32 devices in a mesh: blocks: 16 (over z, y, x), cross: 2 (over core).
Axes of the slice: x: 2, y: 2, z: 4, core: 2. Of those that a mesh axis runs over, the one named last changes fastest.
Arguments:
- f_home: float32 [1024, 19, 512], P(('blocks', 'cross')), may hold values from -0.5 to 1.5
- levels: int32 [1024], P(('blocks', 'cross')), may hold values from 0 to 1, as said below
- plan: int32 [1024], P(('blocks', 'cross')), may hold values from 0 to 1023, as said below
Outputs:
- f_owner: float32 [1024, 19, 512], P(('blocks', 'cross'))
The draws below stay inside these ranges and needn't reach their ends.
Inputs may be any that keep to these rules, and one draw needn't show every extreme that they name: `levels`: exactly a quarter of the patches, 8 times the number of devices, have level 1. plan is a permutation of the patch numbers. Of the patches in the slots of one device of f_home, at most 2 have owner slots on one device, and in every draw some device sends exactly 2 to one owner; every device's owner slots receive exactly 8 patches of level 1.
All inputs are finite; a program needn't handle non-finite values.
Results may differ from the reference program's by a relative error of at most 0.0001.
Values sent between devices are 32-bit elements; how exact they have to be, the bound alone decides.
A program may use at most 256 MiB of HBM per device.

```python
import jax
import jax.numpy as jnp
from jax import lax

FLOW_PATCHES = 1
SPAN_PATCHES = 4
DEPTH_PATCHES = 8
EDGE = 8
STEPS = 2
CELLS = 512
PATCH_DEV = 32
FINE_DEV = 8
PATCHES = 1024
N_BLOCKS = 16
N_CROSS = 2
DEVICES = 32


VELOCITIES = ((0, 0, 0), (1, 0, 0), (-1, 0, 0), (0, 1, 0), (0, -1, 0), (0, 0, 1), (0, 0, -1), (1, 1, 0), (-1, -1, 0), (1, -1, 0), (-1, 1, 0), (1, 0, 1), (-1, 0, -1), (1, 0, -1), (-1, 0, 1), (0, 1, 1), (0, -1, -1), (0, 1, -1), (0, -1, 1))


WEIGHTS = (1.0 / 3.0,) + (1.0 / 18.0,) * 6 + (1.0 / 36.0,) * 12


def wake_layout(key):
    key_tie = jax.random.fold_in(key, 7)
    key_owner = jax.random.fold_in(key, 8)
    key_slot = jax.random.fold_in(key, 9)
    key_jitter = jax.random.fold_in(key, 10)
    ident = jnp.arange(PATCHES, dtype=jnp.int32)
    home = ident // PATCH_DEV
    local_id = ident % PATCH_DEV
    flow_x = home // N_CROSS * FLOW_PATCHES + local_id // (SPAN_PATCHES * DEPTH_PATCHES)
    span_y = home % N_CROSS * SPAN_PATCHES + local_id // DEPTH_PATCHES % SPAN_PATCHES
    total_x = FLOW_PATCHES * N_BLOCKS
    total_y = SPAN_PATCHES * N_CROSS
    behind = flow_x - total_x // 8
    lateral = jnp.abs(2 * span_y + 1 - total_y)
    jitter = jax.random.randint(key_jitter, (PATCHES,), 0, 3 * total_x)
    score = jnp.where(behind >= 0, 8 * total_x * total_y, 0) - lateral * total_x - jnp.abs(behind - total_x // 4) * total_y + jitter
    ties = jax.random.permutation(key_tie, PATCHES).astype(jnp.int32)
    order = jnp.argsort(-(score * PATCHES + ties))
    fine_mask = jnp.zeros((PATCHES,), jnp.int32).at[order[:PATCHES // 4]].set(1)
    fine_rank = jnp.cumsum(fine_mask) - 1
    coarse_rank = jnp.cumsum(1 - fine_mask) - 1
    home_fine = jnp.sum(fine_mask.reshape(DEVICES, PATCH_DEV), axis=1)
    home_coarse = PATCH_DEV - home_fine
    fine_before = jnp.cumsum(home_fine) - home_fine
    coarse_before = jnp.arange(DEVICES, dtype=jnp.int32) * PATCH_DEV - fine_before
    chosen = jnp.argmax(jnp.where(home_coarse > 0, home_fine, -1))
    offset = (fine_before[chosen] - coarse_before[chosen] - home_coarse[chosen] + 1) % DEVICES
    coarse_total = PATCHES - PATCHES // 4
    coarse_index = (coarse_rank + offset) % coarse_total
    owner_pos = jnp.where(fine_mask == 1, fine_rank % DEVICES, coarse_index % DEVICES)
    slot_rank = jnp.where(fine_mask == 1, fine_rank // DEVICES, FINE_DEV + coarse_index // DEVICES)
    relabel = jax.random.permutation(key_owner, DEVICES).astype(jnp.int32)
    slot_scores = jax.random.randint(key_slot, (DEVICES, PATCH_DEV), 0, 1 << 20) * PATCH_DEV + jnp.arange(PATCH_DEV, dtype=jnp.int32)[None, :]
    shuffle = jnp.argsort(slot_scores, axis=1).astype(jnp.int32)
    plan = relabel[owner_pos] * PATCH_DEV + shuffle[owner_pos, slot_rank]
    return (fine_mask.astype(jnp.int32), plan.astype(jnp.int32))


def draw_levels(key, part):
    return wake_layout(key)[0]


def draw_plan(key, part):
    return wake_layout(key)[1]


def draw_f_home(key, part):
    key_density = jax.random.fold_in(key, 21)
    key_velocity = jax.random.fold_in(key, 22)
    key_jitter = jax.random.fold_in(key, 23)
    density = 1.0 + 0.05 * jax.random.truncated_normal(key_density, -3.0, 3.0, (PATCHES, CELLS), jnp.float32)
    velocity = 0.03 * jax.random.truncated_normal(key_velocity, -3.0, 3.0, (3, PATCHES, CELLS), jnp.float32)
    velocity = velocity.at[0].add(0.05)
    jitter = jax.random.truncated_normal(key_jitter, -3.0, 3.0, (PATCHES, 19, CELLS), jnp.float32)
    speed_sq = velocity[0] * velocity[0] + velocity[1] * velocity[1] + velocity[2] * velocity[2]
    columns = []
    for speed in range(19):
        step_x, step_y, step_z = VELOCITIES[speed]
        along = step_x * velocity[0] + step_y * velocity[1] + step_z * velocity[2]
        columns.append(WEIGHTS[speed] * (density * (1.0 + 3.0 * along + 4.5 * along * along - 1.5 * speed_sq) + 0.3 * jitter[:, speed]))
    return jnp.stack(columns, axis=1).astype(jnp.float32)


def block_scale(rng, shape, split, low, top_value):
    loudness = 1.0
    for dim, shards_of in split:
        steps = jax.random.uniform(jax.random.fold_in(jax.random.fold_in(rng, 6), dim), (shards_of,), jnp.float32, low / len(split), top_value / len(split))
        loudness = loudness * jnp.repeat(jnp.exp(steps), shape[dim] // shards_of).reshape((-1,) + (1,) * (len(shape) - 1 - dim))
    return loudness


def setup_inputs(seed: int = 0) -> dict:
    seeds = jax.random.split(jax.random.key(seed), 4)
    f_home = draw_f_home(jax.random.fold_in(seeds[3], 71), 0)
    levels = draw_levels(jax.random.fold_in(seeds[3], 71), 0)
    plan = draw_plan(jax.random.fold_in(seeds[3], 71), 0)
    return dict(f_home=f_home, levels=levels, plan=plan)


VELOCITIES = ((0, 0, 0), (1, 0, 0), (-1, 0, 0), (0, 1, 0), (0, -1, 0), (0, 0, 1), (0, 0, -1), (1, 1, 0), (-1, -1, 0), (1, -1, 0), (-1, 1, 0), (1, 0, 1), (-1, 0, -1), (1, 0, -1), (-1, 0, 1), (0, 1, 1), (0, -1, -1), (0, 1, -1), (0, -1, 1))
WEIGHTS = (1.0 / 3.0,) + (1.0 / 18.0,) * 6 + (1.0 / 36.0,) * 12
FACE_SPEEDS = ((2, 8, 10, 12, 14), (1, 7, 9, 11, 13), (4, 8, 9, 16, 18), (3, 7, 10, 15, 17), (6, 12, 13, 16, 17), (5, 11, 14, 15, 18))
TAU_COARSE = 0.55
TAU_FINE = 2.0 * TAU_COARSE - 0.5
RESCALE = TAU_FINE / (2.0 * TAU_COARSE)
INFLOW = 0.08


def moments(field):
    density = jnp.sum(field, axis=1)
    velocity = []
    for axis_id in range(3):
        forward = [speed for speed in range(19) if VELOCITIES[speed][axis_id] == 1]
        backward = [speed for speed in range(19) if VELOCITIES[speed][axis_id] == -1]
        velocity.append((jnp.sum(field[:, forward], axis=1) - jnp.sum(field[:, backward], axis=1)) / density)
    return density, velocity


def equilibrium(density, velocity, speeds):
    speed_sq = velocity[0] * velocity[0] + velocity[1] * velocity[1] + velocity[2] * velocity[2]
    columns = []
    for speed in speeds:
        step_x, step_y, step_z = VELOCITIES[speed]
        along = step_x * velocity[0] + step_y * velocity[1] + step_z * velocity[2]
        columns.append(WEIGHTS[speed] * density * (1.0 + 3.0 * along + 4.5 * along * along - 1.5 * speed_sq))
    return jnp.stack(columns, axis=1)


def collide(field, relax_rate):
    density, velocity = moments(field)
    balance = equilibrium(density, velocity, range(19))
    relaxed = field + relax_rate[:, None, None, None, None] * (balance - field)
    return relaxed, balance, density, velocity


def layer(field, face_id):
    layer_at = 0 if face_id % 2 == 0 else field.shape[-1] - 1
    return jnp.take(field, layer_at, axis=2 + face_id // 2)


def face_payload(relaxed, balance, send_scale):
    eq_faces = jnp.stack([layer(balance[:, list(FACE_SPEEDS[face_id])], face_id) for face_id in range(6)], axis=1)
    out_faces = jnp.stack([layer(relaxed[:, list(FACE_SPEEDS[face_id])], face_id) for face_id in range(6)], axis=1)
    return eq_faces, send_scale[:, None, None, None, None] * (out_faces - eq_faces)


def inflow_column(speeds):
    values = []
    for speed in speeds:
        along = VELOCITIES[speed][0] * INFLOW
        values.append(WEIGHTS[speed] * (1.0 + 3.0 * along + 4.5 * along * along - 1.5 * INFLOW * INFLOW))
    return jnp.array(values, jnp.float32)


def framed(center, top_row, bottom_row, left_col, right_col):
    middle = jnp.concatenate([left_col[..., :, None], center, right_col[..., :, None]], axis=-1)
    corner = jnp.zeros(top_row.shape[:-1] + (1,), top_row.dtype)
    upper = jnp.concatenate([corner, top_row, corner], axis=-1)[..., None, :]
    lower = jnp.concatenate([corner, bottom_row, corner], axis=-1)[..., None, :]
    return jnp.concatenate([upper, middle, lower], axis=-2)


def bordered(center, left_col, right_col):
    return jnp.concatenate([left_col[..., None], center, right_col[..., None]], axis=-1)


def assemble(eq_ext, neq_ext, recv_scale, inflow_side, outflow_side):
    size_x, size_y, size_z = recv_scale.shape
    factor = recv_scale[:, :, :, None, None, None]

    def neighbour(shift_x, shift_y, shift_z, face_id):
        window = (slice(1 + shift_x, 1 + shift_x + size_x), slice(1 + shift_y, 1 + shift_y + size_y), slice(1 + shift_z, 1 + shift_z + size_z), face_id)
        return eq_ext[window] + factor * neq_ext[window]

    plane_west = framed(neighbour(-1, 0, 0, 1), neighbour(-1, -1, 0, 1)[..., -1, :], neighbour(-1, 1, 0, 1)[..., 0, :], neighbour(-1, 0, -1, 1)[..., :, -1], neighbour(-1, 0, 1, 1)[..., :, 0])
    plane_east = framed(neighbour(1, 0, 0, 0), neighbour(1, -1, 0, 0)[..., -1, :], neighbour(1, 1, 0, 0)[..., 0, :], neighbour(1, 0, -1, 0)[..., :, -1], neighbour(1, 0, 1, 0)[..., :, 0])
    plane_south = bordered(neighbour(0, -1, 0, 3), neighbour(0, -1, -1, 3)[..., :, -1], neighbour(0, -1, 1, 3)[..., :, 0])
    plane_north = bordered(neighbour(0, 1, 0, 2), neighbour(0, 1, -1, 2)[..., :, -1], neighbour(0, 1, 1, 2)[..., :, 0])
    plane_below = neighbour(0, 0, -1, 5)
    plane_above = neighbour(0, 0, 1, 4)
    plane_west = jnp.where(inflow_side[:, None, None, None, None, None], inflow_column(FACE_SPEEDS[1])[:, None, None], plane_west)
    plane_east = jnp.where(outflow_side[:, None, None, None, None, None], inflow_column(FACE_SPEEDS[0])[:, None, None], plane_east)
    return plane_west, plane_east, plane_south, plane_north, plane_below, plane_above


def propagate(relaxed, planes):
    patch_total = relaxed.shape[0]
    extent = relaxed.shape[-1]
    padded = jnp.zeros((patch_total, 19, extent + 2, extent + 2, extent + 2), relaxed.dtype)
    padded = padded.at[:, :, 1:extent + 1, 1:extent + 1, 1:extent + 1].set(relaxed)
    plane_west, plane_east, plane_south, plane_north, plane_below, plane_above = planes
    for column, speed in enumerate(FACE_SPEEDS[1]):
        padded = padded.at[:, speed, 0, :, :].set(plane_west[:, column])
    for column, speed in enumerate(FACE_SPEEDS[0]):
        padded = padded.at[:, speed, extent + 1, :, :].set(plane_east[:, column])
    for column, speed in enumerate(FACE_SPEEDS[3]):
        padded = padded.at[:, speed, 1:extent + 1, 0, :].set(plane_south[:, column])
    for column, speed in enumerate(FACE_SPEEDS[2]):
        padded = padded.at[:, speed, 1:extent + 1, extent + 1, :].set(plane_north[:, column])
    for column, speed in enumerate(FACE_SPEEDS[5]):
        padded = padded.at[:, speed, 1:extent + 1, 1:extent + 1, 0].set(plane_below[:, column])
    for column, speed in enumerate(FACE_SPEEDS[4]):
        padded = padded.at[:, speed, 1:extent + 1, 1:extent + 1, extent + 1].set(plane_above[:, column])
    shifted = []
    for speed in range(19):
        step_x, step_y, step_z = VELOCITIES[speed]
        shifted.append(padded[:, speed, 1 - step_x:1 - step_x + extent, 1 - step_y:1 - step_y + extent, 1 - step_z:1 - step_z + extent])
    return jnp.stack(shifted, axis=1)


def lattice_order(values):
    trailing = values.shape[1:]
    lattice = values.reshape((N_BLOCKS, N_CROSS, FLOW_PATCHES, SPAN_PATCHES, DEPTH_PATCHES) + trailing)
    lattice = jnp.moveaxis(lattice, 2, 1)
    return lattice.reshape((N_BLOCKS * FLOW_PATCHES, N_CROSS * SPAN_PATCHES, DEPTH_PATCHES) + trailing)


def id_order(lattice):
    trailing = lattice.shape[3:]
    grouped = lattice.reshape((N_BLOCKS, FLOW_PATCHES, N_CROSS, SPAN_PATCHES, DEPTH_PATCHES) + trailing)
    grouped = jnp.moveaxis(grouped, 1, 2)
    return grouped.reshape((PATCHES,) + trailing)


def wrap_axis(values, axis_id):
    length = values.shape[axis_id]
    return jnp.concatenate([lax.slice_in_dim(values, length - 1, length, axis=axis_id), values, lax.slice_in_dim(values, 0, 1, axis=axis_id)], axis=axis_id)


def grouped(values):
    return values.reshape((N_BLOCKS * N_CROSS, PATCH_DEV) + values.shape[1:])


def reference(f_home, levels, plan):
    populations = f_home.reshape(PATCHES, 19, EDGE, EDGE, EDGE)
    fine_mask = levels == 1
    relax_rate = jnp.where(fine_mask, 1.0 / TAU_FINE, 1.0 / TAU_COARSE).astype(jnp.float32)
    send_scale = jnp.where(fine_mask, 1.0 / RESCALE, 1.0).astype(jnp.float32)
    recv_scale = lattice_order(jnp.where(fine_mask, RESCALE, 1.0).astype(jnp.float32))
    span_x = FLOW_PATCHES * N_BLOCKS
    position = jnp.arange(span_x, dtype=jnp.int32)

    def group_faces(pieces):
        relaxed, balance, density, velocity = collide(pieces[0], pieces[1])
        return face_payload(relaxed, balance, pieces[2])

    def group_step(pieces):
        fine_rate = jnp.full((PATCH_DEV,), 1.0 / TAU_FINE, jnp.float32)
        planes = pieces[3:]
        relaxed = collide(pieces[0], pieces[1])[0]
        moved = propagate(relaxed, planes)
        updated = propagate(collide(moved, fine_rate)[0], planes)
        return jnp.where(pieces[2][:, None, None, None, None], updated, moved)

    for round_id in range(STEPS):
        eq_faces, neq_faces = lax.map(group_faces, (grouped(populations), grouped(relax_rate), grouped(send_scale)))
        eq_ext = lattice_order(eq_faces.reshape((PATCHES,) + eq_faces.shape[2:]))
        neq_ext = lattice_order(neq_faces.reshape((PATCHES,) + neq_faces.shape[2:]))
        for axis_id in range(3):
            eq_ext = wrap_axis(eq_ext, axis_id)
            neq_ext = wrap_axis(neq_ext, axis_id)
        planes = assemble(eq_ext, neq_ext, recv_scale, position == 0, position == span_x - 1)
        planes = tuple(grouped(id_order(plane)) for plane in planes)
        populations = lax.map(group_step, (grouped(populations), grouped(relax_rate), grouped(fine_mask)) + planes)
        populations = populations.reshape(PATCHES, 19, EDGE, EDGE, EDGE)
    flattened = populations.reshape(PATCHES, 19, CELLS)
    return jnp.zeros_like(flattened).at[plan].set(flattened)
```

```python
import jax
import jax.numpy as jnp
from jax import lax
from jax.experimental import pallas as pl
from jax.experimental.pallas import tpu as pltpu
from jax.sharding import PartitionSpec as P

SPAN_PATCHES = 4
DEPTH_PATCHES = 8
STEPS = 2
CELLS = 512
VELOCITIES = (
    (0, 0, 0),
    (1, 0, 0),
    (-1, 0, 0),
    (0, 1, 0),
    (0, -1, 0),
    (0, 0, 1),
    (0, 0, -1),
    (1, 1, 0),
    (-1, -1, 0),
    (1, -1, 0),
    (-1, 1, 0),
    (1, 0, 1),
    (-1, 0, -1),
    (1, 0, -1),
    (-1, 0, 1),
    (0, 1, 1),
    (0, -1, -1),
    (0, 1, -1),
    (0, -1, 1),
)
WEIGHTS = (1.0 / 3.0,) + (1.0 / 18.0,) * 6 + (1.0 / 36.0,) * 12
TAU_COARSE = 0.55
TAU_FINE = 2.0 * TAU_COARSE - 0.5
RESCALE = TAU_FINE / (2.0 * TAU_COARSE)
INFLOW = 0.08
MESH = pl.DeviceIdType.MESH
ROWS = 152
MAIN = 16
TAIL = 3
LANES = 128
TILES = CELLS // LANES
Y_UP = [q for q in range(19) if VELOCITIES[q][1] == 1]
Y_DOWN = [q for q in range(19) if VELOCITIES[q][1] == -1]
X_UP = [q for q in range(19) if VELOCITIES[q][0] == 1]
X_DOWN = [q for q in range(19) if VELOCITIES[q][0] == -1]
AROUND = [(dx, dy) for dx in (-1, 0, 1) for dy in (-1, 0, 1) if (dx, dy) != (0, 0)]


def relax_into(load, store, coef):
    f = [load(q) for q in range(19)]
    terms = list(f)
    while len(terms) > 1:
        pairs = [a + b for a, b in zip(terms[::2], terms[1::2])]
        terms = pairs + ([terms[-1]] if len(terms) % 2 else [])
    rho = terms[0]
    inv = 1.0 / rho
    u = []
    for axis in range(3):
        up = [f[q] for q in range(19) if VELOCITIES[q][axis] == 1]
        down = [f[q] for q in range(19) if VELOCITIES[q][axis] == -1]
        d = [a - b for a, b in zip(up, down)]
        u.append((((d[0] + d[1]) + (d[2] + d[3])) + d[4]) * inv)
    base = 1.0 - 1.5 * (u[0] * u[0] + u[1] * u[1] + u[2] * u[2])
    scaled = {w: w * rho for w in set(WEIGHTS)}
    for q in range(19):
        along = None
        for axis in range(3):
            e = VELOCITIES[q][axis]
            if e:
                term = u[axis] if e == 1 else -u[axis]
                along = term if along is None else along + term
        poly = base if along is None else base + along * (3.0 + 4.5 * along)
        balance = scaled[WEIGHTS[q]] * poly
        store(q, balance + coef(q) * (f[q] - balance))


def lattice_kernel(nb, nc, sidx, slot_of, level, f_ref, got_ref, table_ref, st, pb, cq, pm, sent, marks, mark_ref,
                   lev_ref, lv, ys, yr, xs, xr, send_sem, recv_sem, lsend, lrecv, psend, precv,
                   msend, mrecv):
    others = nb * nc - 1
    side = nb * nc // 2
    b = lax.axis_index("blocks")
    c = lax.axis_index("cross")

    def at(dx, dy):
        return (lax.rem(b + dx + nb, nb), lax.rem(c + dy + nc, nc))

    me = b * nc + c

    def peer(k):
        return lax.bitwise_xor(me, jnp.where(k < side, side + k, k - side + 1))

    def device(d):
        return (d // nc, lax.rem(d, nc))

    barrier = pltpu.get_barrier_semaphore()

    def greet(k, carry):
        pl.semaphore_signal(barrier, inc=1, device_id=device(peer(k)), device_id_type=MESH)
        return carry

    lax.fori_loop(0, others, greet, 0)

    spot = lax.broadcasted_iota(jnp.int32, (SPAN_PATCHES, 8, LANES), 0) * 8
    spot = spot + lax.broadcasted_iota(jnp.int32, (SPAN_PATCHES, 8, LANES), 1)
    own = jnp.zeros((SPAN_PATCHES, 8, LANES), jnp.float32)
    for p in range(SPAN_PATCHES * 8):
        own = jnp.where(spot == p, level[p].astype(jnp.float32), own)
    lev_ref[...] = own

    def note(d, carry):
        row = lax.broadcasted_iota(jnp.int32, (8, LANES), 0)
        first = slot_of[2 * d].astype(jnp.float32)
        second = slot_of[2 * d + 1].astype(jnp.float32)
        marks[d] = jnp.where(row == 0, first, second)
        return carry

    lax.fori_loop(0, others + 1, note, 0)
    for q in range(19):
        for r in range(SPAN_PATCHES):
            st[q, r] = f_ref[q, r * 8 : r * 8 + 8, :]
    pl.semaphore_wait(barrier, others)

    level_copies = []
    for n, (dx, dy) in enumerate(AROUND):
        copy = pltpu.make_async_remote_copy(
            src_ref=lev_ref, dst_ref=lv.at[n], send_sem=lsend.at[n], recv_sem=lrecv.at[n],
            device_id=at(-dx, -dy), device_id_type=MESH)
        copy.start()
        level_copies.append(copy)

    def mark_copy(k):
        d = peer(k)
        return pltpu.make_async_remote_copy(
            src_ref=marks.at[d], dst_ref=mark_ref.at[me], send_sem=msend.at[k],
            recv_sem=mrecv.at[k], device_id=device(d), device_id_type=MESH)

    def patch_copy(k):
        d = peer(k)
        return pltpu.make_async_remote_copy(
            src_ref=sent.at[d], dst_ref=got_ref.at[me], send_sem=psend.at[k],
            recv_sem=precv.at[k], device_id=device(d), device_id_type=MESH)

    def start_mark(k, carry):
        mark_copy(k).start()
        return carry

    lax.fori_loop(0, others, start_mark, 0)
    mark_ref[me] = marks[me]

    for copy in level_copies:
        copy.wait()

    scale = {(0, 0): jnp.where(own > 0.5, RESCALE, 1.0)}
    for n, key in enumerate(AROUND):
        scale[key] = jnp.where(lv[n] > 0.5, RESCALE, 1.0)
    patch_scale = {}
    for dx in (-1, 0, 1):
        patch_scale[dx, 0] = scale[dx, 0]
        patch_scale[dx, 1] = jnp.concatenate([scale[dx, 0][1:], scale[dx, 1][:1]], axis=0)
        patch_scale[dx, -1] = jnp.concatenate([scale[dx, -1][-1:], scale[dx, 0][:-1]], axis=0)
    gain = jnp.where(own > 0.5, (1.0 - 1.0 / TAU_FINE) / RESCALE, 1.0 - 1.0 / TAU_COARSE)

    def target_scale(dx, dy, dz):
        value = patch_scale[dx, dy]
        return pltpu.roll(value, (-dz) % 8, axis=1) if dz else value

    shape = (SPAN_PATCHES, 8, LANES)
    lane = lax.broadcasted_iota(jnp.int32, shape, 2)
    for q in range(1, 19):
        e = VELOCITIES[q]
        kinds = [{}]
        for axis in range(3):
            if e[axis]:
                kinds = [{**k, axis: v} for k in kinds for v in (0, 1)]
        table = [(k, target_scale(*[e[a] * k.get(a, 0) for a in range(3)])) for k in kinds]
        for tile in range(TILES):
            cell = lane + tile * LANES
            coord = (cell // 64, (cell // 8) % 8, cell % 8)
            result = table[0][1]
            for k, value in table[1:]:
                mask = None
                for axis, on in k.items():
                    if on:
                        hit = coord[axis] == (7 if e[axis] == 1 else 0)
                        mask = hit if mask is None else mask & hit
                result = jnp.where(mask, value, result)
            cq[q - 1, :, :, tile * LANES : (tile + 1) * LANES] = gain * result

    full = (SPAN_PATCHES, 8, CELLS)
    cell = lax.broadcasted_iota(jnp.int32, full, 2)
    coord = (cell // 64, (cell // 8) % 8, cell % 8)
    entry = {
        (axis, e): coord[axis] == (0 if e == 1 else 7) for axis in range(3) for e in (1, -1)
    }
    half = lax.broadcasted_iota(jnp.int32, (2, 8, LANES), 2) < 64
    fine = jnp.broadcast_to(own[:, :, :1] > 0.5, full)

    def roll(v, amount):
        return pltpu.roll(v, amount % CELLS, axis=2)

    def step(s, carry):
        def first(r, tile):
            lanes = slice(tile * LANES, (tile + 1) * LANES)
            plain = jnp.where(lev_ref[r] > 0.5, 1.0 - 1.0 / TAU_FINE, 1.0 - 1.0 / TAU_COARSE)

            def put(q, value):
                pb[q, r, :, lanes] = value

            relax_into(lambda q: st[q, r, :, lanes], put,
                       lambda q: cq[q - 1, r, :, lanes] if q else plain)

        def shift_z(q, rows):
            e = VELOCITIES[q][2]
            if e:
                v = pb[q, rows]
                wrapped = pltpu.roll(roll(v, e - 8 * e), e % 8, axis=1)
                pb[q, rows] = jnp.where(entry[2, e][rows], wrapped, roll(v, e))

        def outer(m, carry):
            for tile in range(TILES):
                first(m * (SPAN_PATCHES - 1), tile)
            return carry

        lax.fori_loop(0, 2, outer, 0)
        for r in (0, SPAN_PATCHES - 1):
            for q in range(19):
                shift_z(q, slice(r, r + 1))
        for n in range(5):
            ys[s, 0, n] = pb[Y_UP[n], SPAN_PATCHES - 1]
            ys[s, 1, n] = pb[Y_DOWN[n], 0]
        y_copies = []
        for way, dy in ((0, 1), (1, -1)):
            copy = pltpu.make_async_remote_copy(
                src_ref=ys.at[s, way], dst_ref=yr.at[s, way], send_sem=send_sem.at[s, way],
                recv_sem=recv_sem.at[s, way], device_id=at(0, dy), device_id_type=MESH)
            copy.start()
            y_copies.append(copy)

        def inner(r, carry):
            for tile in range(TILES):
                first(r, tile)
            return carry

        lax.fori_loop(1, SPAN_PATCHES - 1, inner, 0)
        for q in range(19):
            shift_z(q, slice(1, SPAN_PATCHES - 1))
        st[0] = pb[0]
        st[5] = pb[5]
        st[6] = pb[6]
        def shift_x(wanted):
            for way, e, group in ((0, 1, X_UP), (1, -1, X_DOWN)):
                for n, q in enumerate(group):
                    if (VELOCITIES[q][1] != 0) != wanted:
                        continue
                    v = roll(pb[q], 64 * e)
                    pb[q] = v
                    edge = v[:, :, :LANES] if e == 1 else v[:, :, CELLS - LANES :]
                    turned = pltpu.roll(edge, 64, axis=2)
                    if e == 1:
                        xs[s, way, n] = jnp.where(half, edge[:2], turned[2:])
                    else:
                        xs[s, way, n] = jnp.where(half, turned[:2], edge[2:])

        def shift_y(wanted):
            for way, e, group in ((0, 1, Y_UP), (1, -1, Y_DOWN)):
                for n, q in enumerate(group):
                    if (VELOCITIES[q][0] != 0) != wanted:
                        continue
                    v = pb[q]
                    halo = yr[s, way, n][None]
                    if e == 1:
                        moved = jnp.concatenate([halo, v[:-1]], axis=0)
                    else:
                        moved = jnp.concatenate([v[1:], halo], axis=0)
                    v = jnp.where(entry[1, e], roll(moved, 8 * e - 64 * e), roll(v, 8 * e))
                    if wanted:
                        pb[q] = v
                    else:
                        st[q] = v

        shift_x(False)
        for copy in y_copies:
            copy.wait()
        shift_y(True)
        shift_x(True)
        x_copies = []
        for way, dx in ((0, 1), (1, -1)):
            copy = pltpu.make_async_remote_copy(
                src_ref=xs.at[s, way], dst_ref=xr.at[s, way], send_sem=send_sem.at[s, 2 + way],
                recv_sem=recv_sem.at[s, 2 + way], device_id=at(dx, 0), device_id_type=MESH)
            copy.start()
            x_copies.append(copy)
        shift_y(False)
        for q in X_UP + X_DOWN:
            st[q] = pb[q]

        def again(r, tiles):
            for tile in tiles:
                lanes = slice(tile * LANES, (tile + 1) * LANES)

                def put(q, value):
                    pb[q, r, :, lanes] = value

                relax_into(lambda q: st[q, r, :, lanes], put, lambda q: 1.0 - 1.0 / TAU_FINE)

        def middle(r, carry):
            again(r, range(1, TILES - 1))
            return carry

        lax.fori_loop(0, SPAN_PATCHES, middle, 0)
        for copy in x_copies:
            copy.wait()
        for way, e, group in ((0, 1, X_UP), (1, -1, X_DOWN)):
            outside = b == (0 if e == 1 else nb - 1)
            for n, q in enumerate(group):
                h = xr[s, way, n]
                turned = pltpu.roll(h, 64, axis=2)
                halo = jnp.concatenate([h, turned] if e == 1 else [turned, h], axis=0)
                along = e * INFLOW
                const = WEIGHTS[q] * (1.0 + 3.0 * along + 4.5 * along * along - 1.5 * INFLOW * INFLOW)
                halo = jnp.where(outside, jnp.full(halo.shape, const, jnp.float32), halo)
                if e == 1:
                    st[q, :, :, :LANES] = jnp.where(lane < 64, halo, st[q, :, :, :LANES])
                else:
                    st[q, :, :, CELLS - LANES :] = jnp.where(lane >= 64, halo, st[q, :, :, CELLS - LANES :])

        def ends(r, carry):
            again(r, (0, TILES - 1))
            return carry

        lax.fori_loop(0, SPAN_PATCHES, ends, 0)
        for q in range(19):
            e = VELOCITIES[q]
            take = fine
            for axis in range(3):
                if e[axis]:
                    take = take & ~entry[axis, e[axis]]
            moved = pb[q]
            if q:
                moved = roll(moved, 64 * e[0] + 8 * e[1] + e[2])
            st[q] = jnp.where(take, moved, st[q])
        return carry

    lax.fori_loop(0, STEPS, step, 0)

    for q in range(19):
        for r in range(SPAN_PATCHES):
            pm[r * 8 : r * 8 + 8, q, :] = st[q, r]

    def pack(d):
        for slot in range(2):
            p = sidx[2 * d + slot]
            for tile in range(TILES):
                lanes = slice(tile * LANES, (tile + 1) * LANES)
                at_row = slot * TILES + tile
                sent[d, at_row * MAIN : (at_row + 1) * MAIN, :] = pm[p, :MAIN, lanes]
                low = 2 * TILES * MAIN + at_row * TAIL
                sent[d, low : low + TAIL, :] = pm[p, MAIN:, lanes]

    def post(k, carry):
        pack(peer(k))

        @pl.when(k > 0)
        def _():
            patch_copy(k - 1).start()

        return carry

    lax.fori_loop(0, others, post, 0)
    pack(me)
    patch_copy(others - 1).start()
    got_ref[me] = sent[me]

    def marked(k, carry):
        mark_copy(k).wait()
        return carry

    lax.fori_loop(0, others, marked, 0)
    source = lax.broadcasted_iota(jnp.int32, (others + 1, LANES), 0) * 2
    wanted = lax.broadcasted_iota(jnp.int32, (others + 1, LANES), 1).astype(jnp.float32)
    index = jnp.where(mark_ref[:, 0, :] == wanted, source, 0)
    index = index + jnp.where(mark_ref[:, 1, :] == wanted, source + 1, 0)
    table_ref[...] = jnp.broadcast_to(jnp.sum(index, axis=0, keepdims=True), (8, LANES))

    def finish(k, carry):
        patch_copy(k).wait()
        return carry

    lax.fori_loop(0, others, finish, 0)


def unpack_kernel(ridx, got_ref, out_ref):
    def place(t, carry):
        a = ridx[0, t]
        src = a // 2
        slot = lax.rem(a, 2)
        tail = got_ref[src, 2 * TILES * MAIN : ROWS, :]
        for tile in range(TILES):
            lanes = slice(tile * LANES, (tile + 1) * LANES)
            low = pl.multiple_of((slot * TILES + tile) * MAIN, MAIN)
            out_ref[:MAIN, t, lanes] = got_ref[src, pl.ds(low, MAIN), :]
            other = TAIL * (TILES + tile)
            rest = jnp.where(
                slot == 0, tail[TAIL * tile : TAIL * (tile + 1)], tail[other : other + TAIL]
            )
            out_ref[MAIN:, t, lanes] = rest
        return carry

    for t in range(out_ref.shape[1]):
        place(t, 0)


def body(nb, nc, f_home, levels, plan):
    devices = nb * nc
    patches = f_home.shape[0]
    target = plan // patches
    order = jnp.arange(patches, dtype=jnp.int32)
    earlier = (target[:, None] == target[None, :]) & (order[None, :] < order[:, None])
    place = 2 * target + jnp.sum(earlier.astype(jnp.int32), axis=1)
    hit = place[None, :] == jnp.arange(2 * devices, dtype=jnp.int32)[:, None]
    sidx = jnp.sum(jnp.where(hit, order[None, :], 0), axis=1)
    slot_of = jnp.sum(jnp.where(hit, plan[None, :] % patches + 1, 0), axis=1) - 1
    vmem = pl.BlockSpec(memory_space=pltpu.VMEM)
    smem = pl.BlockSpec(memory_space=pltpu.SMEM)
    state = (19, SPAN_PATCHES, 8, CELLS)
    small = (SPAN_PATCHES, 8, LANES)
    f32 = jnp.float32
    dma = pltpu.SemaphoreType.DMA
    got, ridx = pl.pallas_call(
        lambda *refs: lattice_kernel(nb, nc, *refs),
        out_shape=(
            jax.ShapeDtypeStruct((devices, ROWS, LANES), f32),
            jax.ShapeDtypeStruct((8, LANES), jnp.int32),
        ),
        in_specs=[smem, smem, smem, vmem],
        out_specs=(vmem, vmem),
        scratch_shapes=[
            pltpu.VMEM(state, f32),
            pltpu.VMEM(state, f32),
            pltpu.VMEM((18,) + state[1:], f32),
            pltpu.VMEM((patches, 19, CELLS), f32),
            pltpu.VMEM((devices, ROWS, LANES), f32),
            pltpu.VMEM((devices, 8, LANES), f32),
            pltpu.VMEM((devices, 8, LANES), f32),
            pltpu.VMEM(small, f32),
            pltpu.VMEM((len(AROUND),) + small, f32),
            pltpu.VMEM((STEPS, 2, 5, 8, CELLS), f32),
            pltpu.VMEM((STEPS, 2, 5, 8, CELLS), f32),
            pltpu.VMEM((STEPS, 2, 5, 2, 8, LANES), f32),
            pltpu.VMEM((STEPS, 2, 5, 2, 8, LANES), f32),
            dma((STEPS, 4)),
            dma((STEPS, 4)),
            dma((len(AROUND),)),
            dma((len(AROUND),)),
            dma((devices - 1,)),
            dma((devices - 1,)),
            dma((devices - 1,)),
            dma((devices - 1,)),
        ],
        compiler_params=pltpu.CompilerParams(collective_id=0, has_side_effects=True,
                                             vmem_limit_bytes=60 * 1024 * 1024),
    )(sidx, slot_of, levels, jnp.transpose(f_home, (1, 0, 2)))
    out = pl.pallas_call(
        unpack_kernel,
        out_shape=jax.ShapeDtypeStruct((19, patches, CELLS), f32),
        in_specs=[smem, vmem],
        out_specs=vmem,
        compiler_params=pltpu.CompilerParams(vmem_limit_bytes=40 * 1024 * 1024),
    )(ridx, got)
    return jnp.transpose(out, (1, 0, 2))


def solution(mesh):
    nb, nc = mesh.shape["blocks"], mesh.shape["cross"]
    in_specs = (P(("blocks", "cross"), None, None), P(("blocks", "cross")), P(("blocks", "cross")))
    out_specs = P(("blocks", "cross"), None, None)
    return jax.shard_map(
        lambda f, l, p: body(nb, nc, f, l, p),
        mesh=mesh, in_specs=in_specs, out_specs=out_specs, check_vma=False)
```

```python
import jax
import jax.numpy as jnp
from jax import lax
from jax.experimental import pallas as pl
from jax.experimental.pallas import tpu as pltpu
from jax.sharding import PartitionSpec as P

SPAN_PATCHES = 4
DEPTH_PATCHES = 8
STEPS = 2
CELLS = 512
VELOCITIES = (
    (0, 0, 0),
    (1, 0, 0),
    (-1, 0, 0),
    (0, 1, 0),
    (0, -1, 0),
    (0, 0, 1),
    (0, 0, -1),
    (1, 1, 0),
    (-1, -1, 0),
    (1, -1, 0),
    (-1, 1, 0),
    (1, 0, 1),
    (-1, 0, -1),
    (1, 0, -1),
    (-1, 0, 1),
    (0, 1, 1),
    (0, -1, -1),
    (0, 1, -1),
    (0, -1, 1),
)
WEIGHTS = (1.0 / 3.0,) + (1.0 / 18.0,) * 6 + (1.0 / 36.0,) * 12
TAU_COARSE = 0.55
TAU_FINE = 2.0 * TAU_COARSE - 0.5
RESCALE = TAU_FINE / (2.0 * TAU_COARSE)
INFLOW = 0.08
MESH = pl.DeviceIdType.MESH
MAIN = 16
TAIL = 3
HALF = 40
MARK = 38
FLAG = 39
LANES = 128
TILES = CELLS // LANES
Y_UP = [q for q in range(19) if VELOCITIES[q][1] == 1]
Y_DOWN = [q for q in range(19) if VELOCITIES[q][1] == -1]
X_UP = [q for q in range(19) if VELOCITIES[q][0] == 1]
X_DOWN = [q for q in range(19) if VELOCITIES[q][0] == -1]
AROUND = [(dx, dy) for dx in (-1, 0, 1) for dy in (-1, 0, 1) if (dx, dy) != (0, 0)]


def relax_into(load, store, coef):
    f = [load(q) for q in range(19)]
    terms = list(f)
    while len(terms) > 1:
        pairs = [a + b for a, b in zip(terms[::2], terms[1::2])]
        terms = pairs + ([terms[-1]] if len(terms) % 2 else [])
    rho = terms[0]
    inv = 1.0 / rho
    u = []
    for axis in range(3):
        up = [f[q] for q in range(19) if VELOCITIES[q][axis] == 1]
        down = [f[q] for q in range(19) if VELOCITIES[q][axis] == -1]
        d = [a - b for a, b in zip(up, down)]
        u.append((((d[0] + d[1]) + (d[2] + d[3])) + d[4]) * inv)
    base = 1.0 - 1.5 * (u[0] * u[0] + u[1] * u[1] + u[2] * u[2])
    scaled = {w: w * rho for w in set(WEIGHTS)}
    for q in range(19):
        along = None
        for axis in range(3):
            e = VELOCITIES[q][axis]
            if e:
                term = u[axis] if e == 1 else -u[axis]
                along = term if along is None else along + term
        poly = base if along is None else base + along * (3.0 + 4.5 * along)
        balance = scaled[WEIGHTS[q]] * poly
        store(q, balance + coef(q) * (f[q] - balance))


def low_row(q, tile):
    return tile % 2 * MAIN + q if q < MAIN else 2 * MAIN + tile % 2 * TAIL + q - MAIN


def lattice_kernel(nb, nc, sidx, slot_of, level, f_ref, got_ref, left_ref, table_ref, st, pb, cq, pm, sent, second,
                   extra, theirs, lev_ref, lv, ys, yr, xs, xr, send_sem, recv_sem, lsend, lrecv, psend,
                   precv, esend, erecv, csend, crecv):
    others = nb * nc - 1
    side = nb * nc // 2
    b = lax.axis_index("blocks")
    c = lax.axis_index("cross")

    def at(dx, dy):
        return (lax.rem(b + dx + nb, nb), lax.rem(c + dy + nc, nc))

    me = b * nc + c

    def peer(k):
        return lax.bitwise_xor(me, jnp.where(k < side, side + k, k - side + 1))

    def device(d):
        return (d // nc, lax.rem(d, nc))

    barrier = pltpu.get_barrier_semaphore()

    def greet(k, carry):
        pl.semaphore_signal(barrier, inc=1, device_id=device(peer(k)), device_id_type=MESH)
        return carry

    lax.fori_loop(0, others, greet, 0)

    spot = lax.broadcasted_iota(jnp.int32, (SPAN_PATCHES, 8, LANES), 0) * 8
    spot = spot + lax.broadcasted_iota(jnp.int32, (SPAN_PATCHES, 8, LANES), 1)
    own = jnp.zeros((SPAN_PATCHES, 8, LANES), jnp.float32)
    for p in range(SPAN_PATCHES * 8):
        own = jnp.where(spot == p, level[p].astype(jnp.float32), own)
    lev_ref[...] = own

    for q in range(19):
        for r in range(SPAN_PATCHES):
            st[q, r] = f_ref[q, r * 8 : r * 8 + 8, :]
    pl.semaphore_wait(barrier, others)

    level_copies = []
    for n, (dx, dy) in enumerate(AROUND):
        copy = pltpu.make_async_remote_copy(
            src_ref=lev_ref, dst_ref=lv.at[n], send_sem=lsend.at[n], recv_sem=lrecv.at[n],
            device_id=at(-dx, -dy), device_id_type=MESH)
        copy.start()
        level_copies.append(copy)

    count = others + 1

    def patch_copy(k):
        d = peer(k)
        return pltpu.make_async_remote_copy(
            src_ref=sent.at[d], dst_ref=got_ref.at[pl.ds(2 * me, 2)], send_sem=psend.at[k],
            recv_sem=precv.at[k], device_id=device(d), device_id_type=MESH)

    def extra_copy(k):
        d = peer(k)
        return pltpu.make_async_remote_copy(
            src_ref=extra.at[d], dst_ref=got_ref.at[2 * count + me], send_sem=esend.at[k],
            recv_sem=erecv.at[k], device_id=device(d), device_id_type=MESH)

    for copy in level_copies:
        copy.wait()

    scale = {(0, 0): jnp.where(own > 0.5, RESCALE, 1.0)}
    for n, key in enumerate(AROUND):
        scale[key] = jnp.where(lv[n] > 0.5, RESCALE, 1.0)
    patch_scale = {}
    for dx in (-1, 0, 1):
        patch_scale[dx, 0] = scale[dx, 0]
        patch_scale[dx, 1] = jnp.concatenate([scale[dx, 0][1:], scale[dx, 1][:1]], axis=0)
        patch_scale[dx, -1] = jnp.concatenate([scale[dx, -1][-1:], scale[dx, 0][:-1]], axis=0)
    gain = jnp.where(own > 0.5, (1.0 - 1.0 / TAU_FINE) / RESCALE, 1.0 - 1.0 / TAU_COARSE)

    def target_scale(dx, dy, dz):
        value = patch_scale[dx, dy]
        return pltpu.roll(value, (-dz) % 8, axis=1) if dz else value

    shape = (SPAN_PATCHES, 8, LANES)
    lane = lax.broadcasted_iota(jnp.int32, shape, 2)
    for q in range(1, 19):
        e = VELOCITIES[q]
        kinds = [{}]
        for axis in range(3):
            if e[axis]:
                kinds = [{**k, axis: v} for k in kinds for v in (0, 1)]
        table = [(k, target_scale(*[e[a] * k.get(a, 0) for a in range(3)])) for k in kinds]
        for tile in range(TILES):
            cell = lane + tile * LANES
            coord = (cell // 64, (cell // 8) % 8, cell % 8)
            result = table[0][1]
            for k, value in table[1:]:
                mask = None
                for axis, on in k.items():
                    if on:
                        hit = coord[axis] == (7 if e[axis] == 1 else 0)
                        mask = hit if mask is None else mask & hit
                result = jnp.where(mask, value, result)
            cq[q - 1, :, :, tile * LANES : (tile + 1) * LANES] = gain * result

    full = (SPAN_PATCHES, 8, CELLS)
    cell = lax.broadcasted_iota(jnp.int32, full, 2)
    coord = (cell // 64, (cell // 8) % 8, cell % 8)
    entry = {
        (axis, e): coord[axis] == (0 if e == 1 else 7) for axis in range(3) for e in (1, -1)
    }
    half = lax.broadcasted_iota(jnp.int32, (2, 8, LANES), 2) < 64
    fine = jnp.broadcast_to(own[:, :, :1] > 0.5, full)

    def roll(v, amount):
        return pltpu.roll(v, amount % CELLS, axis=2)

    def step(s, carry):
        def first(r, tile):
            lanes = slice(tile * LANES, (tile + 1) * LANES)
            plain = jnp.where(lev_ref[r] > 0.5, 1.0 - 1.0 / TAU_FINE, 1.0 - 1.0 / TAU_COARSE)

            def put(q, value):
                pb[q, r, :, lanes] = value

            relax_into(lambda q: st[q, r, :, lanes], put,
                       lambda q: cq[q - 1, r, :, lanes] if q else plain)

        def shift_z(q, rows):
            e = VELOCITIES[q][2]
            if e:
                v = pb[q, rows]
                wrapped = pltpu.roll(roll(v, e - 8 * e), e % 8, axis=1)
                pb[q, rows] = jnp.where(entry[2, e][rows], wrapped, roll(v, e))

        def outer(m, carry):
            for tile in range(TILES):
                first(m * (SPAN_PATCHES - 1), tile)
            return carry

        lax.fori_loop(0, 2, outer, 0)
        for r in (0, SPAN_PATCHES - 1):
            for q in range(19):
                shift_z(q, slice(r, r + 1))
        for n in range(5):
            ys[s, 0, n] = pb[Y_UP[n], SPAN_PATCHES - 1]
            ys[s, 1, n] = pb[Y_DOWN[n], 0]
        y_copies = []
        for way, dy in ((0, 1), (1, -1)):
            copy = pltpu.make_async_remote_copy(
                src_ref=ys.at[s, way], dst_ref=yr.at[s, way], send_sem=send_sem.at[s, way],
                recv_sem=recv_sem.at[s, way], device_id=at(0, dy), device_id_type=MESH)
            copy.start()
            y_copies.append(copy)

        def inner(r, carry):
            for tile in range(TILES):
                first(r, tile)
            return carry

        lax.fori_loop(1, SPAN_PATCHES - 1, inner, 0)
        for q in range(19):
            shift_z(q, slice(1, SPAN_PATCHES - 1))
        st[0] = pb[0]
        st[5] = pb[5]
        st[6] = pb[6]
        def shift_x(wanted):
            for way, e, group in ((0, 1, X_UP), (1, -1, X_DOWN)):
                for n, q in enumerate(group):
                    if (VELOCITIES[q][1] != 0) != wanted:
                        continue
                    v = roll(pb[q], 64 * e)
                    pb[q] = v
                    edge = v[:, :, :LANES] if e == 1 else v[:, :, CELLS - LANES :]
                    turned = pltpu.roll(edge, 64, axis=2)
                    if e == 1:
                        xs[s, way, n] = jnp.where(half, edge[:2], turned[2:])
                    else:
                        xs[s, way, n] = jnp.where(half, turned[:2], edge[2:])

        def shift_y(wanted):
            for way, e, group in ((0, 1, Y_UP), (1, -1, Y_DOWN)):
                for n, q in enumerate(group):
                    if (VELOCITIES[q][0] != 0) != wanted:
                        continue
                    v = pb[q]
                    halo = yr[s, way, n][None]
                    if e == 1:
                        moved = jnp.concatenate([halo, v[:-1]], axis=0)
                    else:
                        moved = jnp.concatenate([v[1:], halo], axis=0)
                    v = jnp.where(entry[1, e], roll(moved, 8 * e - 64 * e), roll(v, 8 * e))
                    if wanted:
                        pb[q] = v
                    else:
                        st[q] = v

        shift_x(False)
        for copy in y_copies:
            copy.wait()
        shift_y(True)
        shift_x(True)
        x_copies = []
        for way, dx in ((0, 1), (1, -1)):
            copy = pltpu.make_async_remote_copy(
                src_ref=xs.at[s, way], dst_ref=xr.at[s, way], send_sem=send_sem.at[s, 2 + way],
                recv_sem=recv_sem.at[s, 2 + way], device_id=at(dx, 0), device_id_type=MESH)
            copy.start()
            x_copies.append(copy)
        shift_y(False)
        for q in X_UP + X_DOWN:
            st[q] = pb[q]

        def again(r, tiles):
            for tile in tiles:
                lanes = slice(tile * LANES, (tile + 1) * LANES)

                def put(q, value):
                    pb[q, r, :, lanes] = value

                relax_into(lambda q: st[q, r, :, lanes], put, lambda q: 1.0 - 1.0 / TAU_FINE)

        def middle(r, carry):
            again(r, range(1, TILES - 1))
            return carry

        lax.fori_loop(0, SPAN_PATCHES, middle, 0)
        for copy in x_copies:
            copy.wait()
        for way, e, group in ((0, 1, X_UP), (1, -1, X_DOWN)):
            outside = b == (0 if e == 1 else nb - 1)
            for n, q in enumerate(group):
                h = xr[s, way, n]
                turned = pltpu.roll(h, 64, axis=2)
                halo = jnp.concatenate([h, turned] if e == 1 else [turned, h], axis=0)
                along = e * INFLOW
                const = WEIGHTS[q] * (1.0 + 3.0 * along + 4.5 * along * along - 1.5 * INFLOW * INFLOW)
                halo = jnp.where(outside, jnp.full(halo.shape, const, jnp.float32), halo)
                if e == 1:
                    st[q, :, :, :LANES] = jnp.where(lane < 64, halo, st[q, :, :, :LANES])
                else:
                    st[q, :, :, CELLS - LANES :] = jnp.where(lane >= 64, halo, st[q, :, :, CELLS - LANES :])

        def ends(r, carry):
            again(r, (0, TILES - 1))
            return carry

        lax.fori_loop(0, SPAN_PATCHES, ends, 0)
        for q in range(19):
            e = VELOCITIES[q]
            take = fine
            for axis in range(3):
                if e[axis]:
                    take = take & ~entry[axis, e[axis]]
            moved = pb[q]
            if q:
                moved = roll(moved, 64 * e[0] + 8 * e[1] + e[2])
            st[q] = jnp.where(take, moved, st[q])
        return carry

    lax.fori_loop(0, STEPS, step, 0)

    pm[:, 2 * MAIN : HALF, :] = jnp.zeros((pm.shape[0], HALF - 2 * MAIN, LANES), jnp.float32)
    pm[:, HALF + 2 * MAIN :, :] = jnp.zeros((pm.shape[0], HALF - 2 * MAIN, LANES), jnp.float32)
    for q in range(19):
        for r in range(SPAN_PATCHES):
            for tile in range(TILES):
                row = tile // 2 * HALF + low_row(q, tile)
                pm[r * 8 : r * 8 + 8, row, :] = st[q, r, :, tile * LANES : (tile + 1) * LANES]

    def tag(value):
        return jnp.full((1, LANES), value.astype(jnp.float32), jnp.float32)

    def pack(d):
        p = sidx[2 * d]
        sent[d, 0] = pm[p, :HALF]
        sent[d, 1] = pm[p, HALF:]
        sent[d, 0, MARK : MARK + 1, :] = tag(slot_of[2 * d])

    def post(k, carry):
        pack(peer(k))

        @pl.when(k > 0)
        def _():
            patch_copy(k - 1).start()

        return carry

    lax.fori_loop(0, others, post, 0)
    pack(me)

    def half_rows(which):
        return pl.ds(pl.multiple_of(which * HALF, HALF), HALF)

    def pack_second(d, carry):
        second[d] = pm[sidx[2 * d + 1], half_rows(1 - c), :]
        second[d, MARK : MARK + 1, :] = tag(slot_of[2 * d + 1])
        return carry

    lax.fori_loop(0, count, pack_second, 0)
    patch_copy(others - 1).start()
    got_ref[2 * me] = sent[me, 0]
    got_ref[2 * me + 1] = sent[me, 1]
    swap = pltpu.make_async_remote_copy(
        src_ref=second, dst_ref=theirs, send_sem=csend, recv_sem=crecv,
        device_id=at(0, 1), device_id_type=MESH)
    swap.start()
    swap.wait()
    both = jnp.where((second[:, MARK, :] > -0.5) & (theirs[:, MARK, :] > -0.5), 1.0, 0.0)
    flag = jnp.max(both, axis=0, keepdims=True)
    zero = c == 0

    def pack_extra(d):
        mine = pm[sidx[2 * d + 1], half_rows(c), :]
        other = theirs[d]
        my_tag = tag(slot_of[2 * d + 1])
        other_tag = other[MARK : MARK + 1]
        has_mine = my_tag > -0.5
        has_other = other_tag > -0.5
        keep = (has_mine & zero) | ~has_other
        extra[d] = jnp.where(keep, mine, other)
        extra[d, MARK : MARK + 1, :] = jnp.where(keep, my_tag, other_tag)
        extra[d, FLAG : FLAG + 1, :] = flag
        left_ref[d] = jnp.where(zero, other, mine)
        left_ref[d, MARK : MARK + 1, :] = jnp.where(
            has_mine & has_other, jnp.where(zero, other_tag, my_tag), -1.0
        )

    def post_extra(k, carry):
        pack_extra(peer(k))

        @pl.when(k > 0)
        def _():
            extra_copy(k - 1).start()

        return carry

    lax.fori_loop(0, others, post_extra, 0)
    pack_extra(me)
    extra_copy(others - 1).start()
    got_ref[2 * count + me] = extra[me]

    def finish(k, carry):
        patch_copy(k).wait()
        extra_copy(k).wait()
        return carry

    lax.fori_loop(0, others, finish, 0)
    source = lax.broadcasted_iota(jnp.int32, (2 * count, LANES), 0)
    wanted = lax.broadcasted_iota(jnp.int32, (2 * count, LANES), 1).astype(jnp.float32)
    first_hit = (got_ref[: 2 * count, MARK, :] == wanted) & (source % 2 == 0)
    index = jnp.sum(jnp.where(first_hit, source, 0), axis=0, keepdims=True)
    source = source[:count]
    extra_hit = (got_ref[2 * count :, MARK, :] == wanted[:count]) & (source % nc == 0)
    index = index + jnp.sum(jnp.where(extra_hit, source + 2 * count, 0), axis=0, keepdims=True)
    over = jnp.max(got_ref[2 * count :, FLAG, :], axis=0, keepdims=True)
    row = lax.broadcasted_iota(jnp.int32, (8, LANES), 0)
    table_ref[...] = jnp.where(row == 0, index, jnp.where(over > 0.5, 1, 0))


def leftover_kernel(nb, nc, left_ref, table_ref, got_ref, new_table_ref, send_sem, recv_sem):
    count = nb * nc
    me = lax.axis_index("blocks") * nc + lax.axis_index("cross")

    def device(d):
        return (d // nc, lax.rem(d, nc))

    barrier = pltpu.get_barrier_semaphore()

    def greet(k, carry):
        pl.semaphore_signal(barrier, inc=1, device_id=device(lax.bitwise_xor(me, k)), device_id_type=MESH)
        return carry

    lax.fori_loop(1, count, greet, 0)
    pl.semaphore_wait(barrier, count - 1)

    def left_copy(k):
        d = lax.bitwise_xor(me, k)
        return pltpu.make_async_remote_copy(
            src_ref=left_ref.at[d], dst_ref=got_ref.at[me], send_sem=send_sem.at[k],
            recv_sem=recv_sem.at[k], device_id=device(d), device_id_type=MESH)

    def post(k, carry):
        left_copy(k).start()
        return carry

    def finish(k, carry):
        left_copy(k).wait()
        return carry

    lax.fori_loop(1, count, post, 0)
    got_ref[me] = left_ref[me]
    lax.fori_loop(1, count, finish, 0)
    source = lax.broadcasted_iota(jnp.int32, (count, LANES), 0)
    wanted = lax.broadcasted_iota(jnp.int32, (count, LANES), 1).astype(jnp.float32)
    hit = (got_ref[:, MARK, :] == wanted) & (source % nc == 0)
    index = jnp.sum(jnp.where(hit, source + 3 * count, 0), axis=0, keepdims=True)
    new_table_ref[...] = table_ref[...] + index


def unpack_kernel(ridx, got_ref, out_ref):
    for t in range(out_ref.shape[1]):
        base = ridx[0, t]
        for tile in range(TILES):
            block = got_ref.at[base + tile // 2]
            lanes = slice(tile * LANES, (tile + 1) * LANES)
            low = low_row(0, tile)
            out_ref[:MAIN, t, lanes] = block[low : low + MAIN, :]
            low = low_row(MAIN, tile)
            out_ref[MAIN:, t, lanes] = block[2 * MAIN :, :][low - 2 * MAIN : low - 2 * MAIN + TAIL]


def body(nb, nc, f_home, levels, plan):
    devices = nb * nc
    patches = f_home.shape[0]
    target = plan // patches
    order = jnp.arange(patches, dtype=jnp.int32)
    earlier = (target[:, None] == target[None, :]) & (order[None, :] < order[:, None])
    place = 2 * target + jnp.sum(earlier.astype(jnp.int32), axis=1)
    hit = place[None, :] == jnp.arange(2 * devices, dtype=jnp.int32)[:, None]
    sidx = jnp.sum(jnp.where(hit, order[None, :], 0), axis=1)
    slot_of = jnp.sum(jnp.where(hit, plan[None, :] % patches + 1, 0), axis=1) - 1
    vmem = pl.BlockSpec(memory_space=pltpu.VMEM)
    smem = pl.BlockSpec(memory_space=pltpu.SMEM)
    state = (19, SPAN_PATCHES, 8, CELLS)
    small = (SPAN_PATCHES, 8, LANES)
    f32 = jnp.float32
    dma = pltpu.SemaphoreType.DMA
    half = (HALF, LANES)
    limit = pltpu.CompilerParams(collective_id=0, has_side_effects=True, vmem_limit_bytes=60 * 1024 * 1024)
    got, left, table = pl.pallas_call(
        lambda *refs: lattice_kernel(nb, nc, *refs),
        out_shape=(
            jax.ShapeDtypeStruct((3 * devices,) + half, f32),
            jax.ShapeDtypeStruct((devices,) + half, f32),
            jax.ShapeDtypeStruct((8, LANES), jnp.int32),
        ),
        in_specs=[smem, smem, smem, vmem],
        out_specs=(vmem, vmem, vmem),
        scratch_shapes=[
            pltpu.VMEM(state, f32),
            pltpu.VMEM(state, f32),
            pltpu.VMEM((18,) + state[1:], f32),
            pltpu.VMEM((patches, 2 * HALF, LANES), f32),
            pltpu.VMEM((devices, 2) + half, f32),
            pltpu.VMEM((devices,) + half, f32),
            pltpu.VMEM((devices,) + half, f32),
            pltpu.VMEM((devices,) + half, f32),
            pltpu.VMEM(small, f32),
            pltpu.VMEM((len(AROUND),) + small, f32),
            pltpu.VMEM((STEPS, 2, 5, 8, CELLS), f32),
            pltpu.VMEM((STEPS, 2, 5, 8, CELLS), f32),
            pltpu.VMEM((STEPS, 2, 5, 2, 8, LANES), f32),
            pltpu.VMEM((STEPS, 2, 5, 2, 8, LANES), f32),
            dma((STEPS, 4)),
            dma((STEPS, 4)),
            dma((len(AROUND),)),
            dma((len(AROUND),)),
            dma((devices - 1,)),
            dma((devices - 1,)),
            dma((devices - 1,)),
            dma((devices - 1,)),
            dma,
            dma,
        ],
        compiler_params=limit,
    )(sidx, slot_of, levels, jnp.transpose(f_home, (1, 0, 2)))

    def unpack(table, got):
        return pl.pallas_call(
            unpack_kernel,
            out_shape=jax.ShapeDtypeStruct((19, patches, CELLS), f32),
            in_specs=[smem, vmem],
            out_specs=vmem,
            compiler_params=pltpu.CompilerParams(vmem_limit_bytes=40 * 1024 * 1024),
        )(table, got)

    def with_leftover(table, got, left):
        more, table = pl.pallas_call(
            lambda *refs: leftover_kernel(nb, nc, *refs),
            out_shape=(
                jax.ShapeDtypeStruct((devices,) + half, f32),
                jax.ShapeDtypeStruct((8, LANES), jnp.int32),
            ),
            in_specs=[vmem, vmem],
            out_specs=(vmem, vmem),
            scratch_shapes=[dma((devices,)), dma((devices,))],
            compiler_params=pltpu.CompilerParams(collective_id=1, has_side_effects=True),
        )(left, table)
        return unpack(table, jnp.concatenate([got, more], axis=0))

    out = lax.cond(table[1, 0] > 0, with_leftover, lambda table, got, left: unpack(table, got), table, got, left)
    return jnp.transpose(out, (1, 0, 2))


def solution(mesh):
    nb, nc = mesh.shape["blocks"], mesh.shape["cross"]
    in_specs = (P(("blocks", "cross"), None, None), P(("blocks", "cross")), P(("blocks", "cross")))
    out_specs = P(("blocks", "cross"), None, None)
    return jax.shard_map(
        lambda f, l, p: body(nb, nc, f, l, p),
        mesh=mesh, in_specs=in_specs, out_specs=out_specs, check_vma=False)
```

```python
import jax
import jax.numpy as jnp
from jax import lax
from jax.experimental import pallas as pl
from jax.experimental.pallas import tpu as pltpu
from jax.sharding import PartitionSpec as P

SPAN_PATCHES = 4
DEPTH_PATCHES = 8
STEPS = 2
CELLS = 512
VELOCITIES = (
    (0, 0, 0),
    (1, 0, 0),
    (-1, 0, 0),
    (0, 1, 0),
    (0, -1, 0),
    (0, 0, 1),
    (0, 0, -1),
    (1, 1, 0),
    (-1, -1, 0),
    (1, -1, 0),
    (-1, 1, 0),
    (1, 0, 1),
    (-1, 0, -1),
    (1, 0, -1),
    (-1, 0, 1),
    (0, 1, 1),
    (0, -1, -1),
    (0, 1, -1),
    (0, -1, 1),
)
WEIGHTS = (1.0 / 3.0,) + (1.0 / 18.0,) * 6 + (1.0 / 36.0,) * 12
TAU_COARSE = 0.55
TAU_FINE = 2.0 * TAU_COARSE - 0.5
RESCALE = TAU_FINE / (2.0 * TAU_COARSE)
INFLOW = 0.08
MESH = pl.DeviceIdType.MESH
MAIN = 16
TAIL = 3
HALF = 40
MARK = 38
FLAG = 39
LANES = 128
TILES = CELLS // LANES
Y_UP = [q for q in range(19) if VELOCITIES[q][1] == 1]
Y_DOWN = [q for q in range(19) if VELOCITIES[q][1] == -1]
X_UP = [q for q in range(19) if VELOCITIES[q][0] == 1]
X_DOWN = [q for q in range(19) if VELOCITIES[q][0] == -1]
DIAGONAL = [q for q in range(19) if VELOCITIES[q][0] and VELOCITIES[q][1]]
AROUND = [(dx, dy) for dx in (-1, 0, 1) for dy in (-1, 0, 1) if (dx, dy) != (0, 0)]


def relax_into(load, store, coef):
    f = [load(q) for q in range(19)]
    terms = list(f)
    while len(terms) > 1:
        pairs = [a + b for a, b in zip(terms[::2], terms[1::2])]
        terms = pairs + ([terms[-1]] if len(terms) % 2 else [])
    rho = terms[0]
    inv = 1.0 / rho
    u = []
    for axis in range(3):
        up = [f[q] for q in range(19) if VELOCITIES[q][axis] == 1]
        down = [f[q] for q in range(19) if VELOCITIES[q][axis] == -1]
        d = [a - b for a, b in zip(up, down)]
        u.append((((d[0] + d[1]) + (d[2] + d[3])) + d[4]) * inv)
    base = 1.0 - 1.5 * (u[0] * u[0] + u[1] * u[1] + u[2] * u[2])
    scaled = {w: w * rho for w in set(WEIGHTS)}
    for q in range(19):
        along = None
        for axis in range(3):
            e = VELOCITIES[q][axis]
            if e:
                term = u[axis] if e == 1 else -u[axis]
                along = term if along is None else along + term
        poly = base if along is None else base + along * (3.0 + 4.5 * along)
        balance = scaled[WEIGHTS[q]] * poly
        store(q, balance + coef(q) * (f[q] - balance))


def low_row(q, tile):
    return tile % 2 * MAIN + q if q < MAIN else 2 * MAIN + tile % 2 * TAIL + q - MAIN


def lattice_kernel(nb, nc, sidx, slot_of, level, f_ref, got_ref, left_ref, table_ref, st, pb, cq, pm, sent, second,
                   extra, theirs, lev_ref, lv, ys, yr, xs, xr, ds, dr, send_sem, recv_sem, lsend, lrecv, psend,
                   precv, esend, erecv, csend, crecv):
    others = nb * nc - 1
    side = nb * nc // 2
    b = lax.axis_index("blocks")
    c = lax.axis_index("cross")

    def at(dx, dy):
        return (lax.rem(b + dx + nb, nb), lax.rem(c + dy + nc, nc))

    me = b * nc + c

    def peer(k):
        return lax.bitwise_xor(me, jnp.where(k < side, side + k, k - side + 1))

    def device(d):
        return (d // nc, lax.rem(d, nc))

    barrier = pltpu.get_barrier_semaphore()

    def greet(k, carry):
        pl.semaphore_signal(barrier, inc=1, device_id=device(peer(k)), device_id_type=MESH)
        return carry

    lax.fori_loop(0, others, greet, 0)

    spot = lax.broadcasted_iota(jnp.int32, (SPAN_PATCHES, 8, LANES), 0) * 8
    spot = spot + lax.broadcasted_iota(jnp.int32, (SPAN_PATCHES, 8, LANES), 1)
    own = jnp.zeros((SPAN_PATCHES, 8, LANES), jnp.float32)
    for p in range(SPAN_PATCHES * 8):
        own = jnp.where(spot == p, level[p].astype(jnp.float32), own)
    lev_ref[...] = own

    for q in range(19):
        for r in range(SPAN_PATCHES):
            st[q, r] = f_ref[q, r * 8 : r * 8 + 8, :]
    pl.semaphore_wait(barrier, others)

    level_copies = []
    for n, (dx, dy) in enumerate(AROUND):
        copy = pltpu.make_async_remote_copy(
            src_ref=lev_ref, dst_ref=lv.at[n], send_sem=lsend.at[n], recv_sem=lrecv.at[n],
            device_id=at(-dx, -dy), device_id_type=MESH)
        copy.start()
        level_copies.append(copy)

    count = others + 1

    def patch_copy(k):
        d = peer(k)
        return pltpu.make_async_remote_copy(
            src_ref=sent.at[d], dst_ref=got_ref.at[pl.ds(2 * me, 2)], send_sem=psend.at[k],
            recv_sem=precv.at[k], device_id=device(d), device_id_type=MESH)

    def extra_copy(k):
        d = peer(k)
        return pltpu.make_async_remote_copy(
            src_ref=extra.at[d], dst_ref=got_ref.at[2 * count + me], send_sem=esend.at[k],
            recv_sem=erecv.at[k], device_id=device(d), device_id_type=MESH)

    for copy in level_copies:
        copy.wait()

    scale = {(0, 0): jnp.where(own > 0.5, RESCALE, 1.0)}
    for n, key in enumerate(AROUND):
        scale[key] = jnp.where(lv[n] > 0.5, RESCALE, 1.0)
    patch_scale = {}
    for dx in (-1, 0, 1):
        patch_scale[dx, 0] = scale[dx, 0]
        patch_scale[dx, 1] = jnp.concatenate([scale[dx, 0][1:], scale[dx, 1][:1]], axis=0)
        patch_scale[dx, -1] = jnp.concatenate([scale[dx, -1][-1:], scale[dx, 0][:-1]], axis=0)
    gain = jnp.where(own > 0.5, (1.0 - 1.0 / TAU_FINE) / RESCALE, 1.0 - 1.0 / TAU_COARSE)

    def target_scale(dx, dy, dz):
        value = patch_scale[dx, dy]
        return pltpu.roll(value, (-dz) % 8, axis=1) if dz else value

    shape = (SPAN_PATCHES, 8, LANES)
    lane = lax.broadcasted_iota(jnp.int32, shape, 2)
    for q in range(1, 19):
        e = VELOCITIES[q]
        kinds = [{}]
        for axis in range(3):
            if e[axis]:
                kinds = [{**k, axis: v} for k in kinds for v in (0, 1)]
        table = [(k, target_scale(*[e[a] * k.get(a, 0) for a in range(3)])) for k in kinds]
        for tile in range(TILES):
            cell = lane + tile * LANES
            coord = (cell // 64, (cell // 8) % 8, cell % 8)
            result = table[0][1]
            for k, value in table[1:]:
                mask = None
                for axis, on in k.items():
                    if on:
                        hit = coord[axis] == (7 if e[axis] == 1 else 0)
                        mask = hit if mask is None else mask & hit
                result = jnp.where(mask, value, result)
            cq[q - 1, :, :, tile * LANES : (tile + 1) * LANES] = gain * result

    full = (SPAN_PATCHES, 8, CELLS)
    cell = lax.broadcasted_iota(jnp.int32, full, 2)
    coord = (cell // 64, (cell // 8) % 8, cell % 8)
    entry = {
        (axis, e): coord[axis] == (0 if e == 1 else 7) for axis in range(3) for e in (1, -1)
    }
    lower = lane < 64
    half = lax.broadcasted_iota(jnp.int32, (2, 8, LANES), 2) < 64
    fine = jnp.broadcast_to(own[:, :, :1] > 0.5, full)
    in_tile = {
        (axis, e): (lane // 8 % 8 if axis == 1 else lane % 8) == (0 if e == 1 else 7)
        for axis in (1, 2) for e in (1, -1)
    }

    def spin(v, amount):
        return pltpu.roll(v, amount % LANES, axis=v.ndim - 1)

    def along_z(q, v):
        e = VELOCITIES[q][2]
        if not e:
            return v
        wrapped = pltpu.roll(spin(v, -7 * e), e % 8, axis=1)
        return jnp.where(in_tile[2, e][: v.shape[0]], wrapped, spin(v, e))

    def along_y(q, v, halo):
        e = VELOCITIES[q][1]
        moved = jnp.concatenate([halo, v[:-1]] if e == 1 else [v[1:], halo], axis=0)
        return jnp.where(in_tile[1, e], spin(moved, -56 * e), spin(v, 8 * e))

    def lanes_of(tile):
        return slice(tile * LANES, (tile + 1) * LANES)

    def step(s, carry):
        def first(r, tiles):
            plain = jnp.where(lev_ref[r] > 0.5, 1.0 - 1.0 / TAU_FINE, 1.0 - 1.0 / TAU_COARSE)
            for tile in tiles:
                lanes = lanes_of(tile)

                def put(q, value):
                    pb[q, r, :, lanes] = value

                relax_into(lambda q: st[q, r, :, lanes], put,
                           lambda q: cq[q - 1, r, :, lanes] if q else plain)

        def faces(r, carry):
            first(r, (0, TILES - 1))
            return carry

        lax.fori_loop(0, SPAN_PATCHES, faces, 0)
        for way, e, group in ((0, 1, X_UP), (1, -1, X_DOWN)):
            for n, q in enumerate(group):
                v = along_z(q, pb[q, :, :, lanes_of(TILES - 1 if e == 1 else 0)])
                turned = spin(v, 64)
                if e == 1:
                    xs[s, way, n] = jnp.where(half, turned[:2], v[2:])
                else:
                    xs[s, way, n] = jnp.where(half, v[:2], turned[2:])
                if q in DIAGONAL:
                    ds[s, DIAGONAL.index(q)] = turned[SPAN_PATCHES - 1 if VELOCITIES[q][1] == 1 else 0]
        x_copies = []

        def send(src, dst, n, to):
            copy = pltpu.make_async_remote_copy(
                src_ref=src, dst_ref=dst, send_sem=send_sem.at[s, n], recv_sem=recv_sem.at[s, n],
                device_id=to, device_id_type=MESH)
            copy.start()
            return copy

        def outer(m, carry):
            first(m * (SPAN_PATCHES - 1), range(1, TILES - 1))
            return carry

        def inner(r, carry):
            first(r, range(1, TILES - 1))
            return carry

        for way, dx in ((0, 1), (1, -1)):
            x_copies.append(send(xs.at[s, way], xr.at[s, way], 2 + way, at(dx, 0)))
        for n, q in enumerate(DIAGONAL):
            x_copies.append(send(ds.at[s, n], dr.at[s, n], 4 + n, at(*VELOCITIES[q][:2])))
        lax.fori_loop(0, 2, outer, 0)
        for way, e, group in ((0, 1, Y_UP), (1, -1, Y_DOWN)):
            r = SPAN_PATCHES - 1 if e == 1 else 0
            for n, q in enumerate(group):
                for tile in range(TILES):
                    ys[s, way, n, :, lanes_of(tile)] = along_z(q, pb[q, r : r + 1, :, lanes_of(tile)])[0]
        y_copies = []
        for way, dy in ((0, 1), (1, -1)):
            y_copies.append(send(ys.at[s, way], yr.at[s, way], way, at(0, dy)))
        lax.fori_loop(1, SPAN_PATCHES - 1, inner, 0)

        def shift(q):
            e = VELOCITIES[q]
            tiles = [along_z(q, pb[q, :, :, lanes_of(tile)]) for tile in range(TILES)]
            if e[1]:
                way, group = (0, Y_UP) if e[1] == 1 else (1, Y_DOWN)
                n = group.index(q)
                tiles = [along_y(q, v, yr[s, way, n, :, lanes_of(tile)][None]) for tile, v in enumerate(tiles)]
            if e[0]:
                turned = [spin(v, 64) for v in tiles]
                for tile in range(TILES):
                    if e[0] == 1:
                        tiles[tile] = jnp.where(lower, turned[tile - 1], turned[tile])
                    else:
                        tiles[tile] = jnp.where(lower, turned[tile], turned[(tile + 1) % TILES])
            for tile in range(TILES):
                st[q, :, :, lanes_of(tile)] = tiles[tile]

        for q in range(19):
            if not VELOCITIES[q][1]:
                shift(q)
        for copy in y_copies:
            copy.wait()
        for q in range(19):
            if VELOCITIES[q][1]:
                shift(q)

        def again(r, tiles):
            for tile in tiles:
                lanes = lanes_of(tile)

                def put(q, value):
                    pb[q, r, :, lanes] = value

                relax_into(lambda q: st[q, r, :, lanes], put, lambda q: 1.0 - 1.0 / TAU_FINE)

        def middle(r, carry):
            again(r, range(1, TILES - 1))
            return carry

        lax.fori_loop(0, SPAN_PATCHES, middle, 0)
        for copy in x_copies:
            copy.wait()
        for way, e, group in ((0, 1, X_UP), (1, -1, X_DOWN)):
            outside = b == (0 if e == 1 else nb - 1)
            for n, q in enumerate(group):
                h = xr[s, way, n]
                turned = spin(h, 64)
                halo = jnp.concatenate([h, turned] if e == 1 else [turned, h], axis=0)
                if q in DIAGONAL:
                    halo = along_y(q, halo, dr[s, DIAGONAL.index(q)][None])
                along = e * INFLOW
                const = WEIGHTS[q] * (1.0 + 3.0 * along + 4.5 * along * along - 1.5 * INFLOW * INFLOW)
                halo = jnp.where(outside, jnp.full(halo.shape, const, jnp.float32), halo)
                lanes = lanes_of(0 if e == 1 else TILES - 1)
                keep = st[q, :, :, lanes]
                st[q, :, :, lanes] = jnp.where(lower, halo, keep) if e == 1 else jnp.where(lower, keep, halo)

        def ends(r, carry):
            again(r, (0, TILES - 1))
            return carry

        lax.fori_loop(0, SPAN_PATCHES, ends, 0)
        for q in range(19):
            e = VELOCITIES[q]
            take = fine
            for axis in range(3):
                if e[axis]:
                    take = take & ~entry[axis, e[axis]]
            moved = pb[q]
            if q:
                moved = pltpu.roll(moved, (64 * e[0] + 8 * e[1] + e[2]) % CELLS, axis=2)
            st[q] = jnp.where(take, moved, st[q])
        return carry

    lax.fori_loop(0, STEPS, step, 0)

    pm[:, 2 * MAIN : HALF, :] = jnp.zeros((pm.shape[0], HALF - 2 * MAIN, LANES), jnp.float32)
    pm[:, HALF + 2 * MAIN :, :] = jnp.zeros((pm.shape[0], HALF - 2 * MAIN, LANES), jnp.float32)
    for q in range(19):
        for r in range(SPAN_PATCHES):
            for tile in range(TILES):
                row = tile // 2 * HALF + low_row(q, tile)
                pm[r * 8 : r * 8 + 8, row, :] = st[q, r, :, tile * LANES : (tile + 1) * LANES]

    def tag(value):
        return jnp.full((1, LANES), value.astype(jnp.float32), jnp.float32)

    def pack(d):
        p = sidx[2 * d]
        sent[d, 0] = pm[p, :HALF]
        sent[d, 1] = pm[p, HALF:]
        sent[d, 0, MARK : MARK + 1, :] = tag(slot_of[2 * d])

    def post(k, carry):
        pack(peer(k))

        @pl.when(k > 0)
        def _():
            patch_copy(k - 1).start()

        return carry

    lax.fori_loop(0, others, post, 0)
    pack(me)

    def half_rows(which):
        return pl.ds(pl.multiple_of(which * HALF, HALF), HALF)

    def pack_second(d, carry):
        second[d] = pm[sidx[2 * d + 1], half_rows(1 - c), :]
        second[d, MARK : MARK + 1, :] = tag(slot_of[2 * d + 1])
        return carry

    lax.fori_loop(0, count, pack_second, 0)
    patch_copy(others - 1).start()
    got_ref[2 * me] = sent[me, 0]
    got_ref[2 * me + 1] = sent[me, 1]
    swap = pltpu.make_async_remote_copy(
        src_ref=second, dst_ref=theirs, send_sem=csend, recv_sem=crecv,
        device_id=at(0, 1), device_id_type=MESH)
    swap.start()
    swap.wait()
    both = jnp.where((second[:, MARK, :] > -0.5) & (theirs[:, MARK, :] > -0.5), 1.0, 0.0)
    flag = jnp.max(both, axis=0, keepdims=True)
    zero = c == 0

    def pack_extra(d):
        mine = pm[sidx[2 * d + 1], half_rows(c), :]
        other = theirs[d]
        my_tag = tag(slot_of[2 * d + 1])
        other_tag = other[MARK : MARK + 1]
        has_mine = my_tag > -0.5
        has_other = other_tag > -0.5
        keep = (has_mine & zero) | ~has_other
        extra[d] = jnp.where(keep, mine, other)
        extra[d, MARK : MARK + 1, :] = jnp.where(keep, my_tag, other_tag)
        extra[d, FLAG : FLAG + 1, :] = flag
        left_ref[d] = jnp.where(zero, other, mine)
        left_ref[d, MARK : MARK + 1, :] = jnp.where(
            has_mine & has_other, jnp.where(zero, other_tag, my_tag), -1.0
        )

    def post_extra(k, carry):
        pack_extra(peer(k))

        @pl.when(k > 0)
        def _():
            extra_copy(k - 1).start()

        return carry

    lax.fori_loop(0, others, post_extra, 0)
    pack_extra(me)
    extra_copy(others - 1).start()
    got_ref[2 * count + me] = extra[me]

    def finish(k, carry):
        patch_copy(k).wait()
        extra_copy(k).wait()
        return carry

    lax.fori_loop(0, others, finish, 0)
    source = lax.broadcasted_iota(jnp.int32, (2 * count, LANES), 0)
    wanted = lax.broadcasted_iota(jnp.int32, (2 * count, LANES), 1).astype(jnp.float32)
    first_hit = (got_ref[: 2 * count, MARK, :] == wanted) & (source % 2 == 0)
    index = jnp.sum(jnp.where(first_hit, source, 0), axis=0, keepdims=True)
    source = source[:count]
    extra_hit = (got_ref[2 * count :, MARK, :] == wanted[:count]) & (source % nc == 0)
    index = index + jnp.sum(jnp.where(extra_hit, source + 2 * count, 0), axis=0, keepdims=True)
    over = jnp.max(got_ref[2 * count :, FLAG, :], axis=0, keepdims=True)
    row = lax.broadcasted_iota(jnp.int32, (8, LANES), 0)
    table_ref[...] = jnp.where(row == 0, index, jnp.where(over > 0.5, 1, 0))


def leftover_kernel(nb, nc, left_ref, table_ref, got_ref, new_table_ref, send_sem, recv_sem):
    count = nb * nc
    me = lax.axis_index("blocks") * nc + lax.axis_index("cross")

    def device(d):
        return (d // nc, lax.rem(d, nc))

    barrier = pltpu.get_barrier_semaphore()

    def greet(k, carry):
        pl.semaphore_signal(barrier, inc=1, device_id=device(lax.bitwise_xor(me, k)), device_id_type=MESH)
        return carry

    lax.fori_loop(1, count, greet, 0)
    pl.semaphore_wait(barrier, count - 1)

    def left_copy(k):
        d = lax.bitwise_xor(me, k)
        return pltpu.make_async_remote_copy(
            src_ref=left_ref.at[d], dst_ref=got_ref.at[me], send_sem=send_sem.at[k],
            recv_sem=recv_sem.at[k], device_id=device(d), device_id_type=MESH)

    def post(k, carry):
        left_copy(k).start()
        return carry

    def finish(k, carry):
        left_copy(k).wait()
        return carry

    lax.fori_loop(1, count, post, 0)
    got_ref[me] = left_ref[me]
    lax.fori_loop(1, count, finish, 0)
    source = lax.broadcasted_iota(jnp.int32, (count, LANES), 0)
    wanted = lax.broadcasted_iota(jnp.int32, (count, LANES), 1).astype(jnp.float32)
    hit = (got_ref[:, MARK, :] == wanted) & (source % nc == 0)
    index = jnp.sum(jnp.where(hit, source + 3 * count, 0), axis=0, keepdims=True)
    new_table_ref[...] = table_ref[...] + index


def unpack_kernel(ridx, got_ref, out_ref):
    for t in range(out_ref.shape[1]):
        base = ridx[0, t]
        for tile in range(TILES):
            block = got_ref.at[base + tile // 2]
            lanes = slice(tile * LANES, (tile + 1) * LANES)
            low = low_row(0, tile)
            out_ref[:MAIN, t, lanes] = block[low : low + MAIN, :]
            low = low_row(MAIN, tile)
            out_ref[MAIN:, t, lanes] = block[2 * MAIN :, :][low - 2 * MAIN : low - 2 * MAIN + TAIL]


def body(nb, nc, f_home, levels, plan):
    devices = nb * nc
    patches = f_home.shape[0]
    target = plan // patches
    order = jnp.arange(patches, dtype=jnp.int32)
    earlier = (target[:, None] == target[None, :]) & (order[None, :] < order[:, None])
    place = 2 * target + jnp.sum(earlier.astype(jnp.int32), axis=1)
    hit = place[None, :] == jnp.arange(2 * devices, dtype=jnp.int32)[:, None]
    sidx = jnp.sum(jnp.where(hit, order[None, :], 0), axis=1)
    slot_of = jnp.sum(jnp.where(hit, plan[None, :] % patches + 1, 0), axis=1) - 1
    vmem = pl.BlockSpec(memory_space=pltpu.VMEM)
    smem = pl.BlockSpec(memory_space=pltpu.SMEM)
    state = (19, SPAN_PATCHES, 8, CELLS)
    small = (SPAN_PATCHES, 8, LANES)
    f32 = jnp.float32
    dma = pltpu.SemaphoreType.DMA
    half = (HALF, LANES)
    limit = pltpu.CompilerParams(collective_id=0, has_side_effects=True, vmem_limit_bytes=60 * 1024 * 1024)
    got, left, table = pl.pallas_call(
        lambda *refs: lattice_kernel(nb, nc, *refs),
        out_shape=(
            jax.ShapeDtypeStruct((3 * devices,) + half, f32),
            jax.ShapeDtypeStruct((devices,) + half, f32),
            jax.ShapeDtypeStruct((8, LANES), jnp.int32),
        ),
        in_specs=[smem, smem, smem, vmem],
        out_specs=(vmem, vmem, vmem),
        scratch_shapes=[
            pltpu.VMEM(state, f32),
            pltpu.VMEM(state, f32),
            pltpu.VMEM((18,) + state[1:], f32),
            pltpu.VMEM((patches, 2 * HALF, LANES), f32),
            pltpu.VMEM((devices, 2) + half, f32),
            pltpu.VMEM((devices,) + half, f32),
            pltpu.VMEM((devices,) + half, f32),
            pltpu.VMEM((devices,) + half, f32),
            pltpu.VMEM(small, f32),
            pltpu.VMEM((len(AROUND),) + small, f32),
            pltpu.VMEM((STEPS, 2, 5, 8, CELLS), f32),
            pltpu.VMEM((STEPS, 2, 5, 8, CELLS), f32),
            pltpu.VMEM((STEPS, 2, 5, 2, 8, LANES), f32),
            pltpu.VMEM((STEPS, 2, 5, 2, 8, LANES), f32),
            pltpu.VMEM((STEPS, len(DIAGONAL), 8, LANES), f32),
            pltpu.VMEM((STEPS, len(DIAGONAL), 8, LANES), f32),
            dma((STEPS, 8)),
            dma((STEPS, 8)),
            dma((len(AROUND),)),
            dma((len(AROUND),)),
            dma((devices - 1,)),
            dma((devices - 1,)),
            dma((devices - 1,)),
            dma((devices - 1,)),
            dma,
            dma,
        ],
        compiler_params=limit,
    )(sidx, slot_of, levels, jnp.transpose(f_home, (1, 0, 2)))

    def unpack(table, got):
        return pl.pallas_call(
            unpack_kernel,
            out_shape=jax.ShapeDtypeStruct((19, patches, CELLS), f32),
            in_specs=[smem, vmem],
            out_specs=vmem,
            compiler_params=pltpu.CompilerParams(vmem_limit_bytes=40 * 1024 * 1024),
        )(table, got)

    def with_leftover(table, got, left):
        more, table = pl.pallas_call(
            lambda *refs: leftover_kernel(nb, nc, *refs),
            out_shape=(
                jax.ShapeDtypeStruct((devices,) + half, f32),
                jax.ShapeDtypeStruct((8, LANES), jnp.int32),
            ),
            in_specs=[vmem, vmem],
            out_specs=(vmem, vmem),
            scratch_shapes=[dma((devices,)), dma((devices,))],
            compiler_params=pltpu.CompilerParams(collective_id=1, has_side_effects=True),
        )(left, table)
        return unpack(table, jnp.concatenate([got, more], axis=0))

    out = lax.cond(table[1, 0] > 0, with_leftover, lambda table, got, left: unpack(table, got), table, got, left)
    return jnp.transpose(out, (1, 0, 2))


def solution(mesh):
    nb, nc = mesh.shape["blocks"], mesh.shape["cross"]
    in_specs = (P(("blocks", "cross"), None, None), P(("blocks", "cross")), P(("blocks", "cross")))
    out_specs = P(("blocks", "cross"), None, None)
    return jax.shard_map(
        lambda f, l, p: body(nb, nc, f, l, p),
        mesh=mesh, in_specs=in_specs, out_specs=out_specs, check_vma=False)
```

```python
import jax
import jax.numpy as jnp
from jax import lax
from jax.experimental import pallas as pl
from jax.experimental.pallas import tpu as pltpu
from jax.sharding import PartitionSpec as P

SPAN_PATCHES = 4
DEPTH_PATCHES = 8
STEPS = 2
CELLS = 512
VELOCITIES = (
    (0, 0, 0),
    (1, 0, 0),
    (-1, 0, 0),
    (0, 1, 0),
    (0, -1, 0),
    (0, 0, 1),
    (0, 0, -1),
    (1, 1, 0),
    (-1, -1, 0),
    (1, -1, 0),
    (-1, 1, 0),
    (1, 0, 1),
    (-1, 0, -1),
    (1, 0, -1),
    (-1, 0, 1),
    (0, 1, 1),
    (0, -1, -1),
    (0, 1, -1),
    (0, -1, 1),
)
WEIGHTS = (1.0 / 3.0,) + (1.0 / 18.0,) * 6 + (1.0 / 36.0,) * 12
TAU_COARSE = 0.55
TAU_FINE = 2.0 * TAU_COARSE - 0.5
RESCALE = TAU_FINE / (2.0 * TAU_COARSE)
INFLOW = 0.08
MESH = pl.DeviceIdType.MESH
MAIN = 16
TAIL = 3
HALF = 40
MARK = 38
FLAG = 39
LANES = 128
TILES = CELLS // LANES
Y_UP = [q for q in range(19) if VELOCITIES[q][1] == 1]
Y_DOWN = [q for q in range(19) if VELOCITIES[q][1] == -1]
X_UP = [q for q in range(19) if VELOCITIES[q][0] == 1]
X_DOWN = [q for q in range(19) if VELOCITIES[q][0] == -1]
DIAGONAL = [q for q in range(19) if VELOCITIES[q][0] and VELOCITIES[q][1]]
AROUND = [(dx, dy) for dx in (-1, 0, 1) for dy in (-1, 0, 1) if (dx, dy) != (0, 0)]


def relax_into(load, store, coef):
    f = [load(q) for q in range(19)]
    terms = list(f)
    while len(terms) > 1:
        pairs = [a + b for a, b in zip(terms[::2], terms[1::2])]
        terms = pairs + ([terms[-1]] if len(terms) % 2 else [])
    rho = terms[0]
    inv = 1.0 / rho
    u = []
    for axis in range(3):
        up = [f[q] for q in range(19) if VELOCITIES[q][axis] == 1]
        down = [f[q] for q in range(19) if VELOCITIES[q][axis] == -1]
        d = [a - b for a, b in zip(up, down)]
        u.append((((d[0] + d[1]) + (d[2] + d[3])) + d[4]) * inv)
    base = 1.0 - 1.5 * (u[0] * u[0] + u[1] * u[1] + u[2] * u[2])
    scaled = {w: w * rho for w in set(WEIGHTS)}
    for q in range(19):
        along = None
        for axis in range(3):
            e = VELOCITIES[q][axis]
            if e:
                term = u[axis] if e == 1 else -u[axis]
                along = term if along is None else along + term
        poly = base if along is None else base + along * (3.0 + 4.5 * along)
        balance = scaled[WEIGHTS[q]] * poly
        store(q, balance + coef(q) * (f[q] - balance))


def low_row(q, tile):
    return tile % 2 * MAIN + q if q < MAIN else 2 * MAIN + tile % 2 * TAIL + q - MAIN


def lattice_kernel(nb, nc, level, plan_ref, f_ref, got_ref, left_ref, table_ref, st, pb, cq, pm, sent, second,
                   extra, theirs, lev_ref, lv, ys, yr, xs, xr, ds, dr, pick, pick_s, tags, send_sem, recv_sem, lsend, lrecv, psend,
                   precv, esend, erecv, csend, crecv, pick_sem, up_sem, down_sem):
    others = nb * nc - 1
    rounds = max(2 * STEPS + 1, (nb - 1).bit_length())
    side = nb * nc // 2
    b = lax.axis_index("blocks")
    c = lax.axis_index("cross")

    def at(dx, dy):
        return (lax.rem(b + dx + nb, nb), lax.rem(c + dy + nc, nc))

    me = b * nc + c

    def peer(k):
        return lax.bitwise_xor(me, jnp.where(k < side, side + k, k - side + 1))

    def device(d):
        return (d // nc, lax.rem(d, nc))

    barrier = pltpu.get_barrier_semaphore()
    above = b < nb - 1
    below = b > 0

    def signal(sem, to):
        pl.semaphore_signal(sem, inc=1, device_id=to, device_id_type=MESH)

    for k in range(1, nc):
        signal(barrier, at(0, k))
    for there, dx in ((above, 1), (below, -1)):
        @pl.when(there)
        def _():
            for k in range(nc):
                signal(barrier, at(dx, k))

    def tell(k):
        hop = lax.shift_left(jnp.int32(1), jnp.int32(k))

        @pl.when(b + hop < nb)
        def _():
            signal(up_sem.at[k], (b + hop, c))

        @pl.when(b >= hop)
        def _():
            signal(down_sem.at[k], (b - hop, c))

    def hear(k):
        hop = lax.shift_left(jnp.int32(1), jnp.int32(k))

        @pl.when(b >= hop)
        def _():
            pl.semaphore_wait(up_sem.at[k], 1)

        @pl.when(b + hop < nb)
        def _():
            pl.semaphore_wait(down_sem.at[k], 1)

    patches = f_ref.shape[1]
    count = nb * nc
    target = lax.broadcasted_iota(jnp.int32, (count, patches), 0)
    where = jnp.broadcast_to(plan_ref[...], (count, patches))
    member = where // patches == target
    key = lax.broadcasted_iota(jnp.int32, (count, patches), 1) * patches + where % patches
    low_key = jnp.min(jnp.where(member, key, patches * patches), axis=1, keepdims=True)
    high_key = jnp.max(jnp.where(member, key, -1), axis=1, keepdims=True)
    some = high_key >= 0
    two = high_key > low_key
    column = lax.broadcasted_iota(jnp.int32, (count, LANES), 1)
    pick[...] = jnp.where(column == 0, jnp.where(some, low_key // patches, 0),
                          jnp.where(two, high_key // patches, 0))
    to_scalars = pltpu.make_async_copy(pick, pick_s, pick_sem)
    to_scalars.start()
    tags[0] = jnp.broadcast_to(jnp.where(some, low_key % patches, -1), (count, LANES)).astype(jnp.float32)
    tags[1] = jnp.broadcast_to(jnp.where(two, high_key % patches, -1), (count, LANES)).astype(jnp.float32)

    spot = lax.broadcasted_iota(jnp.int32, (SPAN_PATCHES, 8, LANES), 0) * 8
    spot = spot + lax.broadcasted_iota(jnp.int32, (SPAN_PATCHES, 8, LANES), 1)
    own = jnp.zeros((SPAN_PATCHES, 8, LANES), jnp.float32)
    for p in range(SPAN_PATCHES * 8):
        own = jnp.where(spot == p, level[p].astype(jnp.float32), own)
    lev_ref[...] = own

    for q in range(19):
        for r in range(SPAN_PATCHES):
            st[q, r] = f_ref[q, r * 8 : r * 8 + 8, :]
    pl.semaphore_wait(barrier, nc - 1 + nc * (jnp.where(above, 1, 0) + jnp.where(below, 1, 0)))
    tell(0)

    def start_to(there, copy):
        if there is None:
            copy.start()
        else:
            pl.when(there)(copy.start)

    def wait_for(outgoing, incoming, copy):
        if outgoing is None:
            copy.wait()
        else:
            pl.when(outgoing)(copy.wait_send)
            pl.when(incoming)(copy.wait_recv)

    def ends_of(dx):
        return {0: (None, None), 1: (above, below), -1: (below, above)}[dx]

    level_copies = []
    for n, (dx, dy) in enumerate(AROUND):
        copy = pltpu.make_async_remote_copy(
            src_ref=lev_ref, dst_ref=lv.at[n], send_sem=lsend.at[n], recv_sem=lrecv.at[n],
            device_id=at(-dx, -dy), device_id_type=MESH)
        outgoing, incoming = ends_of(-dx)
        start_to(outgoing, copy)
        level_copies.append((outgoing, incoming, copy))

    def patch_copy(k):
        d = peer(k)
        return pltpu.make_async_remote_copy(
            src_ref=sent.at[d], dst_ref=got_ref.at[pl.ds(2 * me, 2)], send_sem=psend.at[k],
            recv_sem=precv.at[k], device_id=device(d), device_id_type=MESH)

    def extra_copy(k):
        d = peer(k)
        return pltpu.make_async_remote_copy(
            src_ref=extra.at[d], dst_ref=got_ref.at[2 * count + me], send_sem=esend.at[k],
            recv_sem=erecv.at[k], device_id=device(d), device_id_type=MESH)

    for copy in level_copies:
        wait_for(*copy)

    scale = {(0, 0): jnp.where(own > 0.5, RESCALE, 1.0)}
    for n, key in enumerate(AROUND):
        scale[key] = jnp.where(lv[n] > 0.5, RESCALE, 1.0)
    patch_scale = {}
    for dx in (-1, 0, 1):
        patch_scale[dx, 0] = scale[dx, 0]
        patch_scale[dx, 1] = jnp.concatenate([scale[dx, 0][1:], scale[dx, 1][:1]], axis=0)
        patch_scale[dx, -1] = jnp.concatenate([scale[dx, -1][-1:], scale[dx, 0][:-1]], axis=0)
    gain = jnp.where(own > 0.5, (1.0 - 1.0 / TAU_FINE) / RESCALE, 1.0 - 1.0 / TAU_COARSE)

    def target_scale(dx, dy, dz):
        value = patch_scale[dx, dy]
        return pltpu.roll(value, (-dz) % 8, axis=1) if dz else value

    shape = (SPAN_PATCHES, 8, LANES)
    lane = lax.broadcasted_iota(jnp.int32, shape, 2)
    for q in range(1, 19):
        e = VELOCITIES[q]
        kinds = [{}]
        for axis in range(3):
            if e[axis]:
                kinds = [{**k, axis: v} for k in kinds for v in (0, 1)]
        table = [(k, target_scale(*[e[a] * k.get(a, 0) for a in range(3)])) for k in kinds]
        for tile in range(TILES):
            cell = lane + tile * LANES
            coord = (cell // 64, (cell // 8) % 8, cell % 8)
            result = table[0][1]
            for k, value in table[1:]:
                mask = None
                for axis, on in k.items():
                    if on:
                        hit = coord[axis] == (7 if e[axis] == 1 else 0)
                        mask = hit if mask is None else mask & hit
                result = jnp.where(mask, value, result)
            cq[q - 1, :, :, tile * LANES : (tile + 1) * LANES] = gain * result

    full = (SPAN_PATCHES, 8, CELLS)
    cell = lax.broadcasted_iota(jnp.int32, full, 2)
    coord = (cell // 64, (cell // 8) % 8, cell % 8)
    entry = {
        (axis, e): coord[axis] == (0 if e == 1 else 7) for axis in range(3) for e in (1, -1)
    }
    lower = lane < 64
    half = lax.broadcasted_iota(jnp.int32, (2, 8, LANES), 2) < 64
    fine = jnp.broadcast_to(own[:, :, :1] > 0.5, full)
    in_tile = {
        (axis, e): (lane // 8 % 8 if axis == 1 else lane % 8) == (0 if e == 1 else 7)
        for axis in (1, 2) for e in (1, -1)
    }

    def spin(v, amount):
        return pltpu.roll(v, amount % LANES, axis=v.ndim - 1)

    def along_z(q, v):
        e = VELOCITIES[q][2]
        if not e:
            return v
        wrapped = pltpu.roll(spin(v, -7 * e), e % 8, axis=1)
        return jnp.where(in_tile[2, e][: v.shape[0]], wrapped, spin(v, e))

    def along_y(q, v, halo):
        e = VELOCITIES[q][1]
        moved = jnp.concatenate([halo, v[:-1]] if e == 1 else [v[1:], halo], axis=0)
        return jnp.where(in_tile[1, e], spin(moved, -56 * e), spin(v, 8 * e))

    def lanes_of(tile):
        return slice(tile * LANES, (tile + 1) * LANES)

    def step(s, carry):
        def first(r, tiles):
            plain = jnp.where(lev_ref[r] > 0.5, 1.0 - 1.0 / TAU_FINE, 1.0 - 1.0 / TAU_COARSE)
            for tile in tiles:
                lanes = lanes_of(tile)

                def put(q, value):
                    pb[q, r, :, lanes] = value

                relax_into(lambda q: st[q, r, :, lanes], put,
                           lambda q: cq[q - 1, r, :, lanes] if q else plain)

        def faces(r, carry):
            first(r, (0, TILES - 1))
            return carry

        lax.fori_loop(0, SPAN_PATCHES, faces, 0)
        for way, e, group in ((0, 1, X_UP), (1, -1, X_DOWN)):
            for n, q in enumerate(group):
                v = along_z(q, pb[q, :, :, lanes_of(TILES - 1 if e == 1 else 0)])
                turned = spin(v, 64)
                if e == 1:
                    xs[s, way, n] = jnp.where(half, turned[:2], v[2:])
                else:
                    xs[s, way, n] = jnp.where(half, v[:2], turned[2:])
                if q in DIAGONAL:
                    ds[s, DIAGONAL.index(q)] = turned[SPAN_PATCHES - 1 if VELOCITIES[q][1] == 1 else 0]
        x_copies = []

        def send(src, dst, n, dx, dy):
            copy = pltpu.make_async_remote_copy(
                src_ref=src, dst_ref=dst, send_sem=send_sem.at[s, n], recv_sem=recv_sem.at[s, n],
                device_id=at(dx, dy), device_id_type=MESH)
            outgoing, incoming = ends_of(dx)
            start_to(outgoing, copy)
            return outgoing, incoming, copy

        def outer(m, carry):
            first(m * (SPAN_PATCHES - 1), range(1, TILES - 1))
            return carry

        def inner(r, carry):
            first(r, range(1, TILES - 1))
            return carry

        for way, dx in ((0, 1), (1, -1)):
            x_copies.append(send(xs.at[s, way], xr.at[s, way], 2 + way, dx, 0))
        for n, q in enumerate(DIAGONAL):
            x_copies.append(send(ds.at[s, n], dr.at[s, n], 4 + n, *VELOCITIES[q][:2]))
        lax.fori_loop(0, 2, outer, 0)
        for way, e, group in ((0, 1, Y_UP), (1, -1, Y_DOWN)):
            r = SPAN_PATCHES - 1 if e == 1 else 0
            for n, q in enumerate(group):
                for tile in range(TILES):
                    ys[s, way, n, :, lanes_of(tile)] = along_z(q, pb[q, r : r + 1, :, lanes_of(tile)])[0]
        y_copies = []
        for way, dy in ((0, 1), (1, -1)):
            y_copies.append(send(ys.at[s, way], yr.at[s, way], way, 0, dy))
        lax.fori_loop(1, SPAN_PATCHES - 1, inner, 0)

        def shift(q):
            e = VELOCITIES[q]
            tiles = [along_z(q, pb[q, :, :, lanes_of(tile)]) for tile in range(TILES)]
            if e[1]:
                way, group = (0, Y_UP) if e[1] == 1 else (1, Y_DOWN)
                n = group.index(q)
                tiles = [along_y(q, v, yr[s, way, n, :, lanes_of(tile)][None]) for tile, v in enumerate(tiles)]
            if e[0]:
                turned = [spin(v, 64) for v in tiles]
                for tile in range(TILES):
                    if e[0] == 1:
                        tiles[tile] = jnp.where(lower, turned[tile - 1], turned[tile])
                    else:
                        tiles[tile] = jnp.where(lower, turned[tile], turned[(tile + 1) % TILES])
            for tile in range(TILES):
                st[q, :, :, lanes_of(tile)] = tiles[tile]

        for q in range(19):
            if not VELOCITIES[q][1]:
                shift(q)
        for copy in y_copies:
            wait_for(*copy)
        hear(2 * s)
        tell(2 * s + 1)
        for q in range(19):
            if VELOCITIES[q][1]:
                shift(q)

        def again(r, tiles):
            for tile in tiles:
                lanes = lanes_of(tile)

                def put(q, value):
                    pb[q, r, :, lanes] = value

                relax_into(lambda q: st[q, r, :, lanes], put, lambda q: 1.0 - 1.0 / TAU_FINE)

        def middle(r, carry):
            again(r, range(1, TILES - 1))
            return carry

        lax.fori_loop(0, SPAN_PATCHES, middle, 0)
        for copy in x_copies:
            wait_for(*copy)
        hear(2 * s + 1)
        tell(2 * s + 2)
        for way, e, group in ((0, 1, X_UP), (1, -1, X_DOWN)):
            outside = b == (0 if e == 1 else nb - 1)
            for n, q in enumerate(group):
                h = xr[s, way, n]
                turned = spin(h, 64)
                halo = jnp.concatenate([h, turned] if e == 1 else [turned, h], axis=0)
                if q in DIAGONAL:
                    halo = along_y(q, halo, dr[s, DIAGONAL.index(q)][None])
                along = e * INFLOW
                const = WEIGHTS[q] * (1.0 + 3.0 * along + 4.5 * along * along - 1.5 * INFLOW * INFLOW)
                halo = jnp.where(outside, jnp.full(halo.shape, const, jnp.float32), halo)
                lanes = lanes_of(0 if e == 1 else TILES - 1)
                keep = st[q, :, :, lanes]
                st[q, :, :, lanes] = jnp.where(lower, halo, keep) if e == 1 else jnp.where(lower, keep, halo)

        def ends(r, carry):
            again(r, (0, TILES - 1))
            return carry

        lax.fori_loop(0, SPAN_PATCHES, ends, 0)
        for q in range(19):
            e = VELOCITIES[q]
            take = fine
            for axis in range(3):
                if e[axis]:
                    take = take & ~entry[axis, e[axis]]
            moved = pb[q]
            if q:
                moved = pltpu.roll(moved, (64 * e[0] + 8 * e[1] + e[2]) % CELLS, axis=2)
            st[q] = jnp.where(take, moved, st[q])
        return carry

    lax.fori_loop(0, STEPS, step, 0)
    for k in range(2 * STEPS, rounds - 1):
        hear(k)
        tell(k + 1)
    hear(rounds - 1)
    to_scalars.wait()

    pm[:, 2 * MAIN : HALF, :] = jnp.zeros((pm.shape[0], HALF - 2 * MAIN, LANES), jnp.float32)
    pm[:, HALF + 2 * MAIN :, :] = jnp.zeros((pm.shape[0], HALF - 2 * MAIN, LANES), jnp.float32)
    for q in range(19):
        for r in range(SPAN_PATCHES):
            for tile in range(TILES):
                row = tile // 2 * HALF + low_row(q, tile)
                pm[r * 8 : r * 8 + 8, row, :] = st[q, r, :, tile * LANES : (tile + 1) * LANES]

    def pack(d):
        p = pick_s[d, 0]
        sent[d, 0] = pm[p, :HALF]
        sent[d, 1] = pm[p, HALF:]
        sent[d, 0, MARK : MARK + 1, :] = tags[0, pl.ds(d, 1), :]

    def post(k, carry):
        pack(peer(k))

        @pl.when(k > 0)
        def _():
            patch_copy(k - 1).start()

        return carry

    lax.fori_loop(0, others, post, 0)
    pack(me)

    def half_rows(which):
        return pl.ds(pl.multiple_of(which * HALF, HALF), HALF)

    def pack_second(d, carry):
        second[d] = pm[pick_s[d, 1], half_rows(1 - c), :]
        second[d, MARK : MARK + 1, :] = tags[1, pl.ds(d, 1), :]
        return carry

    lax.fori_loop(0, count, pack_second, 0)
    patch_copy(others - 1).start()
    got_ref[2 * me] = sent[me, 0]
    got_ref[2 * me + 1] = sent[me, 1]
    swap = pltpu.make_async_remote_copy(
        src_ref=second, dst_ref=theirs, send_sem=csend, recv_sem=crecv,
        device_id=at(0, 1), device_id_type=MESH)
    swap.start()
    swap.wait()
    both = jnp.where((second[:, MARK, :] > -0.5) & (theirs[:, MARK, :] > -0.5), 1.0, 0.0)
    flag = jnp.max(both, axis=0, keepdims=True)
    zero = c == 0

    def pack_extra(d):
        mine = pm[pick_s[d, 1], half_rows(c), :]
        other = theirs[d]
        my_tag = tags[1, pl.ds(d, 1), :]
        other_tag = other[MARK : MARK + 1]
        has_mine = my_tag > -0.5
        has_other = other_tag > -0.5
        keep = (has_mine & zero) | ~has_other
        extra[d] = jnp.where(keep, mine, other)
        extra[d, MARK : MARK + 1, :] = jnp.where(keep, my_tag, other_tag)
        extra[d, FLAG : FLAG + 1, :] = flag
        left_ref[d] = jnp.where(zero, other, mine)
        left_ref[d, MARK : MARK + 1, :] = jnp.where(
            has_mine & has_other, jnp.where(zero, other_tag, my_tag), -1.0
        )

    def post_extra(k, carry):
        pack_extra(peer(k))

        @pl.when(k > 0)
        def _():
            extra_copy(k - 1).start()

        return carry

    lax.fori_loop(0, others, post_extra, 0)
    pack_extra(me)
    extra_copy(others - 1).start()
    got_ref[2 * count + me] = extra[me]

    def finish(k, carry):
        patch_copy(k).wait()
        extra_copy(k).wait()
        return carry

    lax.fori_loop(0, others, finish, 0)
    source = lax.broadcasted_iota(jnp.int32, (2 * count, LANES), 0)
    wanted = lax.broadcasted_iota(jnp.int32, (2 * count, LANES), 1).astype(jnp.float32)
    first_hit = (got_ref[: 2 * count, MARK, :] == wanted) & (source % 2 == 0)
    index = jnp.sum(jnp.where(first_hit, source, 0), axis=0, keepdims=True)
    source = source[:count]
    extra_hit = (got_ref[2 * count :, MARK, :] == wanted[:count]) & (source % nc == 0)
    index = index + jnp.sum(jnp.where(extra_hit, source + 2 * count, 0), axis=0, keepdims=True)
    over = jnp.max(got_ref[2 * count :, FLAG, :], axis=0, keepdims=True)
    row = lax.broadcasted_iota(jnp.int32, (8, LANES), 0)
    table_ref[...] = jnp.where(row == 0, index, jnp.where(over > 0.5, 1, 0))


def leftover_kernel(nb, nc, left_ref, table_ref, got_ref, new_table_ref, send_sem, recv_sem):
    count = nb * nc
    me = lax.axis_index("blocks") * nc + lax.axis_index("cross")

    def device(d):
        return (d // nc, lax.rem(d, nc))

    barrier = pltpu.get_barrier_semaphore()

    def greet(k, carry):
        pl.semaphore_signal(barrier, inc=1, device_id=device(lax.bitwise_xor(me, k)), device_id_type=MESH)
        return carry

    lax.fori_loop(1, count, greet, 0)
    pl.semaphore_wait(barrier, count - 1)

    def left_copy(k):
        d = lax.bitwise_xor(me, k)
        return pltpu.make_async_remote_copy(
            src_ref=left_ref.at[d], dst_ref=got_ref.at[me], send_sem=send_sem.at[k],
            recv_sem=recv_sem.at[k], device_id=device(d), device_id_type=MESH)

    def post(k, carry):
        left_copy(k).start()
        return carry

    def finish(k, carry):
        left_copy(k).wait()
        return carry

    lax.fori_loop(1, count, post, 0)
    got_ref[me] = left_ref[me]
    lax.fori_loop(1, count, finish, 0)
    source = lax.broadcasted_iota(jnp.int32, (count, LANES), 0)
    wanted = lax.broadcasted_iota(jnp.int32, (count, LANES), 1).astype(jnp.float32)
    hit = (got_ref[:, MARK, :] == wanted) & (source % nc == 0)
    index = jnp.sum(jnp.where(hit, source + 3 * count, 0), axis=0, keepdims=True)
    new_table_ref[...] = table_ref[...] + index


def unpack_kernel(ridx, got_ref, out_ref):
    for t in range(out_ref.shape[1]):
        base = ridx[0, t]
        for tile in range(TILES):
            block = got_ref.at[base + tile // 2]
            lanes = slice(tile * LANES, (tile + 1) * LANES)
            low = low_row(0, tile)
            out_ref[:MAIN, t, lanes] = block[low : low + MAIN, :]
            low = low_row(MAIN, tile)
            out_ref[MAIN:, t, lanes] = block[2 * MAIN :, :][low - 2 * MAIN : low - 2 * MAIN + TAIL]


def body(nb, nc, f_home, levels, plan):
    devices = nb * nc
    patches = f_home.shape[0]
    vmem = pl.BlockSpec(memory_space=pltpu.VMEM)
    smem = pl.BlockSpec(memory_space=pltpu.SMEM)
    state = (19, SPAN_PATCHES, 8, CELLS)
    small = (SPAN_PATCHES, 8, LANES)
    f32 = jnp.float32
    dma = pltpu.SemaphoreType.DMA
    half = (HALF, LANES)
    rounds = max(2 * STEPS + 1, (nb - 1).bit_length())
    limit = pltpu.CompilerParams(collective_id=0, has_side_effects=True, vmem_limit_bytes=60 * 1024 * 1024)
    got, left, table = pl.pallas_call(
        lambda *refs: lattice_kernel(nb, nc, *refs),
        out_shape=(
            jax.ShapeDtypeStruct((3 * devices,) + half, f32),
            jax.ShapeDtypeStruct((devices,) + half, f32),
            jax.ShapeDtypeStruct((8, LANES), jnp.int32),
        ),
        in_specs=[smem, vmem, vmem],
        out_specs=(vmem, vmem, vmem),
        scratch_shapes=[
            pltpu.VMEM(state, f32),
            pltpu.VMEM(state, f32),
            pltpu.VMEM((18,) + state[1:], f32),
            pltpu.VMEM((patches, 2 * HALF, LANES), f32),
            pltpu.VMEM((devices, 2) + half, f32),
            pltpu.VMEM((devices,) + half, f32),
            pltpu.VMEM((devices,) + half, f32),
            pltpu.VMEM((devices,) + half, f32),
            pltpu.VMEM(small, f32),
            pltpu.VMEM((len(AROUND),) + small, f32),
            pltpu.VMEM((STEPS, 2, 5, 8, CELLS), f32),
            pltpu.VMEM((STEPS, 2, 5, 8, CELLS), f32),
            pltpu.VMEM((STEPS, 2, 5, 2, 8, LANES), f32),
            pltpu.VMEM((STEPS, 2, 5, 2, 8, LANES), f32),
            pltpu.VMEM((STEPS, len(DIAGONAL), 8, LANES), f32),
            pltpu.VMEM((STEPS, len(DIAGONAL), 8, LANES), f32),
            pltpu.VMEM((devices, LANES), jnp.int32),
            pltpu.SMEM((devices, LANES), jnp.int32),
            pltpu.VMEM((2, devices, LANES), f32),
            dma((STEPS, 8)),
            dma((STEPS, 8)),
            dma((len(AROUND),)),
            dma((len(AROUND),)),
            dma((devices - 1,)),
            dma((devices - 1,)),
            dma((devices - 1,)),
            dma((devices - 1,)),
            dma,
            dma,
            dma,
            pltpu.SemaphoreType.REGULAR((rounds,)),
            pltpu.SemaphoreType.REGULAR((rounds,)),
        ],
        compiler_params=limit,
    )(levels, plan[None, :], jnp.transpose(f_home, (1, 0, 2)))

    def unpack(table, got):
        return pl.pallas_call(
            unpack_kernel,
            out_shape=jax.ShapeDtypeStruct((19, patches, CELLS), f32),
            in_specs=[smem, vmem],
            out_specs=vmem,
            compiler_params=pltpu.CompilerParams(vmem_limit_bytes=40 * 1024 * 1024),
        )(table, got)

    def with_leftover(table, got, left):
        more, table = pl.pallas_call(
            lambda *refs: leftover_kernel(nb, nc, *refs),
            out_shape=(
                jax.ShapeDtypeStruct((devices,) + half, f32),
                jax.ShapeDtypeStruct((8, LANES), jnp.int32),
            ),
            in_specs=[vmem, vmem],
            out_specs=(vmem, vmem),
            scratch_shapes=[dma((devices,)), dma((devices,))],
            compiler_params=pltpu.CompilerParams(collective_id=1, has_side_effects=True),
        )(left, table)
        return unpack(table, jnp.concatenate([got, more], axis=0))

    out = lax.cond(table[1, 0] > 0, with_leftover, lambda table, got, left: unpack(table, got), table, got, left)
    return jnp.transpose(out, (1, 0, 2))


def solution(mesh):
    nb, nc = mesh.shape["blocks"], mesh.shape["cross"]
    in_specs = (P(("blocks", "cross"), None, None), P(("blocks", "cross")), P(("blocks", "cross")))
    out_specs = P(("blocks", "cross"), None, None)
    return jax.shard_map(
        lambda f, l, p: body(nb, nc, f, l, p),
        mesh=mesh, in_specs=in_specs, out_specs=out_specs, check_vma=False)
```

```python
import jax
import jax.numpy as jnp
from jax import lax
from jax.experimental import pallas as pl
from jax.experimental.pallas import tpu as pltpu
from jax.sharding import PartitionSpec as P

SPAN_PATCHES = 4
DEPTH_PATCHES = 8
STEPS = 2
CELLS = 512
VELOCITIES = (
    (0, 0, 0),
    (1, 0, 0),
    (-1, 0, 0),
    (0, 1, 0),
    (0, -1, 0),
    (0, 0, 1),
    (0, 0, -1),
    (1, 1, 0),
    (-1, -1, 0),
    (1, -1, 0),
    (-1, 1, 0),
    (1, 0, 1),
    (-1, 0, -1),
    (1, 0, -1),
    (-1, 0, 1),
    (0, 1, 1),
    (0, -1, -1),
    (0, 1, -1),
    (0, -1, 1),
)
WEIGHTS = (1.0 / 3.0,) + (1.0 / 18.0,) * 6 + (1.0 / 36.0,) * 12
TAU_COARSE = 0.55
TAU_FINE = 2.0 * TAU_COARSE - 0.5
RESCALE = TAU_FINE / (2.0 * TAU_COARSE)
INFLOW = 0.08
MESH = pl.DeviceIdType.MESH
MAIN = 16
TAIL = 3
HALF = 40
MARK = 38
FIRST = 39
QUARTER = 20
TAG = 19
OVER = 1000.0
GROUP = 4
LANES = 128
TILES = CELLS // LANES
Y_UP = [q for q in range(19) if VELOCITIES[q][1] == 1]
Y_DOWN = [q for q in range(19) if VELOCITIES[q][1] == -1]
X_UP = [q for q in range(19) if VELOCITIES[q][0] == 1]
X_DOWN = [q for q in range(19) if VELOCITIES[q][0] == -1]
DIAGONAL = [q for q in range(19) if VELOCITIES[q][0] and VELOCITIES[q][1]]
AROUND = [(dx, dy) for dx in (-1, 0, 1) for dy in (-1, 0, 1) if (dx, dy) != (0, 0)]


def relax_into(load, store, coef):
    f = [load(q) for q in range(19)]
    terms = list(f)
    while len(terms) > 1:
        pairs = [a + b for a, b in zip(terms[::2], terms[1::2])]
        terms = pairs + ([terms[-1]] if len(terms) % 2 else [])
    rho = terms[0]
    inv = 1.0 / rho
    u = []
    for axis in range(3):
        up = [f[q] for q in range(19) if VELOCITIES[q][axis] == 1]
        down = [f[q] for q in range(19) if VELOCITIES[q][axis] == -1]
        d = [a - b for a, b in zip(up, down)]
        u.append((((d[0] + d[1]) + (d[2] + d[3])) + d[4]) * inv)
    base = 1.0 - 1.5 * (u[0] * u[0] + u[1] * u[1] + u[2] * u[2])
    scaled = {w: w * rho for w in set(WEIGHTS)}
    for q in range(19):
        along = None
        for axis in range(3):
            e = VELOCITIES[q][axis]
            if e:
                term = u[axis] if e == 1 else -u[axis]
                along = term if along is None else along + term
        poly = base if along is None else base + along * (3.0 + 4.5 * along)
        balance = scaled[WEIGHTS[q]] * poly
        store(q, balance + coef(q) * (f[q] - balance))


def low_row(q, tile):
    return tile % 2 * MAIN + q if q < MAIN else 2 * MAIN + tile % 2 * TAIL + q - MAIN


def lattice_kernel(nb, nc, level, plan_ref, f_ref, got_ref, pm, table_ref, st, pb, cq, sent, second, theirs,
                   away, kept, across, extra, got_extra, lev_ref, lv, ys, yr, xs, xr, ds, dr, pick, pick_s, tags, send_sem, recv_sem, lsend, lrecv, psend,
                   precv, esend, erecv, csend, crecv, qsend, qrecv, pick_sem, up_sem, down_sem):
    others = nb * nc - 1
    rounds = max(2 * STEPS + 1, (nb - 1).bit_length())
    b = lax.axis_index("blocks")
    c = lax.axis_index("cross")

    def at(dx, dy):
        return (lax.rem(b + dx + nb, nb), lax.rem(c + dy + nc, nc))

    me = b * nc + c

    def peer(k):
        return lax.bitwise_xor(me, k)

    def device(d):
        return (d // nc, lax.rem(d, nc))

    barrier = pltpu.get_barrier_semaphore()
    above = b < nb - 1
    below = b > 0

    def signal(sem, to):
        pl.semaphore_signal(sem, inc=1, device_id=to, device_id_type=MESH)

    for k in range(1, nc):
        signal(barrier, at(0, k))
    for there, dx in ((above, 1), (below, -1)):
        @pl.when(there)
        def _():
            for k in range(nc):
                signal(barrier, at(dx, k))

    def tell(k):
        hop = lax.shift_left(jnp.int32(1), jnp.int32(k))

        @pl.when(b + hop < nb)
        def _():
            signal(up_sem.at[k], (b + hop, c))

        @pl.when(b >= hop)
        def _():
            signal(down_sem.at[k], (b - hop, c))

    def hear(k):
        hop = lax.shift_left(jnp.int32(1), jnp.int32(k))

        @pl.when(b >= hop)
        def _():
            pl.semaphore_wait(up_sem.at[k], 1)

        @pl.when(b + hop < nb)
        def _():
            pl.semaphore_wait(down_sem.at[k], 1)

    patches = f_ref.shape[1]
    count = nb * nc
    target = lax.broadcasted_iota(jnp.int32, (count, patches), 0)
    where = jnp.broadcast_to(plan_ref[...], (count, patches))
    member = where // patches == target
    key = lax.broadcasted_iota(jnp.int32, (count, patches), 1) * patches + where % patches
    low_key = jnp.min(jnp.where(member, key, patches * patches), axis=1, keepdims=True)
    high_key = jnp.max(jnp.where(member, key, -1), axis=1, keepdims=True)
    some = high_key >= 0
    two = high_key > low_key
    column = lax.broadcasted_iota(jnp.int32, (count, LANES), 1)
    pick[...] = jnp.where(column == 0, jnp.where(some, low_key // patches, 0),
                          jnp.where(two, high_key // patches, 0))
    to_scalars = pltpu.make_async_copy(pick, pick_s, pick_sem)
    to_scalars.start()
    tags[0] = jnp.broadcast_to(jnp.where(some, low_key % patches, -1), (count, LANES)).astype(jnp.float32)
    tags[1] = jnp.broadcast_to(jnp.where(two, high_key % patches, -1), (count, LANES)).astype(jnp.float32)

    spot = lax.broadcasted_iota(jnp.int32, (SPAN_PATCHES, 8, LANES), 0) * 8
    spot = spot + lax.broadcasted_iota(jnp.int32, (SPAN_PATCHES, 8, LANES), 1)
    own = jnp.zeros((SPAN_PATCHES, 8, LANES), jnp.float32)
    for p in range(SPAN_PATCHES * 8):
        own = jnp.where(spot == p, level[p].astype(jnp.float32), own)
    lev_ref[...] = own

    for q in range(19):
        for r in range(SPAN_PATCHES):
            st[q, r] = f_ref[q, r * 8 : r * 8 + 8, :]
    pl.semaphore_wait(barrier, nc - 1 + nc * (jnp.where(above, 1, 0) + jnp.where(below, 1, 0)))
    tell(0)

    def start_to(there, copy):
        if there is None:
            copy.start()
        else:
            pl.when(there)(copy.start)

    def wait_for(outgoing, incoming, copy):
        if outgoing is None:
            copy.wait()
        else:
            pl.when(outgoing)(copy.wait_send)
            pl.when(incoming)(copy.wait_recv)

    def ends_of(dx):
        return {0: (None, None), 1: (above, below), -1: (below, above)}[dx]

    level_copies = []
    for n, (dx, dy) in enumerate(AROUND):
        copy = pltpu.make_async_remote_copy(
            src_ref=lev_ref, dst_ref=lv.at[n], send_sem=lsend.at[n], recv_sem=lrecv.at[n],
            device_id=at(-dx, -dy), device_id_type=MESH)
        outgoing, incoming = ends_of(-dx)
        start_to(outgoing, copy)
        level_copies.append((outgoing, incoming, copy))

    def patch_copy(k):
        d = peer(k)
        return pltpu.make_async_remote_copy(
            src_ref=sent.at[d], dst_ref=got_ref.at[pl.ds(2 * me, 2)], send_sem=psend.at[k],
            recv_sem=precv.at[k], device_id=device(d), device_id_type=MESH)

    def extra_copy(k):
        d = peer(k)
        return pltpu.make_async_remote_copy(
            src_ref=extra.at[d], dst_ref=got_extra.at[me], send_sem=esend.at[k],
            recv_sem=erecv.at[k], device_id=device(d), device_id_type=MESH)

    for copy in level_copies:
        wait_for(*copy)

    scale = {(0, 0): jnp.where(own > 0.5, RESCALE, 1.0)}
    for n, key in enumerate(AROUND):
        scale[key] = jnp.where(lv[n] > 0.5, RESCALE, 1.0)
    patch_scale = {}
    for dx in (-1, 0, 1):
        patch_scale[dx, 0] = scale[dx, 0]
        patch_scale[dx, 1] = jnp.concatenate([scale[dx, 0][1:], scale[dx, 1][:1]], axis=0)
        patch_scale[dx, -1] = jnp.concatenate([scale[dx, -1][-1:], scale[dx, 0][:-1]], axis=0)
    gain = jnp.where(own > 0.5, (1.0 - 1.0 / TAU_FINE) / RESCALE, 1.0 - 1.0 / TAU_COARSE)

    def target_scale(dx, dy, dz):
        value = patch_scale[dx, dy]
        return pltpu.roll(value, (-dz) % 8, axis=1) if dz else value

    shape = (SPAN_PATCHES, 8, LANES)
    lane = lax.broadcasted_iota(jnp.int32, shape, 2)
    for q in range(1, 19):
        e = VELOCITIES[q]
        kinds = [{}]
        for axis in range(3):
            if e[axis]:
                kinds = [{**k, axis: v} for k in kinds for v in (0, 1)]
        table = [(k, target_scale(*[e[a] * k.get(a, 0) for a in range(3)])) for k in kinds]
        for tile in range(TILES):
            cell = lane + tile * LANES
            coord = (cell // 64, (cell // 8) % 8, cell % 8)
            result = table[0][1]
            for k, value in table[1:]:
                mask = None
                for axis, on in k.items():
                    if on:
                        hit = coord[axis] == (7 if e[axis] == 1 else 0)
                        mask = hit if mask is None else mask & hit
                result = jnp.where(mask, value, result)
            cq[q - 1, :, :, tile * LANES : (tile + 1) * LANES] = gain * result

    full = (SPAN_PATCHES, 8, CELLS)
    cell = lax.broadcasted_iota(jnp.int32, full, 2)
    coord = (cell // 64, (cell // 8) % 8, cell % 8)
    entry = {
        (axis, e): coord[axis] == (0 if e == 1 else 7) for axis in range(3) for e in (1, -1)
    }
    lower = lane < 64
    half = lax.broadcasted_iota(jnp.int32, (2, 8, LANES), 2) < 64
    fine = jnp.broadcast_to(own[:, :, :1] > 0.5, full)
    in_tile = {
        (axis, e): (lane // 8 % 8 if axis == 1 else lane % 8) == (0 if e == 1 else 7)
        for axis in (1, 2) for e in (1, -1)
    }

    def spin(v, amount):
        return pltpu.roll(v, amount % LANES, axis=v.ndim - 1)

    def along_z(q, v):
        e = VELOCITIES[q][2]
        if not e:
            return v
        wrapped = pltpu.roll(spin(v, -7 * e), e % 8, axis=1)
        return jnp.where(in_tile[2, e][: v.shape[0]], wrapped, spin(v, e))

    def along_y(q, v, halo):
        e = VELOCITIES[q][1]
        moved = jnp.concatenate([halo, v[:-1]] if e == 1 else [v[1:], halo], axis=0)
        return jnp.where(in_tile[1, e], spin(moved, -56 * e), spin(v, 8 * e))

    def lanes_of(tile):
        return slice(tile * LANES, (tile + 1) * LANES)

    def step(s, carry):
        def first(r, tiles):
            plain = jnp.where(lev_ref[r] > 0.5, 1.0 - 1.0 / TAU_FINE, 1.0 - 1.0 / TAU_COARSE)
            for tile in tiles:
                lanes = lanes_of(tile)

                def put(q, value):
                    pb[q, r, :, lanes] = value

                relax_into(lambda q: st[q, r, :, lanes], put,
                           lambda q: cq[q - 1, r, :, lanes] if q else plain)

        def faces(r, carry):
            first(r, (0, TILES - 1))
            return carry

        lax.fori_loop(0, SPAN_PATCHES, faces, 0)
        for way, e, group in ((0, 1, X_UP), (1, -1, X_DOWN)):
            for n, q in enumerate(group):
                v = along_z(q, pb[q, :, :, lanes_of(TILES - 1 if e == 1 else 0)])
                turned = spin(v, 64)
                if e == 1:
                    xs[s, way, n] = jnp.where(half, turned[:2], v[2:])
                else:
                    xs[s, way, n] = jnp.where(half, v[:2], turned[2:])
                if q in DIAGONAL:
                    ds[s, DIAGONAL.index(q)] = turned[SPAN_PATCHES - 1 if VELOCITIES[q][1] == 1 else 0]
        x_copies = []

        def send(src, dst, n, dx, dy):
            copy = pltpu.make_async_remote_copy(
                src_ref=src, dst_ref=dst, send_sem=send_sem.at[s, n], recv_sem=recv_sem.at[s, n],
                device_id=at(dx, dy), device_id_type=MESH)
            outgoing, incoming = ends_of(dx)
            start_to(outgoing, copy)
            return outgoing, incoming, copy

        def outer(m, carry):
            first(m * (SPAN_PATCHES - 1), range(1, TILES - 1))
            return carry

        def inner(r, carry):
            first(r, range(1, TILES - 1))
            return carry

        for way, dx in ((0, 1), (1, -1)):
            x_copies.append(send(xs.at[s, way], xr.at[s, way], 2 + way, dx, 0))
        for n, q in enumerate(DIAGONAL):
            x_copies.append(send(ds.at[s, n], dr.at[s, n], 4 + n, *VELOCITIES[q][:2]))
        lax.fori_loop(0, 2, outer, 0)
        for way, e, group in ((0, 1, Y_UP), (1, -1, Y_DOWN)):
            r = SPAN_PATCHES - 1 if e == 1 else 0
            for n, q in enumerate(group):
                for tile in range(TILES):
                    ys[s, way, n, :, lanes_of(tile)] = along_z(q, pb[q, r : r + 1, :, lanes_of(tile)])[0]
        y_copies = []
        for way, dy in ((0, 1), (1, -1)):
            y_copies.append(send(ys.at[s, way], yr.at[s, way], way, 0, dy))
        lax.fori_loop(1, SPAN_PATCHES - 1, inner, 0)

        def shift(q):
            e = VELOCITIES[q]
            tiles = [along_z(q, pb[q, :, :, lanes_of(tile)]) for tile in range(TILES)]
            if e[1]:
                way, group = (0, Y_UP) if e[1] == 1 else (1, Y_DOWN)
                n = group.index(q)
                tiles = [along_y(q, v, yr[s, way, n, :, lanes_of(tile)][None]) for tile, v in enumerate(tiles)]
            if e[0]:
                turned = [spin(v, 64) for v in tiles]
                for tile in range(TILES):
                    if e[0] == 1:
                        tiles[tile] = jnp.where(lower, turned[tile - 1], turned[tile])
                    else:
                        tiles[tile] = jnp.where(lower, turned[tile], turned[(tile + 1) % TILES])
            for tile in range(TILES):
                st[q, :, :, lanes_of(tile)] = tiles[tile]

        for q in range(19):
            if not VELOCITIES[q][1]:
                shift(q)
        for copy in y_copies:
            wait_for(*copy)
        hear(2 * s)
        tell(2 * s + 1)
        for q in range(19):
            if VELOCITIES[q][1]:
                shift(q)

        def again(r, tiles):
            for tile in tiles:
                lanes = lanes_of(tile)

                def put(q, value):
                    pb[q, r, :, lanes] = value

                relax_into(lambda q: st[q, r, :, lanes], put, lambda q: 1.0 - 1.0 / TAU_FINE)

        def middle(r, carry):
            again(r, range(1, TILES - 1))
            return carry

        lax.fori_loop(0, SPAN_PATCHES, middle, 0)
        for copy in x_copies:
            wait_for(*copy)
        hear(2 * s + 1)
        tell(2 * s + 2)
        for way, e, group in ((0, 1, X_UP), (1, -1, X_DOWN)):
            outside = b == (0 if e == 1 else nb - 1)
            for n, q in enumerate(group):
                h = xr[s, way, n]
                turned = spin(h, 64)
                halo = jnp.concatenate([h, turned] if e == 1 else [turned, h], axis=0)
                if q in DIAGONAL:
                    halo = along_y(q, halo, dr[s, DIAGONAL.index(q)][None])
                along = e * INFLOW
                const = WEIGHTS[q] * (1.0 + 3.0 * along + 4.5 * along * along - 1.5 * INFLOW * INFLOW)
                halo = jnp.where(outside, jnp.full(halo.shape, const, jnp.float32), halo)
                lanes = lanes_of(0 if e == 1 else TILES - 1)
                keep = st[q, :, :, lanes]
                st[q, :, :, lanes] = jnp.where(lower, halo, keep) if e == 1 else jnp.where(lower, keep, halo)

        def ends(r, carry):
            again(r, (0, TILES - 1))
            return carry

        lax.fori_loop(0, SPAN_PATCHES, ends, 0)
        for q in range(19):
            e = VELOCITIES[q]
            take = fine
            for axis in range(3):
                if e[axis]:
                    take = take & ~entry[axis, e[axis]]
            moved = pb[q]
            if q:
                moved = pltpu.roll(moved, (64 * e[0] + 8 * e[1] + e[2]) % CELLS, axis=2)
            st[q] = jnp.where(take, moved, st[q])
        return carry

    lax.fori_loop(0, STEPS, step, 0)
    for k in range(2 * STEPS, rounds - 1):
        hear(k)
        tell(k + 1)
    hear(rounds - 1)
    to_scalars.wait()

    pm[:, 2 * MAIN : HALF, :] = jnp.zeros((pm.shape[0], HALF - 2 * MAIN, LANES), jnp.float32)
    pm[:, HALF + 2 * MAIN :, :] = jnp.zeros((pm.shape[0], HALF - 2 * MAIN, LANES), jnp.float32)
    for q in range(19):
        for r in range(SPAN_PATCHES):
            for tile in range(TILES):
                row = tile // 2 * HALF + low_row(q, tile)
                pm[r * 8 : r * 8 + 8, row, :] = st[q, r, :, tile * LANES : (tile + 1) * LANES]

    part = lax.rem(me, GROUP)
    base = me - part
    far_chip = part // nc
    chunks = count // GROUP

    def chunk_at(j):
        return lax.rem(j + chunks // 2, chunks)

    def rows_of(j):
        return pl.ds(chunk_at(j) * GROUP, GROUP)

    def swap_copy(j):
        return pltpu.make_async_remote_copy(
            src_ref=second.at[rows_of(j)], dst_ref=theirs.at[rows_of(j)], send_sem=csend.at[j],
            recv_sem=crecv.at[j], device_id=at(0, 1), device_id_type=MESH)

    def shuffle_copy(j):
        return pltpu.make_async_remote_copy(
            src_ref=away.at[rows_of(j)], dst_ref=across.at[rows_of(j)], send_sem=qsend.at[j],
            recv_sem=qrecv.at[j], device_id=device(lax.bitwise_xor(me, nc)), device_id_type=MESH)

    def tag_of(which, d):
        return tags[which, pl.ds(d, 1), :]

    def pack_second(j, carry):
        for i in range(GROUP):
            m = chunk_at(j) * GROUP + i
            d = lax.bitwise_xor(base, m)
            p = pick_s[d, 1]
            second[m, 0] = pm[p, :HALF]
            second[m, 1] = pm[p, HALF:]
            second[m, 0, MARK : MARK + 1, :] = tag_of(1, d)
            second[m, 0, FIRST : FIRST + 1, :] = tag_of(0, d)

        @pl.when(j > 0)
        def _():
            swap_copy(j - 1).start()

        return carry

    lax.fori_loop(0, chunks, pack_second, 0)
    swap_copy(chunks - 1).start()
    zero = c == 0

    def piece(p, m, t):
        top = pl.multiple_of(t // 2 * HALF + lax.rem(t, 2) * MAIN, 8)
        low = pl.multiple_of(t // 2 * HALF + 2 * MAIN, 8)
        their_top = pl.multiple_of(lax.rem(t, 2) * MAIN, 8)
        return (pm[p, pl.ds(top, MAIN), :], pm[p, pl.ds(low, 8), :],
                theirs[m, t // 2, pl.ds(their_top, MAIN), :], theirs[m, t // 2, 2 * MAIN : HALF, :])

    def pack_chunk(j):
        for i in range(GROUP):
            k = chunk_at(j) * GROUP + i
            d = peer(k)
            m = lax.bitwise_xor(k, part)
            p = pick_s[d, 0]
            my_first = tag_of(0, d)
            my_second = tag_of(1, d)
            their_second = theirs[m, 0, MARK : MARK + 1, :]
            their_first = theirs[m, 0, FIRST : FIRST + 1, :]
            own = my_first > -0.5
            sent[d, 0] = jnp.where(own, pm[p, :HALF], theirs[m, 0])
            sent[d, 1] = jnp.where(own, pm[p, HALF:], theirs[m, 1])
            sent[d, 0, MARK : MARK + 1, :] = jnp.where(own, my_first, their_second)
            mine_extra = (my_second > -0.5) & (their_first > -0.5)
            their_extra = (their_second > -0.5) & own
            use_mine = mine_extra & (zero | ~their_extra)
            tag = jnp.where(use_mine, my_second, jnp.where(their_extra, their_second, -1.0))
            tag = jnp.where(mine_extra & their_extra, OVER, tag)
            p = pick_s[d, 1]
            for ref, t in ((kept, part), (away, lax.bitwise_xor(part, nc))):
                my_top, my_low, their_top, their_low = piece(p, m, t)
                ref[m, :MAIN, :] = jnp.where(use_mine, my_top, their_top)
                low = jnp.where(use_mine, my_low, their_low)
                low = jnp.where(lax.rem(t, 2) == 1, pltpu.roll(low, 8 - TAIL, axis=0), low)
                ref[m, MAIN : MAIN + TAIL, :] = low[:TAIL]
                ref[m, TAG : TAG + 1, :] = tag

    def send_chunk(j):
        shuffle_copy(j).start()
        for i in range(GROUP):
            k = chunk_at(j) * GROUP + i

            @pl.when(k > 0)
            def _():
                patch_copy(k).start()

    def post(j, carry):
        swap_copy(j).wait_recv()
        pack_chunk(j)

        @pl.when(j > 0)
        def _():
            send_chunk(j - 1)

        return carry

    lax.fori_loop(0, chunks, post, 0)
    send_chunk(chunks - 1)
    got_ref[2 * me] = sent[me, 0]
    got_ref[2 * me + 1] = sent[me, 1]

    def swapped(j, carry):
        swap_copy(j).wait_send()
        shuffle_copy(j).wait()
        return carry

    lax.fori_loop(0, chunks, swapped, 0)
    near_tags = kept[:, TAG, :]
    far_tags = across[:, TAG, :]
    over = (near_tags > OVER / 2) | (far_tags > OVER / 2) | ((near_tags > -0.5) & (far_tags > -0.5))
    flag = jnp.max(jnp.where(over, OVER, 0.0), axis=0, keepdims=True)

    def pack_extra(d):
        m = lax.bitwise_xor(base, d)
        mine = kept[m]
        other = across[m]
        keep = ((mine[TAG:] > -0.5) & (far_chip == 0)) | ~(other[TAG:] > -0.5)
        extra[d] = jnp.where(keep, mine, other)
        extra[d, TAG : TAG + 1, :] = jnp.where(keep, mine[TAG:], other[TAG:]) + flag

    def mask_at(i):
        return lax.rem(i + count // 2, count)

    def post_extra(i, carry):
        pack_extra(peer(mask_at(i)))

        @pl.when((i > 0) & (mask_at(i - 1) > 0))
        def _():
            extra_copy(mask_at(i - 1)).start()

        return carry

    lax.fori_loop(0, count, post_extra, 0)
    extra_copy(mask_at(count - 1)).start()
    got_extra[me] = extra[me]

    def finish(k, carry):
        patch_copy(k).wait()
        extra_copy(k).wait()
        return carry

    lax.fori_loop(1, count, finish, 0)

    def assemble(g, carry):
        for t in range(TILES):
            whole = got_ref.at[2 * count + 2 * g + t // 2]
            block = got_extra.at[g * GROUP + t]
            whole[t % 2 * MAIN : (t % 2 + 1) * MAIN, :] = block[:MAIN, :]
            low = 2 * MAIN + t % 2 * TAIL
            whole[low : low + TAIL, :] = block[MAIN : MAIN + TAIL, :]
        return carry

    lax.fori_loop(0, chunks, assemble, 0)
    source = lax.broadcasted_iota(jnp.int32, (2 * count, LANES), 0)
    wanted = lax.broadcasted_iota(jnp.int32, (2 * count, LANES), 1).astype(jnp.float32)
    first_hit = (got_ref[: 2 * count, MARK, :] == wanted) & (source % 2 == 0)
    index = jnp.sum(jnp.where(first_hit, source, 0), axis=0, keepdims=True)
    source = source[:count]
    extra_tags = got_extra[:, TAG, :]
    extra_hit = (extra_tags == wanted[:count]) & (source % GROUP == 0)
    place = source // GROUP * 2 + 2 * count
    index = index + jnp.sum(jnp.where(extra_hit, place, 0), axis=0, keepdims=True)
    over = jnp.max(extra_tags, axis=0, keepdims=True)
    row = lax.broadcasted_iota(jnp.int32, (8, LANES), 0)
    table_ref[...] = jnp.where(row == 0, index, jnp.where(over > OVER / 2, 1, 0))


def full_kernel(nb, nc, sidx, slot_of, pm, got_ref, table_ref, sent, send_sem, recv_sem):
    count = nb * nc
    me = lax.axis_index("blocks") * nc + lax.axis_index("cross")

    def device(d):
        return (d // nc, lax.rem(d, nc))

    barrier = pltpu.get_barrier_semaphore()

    def greet(k, carry):
        pl.semaphore_signal(barrier, inc=1, device_id=device(lax.bitwise_xor(me, k)), device_id_type=MESH)
        return carry

    lax.fori_loop(1, count, greet, 0)
    pl.semaphore_wait(barrier, count - 1)

    def pack(d, carry):
        for slot in range(2):
            p = sidx[2 * d + slot]
            sent[d, 2 * slot] = pm[p, :HALF]
            sent[d, 2 * slot + 1] = pm[p, HALF:]
            tag = jnp.full((1, LANES), slot_of[2 * d + slot].astype(jnp.float32), jnp.float32)
            sent[d, 2 * slot, MARK : MARK + 1, :] = tag
        return carry

    lax.fori_loop(0, count, pack, 0)

    def copy(k):
        d = lax.bitwise_xor(me, k)
        return pltpu.make_async_remote_copy(
            src_ref=sent.at[d], dst_ref=got_ref.at[pl.ds(4 * me, 4)], send_sem=send_sem.at[k],
            recv_sem=recv_sem.at[k], device_id=device(d), device_id_type=MESH)

    def post(k, carry):
        copy(k).start()
        return carry

    def finish(k, carry):
        copy(k).wait()
        return carry

    lax.fori_loop(1, count, post, 0)
    for i in range(4):
        got_ref[4 * me + i] = sent[me, i]
    lax.fori_loop(1, count, finish, 0)
    source = lax.broadcasted_iota(jnp.int32, (4 * count, LANES), 0)
    wanted = lax.broadcasted_iota(jnp.int32, (4 * count, LANES), 1).astype(jnp.float32)
    hit = (got_ref[:, MARK, :] == wanted) & (source % 2 == 0)
    index = jnp.sum(jnp.where(hit, source, 0), axis=0, keepdims=True)
    table_ref[...] = jnp.broadcast_to(index, table_ref.shape)


def unpack_kernel(ridx, got_ref, out_ref):
    for t in range(out_ref.shape[1]):
        base = ridx[0, t]
        for tile in range(TILES):
            block = got_ref.at[base + tile // 2]
            lanes = slice(tile * LANES, (tile + 1) * LANES)
            low = low_row(0, tile)
            out_ref[:MAIN, t, lanes] = block[low : low + MAIN, :]
            low = low_row(MAIN, tile)
            out_ref[MAIN:, t, lanes] = block[2 * MAIN :, :][low - 2 * MAIN : low - 2 * MAIN + TAIL]


def body(nb, nc, f_home, levels, plan):
    devices = nb * nc
    patches = f_home.shape[0]
    vmem = pl.BlockSpec(memory_space=pltpu.VMEM)
    smem = pl.BlockSpec(memory_space=pltpu.SMEM)
    state = (19, SPAN_PATCHES, 8, CELLS)
    small = (SPAN_PATCHES, 8, LANES)
    f32 = jnp.float32
    dma = pltpu.SemaphoreType.DMA
    half = (HALF, LANES)
    quarter = (QUARTER, LANES)
    rounds = max(2 * STEPS + 1, (nb - 1).bit_length())
    limit = pltpu.CompilerParams(collective_id=0, has_side_effects=True, vmem_limit_bytes=60 * 1024 * 1024)
    got, packed, table = pl.pallas_call(
        lambda *refs: lattice_kernel(nb, nc, *refs),
        out_shape=(
            jax.ShapeDtypeStruct((2 * devices + 2 * devices // GROUP,) + half, f32),
            jax.ShapeDtypeStruct((patches, 2 * HALF, LANES), f32),
            jax.ShapeDtypeStruct((8, LANES), jnp.int32),
        ),
        in_specs=[smem, vmem, vmem],
        out_specs=(vmem, vmem, vmem),
        scratch_shapes=[
            pltpu.VMEM(state, f32),
            pltpu.VMEM(state, f32),
            pltpu.VMEM((18,) + state[1:], f32),
            pltpu.VMEM((devices, 2) + half, f32),
            pltpu.VMEM((devices, 2) + half, f32),
            pltpu.VMEM((devices, 2) + half, f32),
            pltpu.VMEM((devices,) + quarter, f32),
            pltpu.VMEM((devices,) + quarter, f32),
            pltpu.VMEM((devices,) + quarter, f32),
            pltpu.VMEM((devices,) + quarter, f32),
            pltpu.VMEM((devices,) + quarter, f32),
            pltpu.VMEM(small, f32),
            pltpu.VMEM((len(AROUND),) + small, f32),
            pltpu.VMEM((STEPS, 2, 5, 8, CELLS), f32),
            pltpu.VMEM((STEPS, 2, 5, 8, CELLS), f32),
            pltpu.VMEM((STEPS, 2, 5, 2, 8, LANES), f32),
            pltpu.VMEM((STEPS, 2, 5, 2, 8, LANES), f32),
            pltpu.VMEM((STEPS, len(DIAGONAL), 8, LANES), f32),
            pltpu.VMEM((STEPS, len(DIAGONAL), 8, LANES), f32),
            pltpu.VMEM((devices, LANES), jnp.int32),
            pltpu.SMEM((devices, LANES), jnp.int32),
            pltpu.VMEM((2, devices, LANES), f32),
            dma((STEPS, 8)),
            dma((STEPS, 8)),
            dma((len(AROUND),)),
            dma((len(AROUND),)),
            dma((devices,)),
            dma((devices,)),
            dma((devices,)),
            dma((devices,)),
            dma((devices // GROUP,)),
            dma((devices // GROUP,)),
            dma((devices // GROUP,)),
            dma((devices // GROUP,)),
            dma,
            pltpu.SemaphoreType.REGULAR((rounds,)),
            pltpu.SemaphoreType.REGULAR((rounds,)),
        ],
        compiler_params=limit,
    )(levels, plan[None, :], jnp.transpose(f_home, (1, 0, 2)))

    def unpack(table, got):
        return pl.pallas_call(
            unpack_kernel,
            out_shape=jax.ShapeDtypeStruct((19, patches, CELLS), f32),
            in_specs=[smem, vmem],
            out_specs=vmem,
            compiler_params=pltpu.CompilerParams(vmem_limit_bytes=40 * 1024 * 1024),
        )(table, got)

    def in_full(table, got, packed, plan):
        target = plan // patches
        order = jnp.arange(patches, dtype=jnp.int32)
        earlier = (target[:, None] == target[None, :]) & (order[None, :] < order[:, None])
        place = 2 * target + jnp.sum(earlier.astype(jnp.int32), axis=1)
        hit = place[None, :] == jnp.arange(2 * devices, dtype=jnp.int32)[:, None]
        sidx = jnp.sum(jnp.where(hit, order[None, :], 0), axis=1)
        slot_of = jnp.sum(jnp.where(hit, plan[None, :] % patches + 1, 0), axis=1) - 1
        got, table = pl.pallas_call(
            lambda *refs: full_kernel(nb, nc, *refs),
            out_shape=(
                jax.ShapeDtypeStruct((4 * devices,) + half, f32),
                jax.ShapeDtypeStruct((8, LANES), jnp.int32),
            ),
            in_specs=[smem, smem, vmem],
            out_specs=(vmem, vmem),
            scratch_shapes=[
                pltpu.VMEM((devices, 4) + half, f32), dma((devices,)), dma((devices,))
            ],
            compiler_params=pltpu.CompilerParams(collective_id=1, has_side_effects=True,
                                                 vmem_limit_bytes=48 * 1024 * 1024),
        )(sidx, slot_of, packed)
        return unpack(table, got)

    out = lax.cond(table[1, 0] > 0, in_full, lambda table, got, packed, plan: unpack(table, got),
                   table, got, packed, plan)
    return jnp.transpose(out, (1, 0, 2))


def solution(mesh):
    nb, nc = mesh.shape["blocks"], mesh.shape["cross"]
    in_specs = (P(("blocks", "cross"), None, None), P(("blocks", "cross")), P(("blocks", "cross")))
    out_specs = P(("blocks", "cross"), None, None)
    return jax.shard_map(
        lambda f, l, p: body(nb, nc, f, l, p),
        mesh=mesh, in_specs=in_specs, out_specs=out_specs, check_vma=False)
```

```python
import jax
import jax.numpy as jnp
from jax import lax
from jax.experimental import pallas as pl
from jax.experimental.pallas import tpu as pltpu
from jax.sharding import PartitionSpec as P

SPAN_PATCHES = 4
DEPTH_PATCHES = 8
STEPS = 2
CELLS = 512
VELOCITIES = (
    (0, 0, 0),
    (1, 0, 0),
    (-1, 0, 0),
    (0, 1, 0),
    (0, -1, 0),
    (0, 0, 1),
    (0, 0, -1),
    (1, 1, 0),
    (-1, -1, 0),
    (1, -1, 0),
    (-1, 1, 0),
    (1, 0, 1),
    (-1, 0, -1),
    (1, 0, -1),
    (-1, 0, 1),
    (0, 1, 1),
    (0, -1, -1),
    (0, 1, -1),
    (0, -1, 1),
)
WEIGHTS = (1.0 / 3.0,) + (1.0 / 18.0,) * 6 + (1.0 / 36.0,) * 12
TAU_COARSE = 0.55
TAU_FINE = 2.0 * TAU_COARSE - 0.5
RESCALE = TAU_FINE / (2.0 * TAU_COARSE)
INFLOW = 0.08
MESH = pl.DeviceIdType.MESH
MAIN = 16
TAIL = 3
HALF = 40
MARK = 38
FIRST = 39
QUARTER = 20
TAG = 19
OVER = 1000.0
GROUP = 4
LANES = 128
TILES = CELLS // LANES
Y_UP = [q for q in range(19) if VELOCITIES[q][1] == 1]
Y_DOWN = [q for q in range(19) if VELOCITIES[q][1] == -1]
X_UP = [q for q in range(19) if VELOCITIES[q][0] == 1]
X_DOWN = [q for q in range(19) if VELOCITIES[q][0] == -1]
DIAGONAL = [q for q in range(19) if VELOCITIES[q][0] and VELOCITIES[q][1]]
AROUND = [(dx, dy) for dx in (-1, 0, 1) for dy in (-1, 0, 1) if (dx, dy) != (0, 0)]


def relax_into(load, store, coef):
    f = [load(q) for q in range(19)]
    terms = list(f)
    while len(terms) > 1:
        pairs = [a + b for a, b in zip(terms[::2], terms[1::2])]
        terms = pairs + ([terms[-1]] if len(terms) % 2 else [])
    rho = terms[0]
    inv = 1.0 / rho
    u = []
    for axis in range(3):
        up = [f[q] for q in range(19) if VELOCITIES[q][axis] == 1]
        down = [f[q] for q in range(19) if VELOCITIES[q][axis] == -1]
        d = [a - b for a, b in zip(up, down)]
        u.append((((d[0] + d[1]) + (d[2] + d[3])) + d[4]) * inv)
    base = 1.0 - 1.5 * (u[0] * u[0] + u[1] * u[1] + u[2] * u[2])
    scaled = {w: w * rho for w in set(WEIGHTS)}
    for q in range(19):
        along = None
        for axis in range(3):
            e = VELOCITIES[q][axis]
            if e:
                term = u[axis] if e == 1 else -u[axis]
                along = term if along is None else along + term
        poly = base if along is None else base + along * (3.0 + 4.5 * along)
        balance = scaled[WEIGHTS[q]] * poly
        store(q, balance + coef(q) * (f[q] - balance))


def half_of(tile):
    return 1 if tile in (0, TILES - 1) else 0


def place_of(tile):
    return tile // 2 if half_of(tile) else tile - 1


def low_row(q, tile):
    place = place_of(tile)
    return place * MAIN + q if q < MAIN else 2 * MAIN + place * TAIL + q - MAIN


def lattice_kernel(nb, nc, level, plan_ref, f_ref, got_ref, pm, table_ref, st, pb, cq, sent, second, theirs,
                   away, kept, across, extra, got_extra, lev_ref, lv, ys, yr, xs, xr, ds, dr, pick, pick_s, tags, send_sem, recv_sem, lsend, lrecv, psend,
                   precv, esend, erecv, csend, crecv, qsend, qrecv, pick_sem, up_sem, down_sem):
    others = nb * nc - 1
    rounds = max(2 * STEPS, (nb - 1).bit_length())
    b = lax.axis_index("blocks")
    c = lax.axis_index("cross")

    def at(dx, dy):
        return (lax.rem(b + dx + nb, nb), lax.rem(c + dy + nc, nc))

    me = b * nc + c

    def peer(k):
        return lax.bitwise_xor(me, k)

    def device(d):
        return (d // nc, lax.rem(d, nc))

    barrier = pltpu.get_barrier_semaphore()
    above = b < nb - 1
    below = b > 0

    def signal(sem, to):
        pl.semaphore_signal(sem, inc=1, device_id=to, device_id_type=MESH)

    for k in range(1, nc):
        signal(barrier, at(0, k))
    for there, dx in ((above, 1), (below, -1)):
        @pl.when(there)
        def _():
            for k in range(nc):
                signal(barrier, at(dx, k))

    def tell(k):
        hop = lax.shift_left(jnp.int32(1), jnp.int32(k))

        @pl.when(b + hop < nb)
        def _():
            signal(up_sem.at[k], (b + hop, c))

        @pl.when(b >= hop)
        def _():
            signal(down_sem.at[k], (b - hop, c))

    def hear(k):
        hop = lax.shift_left(jnp.int32(1), jnp.int32(k))

        @pl.when(b >= hop)
        def _():
            pl.semaphore_wait(up_sem.at[k], 1)

        @pl.when(b + hop < nb)
        def _():
            pl.semaphore_wait(down_sem.at[k], 1)

    patches = f_ref.shape[1]
    count = nb * nc
    target = lax.broadcasted_iota(jnp.int32, (count, patches), 0)
    where = jnp.broadcast_to(plan_ref[...], (count, patches))
    member = where // patches == target
    key = lax.broadcasted_iota(jnp.int32, (count, patches), 1) * patches + where % patches
    low_key = jnp.min(jnp.where(member, key, patches * patches), axis=1, keepdims=True)
    high_key = jnp.max(jnp.where(member, key, -1), axis=1, keepdims=True)
    some = high_key >= 0
    two = high_key > low_key
    column = lax.broadcasted_iota(jnp.int32, (count, LANES), 1)
    pick[...] = jnp.where(column == 0, jnp.where(some, low_key // patches, 0),
                          jnp.where(two, high_key // patches, 0))
    to_scalars = pltpu.make_async_copy(pick, pick_s, pick_sem)
    to_scalars.start()
    tags[0] = jnp.broadcast_to(jnp.where(some, low_key % patches, -1), (count, LANES)).astype(jnp.float32)
    tags[1] = jnp.broadcast_to(jnp.where(two, high_key % patches, -1), (count, LANES)).astype(jnp.float32)

    spot = lax.broadcasted_iota(jnp.int32, (SPAN_PATCHES, 8, LANES), 0) * 8
    spot = spot + lax.broadcasted_iota(jnp.int32, (SPAN_PATCHES, 8, LANES), 1)
    own = jnp.zeros((SPAN_PATCHES, 8, LANES), jnp.float32)
    for p in range(SPAN_PATCHES * 8):
        own = jnp.where(spot == p, level[p].astype(jnp.float32), own)
    lev_ref[...] = own

    for q in range(19):
        for r in range(SPAN_PATCHES):
            st[q, r] = f_ref[q, r * 8 : r * 8 + 8, :]
    pl.semaphore_wait(barrier, nc - 1 + nc * (jnp.where(above, 1, 0) + jnp.where(below, 1, 0)))
    tell(0)

    def start_to(there, copy):
        if there is None:
            copy.start()
        else:
            pl.when(there)(copy.start)

    def wait_for(outgoing, incoming, copy):
        if outgoing is None:
            copy.wait()
        else:
            pl.when(outgoing)(copy.wait_send)
            pl.when(incoming)(copy.wait_recv)

    def ends_of(dx):
        return {0: (None, None), 1: (above, below), -1: (below, above)}[dx]

    level_copies = []
    for n, (dx, dy) in enumerate(AROUND):
        copy = pltpu.make_async_remote_copy(
            src_ref=lev_ref, dst_ref=lv.at[n], send_sem=lsend.at[n], recv_sem=lrecv.at[n],
            device_id=at(-dx, -dy), device_id_type=MESH)
        outgoing, incoming = ends_of(-dx)
        start_to(outgoing, copy)
        level_copies.append((outgoing, incoming, copy))

    def patch_copy(half, k):
        d = peer(k)
        return pltpu.make_async_remote_copy(
            src_ref=sent.at[half, d], dst_ref=got_ref.at[2 * me + half], send_sem=psend.at[half, k],
            recv_sem=precv.at[half, k], device_id=device(d), device_id_type=MESH)

    def extra_copy(k):
        d = peer(k)
        return pltpu.make_async_remote_copy(
            src_ref=extra.at[d], dst_ref=got_extra.at[me], send_sem=esend.at[k],
            recv_sem=erecv.at[k], device_id=device(d), device_id_type=MESH)

    for copy in level_copies:
        wait_for(*copy)

    scale = {(0, 0): jnp.where(own > 0.5, RESCALE, 1.0)}
    for n, key in enumerate(AROUND):
        scale[key] = jnp.where(lv[n] > 0.5, RESCALE, 1.0)
    patch_scale = {}
    for dx in (-1, 0, 1):
        patch_scale[dx, 0] = scale[dx, 0]
        patch_scale[dx, 1] = jnp.concatenate([scale[dx, 0][1:], scale[dx, 1][:1]], axis=0)
        patch_scale[dx, -1] = jnp.concatenate([scale[dx, -1][-1:], scale[dx, 0][:-1]], axis=0)
    gain = jnp.where(own > 0.5, (1.0 - 1.0 / TAU_FINE) / RESCALE, 1.0 - 1.0 / TAU_COARSE)

    def target_scale(dx, dy, dz):
        value = patch_scale[dx, dy]
        return pltpu.roll(value, (-dz) % 8, axis=1) if dz else value

    shape = (SPAN_PATCHES, 8, LANES)
    lane = lax.broadcasted_iota(jnp.int32, shape, 2)
    for q in range(1, 19):
        e = VELOCITIES[q]
        kinds = [{}]
        for axis in range(3):
            if e[axis]:
                kinds = [{**k, axis: v} for k in kinds for v in (0, 1)]
        table = [(k, target_scale(*[e[a] * k.get(a, 0) for a in range(3)])) for k in kinds]
        for tile in range(TILES):
            cell = lane + tile * LANES
            coord = (cell // 64, (cell // 8) % 8, cell % 8)
            result = table[0][1]
            for k, value in table[1:]:
                mask = None
                for axis, on in k.items():
                    if on:
                        hit = coord[axis] == (7 if e[axis] == 1 else 0)
                        mask = hit if mask is None else mask & hit
                result = jnp.where(mask, value, result)
            cq[q - 1, :, :, tile * LANES : (tile + 1) * LANES] = gain * result

    lower = lane < 64
    half = lax.broadcasted_iota(jnp.int32, (2, 8, LANES), 2) < 64
    fine = own > 0.5
    in_tile = {
        (axis, e): (lane // 8 % 8 if axis == 1 else lane % 8) == (0 if e == 1 else 7)
        for axis in (1, 2) for e in (1, -1)
    }

    def spin(v, amount):
        return pltpu.roll(v, amount % LANES, axis=v.ndim - 1)

    def along_z(q, v):
        e = VELOCITIES[q][2]
        if not e:
            return v
        wrapped = pltpu.roll(spin(v, -7 * e), e % 8, axis=1)
        return jnp.where(in_tile[2, e][: v.shape[0]], wrapped, spin(v, e))

    def along_y(q, v, halo):
        e = VELOCITIES[q][1]
        moved = jnp.concatenate([halo, v[:-1]] if e == 1 else [v[1:], halo], axis=0)
        return jnp.where(in_tile[1, e], spin(moved, -56 * e), spin(v, 8 * e))

    def lanes_of(tile):
        return slice(tile * LANES, (tile + 1) * LANES)

    def step(s, stage=None):
        def first(r, tiles):
            plain = jnp.where(lev_ref[r] > 0.5, 1.0 - 1.0 / TAU_FINE, 1.0 - 1.0 / TAU_COARSE)
            for tile in tiles:
                lanes = lanes_of(tile)

                def put(q, value):
                    pb[q, r, :, lanes] = value

                relax_into(lambda q: st[q, r, :, lanes], put,
                           lambda q: cq[q - 1, r, :, lanes] if q else plain)

        def faces(r, carry):
            first(r, (0, TILES - 1))
            return carry

        lax.fori_loop(0, SPAN_PATCHES, faces, 0)
        for way, e, group in ((0, 1, X_UP), (1, -1, X_DOWN)):
            for n, q in enumerate(group):
                v = along_z(q, pb[q, :, :, lanes_of(TILES - 1 if e == 1 else 0)])
                turned = spin(v, 64)
                if e == 1:
                    xs[s, way, n] = jnp.where(half, turned[:2], v[2:])
                else:
                    xs[s, way, n] = jnp.where(half, v[:2], turned[2:])
                if q in DIAGONAL:
                    ds[s, DIAGONAL.index(q)] = turned[SPAN_PATCHES - 1 if VELOCITIES[q][1] == 1 else 0]
        x_copies = []

        def send(src, dst, n, dx, dy):
            copy = pltpu.make_async_remote_copy(
                src_ref=src, dst_ref=dst, send_sem=send_sem.at[s, n], recv_sem=recv_sem.at[s, n],
                device_id=at(dx, dy), device_id_type=MESH)
            outgoing, incoming = ends_of(dx)
            start_to(outgoing, copy)
            return outgoing, incoming, copy

        def outer(m, carry):
            first(m * (SPAN_PATCHES - 1), range(1, TILES - 1))
            return carry

        def inner(r, carry):
            first(r, range(1, TILES - 1))
            return carry

        for way, dx in ((0, 1), (1, -1)):
            x_copies.append(send(xs.at[s, way], xr.at[s, way], 2 + way, dx, 0))
        for n, q in enumerate(DIAGONAL):
            x_copies.append(send(ds.at[s, n], dr.at[s, n], 4 + n, *VELOCITIES[q][:2]))
        lax.fori_loop(0, 2, outer, 0)
        for way, e, group in ((0, 1, Y_UP), (1, -1, Y_DOWN)):
            r = SPAN_PATCHES - 1 if e == 1 else 0
            for n, q in enumerate(group):
                for tile in range(TILES):
                    ys[s, way, n, :, lanes_of(tile)] = along_z(q, pb[q, r : r + 1, :, lanes_of(tile)])[0]
        y_copies = []
        for way, dy in ((0, 1), (1, -1)):
            y_copies.append(send(ys.at[s, way], yr.at[s, way], way, 0, dy))
        lax.fori_loop(1, SPAN_PATCHES - 1, inner, 0)

        def shift(q):
            e = VELOCITIES[q]
            tiles = [along_z(q, pb[q, :, :, lanes_of(tile)]) for tile in range(TILES)]
            if e[1]:
                way, group = (0, Y_UP) if e[1] == 1 else (1, Y_DOWN)
                n = group.index(q)
                tiles = [along_y(q, v, yr[s, way, n, :, lanes_of(tile)][None]) for tile, v in enumerate(tiles)]
            if e[0]:
                turned = [spin(v, 64) for v in tiles]
                for tile in range(TILES):
                    if e[0] == 1:
                        tiles[tile] = jnp.where(lower, turned[tile - 1], turned[tile])
                    else:
                        tiles[tile] = jnp.where(lower, turned[tile], turned[(tile + 1) % TILES])
            for tile in range(TILES):
                st[q, :, :, lanes_of(tile)] = tiles[tile]

        for q in range(19):
            if not VELOCITIES[q][1]:
                shift(q)
        for copy in y_copies:
            wait_for(*copy)
        hear(2 * s)
        tell(2 * s + 1)
        for q in range(19):
            if VELOCITIES[q][1]:
                shift(q)

        def again(r, tiles):
            for tile in tiles:
                lanes = lanes_of(tile)

                def put(q, value):
                    pb[q, r, :, lanes] = value

                relax_into(lambda q: st[q, r, :, lanes], put, lambda q: 1.0 - 1.0 / TAU_FINE)

        def settle(tiles):
            for q in range(19):
                e = VELOCITIES[q]
                amount = 64 * e[0] + 8 * e[1] + e[2]
                inside = fine
                for axis in (1, 2):
                    if e[axis]:
                        inside = inside & ~in_tile[axis, e[axis]]
                turned = {}

                def moved_from(tile):
                    if tile not in turned:
                        v = pb[q, :, :, lanes_of(tile)]
                        turned[tile] = spin(v, amount) if amount else v
                    return turned[tile]

                for tile in tiles:
                    take = inside
                    value = moved_from(tile)
                    if e[0] == 1:
                        value = jnp.where(lower, moved_from((tile - 1) % TILES), value)
                        take = take & ~lower if tile == 0 else take
                    elif e[0] == -1:
                        value = jnp.where(lower, value, moved_from((tile + 1) % TILES))
                        take = take & lower if tile == TILES - 1 else take
                    lanes = lanes_of(tile)
                    st[q, :, :, lanes] = jnp.where(take, value, st[q, :, :, lanes])

        def middle(r, carry):
            again(r, range(1, TILES - 1))
            return carry

        def ends(r, carry):
            again(r, (0, TILES - 1))
            return carry

        lax.fori_loop(0, SPAN_PATCHES, middle, 0)
        if stage is not None:
            lax.fori_loop(0, SPAN_PATCHES, ends, 0)
            settle(range(1, TILES - 1))
            stage()
        for copy in x_copies:
            wait_for(*copy)
        if stage is None:
            hear(2 * s + 1)
            tell(2 * s + 2)
        for way, e, group in ((0, 1, X_UP), (1, -1, X_DOWN)):
            outside = b == (0 if e == 1 else nb - 1)
            for n, q in enumerate(group):
                h = xr[s, way, n]
                turned = spin(h, 64)
                halo = jnp.concatenate([h, turned] if e == 1 else [turned, h], axis=0)
                if q in DIAGONAL:
                    halo = along_y(q, halo, dr[s, DIAGONAL.index(q)][None])
                along = e * INFLOW
                const = WEIGHTS[q] * (1.0 + 3.0 * along + 4.5 * along * along - 1.5 * INFLOW * INFLOW)
                halo = jnp.where(outside, jnp.full(halo.shape, const, jnp.float32), halo)
                lanes = lanes_of(0 if e == 1 else TILES - 1)
                keep = st[q, :, :, lanes]
                st[q, :, :, lanes] = jnp.where(lower, halo, keep) if e == 1 else jnp.where(lower, keep, halo)

        lax.fori_loop(0, SPAN_PATCHES, ends, 0)
        settle(range(TILES) if stage is None else (0, TILES - 1))

    def fill(half):
        pm[:, half * HALF + 2 * MAIN : (half + 1) * HALF, :] = jnp.zeros(
            (pm.shape[0], HALF - 2 * MAIN, LANES), jnp.float32)
        for q in range(19):
            for r in range(SPAN_PATCHES):
                for tile in range(TILES):
                    if half_of(tile) == half:
                        pm[r * 8 : r * 8 + 8, half * HALF + low_row(q, tile), :] = st[q, r, :, lanes_of(tile)]

    part = lax.rem(me, GROUP)
    base = me - part
    far_chip = part // nc
    chunks = count // GROUP

    def chunk_at(j):
        return lax.rem(j + chunks // 2, chunks)

    def rows_of(j):
        return pl.ds(chunk_at(j) * GROUP, GROUP)

    def swap_copy(half, j):
        return pltpu.make_async_remote_copy(
            src_ref=second.at[half, rows_of(j)], dst_ref=theirs.at[half, rows_of(j)],
            send_sem=csend.at[half, j], recv_sem=crecv.at[half, j], device_id=at(0, 1),
            device_id_type=MESH)

    def shuffle_copy(j):
        return pltpu.make_async_remote_copy(
            src_ref=away.at[rows_of(j)], dst_ref=across.at[rows_of(j)], send_sem=qsend.at[j],
            recv_sem=qrecv.at[j], device_id=device(lax.bitwise_xor(me, nc)), device_id_type=MESH)

    def tag_of(which, d):
        return tags[which, pl.ds(d, 1), :]

    def offer(half):
        def pack_second(j, carry):
            for i in range(GROUP):
                m = chunk_at(j) * GROUP + i
                d = lax.bitwise_xor(base, m)
                second[half, m] = pm[pick_s[d, 1], half * HALF : (half + 1) * HALF]
                if half == 0:
                    second[0, m, MARK : MARK + 1, :] = tag_of(1, d)
                    second[0, m, FIRST : FIRST + 1, :] = tag_of(0, d)

            @pl.when(j > 0)
            def _():
                swap_copy(half, j - 1).start()

            return carry

        lax.fori_loop(0, chunks, pack_second, 0)
        swap_copy(half, chunks - 1).start()

    zero = c == 0

    def pack_quarters(d, m, my_second, their_second, their_first, own):
        mine_extra = (my_second > -0.5) & (their_first > -0.5)
        their_extra = (their_second > -0.5) & own
        use_mine = mine_extra & (zero | ~their_extra)
        tag = jnp.where(use_mine, my_second, jnp.where(their_extra, their_second, -1.0))
        tag = jnp.where(mine_extra & their_extra, OVER, tag)
        p = pick_s[d, 1]
        for ref, t in ((kept, part), (away, lax.bitwise_xor(part, nc))):
            half = lax.rem(t, 2)
            place = t // 2
            top = pl.multiple_of(place * MAIN, 8)
            my_top = pl.multiple_of(half * HALF + place * MAIN, 8)
            my_low = pl.multiple_of(half * HALF + 2 * MAIN, 8)
            ref[m, :MAIN, :] = jnp.where(
                use_mine, pm[p, pl.ds(my_top, MAIN), :], theirs[half, m, pl.ds(top, MAIN), :])
            low = jnp.where(use_mine, pm[p, pl.ds(my_low, 8), :], theirs[half, m, 2 * MAIN : HALF, :])
            low = jnp.where(place == 1, pltpu.roll(low, 8 - TAIL, axis=0), low)
            ref[m, MAIN : MAIN + TAIL, :] = low[:TAIL]
            ref[m, TAG : TAG + 1, :] = tag

    def pack_chunk(half, j):
        for i in range(GROUP):
            k = chunk_at(j) * GROUP + i
            d = peer(k)
            m = lax.bitwise_xor(k, part)
            my_first = tag_of(0, d)
            their_second = theirs[0, m, MARK : MARK + 1, :]
            own = my_first > -0.5
            sent[half, d] = jnp.where(
                own, pm[pick_s[d, 0], half * HALF : (half + 1) * HALF], theirs[half, m])
            if half == 0:
                sent[0, d, MARK : MARK + 1, :] = jnp.where(own, my_first, their_second)
            else:
                pack_quarters(d, m, tag_of(1, d), their_second, theirs[0, m, FIRST : FIRST + 1, :], own)

    def send_chunk(half, j):
        if half:
            shuffle_copy(j).start()
        for i in range(GROUP):
            k = chunk_at(j) * GROUP + i

            @pl.when(k > 0)
            def _():
                patch_copy(half, k).start()

    def exchange(half):
        def post(j, carry):
            swap_copy(half, j).wait_recv()
            pack_chunk(half, j)

            @pl.when(j > 0)
            def _():
                send_chunk(half, j - 1)

            return carry

        lax.fori_loop(0, chunks, post, 0)
        send_chunk(half, chunks - 1)
        got_ref[2 * me + half] = sent[half, me]

    def early():
        fill(0)
        to_scalars.wait()
        offer(0)
        for k in range(2 * STEPS - 1, rounds):
            if k > 2 * STEPS - 1:
                tell(k)
            hear(k)
        exchange(0)

    def whole_step(s, carry):
        step(s)
        return carry

    lax.fori_loop(0, STEPS - 1, whole_step, 0)
    step(STEPS - 1, early)
    fill(1)
    offer(1)
    exchange(1)

    def swapped(j, carry):
        swap_copy(0, j).wait_send()
        swap_copy(1, j).wait_send()
        shuffle_copy(j).wait()
        return carry

    lax.fori_loop(0, chunks, swapped, 0)
    near_tags = kept[:, TAG, :]
    far_tags = across[:, TAG, :]
    over = (near_tags > OVER / 2) | (far_tags > OVER / 2) | ((near_tags > -0.5) & (far_tags > -0.5))
    flag = jnp.max(jnp.where(over, OVER, 0.0), axis=0, keepdims=True)

    def pack_extra(d):
        m = lax.bitwise_xor(base, d)
        mine = kept[m]
        other = across[m]
        keep = ((mine[TAG:] > -0.5) & (far_chip == 0)) | ~(other[TAG:] > -0.5)
        extra[d] = jnp.where(keep, mine, other)
        extra[d, TAG : TAG + 1, :] = jnp.where(keep, mine[TAG:], other[TAG:]) + flag

    def mask_at(i):
        return lax.rem(i + count // 2, count)

    def post_extra(i, carry):
        pack_extra(peer(mask_at(i)))

        @pl.when((i > 0) & (mask_at(i - 1) > 0))
        def _():
            extra_copy(mask_at(i - 1)).start()

        return carry

    lax.fori_loop(0, count, post_extra, 0)
    extra_copy(mask_at(count - 1)).start()
    got_extra[me] = extra[me]

    def finish(k, carry):
        patch_copy(0, k).wait()
        patch_copy(1, k).wait()
        extra_copy(k).wait()
        return carry

    lax.fori_loop(1, count, finish, 0)

    def assemble(g, carry):
        for t in range(TILES):
            whole = got_ref.at[2 * count + 2 * g + t % 2]
            block = got_extra.at[g * GROUP + t]
            whole[t // 2 * MAIN : (t // 2 + 1) * MAIN, :] = block[:MAIN, :]
            low = 2 * MAIN + t // 2 * TAIL
            whole[low : low + TAIL, :] = block[MAIN : MAIN + TAIL, :]
        return carry

    lax.fori_loop(0, chunks, assemble, 0)
    source = lax.broadcasted_iota(jnp.int32, (2 * count, LANES), 0)
    wanted = lax.broadcasted_iota(jnp.int32, (2 * count, LANES), 1).astype(jnp.float32)
    first_hit = (got_ref[: 2 * count, MARK, :] == wanted) & (source % 2 == 0)
    index = jnp.sum(jnp.where(first_hit, source, 0), axis=0, keepdims=True)
    source = source[:count]
    extra_tags = got_extra[:, TAG, :]
    extra_hit = (extra_tags == wanted[:count]) & (source % GROUP == 0)
    place = source // GROUP * 2 + 2 * count
    index = index + jnp.sum(jnp.where(extra_hit, place, 0), axis=0, keepdims=True)
    over = jnp.max(extra_tags, axis=0, keepdims=True)
    row = lax.broadcasted_iota(jnp.int32, (8, LANES), 0)
    table_ref[...] = jnp.where(row == 0, index, jnp.where(over > OVER / 2, 1, 0))


def full_kernel(nb, nc, sidx, slot_of, pm, got_ref, table_ref, sent, send_sem, recv_sem):
    count = nb * nc
    me = lax.axis_index("blocks") * nc + lax.axis_index("cross")

    def device(d):
        return (d // nc, lax.rem(d, nc))

    barrier = pltpu.get_barrier_semaphore()

    def greet(k, carry):
        pl.semaphore_signal(barrier, inc=1, device_id=device(lax.bitwise_xor(me, k)), device_id_type=MESH)
        return carry

    lax.fori_loop(1, count, greet, 0)
    pl.semaphore_wait(barrier, count - 1)

    def pack(d, carry):
        for slot in range(2):
            p = sidx[2 * d + slot]
            sent[d, 2 * slot] = pm[p, :HALF]
            sent[d, 2 * slot + 1] = pm[p, HALF:]
            tag = jnp.full((1, LANES), slot_of[2 * d + slot].astype(jnp.float32), jnp.float32)
            sent[d, 2 * slot, MARK : MARK + 1, :] = tag
        return carry

    lax.fori_loop(0, count, pack, 0)

    def copy(k):
        d = lax.bitwise_xor(me, k)
        return pltpu.make_async_remote_copy(
            src_ref=sent.at[d], dst_ref=got_ref.at[pl.ds(4 * me, 4)], send_sem=send_sem.at[k],
            recv_sem=recv_sem.at[k], device_id=device(d), device_id_type=MESH)

    def post(k, carry):
        copy(k).start()
        return carry

    def finish(k, carry):
        copy(k).wait()
        return carry

    lax.fori_loop(1, count, post, 0)
    for i in range(4):
        got_ref[4 * me + i] = sent[me, i]
    lax.fori_loop(1, count, finish, 0)
    source = lax.broadcasted_iota(jnp.int32, (4 * count, LANES), 0)
    wanted = lax.broadcasted_iota(jnp.int32, (4 * count, LANES), 1).astype(jnp.float32)
    hit = (got_ref[:, MARK, :] == wanted) & (source % 2 == 0)
    index = jnp.sum(jnp.where(hit, source, 0), axis=0, keepdims=True)
    table_ref[...] = jnp.broadcast_to(index, table_ref.shape)


def unpack_kernel(ridx, got_ref, out_ref):
    for t in range(out_ref.shape[1]):
        base = ridx[0, t]
        for tile in range(TILES):
            block = got_ref.at[base + half_of(tile)]
            lanes = slice(tile * LANES, (tile + 1) * LANES)
            low = low_row(0, tile)
            out_ref[:MAIN, t, lanes] = block[low : low + MAIN, :]
            low = low_row(MAIN, tile)
            out_ref[MAIN:, t, lanes] = block[2 * MAIN :, :][low - 2 * MAIN : low - 2 * MAIN + TAIL]


def body(nb, nc, f_home, levels, plan):
    devices = nb * nc
    patches = f_home.shape[0]
    vmem = pl.BlockSpec(memory_space=pltpu.VMEM)
    smem = pl.BlockSpec(memory_space=pltpu.SMEM)
    state = (19, SPAN_PATCHES, 8, CELLS)
    small = (SPAN_PATCHES, 8, LANES)
    f32 = jnp.float32
    dma = pltpu.SemaphoreType.DMA
    half = (HALF, LANES)
    quarter = (QUARTER, LANES)
    rounds = max(2 * STEPS, (nb - 1).bit_length())
    limit = pltpu.CompilerParams(collective_id=0, has_side_effects=True, vmem_limit_bytes=60 * 1024 * 1024)
    got, packed, table = pl.pallas_call(
        lambda *refs: lattice_kernel(nb, nc, *refs),
        out_shape=(
            jax.ShapeDtypeStruct((2 * devices + 2 * devices // GROUP,) + half, f32),
            jax.ShapeDtypeStruct((patches, 2 * HALF, LANES), f32),
            jax.ShapeDtypeStruct((8, LANES), jnp.int32),
        ),
        in_specs=[smem, vmem, vmem],
        out_specs=(vmem, vmem, vmem),
        scratch_shapes=[
            pltpu.VMEM(state, f32),
            pltpu.VMEM(state, f32),
            pltpu.VMEM((18,) + state[1:], f32),
            pltpu.VMEM((2, devices) + half, f32),
            pltpu.VMEM((2, devices) + half, f32),
            pltpu.VMEM((2, devices) + half, f32),
            pltpu.VMEM((devices,) + quarter, f32),
            pltpu.VMEM((devices,) + quarter, f32),
            pltpu.VMEM((devices,) + quarter, f32),
            pltpu.VMEM((devices,) + quarter, f32),
            pltpu.VMEM((devices,) + quarter, f32),
            pltpu.VMEM(small, f32),
            pltpu.VMEM((len(AROUND),) + small, f32),
            pltpu.VMEM((STEPS, 2, 5, 8, CELLS), f32),
            pltpu.VMEM((STEPS, 2, 5, 8, CELLS), f32),
            pltpu.VMEM((STEPS, 2, 5, 2, 8, LANES), f32),
            pltpu.VMEM((STEPS, 2, 5, 2, 8, LANES), f32),
            pltpu.VMEM((STEPS, len(DIAGONAL), 8, LANES), f32),
            pltpu.VMEM((STEPS, len(DIAGONAL), 8, LANES), f32),
            pltpu.VMEM((devices, LANES), jnp.int32),
            pltpu.SMEM((devices, LANES), jnp.int32),
            pltpu.VMEM((2, devices, LANES), f32),
            dma((STEPS, 8)),
            dma((STEPS, 8)),
            dma((len(AROUND),)),
            dma((len(AROUND),)),
            dma((2, devices)),
            dma((2, devices)),
            dma((devices,)),
            dma((devices,)),
            dma((2, devices // GROUP)),
            dma((2, devices // GROUP)),
            dma((devices // GROUP,)),
            dma((devices // GROUP,)),
            dma,
            pltpu.SemaphoreType.REGULAR((rounds,)),
            pltpu.SemaphoreType.REGULAR((rounds,)),
        ],
        compiler_params=limit,
    )(levels, plan[None, :], jnp.transpose(f_home, (1, 0, 2)))

    def unpack(table, got):
        return pl.pallas_call(
            unpack_kernel,
            out_shape=jax.ShapeDtypeStruct((19, patches, CELLS), f32),
            in_specs=[smem, vmem],
            out_specs=vmem,
            compiler_params=pltpu.CompilerParams(vmem_limit_bytes=40 * 1024 * 1024),
        )(table, got)

    def in_full(table, got, packed, plan):
        target = plan // patches
        order = jnp.arange(patches, dtype=jnp.int32)
        earlier = (target[:, None] == target[None, :]) & (order[None, :] < order[:, None])
        place = 2 * target + jnp.sum(earlier.astype(jnp.int32), axis=1)
        hit = place[None, :] == jnp.arange(2 * devices, dtype=jnp.int32)[:, None]
        sidx = jnp.sum(jnp.where(hit, order[None, :], 0), axis=1)
        slot_of = jnp.sum(jnp.where(hit, plan[None, :] % patches + 1, 0), axis=1) - 1
        got, table = pl.pallas_call(
            lambda *refs: full_kernel(nb, nc, *refs),
            out_shape=(
                jax.ShapeDtypeStruct((4 * devices,) + half, f32),
                jax.ShapeDtypeStruct((8, LANES), jnp.int32),
            ),
            in_specs=[smem, smem, vmem],
            out_specs=(vmem, vmem),
            scratch_shapes=[
                pltpu.VMEM((devices, 4) + half, f32), dma((devices,)), dma((devices,))
            ],
            compiler_params=pltpu.CompilerParams(collective_id=1, has_side_effects=True,
                                                 vmem_limit_bytes=48 * 1024 * 1024),
        )(sidx, slot_of, packed)
        return unpack(table, got)

    out = lax.cond(table[1, 0] > 0, in_full, lambda table, got, packed, plan: unpack(table, got),
                   table, got, packed, plan)
    return jnp.transpose(out, (1, 0, 2))


def solution(mesh):
    nb, nc = mesh.shape["blocks"], mesh.shape["cross"]
    in_specs = (P(("blocks", "cross"), None, None), P(("blocks", "cross")), P(("blocks", "cross")))
    out_specs = P(("blocks", "cross"), None, None)
    return jax.shard_map(
        lambda f, l, p: body(nb, nc, f, l, p),
        mesh=mesh, in_specs=in_specs, out_specs=out_specs, check_vma=False)
```

```python
import jax
import jax.numpy as jnp
from jax import lax
from jax.experimental import pallas as pl
from jax.experimental.pallas import tpu as pltpu
from jax.sharding import PartitionSpec as P

SPAN_PATCHES = 4
DEPTH_PATCHES = 8
STEPS = 2
CELLS = 512
VELOCITIES = (
    (0, 0, 0),
    (1, 0, 0),
    (-1, 0, 0),
    (0, 1, 0),
    (0, -1, 0),
    (0, 0, 1),
    (0, 0, -1),
    (1, 1, 0),
    (-1, -1, 0),
    (1, -1, 0),
    (-1, 1, 0),
    (1, 0, 1),
    (-1, 0, -1),
    (1, 0, -1),
    (-1, 0, 1),
    (0, 1, 1),
    (0, -1, -1),
    (0, 1, -1),
    (0, -1, 1),
)
WEIGHTS = (1.0 / 3.0,) + (1.0 / 18.0,) * 6 + (1.0 / 36.0,) * 12
TAU_COARSE = 0.55
TAU_FINE = 2.0 * TAU_COARSE - 0.5
RESCALE = TAU_FINE / (2.0 * TAU_COARSE)
INFLOW = 0.08
MESH = pl.DeviceIdType.MESH
MAIN = 16
TAIL = 3
HALF = 40
MARK = 38
FIRST = 39
QUARTER = 20
TAG = 19
OVER = 1000.0
GROUP = 4
LANES = 128
TILES = CELLS // LANES
Y_UP = [q for q in range(19) if VELOCITIES[q][1] == 1]
Y_DOWN = [q for q in range(19) if VELOCITIES[q][1] == -1]
X_UP = [q for q in range(19) if VELOCITIES[q][0] == 1]
X_DOWN = [q for q in range(19) if VELOCITIES[q][0] == -1]
DIAGONAL = [q for q in range(19) if VELOCITIES[q][0] and VELOCITIES[q][1]]


def relax_into(load, store, coef):
    f = [load(q) for q in range(19)]
    terms = list(f)
    while len(terms) > 1:
        pairs = [a + b for a, b in zip(terms[::2], terms[1::2])]
        terms = pairs + ([terms[-1]] if len(terms) % 2 else [])
    rho = terms[0]
    inv = 1.0 / rho
    u = []
    for axis in range(3):
        up = [f[q] for q in range(19) if VELOCITIES[q][axis] == 1]
        down = [f[q] for q in range(19) if VELOCITIES[q][axis] == -1]
        d = [a - b for a, b in zip(up, down)]
        u.append((((d[0] + d[1]) + (d[2] + d[3])) + d[4]) * inv)
    base = 1.0 - 1.5 * (u[0] * u[0] + u[1] * u[1] + u[2] * u[2])
    scaled = {w: w * rho for w in set(WEIGHTS)}
    for q in range(19):
        along = None
        for axis in range(3):
            e = VELOCITIES[q][axis]
            if e:
                term = u[axis] if e == 1 else -u[axis]
                along = term if along is None else along + term
        poly = base if along is None else base + along * (3.0 + 4.5 * along)
        balance = scaled[WEIGHTS[q]] * poly
        store(q, balance + coef(q) * (f[q] - balance))


def half_of(tile):
    return 1 if tile in (0, TILES - 1) else 0


def place_of(tile):
    return tile // 2 if half_of(tile) else tile - 1


def low_row(q, tile):
    place = place_of(tile)
    return place * MAIN + q if q < MAIN else 2 * MAIN + place * TAIL + q - MAIN


def lattice_kernel(nb, nc, level, plan_ref, f_ref, got_ref, pm, table_ref, st, pb, cq, sent, second, theirs,
                   away, kept, across, extra, got_extra, own_ref, lev_ref, lv, ys, yr, xs, xr, ds, dr, pick, pick_s, tags, send_sem, recv_sem, lsend, lrecv, psend,
                   precv, esend, erecv, csend, crecv, qsend, qrecv, pick_sem, up_sem, down_sem):
    others = nb * nc - 1
    rounds = max(2 * STEPS, (nb - 1).bit_length())
    b = lax.axis_index("blocks")
    c = lax.axis_index("cross")

    def at(dx, dy):
        return (lax.rem(b + dx + nb, nb), lax.rem(c + dy + nc, nc))

    me = b * nc + c

    def peer(k):
        return lax.bitwise_xor(me, k)

    def device(d):
        return (d // nc, lax.rem(d, nc))

    barrier = pltpu.get_barrier_semaphore()
    above = b < nb - 1
    below = b > 0

    def signal(sem, to):
        pl.semaphore_signal(sem, inc=1, device_id=to, device_id_type=MESH)

    for k in range(1, nc):
        signal(barrier, at(0, k))
    for there, dx in ((above, 1), (below, -1)):
        @pl.when(there)
        def _():
            for k in range(nc):
                signal(barrier, at(dx, k))

    def tell(k):
        hop = lax.shift_left(jnp.int32(1), jnp.int32(k))

        @pl.when(b + hop < nb)
        def _():
            signal(up_sem.at[k], (b + hop, c))

        @pl.when(b >= hop)
        def _():
            signal(down_sem.at[k], (b - hop, c))

    def hear(k):
        hop = lax.shift_left(jnp.int32(1), jnp.int32(k))

        @pl.when(b >= hop)
        def _():
            pl.semaphore_wait(up_sem.at[k], 1)

        @pl.when(b + hop < nb)
        def _():
            pl.semaphore_wait(down_sem.at[k], 1)

    patches = f_ref.shape[1]
    count = nb * nc
    target = lax.broadcasted_iota(jnp.int32, (count, patches), 0)
    where = jnp.broadcast_to(plan_ref[...], (count, patches))
    member = where // patches == target
    key = lax.broadcasted_iota(jnp.int32, (count, patches), 1) * patches + where % patches
    low_key = jnp.min(jnp.where(member, key, patches * patches), axis=1, keepdims=True)
    high_key = jnp.max(jnp.where(member, key, -1), axis=1, keepdims=True)
    some = high_key >= 0
    two = high_key > low_key
    column = lax.broadcasted_iota(jnp.int32, (count, LANES), 1)
    pick[...] = jnp.where(column == 0, jnp.where(some, low_key // patches, 0),
                          jnp.where(two, high_key // patches, 0))
    to_scalars = pltpu.make_async_copy(pick, pick_s, pick_sem)
    to_scalars.start()
    tags[0] = jnp.broadcast_to(jnp.where(some, low_key % patches, -1), (count, LANES)).astype(jnp.float32)
    tags[1] = jnp.broadcast_to(jnp.where(two, high_key % patches, -1), (count, LANES)).astype(jnp.float32)

    slot = lax.broadcasted_iota(jnp.int32, (8, LANES), 0)
    slot = slot + 8 * lax.broadcasted_iota(jnp.int32, (8, LANES), 1)
    brief = jnp.zeros((8, LANES), jnp.float32)
    for p in range(SPAN_PATCHES * 8):
        brief = jnp.where(slot == p, level[p].astype(jnp.float32), brief)
    lev_ref[...] = brief

    def spread(values, r):
        return jnp.broadcast_to(values[:, r : r + 1], (8, LANES))[None]

    own = jnp.concatenate([spread(brief, r) for r in range(SPAN_PATCHES)], axis=0)
    own_ref[...] = own
    for q in range(19):
        for r in range(SPAN_PATCHES):
            st[q, r] = f_ref[q, r * 8 : r * 8 + 8, :]
    pl.semaphore_wait(barrier, nc - 1 + nc * (jnp.where(above, 1, 0) + jnp.where(below, 1, 0)))
    tell(0)

    def start_to(there, copy):
        if there is None:
            copy.start()
        else:
            pl.when(there)(copy.start)

    def wait_for(outgoing, incoming, copy):
        if outgoing is None:
            copy.wait()
        else:
            pl.when(outgoing)(copy.wait_send)
            pl.when(incoming)(copy.wait_recv)

    def ends_of(dx):
        return {0: (None, None), 1: (above, below), -1: (below, above)}[dx]

    level_copies = []
    around = [(dx, dy) for dx in (-1, 0, 1) for dy in range(nc) if (dx, dy) != (0, 0)]
    for n, (dx, dy) in enumerate(around):
        copy = pltpu.make_async_remote_copy(
            src_ref=lev_ref, dst_ref=lv.at[n], send_sem=lsend.at[n], recv_sem=lrecv.at[n],
            device_id=at(-dx, -dy), device_id_type=MESH)
        outgoing, incoming = ends_of(-dx)
        start_to(outgoing, copy)
        level_copies.append((outgoing, incoming, copy))

    def patch_copy(half, k):
        d = peer(k)
        rows = slice(0, MARK if half else FIRST)
        return pltpu.make_async_remote_copy(
            src_ref=sent.at[half, d, rows], dst_ref=got_ref.at[2 * me + half, rows],
            send_sem=psend.at[half, k], recv_sem=precv.at[half, k], device_id=device(d),
            device_id_type=MESH)

    def extra_copy(k):
        d = peer(k)
        return pltpu.make_async_remote_copy(
            src_ref=extra.at[d], dst_ref=got_extra.at[me], send_sem=esend.at[k],
            recv_sem=erecv.at[k], device_id=device(d), device_id_type=MESH)

    for copy in level_copies:
        wait_for(*copy)

    patch_scale = {}
    for dx in (-1, 0, 1):
        rows = [spread(lv[around.index((dx, nc - 1))], SPAN_PATCHES - 1)]
        rows += [own[r][None] if dx == 0 else spread(lv[around.index((dx, 0))], r) for r in range(SPAN_PATCHES)]
        rows += [spread(lv[around.index((dx, 1 % nc))], 0)]
        rows = [jnp.where(value > 0.5, RESCALE, 1.0) for value in rows]
        for dy in (-1, 0, 1):
            patch_scale[dx, dy] = jnp.concatenate(rows[1 + dy : 1 + dy + SPAN_PATCHES], axis=0)
    gain = jnp.where(own > 0.5, (1.0 - 1.0 / TAU_FINE) / RESCALE, 1.0 - 1.0 / TAU_COARSE)

    def target_scale(dx, dy, dz):
        value = patch_scale[dx, dy]
        return pltpu.roll(value, (-dz) % 8, axis=1) if dz else value

    shape = (SPAN_PATCHES, 8, LANES)
    lane = lax.broadcasted_iota(jnp.int32, shape, 2)
    for q in range(1, 19):
        e = VELOCITIES[q]
        kinds = [{}]
        for axis in range(3):
            if e[axis]:
                kinds = [{**k, axis: v} for k in kinds for v in (0, 1)]
        table = [(k, target_scale(*[e[a] * k.get(a, 0) for a in range(3)])) for k in kinds]
        for tile in range(TILES):
            cell = lane + tile * LANES
            coord = (cell // 64, (cell // 8) % 8, cell % 8)
            result = table[0][1]
            for k, value in table[1:]:
                mask = None
                for axis, on in k.items():
                    if on:
                        hit = coord[axis] == (7 if e[axis] == 1 else 0)
                        mask = hit if mask is None else mask & hit
                result = jnp.where(mask, value, result)
            cq[q - 1, :, :, tile * LANES : (tile + 1) * LANES] = gain * result

    lower = lane < 64
    half = lax.broadcasted_iota(jnp.int32, (2, 8, LANES), 2) < 64
    fine = own > 0.5
    in_tile = {
        (axis, e): (lane // 8 % 8 if axis == 1 else lane % 8) == (0 if e == 1 else 7)
        for axis in (1, 2) for e in (1, -1)
    }

    def spin(v, amount):
        return pltpu.roll(v, amount % LANES, axis=v.ndim - 1)

    def along_z(q, v, more=0):
        e = VELOCITIES[q][2]
        if not e:
            return spin(v, more) if more else v
        wrapped = pltpu.roll(spin(v, more - 7 * e), e % 8, axis=1)
        return jnp.where(in_tile[2, e][: v.shape[0]], wrapped, spin(v, more + e))

    def along_y(q, v, halo, more=0):
        e = VELOCITIES[q][1]
        moved = jnp.concatenate([halo, v[:-1]] if e == 1 else [v[1:], halo], axis=0)
        return jnp.where(in_tile[1, e], spin(moved, more - 56 * e), spin(v, more + 8 * e))

    def lanes_of(tile):
        return slice(tile * LANES, (tile + 1) * LANES)

    def step(s, stage=None):
        def first(r, tiles):
            plain = jnp.where(own_ref[r] > 0.5, 1.0 - 1.0 / TAU_FINE, 1.0 - 1.0 / TAU_COARSE)
            for tile in tiles:
                lanes = lanes_of(tile)

                def put(q, value):
                    pb[q, r, :, lanes] = value

                relax_into(lambda q: st[q, r, :, lanes], put,
                           lambda q: cq[q - 1, r, :, lanes] if q else plain)

        def faces(r, carry):
            first(r, (0, TILES - 1))
            return carry

        lax.fori_loop(0, SPAN_PATCHES, faces, 0)
        for way, e, group in ((0, 1, X_UP), (1, -1, X_DOWN)):
            for n, q in enumerate(group):
                v = along_z(q, pb[q, :, :, lanes_of(TILES - 1 if e == 1 else 0)])
                turned = spin(v, 64)
                if e == 1:
                    xs[s, way, n] = jnp.where(half, turned[:2], v[2:])
                else:
                    xs[s, way, n] = jnp.where(half, v[:2], turned[2:])
                if q in DIAGONAL:
                    ds[s, DIAGONAL.index(q)] = turned[SPAN_PATCHES - 1 if VELOCITIES[q][1] == 1 else 0]
        x_copies = []

        def send(src, dst, n, dx, dy):
            copy = pltpu.make_async_remote_copy(
                src_ref=src, dst_ref=dst, send_sem=send_sem.at[s, n], recv_sem=recv_sem.at[s, n],
                device_id=at(dx, dy), device_id_type=MESH)
            outgoing, incoming = ends_of(dx)
            start_to(outgoing, copy)
            return outgoing, incoming, copy

        def outer(m, carry):
            first(m * (SPAN_PATCHES - 1), range(1, TILES - 1))
            return carry

        def inner(r, carry):
            first(r, range(1, TILES - 1))
            return carry

        for way, dx in ((0, 1), (1, -1)):
            x_copies.append(send(xs.at[s, way], xr.at[s, way], 2 + way, dx, 0))
        for n, q in enumerate(DIAGONAL):
            x_copies.append(send(ds.at[s, n], dr.at[s, n], 4 + n, *VELOCITIES[q][:2]))
        lax.fori_loop(0, 2, outer, 0)
        for way, e, group in ((0, 1, Y_UP), (1, -1, Y_DOWN)):
            r = SPAN_PATCHES - 1 if e == 1 else 0
            for n, q in enumerate(group):
                for tile in range(TILES):
                    ys[s, way, n, :, lanes_of(tile)] = along_z(q, pb[q, r : r + 1, :, lanes_of(tile)])[0]
        y_copies = []
        for way, dy in ((0, 1), (1, -1)):
            y_copies.append(send(ys.at[s, way], yr.at[s, way], way, 0, dy))
        lax.fori_loop(1, SPAN_PATCHES - 1, inner, 0)

        def shift(q):
            e = VELOCITIES[q]
            half_turn = 64 if e[0] else 0
            tiles = [along_z(q, pb[q, :, :, lanes_of(tile)], 0 if e[1] else half_turn) for tile in range(TILES)]
            if e[1]:
                way, group = (0, Y_UP) if e[1] == 1 else (1, Y_DOWN)
                n = group.index(q)
                tiles = [along_y(q, v, yr[s, way, n, :, lanes_of(tile)][None], half_turn)
                         for tile, v in enumerate(tiles)]
            if e[0]:
                turned = list(tiles)
                for tile in range(TILES):
                    if e[0] == 1:
                        tiles[tile] = jnp.where(lower, turned[tile - 1], turned[tile])
                    else:
                        tiles[tile] = jnp.where(lower, turned[tile], turned[(tile + 1) % TILES])
            for tile in range(TILES):
                st[q, :, :, lanes_of(tile)] = tiles[tile]

        for q in range(19):
            if not VELOCITIES[q][1]:
                shift(q)
        for copy in y_copies:
            wait_for(*copy)
        hear(2 * s)
        tell(2 * s + 1)
        for q in range(19):
            if VELOCITIES[q][1]:
                shift(q)

        def again(r, tiles):
            for tile in tiles:
                lanes = lanes_of(tile)

                def put(q, value):
                    pb[q, r, :, lanes] = value

                relax_into(lambda q: st[q, r, :, lanes], put, lambda q: 1.0 - 1.0 / TAU_FINE)

        def settle(tiles):
            for q in range(19):
                e = VELOCITIES[q]
                amount = 64 * e[0] + 8 * e[1] + e[2]
                inside = fine
                for axis in (1, 2):
                    if e[axis]:
                        inside = inside & ~in_tile[axis, e[axis]]
                turned = {}

                def moved_from(tile):
                    if tile not in turned:
                        v = pb[q, :, :, lanes_of(tile)]
                        turned[tile] = spin(v, amount) if amount else v
                    return turned[tile]

                for tile in tiles:
                    take = inside
                    value = moved_from(tile)
                    if e[0] == 1:
                        value = jnp.where(lower, moved_from((tile - 1) % TILES), value)
                        take = take & ~lower if tile == 0 else take
                    elif e[0] == -1:
                        value = jnp.where(lower, value, moved_from((tile + 1) % TILES))
                        take = take & lower if tile == TILES - 1 else take
                    lanes = lanes_of(tile)
                    st[q, :, :, lanes] = jnp.where(take, value, st[q, :, :, lanes])

        def middle(r, carry):
            again(r, range(1, TILES - 1))
            return carry

        def ends(r, carry):
            again(r, (0, TILES - 1))
            return carry

        lax.fori_loop(0, SPAN_PATCHES, middle, 0)
        if stage is not None:
            lax.fori_loop(0, SPAN_PATCHES, ends, 0)
            settle(range(1, TILES - 1))
            stage()
        for copy in x_copies:
            wait_for(*copy)
        if stage is None:
            hear(2 * s + 1)
            tell(2 * s + 2)
        for way, e, group in ((0, 1, X_UP), (1, -1, X_DOWN)):
            outside = b == (0 if e == 1 else nb - 1)
            for n, q in enumerate(group):
                h = xr[s, way, n]
                turned = spin(h, 64)
                halo = jnp.concatenate([h, turned] if e == 1 else [turned, h], axis=0)
                if q in DIAGONAL:
                    halo = along_y(q, halo, dr[s, DIAGONAL.index(q)][None])
                along = e * INFLOW
                const = WEIGHTS[q] * (1.0 + 3.0 * along + 4.5 * along * along - 1.5 * INFLOW * INFLOW)
                halo = jnp.where(outside, jnp.full(halo.shape, const, jnp.float32), halo)
                lanes = lanes_of(0 if e == 1 else TILES - 1)
                keep = st[q, :, :, lanes]
                st[q, :, :, lanes] = jnp.where(lower, halo, keep) if e == 1 else jnp.where(lower, keep, halo)

        lax.fori_loop(0, SPAN_PATCHES, ends, 0)
        settle(range(TILES) if stage is None else (0, TILES - 1))

    flat = pm.reshape(pm.shape[0] * 2 * HALF, LANES)

    def fill(half):
        pm[:, half * HALF + 2 * MAIN : (half + 1) * HALF, :] = jnp.zeros(
            (pm.shape[0], HALF - 2 * MAIN, LANES), jnp.float32)
        for q in range(19):
            for r in range(SPAN_PATCHES):
                for tile in range(TILES):
                    if half_of(tile) == half:
                        row = r * 8 * 2 * HALF + half * HALF + low_row(q, tile)
                        flat[pl.ds(row, 8, stride=2 * HALF), :] = st[q, r, :, lanes_of(tile)]

    part = lax.rem(me, GROUP)
    base = me - part
    far_chip = part // nc
    chunks = count // GROUP

    def chunk_at(j):
        return lax.rem(j + chunks // 2, chunks)

    def rows_of(j):
        return pl.ds(chunk_at(j) * GROUP, GROUP)

    def swap_copy(half, j):
        return pltpu.make_async_remote_copy(
            src_ref=second.at[half, rows_of(j)], dst_ref=theirs.at[half, rows_of(j)],
            send_sem=csend.at[half, j], recv_sem=crecv.at[half, j], device_id=at(0, 1),
            device_id_type=MESH)

    def shuffle_copy(j):
        return pltpu.make_async_remote_copy(
            src_ref=away.at[rows_of(j)], dst_ref=across.at[rows_of(j)], send_sem=qsend.at[j],
            recv_sem=qrecv.at[j], device_id=device(lax.bitwise_xor(me, nc)), device_id_type=MESH)

    def tag_of(which, d):
        return tags[which, pl.ds(d, 1), :]

    def offer(half):
        def pack_second(j, carry):
            for i in range(GROUP):
                m = chunk_at(j) * GROUP + i
                d = lax.bitwise_xor(base, m)
                second[half, m] = pm[pick_s[d, 1], half * HALF : (half + 1) * HALF]
                if half == 0:
                    second[0, m, MARK : MARK + 1, :] = tag_of(1, d)
                    second[0, m, FIRST : FIRST + 1, :] = tag_of(0, d)

            @pl.when(j > 0)
            def _():
                swap_copy(half, j - 1).start()

            return carry

        lax.fori_loop(0, chunks, pack_second, 0)
        swap_copy(half, chunks - 1).start()

    zero = c == 0

    def pack_quarters(d, m, my_second, their_second, their_first, own):
        mine_extra = (my_second > -0.5) & (their_first > -0.5)
        their_extra = (their_second > -0.5) & own
        use_mine = mine_extra & (zero | ~their_extra)
        tag = jnp.where(use_mine, my_second, jnp.where(their_extra, their_second, -1.0))
        tag = jnp.where(mine_extra & their_extra, OVER, tag)
        p = pick_s[d, 1]
        for ref, t in ((kept, part), (away, lax.bitwise_xor(part, nc))):
            half = lax.rem(t, 2)
            place = t // 2
            top = pl.multiple_of(place * MAIN, 8)
            my_top = pl.multiple_of(half * HALF + place * MAIN, 8)
            my_low = pl.multiple_of(half * HALF + 2 * MAIN, 8)
            ref[m, :MAIN, :] = jnp.where(
                use_mine, pm[p, pl.ds(my_top, MAIN), :], theirs[half, m, pl.ds(top, MAIN), :])
            low = jnp.where(use_mine, pm[p, pl.ds(my_low, 8), :], theirs[half, m, 2 * MAIN : HALF, :])
            low = jnp.where(place == 1, pltpu.roll(low, 8 - TAIL, axis=0), low)
            ref[m, MAIN : MAIN + TAIL, :] = low[:TAIL]
            ref[m, TAG : TAG + 1, :] = tag

    def pack_chunk(half, j):
        for i in range(GROUP):
            k = chunk_at(j) * GROUP + i
            d = peer(k)
            m = lax.bitwise_xor(k, part)
            my_first = tag_of(0, d)
            their_second = theirs[0, m, MARK : MARK + 1, :]
            own = my_first > -0.5
            sent[half, d] = jnp.where(
                own, pm[pick_s[d, 0], half * HALF : (half + 1) * HALF], theirs[half, m])
            if half == 0:
                sent[0, d, MARK : MARK + 1, :] = jnp.where(own, my_first, their_second)
            else:
                pack_quarters(d, m, tag_of(1, d), their_second, theirs[0, m, FIRST : FIRST + 1, :], own)

    def send_chunk(half, j):
        if half:
            shuffle_copy(j).start()
        for i in range(GROUP):
            k = chunk_at(j) * GROUP + i

            @pl.when(k > 0)
            def _():
                patch_copy(half, k).start()

    def exchange(half):
        def post(j, carry):
            swap_copy(half, j).wait_recv()
            pack_chunk(half, j)

            @pl.when(j > 0)
            def _():
                send_chunk(half, j - 1)

            return carry

        lax.fori_loop(0, chunks, post, 0)
        send_chunk(half, chunks - 1)
        got_ref[2 * me + half] = sent[half, me]

    def early():
        fill(0)
        to_scalars.wait()
        offer(0)
        for k in range(2 * STEPS - 1, rounds):
            if k > 2 * STEPS - 1:
                tell(k)
            hear(k)
        exchange(0)

    def whole_step(s, carry):
        step(s)
        return carry

    lax.fori_loop(0, STEPS - 1, whole_step, 0)
    step(STEPS - 1, early)
    fill(1)
    offer(1)
    exchange(1)

    def swapped(j, carry):
        swap_copy(0, j).wait_send()
        swap_copy(1, j).wait_send()
        shuffle_copy(j).wait()
        return carry

    lax.fori_loop(0, chunks, swapped, 0)
    near_tags = kept[:, TAG, :]
    far_tags = across[:, TAG, :]
    over = (near_tags > OVER / 2) | (far_tags > OVER / 2) | ((near_tags > -0.5) & (far_tags > -0.5))
    flag = jnp.max(jnp.where(over, OVER, 0.0), axis=0, keepdims=True)

    def pack_extra(d):
        m = lax.bitwise_xor(base, d)
        mine = kept[m]
        other = across[m]
        keep = ((mine[TAG:] > -0.5) & (far_chip == 0)) | ~(other[TAG:] > -0.5)
        extra[d] = jnp.where(keep, mine, other)
        extra[d, TAG : TAG + 1, :] = jnp.where(keep, mine[TAG:], other[TAG:]) + flag

    def mask_at(i):
        return lax.rem(i + count // 2, count)

    def post_extra(i, carry):
        pack_extra(peer(mask_at(i)))

        @pl.when((i > 0) & (mask_at(i - 1) > 0))
        def _():
            extra_copy(mask_at(i - 1)).start()

        return carry

    lax.fori_loop(0, count, post_extra, 0)
    extra_copy(mask_at(count - 1)).start()
    got_extra[me] = extra[me]

    def finish(k, carry):
        patch_copy(0, k).wait()
        patch_copy(1, k).wait()
        extra_copy(k).wait()
        return carry

    lax.fori_loop(1, count, finish, 0)

    def assemble(g, carry):
        for t in range(TILES):
            whole = got_ref.at[2 * count + 2 * g + t % 2]
            block = got_extra.at[g * GROUP + t]
            whole[t // 2 * MAIN : (t // 2 + 1) * MAIN, :] = block[:MAIN, :]
            low = 2 * MAIN + t // 2 * TAIL
            whole[low : low + TAIL, :] = block[MAIN : MAIN + TAIL, :]
        return carry

    lax.fori_loop(0, chunks, assemble, 0)
    source = lax.broadcasted_iota(jnp.int32, (2 * count, LANES), 0)
    wanted = lax.broadcasted_iota(jnp.int32, (2 * count, LANES), 1).astype(jnp.float32)
    first_hit = (got_ref[: 2 * count, MARK, :] == wanted) & (source % 2 == 0)
    index = jnp.sum(jnp.where(first_hit, source, 0), axis=0, keepdims=True)
    source = source[:count]
    extra_tags = got_extra[:, TAG, :]
    extra_hit = (extra_tags == wanted[:count]) & (source % GROUP == 0)
    place = source // GROUP * 2 + 2 * count
    index = index + jnp.sum(jnp.where(extra_hit, place, 0), axis=0, keepdims=True)
    over = jnp.max(extra_tags, axis=0, keepdims=True)
    row = lax.broadcasted_iota(jnp.int32, (8, LANES), 0)
    table_ref[...] = jnp.where(row == 0, index, jnp.where(over > OVER / 2, 1, 0))


def full_kernel(nb, nc, sidx, slot_of, pm, got_ref, table_ref, sent, send_sem, recv_sem):
    count = nb * nc
    me = lax.axis_index("blocks") * nc + lax.axis_index("cross")

    def device(d):
        return (d // nc, lax.rem(d, nc))

    barrier = pltpu.get_barrier_semaphore()

    def greet(k, carry):
        pl.semaphore_signal(barrier, inc=1, device_id=device(lax.bitwise_xor(me, k)), device_id_type=MESH)
        return carry

    lax.fori_loop(1, count, greet, 0)
    pl.semaphore_wait(barrier, count - 1)

    def pack(d, carry):
        for slot in range(2):
            p = sidx[2 * d + slot]
            sent[d, 2 * slot] = pm[p, :HALF]
            sent[d, 2 * slot + 1] = pm[p, HALF:]
            tag = jnp.full((1, LANES), slot_of[2 * d + slot].astype(jnp.float32), jnp.float32)
            sent[d, 2 * slot, MARK : MARK + 1, :] = tag
        return carry

    lax.fori_loop(0, count, pack, 0)

    def copy(k):
        d = lax.bitwise_xor(me, k)
        return pltpu.make_async_remote_copy(
            src_ref=sent.at[d], dst_ref=got_ref.at[pl.ds(4 * me, 4)], send_sem=send_sem.at[k],
            recv_sem=recv_sem.at[k], device_id=device(d), device_id_type=MESH)

    def post(k, carry):
        copy(k).start()
        return carry

    def finish(k, carry):
        copy(k).wait()
        return carry

    lax.fori_loop(1, count, post, 0)
    for i in range(4):
        got_ref[4 * me + i] = sent[me, i]
    lax.fori_loop(1, count, finish, 0)
    source = lax.broadcasted_iota(jnp.int32, (4 * count, LANES), 0)
    wanted = lax.broadcasted_iota(jnp.int32, (4 * count, LANES), 1).astype(jnp.float32)
    hit = (got_ref[:, MARK, :] == wanted) & (source % 2 == 0)
    index = jnp.sum(jnp.where(hit, source, 0), axis=0, keepdims=True)
    table_ref[...] = jnp.broadcast_to(index, table_ref.shape)


def unpack_kernel(ridx, got_ref, out_ref):
    for t in range(out_ref.shape[1]):
        base = ridx[0, t]
        for tile in range(TILES):
            block = got_ref.at[base + half_of(tile)]
            lanes = slice(tile * LANES, (tile + 1) * LANES)
            low = low_row(0, tile)
            out_ref[:MAIN, t, lanes] = block[low : low + MAIN, :]
            low = low_row(MAIN, tile)
            out_ref[MAIN:, t, lanes] = block[2 * MAIN :, :][low - 2 * MAIN : low - 2 * MAIN + TAIL]


def body(nb, nc, f_home, levels, plan):
    devices = nb * nc
    patches = f_home.shape[0]
    vmem = pl.BlockSpec(memory_space=pltpu.VMEM)
    smem = pl.BlockSpec(memory_space=pltpu.SMEM)
    state = (19, SPAN_PATCHES, 8, CELLS)
    small = (SPAN_PATCHES, 8, LANES)
    f32 = jnp.float32
    dma = pltpu.SemaphoreType.DMA
    half = (HALF, LANES)
    quarter = (QUARTER, LANES)
    rounds = max(2 * STEPS, (nb - 1).bit_length())
    limit = pltpu.CompilerParams(collective_id=0, has_side_effects=True, vmem_limit_bytes=60 * 1024 * 1024)
    got, packed, table = pl.pallas_call(
        lambda *refs: lattice_kernel(nb, nc, *refs),
        out_shape=(
            jax.ShapeDtypeStruct((2 * devices + 2 * devices // GROUP,) + half, f32),
            jax.ShapeDtypeStruct((patches, 2 * HALF, LANES), f32),
            jax.ShapeDtypeStruct((8, LANES), jnp.int32),
        ),
        in_specs=[smem, vmem, vmem],
        out_specs=(vmem, vmem, vmem),
        scratch_shapes=[
            pltpu.VMEM(state, f32),
            pltpu.VMEM(state, f32),
            pltpu.VMEM((18,) + state[1:], f32),
            pltpu.VMEM((2, devices) + half, f32),
            pltpu.VMEM((2, devices) + half, f32),
            pltpu.VMEM((2, devices) + half, f32),
            pltpu.VMEM((devices,) + quarter, f32),
            pltpu.VMEM((devices,) + quarter, f32),
            pltpu.VMEM((devices,) + quarter, f32),
            pltpu.VMEM((devices,) + quarter, f32),
            pltpu.VMEM((devices,) + quarter, f32),
            pltpu.VMEM(small, f32),
            pltpu.VMEM((8, LANES), f32),
            pltpu.VMEM((3 * nc - 1, 8, LANES), f32),
            pltpu.VMEM((STEPS, 2, 5, 8, CELLS), f32),
            pltpu.VMEM((STEPS, 2, 5, 8, CELLS), f32),
            pltpu.VMEM((STEPS, 2, 5, 2, 8, LANES), f32),
            pltpu.VMEM((STEPS, 2, 5, 2, 8, LANES), f32),
            pltpu.VMEM((STEPS, len(DIAGONAL), 8, LANES), f32),
            pltpu.VMEM((STEPS, len(DIAGONAL), 8, LANES), f32),
            pltpu.VMEM((devices, LANES), jnp.int32),
            pltpu.SMEM((devices, LANES), jnp.int32),
            pltpu.VMEM((2, devices, LANES), f32),
            dma((STEPS, 8)),
            dma((STEPS, 8)),
            dma((3 * nc - 1,)),
            dma((3 * nc - 1,)),
            dma((2, devices)),
            dma((2, devices)),
            dma((devices,)),
            dma((devices,)),
            dma((2, devices // GROUP)),
            dma((2, devices // GROUP)),
            dma((devices // GROUP,)),
            dma((devices // GROUP,)),
            dma,
            pltpu.SemaphoreType.REGULAR((rounds,)),
            pltpu.SemaphoreType.REGULAR((rounds,)),
        ],
        compiler_params=limit,
    )(levels, plan[None, :], jnp.transpose(f_home, (1, 0, 2)))

    def unpack(table, got):
        return pl.pallas_call(
            unpack_kernel,
            out_shape=jax.ShapeDtypeStruct((19, patches, CELLS), f32),
            in_specs=[smem, vmem],
            out_specs=vmem,
            compiler_params=pltpu.CompilerParams(vmem_limit_bytes=40 * 1024 * 1024),
        )(table, got)

    def in_full(table, got, packed, plan):
        target = plan // patches
        order = jnp.arange(patches, dtype=jnp.int32)
        earlier = (target[:, None] == target[None, :]) & (order[None, :] < order[:, None])
        place = 2 * target + jnp.sum(earlier.astype(jnp.int32), axis=1)
        hit = place[None, :] == jnp.arange(2 * devices, dtype=jnp.int32)[:, None]
        sidx = jnp.sum(jnp.where(hit, order[None, :], 0), axis=1)
        slot_of = jnp.sum(jnp.where(hit, plan[None, :] % patches + 1, 0), axis=1) - 1
        got, table = pl.pallas_call(
            lambda *refs: full_kernel(nb, nc, *refs),
            out_shape=(
                jax.ShapeDtypeStruct((4 * devices,) + half, f32),
                jax.ShapeDtypeStruct((8, LANES), jnp.int32),
            ),
            in_specs=[smem, smem, vmem],
            out_specs=(vmem, vmem),
            scratch_shapes=[
                pltpu.VMEM((devices, 4) + half, f32), dma((devices,)), dma((devices,))
            ],
            compiler_params=pltpu.CompilerParams(collective_id=1, has_side_effects=True,
                                                 vmem_limit_bytes=48 * 1024 * 1024),
        )(sidx, slot_of, packed)
        return unpack(table, got)

    out = lax.cond(table[1, 0] > 0, in_full, lambda table, got, packed, plan: unpack(table, got),
                   table, got, packed, plan)
    return jnp.transpose(out, (1, 0, 2))


def solution(mesh):
    nb, nc = mesh.shape["blocks"], mesh.shape["cross"]
    in_specs = (P(("blocks", "cross"), None, None), P(("blocks", "cross")), P(("blocks", "cross")))
    out_specs = P(("blocks", "cross"), None, None)
    return jax.shard_map(
        lambda f, l, p: body(nb, nc, f, l, p),
        mesh=mesh, in_specs=in_specs, out_specs=out_specs, check_vma=False)
```

```python
import jax
import jax.numpy as jnp
from jax import lax
from jax.experimental import pallas as pl
from jax.experimental.pallas import tpu as pltpu
from jax.sharding import PartitionSpec as P

SPAN_PATCHES = 4
DEPTH_PATCHES = 8
STEPS = 2
CELLS = 512
VELOCITIES = (
    (0, 0, 0),
    (1, 0, 0),
    (-1, 0, 0),
    (0, 1, 0),
    (0, -1, 0),
    (0, 0, 1),
    (0, 0, -1),
    (1, 1, 0),
    (-1, -1, 0),
    (1, -1, 0),
    (-1, 1, 0),
    (1, 0, 1),
    (-1, 0, -1),
    (1, 0, -1),
    (-1, 0, 1),
    (0, 1, 1),
    (0, -1, -1),
    (0, 1, -1),
    (0, -1, 1),
)
WEIGHTS = (1.0 / 3.0,) + (1.0 / 18.0,) * 6 + (1.0 / 36.0,) * 12
TAU_COARSE = 0.55
TAU_FINE = 2.0 * TAU_COARSE - 0.5
RESCALE = TAU_FINE / (2.0 * TAU_COARSE)
INFLOW = 0.08
MESH = pl.DeviceIdType.MESH
MAIN = 16
TAIL = 3
HALF = 40
MARK = 38
FIRST = 39
QUARTER = 20
TAG = 19
OVER = 1000.0
GROUP = 4
LANES = 128
TILES = CELLS // LANES
Y_UP = [q for q in range(19) if VELOCITIES[q][1] == 1]
Y_DOWN = [q for q in range(19) if VELOCITIES[q][1] == -1]
X_UP = [q for q in range(19) if VELOCITIES[q][0] == 1]
X_DOWN = [q for q in range(19) if VELOCITIES[q][0] == -1]
DIAGONAL = [q for q in range(19) if VELOCITIES[q][0] and VELOCITIES[q][1]]


def relax_into(load, store, coef):
    f = [load(q) for q in range(19)]
    terms = list(f)
    while len(terms) > 1:
        pairs = [a + b for a, b in zip(terms[::2], terms[1::2])]
        terms = pairs + ([terms[-1]] if len(terms) % 2 else [])
    rho = terms[0]
    inv = 1.0 / rho
    u = []
    for axis in range(3):
        up = [f[q] for q in range(19) if VELOCITIES[q][axis] == 1]
        down = [f[q] for q in range(19) if VELOCITIES[q][axis] == -1]
        d = [a - b for a, b in zip(up, down)]
        u.append((((d[0] + d[1]) + (d[2] + d[3])) + d[4]) * inv)
    base = 1.0 - 1.5 * (u[0] * u[0] + u[1] * u[1] + u[2] * u[2])
    scaled = {w: w * rho for w in set(WEIGHTS)}
    for q in range(19):
        along = None
        for axis in range(3):
            e = VELOCITIES[q][axis]
            if e:
                term = u[axis] if e == 1 else -u[axis]
                along = term if along is None else along + term
        poly = base if along is None else base + along * (3.0 + 4.5 * along)
        balance = scaled[WEIGHTS[q]] * poly
        store(q, balance + coef(q) * (f[q] - balance))


def half_of(tile):
    return 1 if tile in (0, TILES - 1) else 0


def place_of(tile):
    return tile // 2 if half_of(tile) else tile - 1


def low_row(q, tile):
    place = place_of(tile)
    return place * MAIN + q if q < MAIN else 2 * MAIN + place * TAIL + q - MAIN


def lattice_kernel(nb, nc, level, plan_ref, f_ref, got_ref, pm, table_ref, st, pb, pb2, cq, sent, second, theirs,
                   away, kept, across, extra, got_extra, own_ref, lev_ref, lv, ys, yr, xs, xr, ds, dr, pick, pick_s, tags, send_sem, recv_sem, lsend, lrecv, psend,
                   precv, esend, erecv, csend, crecv, qsend, qrecv, pick_sem, up_sem, down_sem):
    others = nb * nc - 1
    rounds = max(2 * STEPS, (nb - 1).bit_length())
    b = lax.axis_index("blocks")
    c = lax.axis_index("cross")

    def at(dx, dy):
        return (lax.rem(b + dx + nb, nb), lax.rem(c + dy + nc, nc))

    me = b * nc + c

    def peer(k):
        return lax.bitwise_xor(me, k)

    def device(d):
        return (d // nc, lax.rem(d, nc))

    barrier = pltpu.get_barrier_semaphore()
    above = b < nb - 1
    below = b > 0

    def signal(sem, to):
        pl.semaphore_signal(sem, inc=1, device_id=to, device_id_type=MESH)

    for k in range(1, nc):
        signal(barrier, at(0, k))
    for there, dx in ((above, 1), (below, -1)):
        @pl.when(there)
        def _():
            for k in range(nc):
                signal(barrier, at(dx, k))

    def tell(k):
        hop = lax.shift_left(jnp.int32(1), jnp.int32(k))

        @pl.when(b + hop < nb)
        def _():
            signal(up_sem.at[k], (b + hop, c))

        @pl.when(b >= hop)
        def _():
            signal(down_sem.at[k], (b - hop, c))

    def hear(k):
        hop = lax.shift_left(jnp.int32(1), jnp.int32(k))

        @pl.when(b >= hop)
        def _():
            pl.semaphore_wait(up_sem.at[k], 1)

        @pl.when(b + hop < nb)
        def _():
            pl.semaphore_wait(down_sem.at[k], 1)

    patches = f_ref.shape[1]
    count = nb * nc
    target = lax.broadcasted_iota(jnp.int32, (count, patches), 0)
    where = jnp.broadcast_to(plan_ref[...], (count, patches))
    member = where // patches == target
    key = lax.broadcasted_iota(jnp.int32, (count, patches), 1) * patches + where % patches
    low_key = jnp.min(jnp.where(member, key, patches * patches), axis=1, keepdims=True)
    high_key = jnp.max(jnp.where(member, key, -1), axis=1, keepdims=True)
    some = high_key >= 0
    two = high_key > low_key
    column = lax.broadcasted_iota(jnp.int32, (count, LANES), 1)
    pick[...] = jnp.where(column == 0, jnp.where(some, low_key // patches, 0),
                          jnp.where(two, high_key // patches, 0))
    to_scalars = pltpu.make_async_copy(pick, pick_s, pick_sem)
    to_scalars.start()
    tags[0] = jnp.broadcast_to(jnp.where(some, low_key % patches, -1), (count, LANES)).astype(jnp.float32)
    tags[1] = jnp.broadcast_to(jnp.where(two, high_key % patches, -1), (count, LANES)).astype(jnp.float32)

    slot = lax.broadcasted_iota(jnp.int32, (8, LANES), 0)
    slot = slot + 8 * lax.broadcasted_iota(jnp.int32, (8, LANES), 1)
    brief = jnp.zeros((8, LANES), jnp.float32)
    for p in range(SPAN_PATCHES * 8):
        brief = jnp.where(slot == p, level[p].astype(jnp.float32), brief)
    lev_ref[...] = brief

    def spread(values, r):
        return jnp.broadcast_to(values[:, r : r + 1], (8, LANES))[None]

    own = jnp.concatenate([spread(brief, r) for r in range(SPAN_PATCHES)], axis=0)
    own_ref[...] = own
    for q in range(19):
        for r in range(SPAN_PATCHES):
            st[q, r] = f_ref[q, r * 8 : r * 8 + 8, :]
    gain = jnp.where(own > 0.5, (1.0 - 1.0 / TAU_FINE) / RESCALE, 1.0 - 1.0 / TAU_COARSE)
    lane = lax.broadcasted_iota(jnp.int32, (SPAN_PATCHES, 8, LANES), 2)
    lower = lane < 64
    half = lax.broadcasted_iota(jnp.int32, (2, 8, LANES), 2) < 64
    fine = own > 0.5
    in_tile = {
        (axis, e): (lane // 8 % 8 if axis == 1 else lane % 8) == (0 if e == 1 else 7)
        for axis in (1, 2) for e in (1, -1)
    }
    around = [(dx, dy) for dx in (-1, 0, 1) for dy in range(nc) if (dx, dy) != (0, 0)]

    def targets(far):
        scales = {}
        for dx in (-1, 0, 1):
            rows = [spread(far(dx, nc - 1), SPAN_PATCHES - 1)]
            rows += [own[r][None] if dx == 0 else spread(far(dx, 0), r) for r in range(SPAN_PATCHES)]
            rows += [spread(far(dx, 1 % nc), 0)]
            rows = [jnp.where(value > 0.5, RESCALE, 1.0) for value in rows]
            for dy in (-1, 0, 1):
                value = jnp.concatenate(rows[1 + dy : 1 + dy + SPAN_PATCHES], axis=0)
                for dz in (-1, 0, 1):
                    scales[dx, dy, dz] = pltpu.roll(value, (-dz) % 8, axis=1) if dz else value
        return scales

    def coefficient(q, tile, scales, rows):
        e = VELOCITIES[q]
        kinds = [{}]
        for axis in range(3):
            if e[axis] and (axis or tile == (TILES - 1 if e[0] == 1 else 0)):
                kinds = [{**k, axis: v} for k in kinds for v in (0, 1)]
        result = None
        for k in kinds:
            value = scales[tuple(e[a] * k.get(a, 0) for a in range(3))][rows]
            mask = None
            for axis, on in k.items():
                if on:
                    hit = in_tile[axis, -e[axis]] if axis else (~lower if e[0] == 1 else lower)
                    mask = hit[rows] if mask is None else mask & hit[rows]
            result = value if result is None else jnp.where(mask, value, result)
        return gain[rows] * result

    def lanes_of(tile):
        return slice(tile * LANES, (tile + 1) * LANES)

    everything = slice(0, SPAN_PATCHES)
    scales = targets(lambda dx, dy: jnp.zeros((8, LANES), jnp.float32))
    for q in range(1, 19):
        for tile in range(TILES):
            cq[q - 1, :, :, lanes_of(tile)] = coefficient(q, tile, scales, everything)

    def first(r, tiles):
        plain = jnp.where(own_ref[r] > 0.5, 1.0 - 1.0 / TAU_FINE, 1.0 - 1.0 / TAU_COARSE)
        for tile in tiles:
            lanes = lanes_of(tile)

            def put(q, value):
                pb[q, r, :, lanes] = value

            relax_into(lambda q: st[q, r, :, lanes], put,
                       lambda q: cq[q - 1, r, :, lanes] if q else plain)

    def first_rows(tiles, start, stop, stride=1):
        def one(n, carry):
            first(start + stride * n, tiles)
            return carry

        lax.fori_loop(0, (stop - start + stride - 1) // stride, one, 0)

    end_tiles = (0, TILES - 1)
    middle_tiles = tuple(range(1, TILES - 1))
    first_rows(end_tiles, 0, SPAN_PATCHES)
    first_rows(middle_tiles, 0, SPAN_PATCHES)
    pl.semaphore_wait(barrier, nc - 1 + nc * (jnp.where(above, 1, 0) + jnp.where(below, 1, 0)))
    tell(0)

    def start_to(there, copy):
        if there is None:
            copy.start()
        else:
            pl.when(there)(copy.start)

    def wait_for(outgoing, incoming, copy):
        if outgoing is None:
            copy.wait()
        else:
            pl.when(outgoing)(copy.wait_send)
            pl.when(incoming)(copy.wait_recv)

    def ends_of(dx):
        return {0: (None, None), 1: (above, below), -1: (below, above)}[dx]

    level_copies = []
    for n, (dx, dy) in enumerate(around):
        copy = pltpu.make_async_remote_copy(
            src_ref=lev_ref, dst_ref=lv.at[n], send_sem=lsend.at[n], recv_sem=lrecv.at[n],
            device_id=at(-dx, -dy), device_id_type=MESH)
        outgoing, incoming = ends_of(-dx)
        start_to(outgoing, copy)
        level_copies.append((outgoing, incoming, copy))

    def patch_copy(half, k):
        d = peer(k)
        rows = slice(0, MARK if half else FIRST)
        return pltpu.make_async_remote_copy(
            src_ref=sent.at[half, d, rows], dst_ref=got_ref.at[2 * me + half, rows],
            send_sem=psend.at[half, k], recv_sem=precv.at[half, k], device_id=device(d),
            device_id_type=MESH)

    def extra_copy(k):
        d = peer(k)
        return pltpu.make_async_remote_copy(
            src_ref=extra.at[d], dst_ref=got_extra.at[me], send_sem=esend.at[k],
            recv_sem=erecv.at[k], device_id=device(d), device_id_type=MESH)

    for copy in level_copies:
        wait_for(*copy)
    scales = targets(lambda dx, dy: lv[around.index((dx, dy))])

    def amend(q, tile, rows):
        spot = (rows, slice(0, 8), lanes_of(tile))
        before = cq[(q - 1,) + spot]
        after = coefficient(q, tile, scales, rows)
        held = pb[(q,) + spot]
        pb[(q,) + spot] = held + (after - before) / (1.0 - before) * (st[(q,) + spot] - held)
        cq[(q - 1,) + spot] = after

    for q in range(1, 19):
        e = VELOCITIES[q]
        outer_tile = {0: None, 1: TILES - 1, -1: 0}[e[0]]
        if e[0]:
            amend(q, outer_tile, everything)
        if e[1]:
            r = SPAN_PATCHES - 1 if e[1] == 1 else 0
            for tile in range(TILES):
                if tile != outer_tile:
                    amend(q, tile, slice(r, r + 1))

    def spin(v, amount):
        return pltpu.roll(v, amount % LANES, axis=v.ndim - 1)

    def along_z(q, v, more=0):
        e = VELOCITIES[q][2]
        if not e:
            return spin(v, more) if more else v
        wrapped = pltpu.roll(spin(v, more - 7 * e), e % 8, axis=1)
        return jnp.where(in_tile[2, e][: v.shape[0]], wrapped, spin(v, more + e))

    def along_y(q, v, halo, more=0):
        e = VELOCITIES[q][1]
        moved = jnp.concatenate([halo, v[:-1]] if e == 1 else [v[1:], halo], axis=0)
        return jnp.where(in_tile[1, e], spin(moved, more - 56 * e), spin(v, more + 8 * e))

    def step(s, stage=None):
        copies = {"x": [], "y": []}

        def send(src, dst, n, dx, dy):
            copy = pltpu.make_async_remote_copy(
                src_ref=src, dst_ref=dst, send_sem=send_sem.at[s, n], recv_sem=recv_sem.at[s, n],
                device_id=at(dx, dy), device_id_type=MESH)
            outgoing, incoming = ends_of(dx)
            start_to(outgoing, copy)
            copies["x" if dx else "y"].append((outgoing, incoming, copy))

        def send_x():
            for way, e, group in ((0, 1, X_UP), (1, -1, X_DOWN)):
                for n, q in enumerate(group):
                    v = along_z(q, pb[q, :, :, lanes_of(TILES - 1 if e == 1 else 0)])
                    turned = spin(v, 64)
                    if e == 1:
                        xs[s, way, n] = jnp.where(half, turned[:2], v[2:])
                    else:
                        xs[s, way, n] = jnp.where(half, v[:2], turned[2:])
                    if q in DIAGONAL:
                        ds[s, DIAGONAL.index(q)] = turned[SPAN_PATCHES - 1 if VELOCITIES[q][1] == 1 else 0]
            for way, dx in ((0, 1), (1, -1)):
                send(xs.at[s, way], xr.at[s, way], 2 + way, dx, 0)
            for n, q in enumerate(DIAGONAL):
                send(ds.at[s, n], dr.at[s, n], 4 + n, *VELOCITIES[q][:2])

        def send_y():
            for way, e, group in ((0, 1, Y_UP), (1, -1, Y_DOWN)):
                r = SPAN_PATCHES - 1 if e == 1 else 0
                for n, q in enumerate(group):
                    for tile in range(TILES):
                        ys[s, way, n, :, lanes_of(tile)] = along_z(q, pb[q, r : r + 1, :, lanes_of(tile)])[0]
            for way, dy in ((0, 1), (1, -1)):
                send(ys.at[s, way], yr.at[s, way], way, 0, dy)

        if s == 0:
            send_x()
            send_y()
        elif stage is None:
            first_rows(end_tiles, 0, SPAN_PATCHES)
            send_x()
            send_y()
        else:
            first_rows(end_tiles, 0, SPAN_PATCHES, SPAN_PATCHES - 1)
            send_y()
            first_rows(end_tiles, 1, SPAN_PATCHES - 1)
            send_x()

        def shift(q):
            e = VELOCITIES[q]
            half_turn = 64 if e[0] else 0
            tiles = [along_z(q, pb[q, :, :, lanes_of(tile)], 0 if e[1] else half_turn) for tile in range(TILES)]
            if e[1]:
                way, group = (0, Y_UP) if e[1] == 1 else (1, Y_DOWN)
                n = group.index(q)
                tiles = [along_y(q, v, yr[s, way, n, :, lanes_of(tile)][None], half_turn)
                         for tile, v in enumerate(tiles)]
            if e[0]:
                turned = list(tiles)
                for tile in range(TILES):
                    if e[0] == 1:
                        tiles[tile] = jnp.where(lower, turned[tile - 1], turned[tile])
                    else:
                        tiles[tile] = jnp.where(lower, turned[tile], turned[(tile + 1) % TILES])
            for tile in range(TILES):
                st[q, :, :, lanes_of(tile)] = tiles[tile]

        for q in range(19):
            if not VELOCITIES[q][1]:
                shift(q)
        for copy in copies["y"]:
            wait_for(*copy)
        hear(2 * s)
        tell(2 * s + 1)
        for q in range(19):
            if VELOCITIES[q][1]:
                shift(q)

        def again(r, tiles):
            for tile in tiles:
                lanes = lanes_of(tile)

                def put(q, value):
                    pb2[q, r, :, lanes] = value

                relax_into(lambda q: st[q, r, :, lanes], put, lambda q: 1.0 - 1.0 / TAU_FINE)

        def settle(tiles):
            for q in range(19):
                e = VELOCITIES[q]
                amount = 64 * e[0] + 8 * e[1] + e[2]
                inside = fine
                for axis in (1, 2):
                    if e[axis]:
                        inside = inside & ~in_tile[axis, e[axis]]
                turned = {}

                def moved_from(tile):
                    if tile not in turned:
                        v = pb2[q, :, :, lanes_of(tile)]
                        turned[tile] = spin(v, amount) if amount else v
                    return turned[tile]

                for tile in tiles:
                    take = inside
                    value = moved_from(tile)
                    if e[0] == 1:
                        value = jnp.where(lower, moved_from((tile - 1) % TILES), value)
                        take = take & ~lower if tile == 0 else take
                    elif e[0] == -1:
                        value = jnp.where(lower, value, moved_from((tile + 1) % TILES))
                        take = take & lower if tile == TILES - 1 else take
                    lanes = lanes_of(tile)
                    st[q, :, :, lanes] = jnp.where(take, value, st[q, :, :, lanes])

        def middle(r, carry):
            again(r, range(1, TILES - 1))
            return carry

        def ends(r, carry):
            again(r, (0, TILES - 1))
            return carry

        lax.fori_loop(0, SPAN_PATCHES, middle, 0)
        lax.fori_loop(0, SPAN_PATCHES, ends, 0)
        settle(middle_tiles)
        if stage is None:
            first_rows(middle_tiles, 0, SPAN_PATCHES)
        else:
            stage()
        for copy in copies["x"]:
            wait_for(*copy)
        if stage is None:
            hear(2 * s + 1)
            tell(2 * s + 2)
        for way, e, group in ((0, 1, X_UP), (1, -1, X_DOWN)):
            outside = b == (0 if e == 1 else nb - 1)
            for n, q in enumerate(group):
                h = xr[s, way, n]
                turned = spin(h, 64)
                halo = jnp.concatenate([h, turned] if e == 1 else [turned, h], axis=0)
                if q in DIAGONAL:
                    halo = along_y(q, halo, dr[s, DIAGONAL.index(q)][None])
                along = e * INFLOW
                const = WEIGHTS[q] * (1.0 + 3.0 * along + 4.5 * along * along - 1.5 * INFLOW * INFLOW)
                halo = jnp.where(outside, jnp.full(halo.shape, const, jnp.float32), halo)
                lanes = lanes_of(0 if e == 1 else TILES - 1)
                keep = st[q, :, :, lanes]
                st[q, :, :, lanes] = jnp.where(lower, halo, keep) if e == 1 else jnp.where(lower, keep, halo)

        lax.fori_loop(0, SPAN_PATCHES, ends, 0)
        settle(end_tiles)

    flat = pm.reshape(pm.shape[0] * 2 * HALF, LANES)

    def fill(half):
        pm[:, half * HALF + 2 * MAIN : (half + 1) * HALF, :] = jnp.zeros(
            (pm.shape[0], HALF - 2 * MAIN, LANES), jnp.float32)
        for q in range(19):
            for r in range(SPAN_PATCHES):
                for tile in range(TILES):
                    if half_of(tile) == half:
                        row = r * 8 * 2 * HALF + half * HALF + low_row(q, tile)
                        flat[pl.ds(row, 8, stride=2 * HALF), :] = st[q, r, :, lanes_of(tile)]

    part = lax.rem(me, GROUP)
    base = me - part
    far_chip = part // nc
    chunks = count // GROUP

    def chunk_at(j):
        return lax.rem(j + chunks // 2, chunks)

    def rows_of(j):
        return pl.ds(chunk_at(j) * GROUP, GROUP)

    def swap_copy(half, j):
        return pltpu.make_async_remote_copy(
            src_ref=second.at[half, rows_of(j)], dst_ref=theirs.at[half, rows_of(j)],
            send_sem=csend.at[half, j], recv_sem=crecv.at[half, j], device_id=at(0, 1),
            device_id_type=MESH)

    def shuffle_copy(j):
        return pltpu.make_async_remote_copy(
            src_ref=away.at[rows_of(j)], dst_ref=across.at[rows_of(j)], send_sem=qsend.at[j],
            recv_sem=qrecv.at[j], device_id=device(lax.bitwise_xor(me, nc)), device_id_type=MESH)

    def tag_of(which, d):
        return tags[which, pl.ds(d, 1), :]

    def offer(half):
        def pack_second(j, carry):
            for i in range(GROUP):
                m = chunk_at(j) * GROUP + i
                d = lax.bitwise_xor(base, m)
                second[half, m] = pm[pick_s[d, 1], half * HALF : (half + 1) * HALF]
                if half == 0:
                    second[0, m, MARK : MARK + 1, :] = tag_of(1, d)
                    second[0, m, FIRST : FIRST + 1, :] = tag_of(0, d)

            @pl.when(j > 0)
            def _():
                swap_copy(half, j - 1).start()

            return carry

        lax.fori_loop(0, chunks, pack_second, 0)
        swap_copy(half, chunks - 1).start()

    zero = c == 0

    def pack_quarters(d, m, my_second, their_second, their_first, own):
        mine_extra = (my_second > -0.5) & (their_first > -0.5)
        their_extra = (their_second > -0.5) & own
        use_mine = mine_extra & (zero | ~their_extra)
        tag = jnp.where(use_mine, my_second, jnp.where(their_extra, their_second, -1.0))
        tag = jnp.where(mine_extra & their_extra, OVER, tag)
        p = pick_s[d, 1]
        for ref, t in ((kept, part), (away, lax.bitwise_xor(part, nc))):
            half = lax.rem(t, 2)
            place = t // 2
            top = pl.multiple_of(place * MAIN, 8)
            my_top = pl.multiple_of(half * HALF + place * MAIN, 8)
            my_low = pl.multiple_of(half * HALF + 2 * MAIN, 8)
            ref[m, :MAIN, :] = jnp.where(
                use_mine, pm[p, pl.ds(my_top, MAIN), :], theirs[half, m, pl.ds(top, MAIN), :])
            low = jnp.where(use_mine, pm[p, pl.ds(my_low, 8), :], theirs[half, m, 2 * MAIN : HALF, :])
            low = jnp.where(place == 1, pltpu.roll(low, 8 - TAIL, axis=0), low)
            ref[m, MAIN : MAIN + TAIL, :] = low[:TAIL]
            ref[m, TAG : TAG + 1, :] = tag

    def pack_chunk(half, j):
        for i in range(GROUP):
            k = chunk_at(j) * GROUP + i
            d = peer(k)
            m = lax.bitwise_xor(k, part)
            my_first = tag_of(0, d)
            their_second = theirs[0, m, MARK : MARK + 1, :]
            own = my_first > -0.5
            sent[half, d] = jnp.where(
                own, pm[pick_s[d, 0], half * HALF : (half + 1) * HALF], theirs[half, m])
            if half == 0:
                sent[0, d, MARK : MARK + 1, :] = jnp.where(own, my_first, their_second)
            else:
                pack_quarters(d, m, tag_of(1, d), their_second, theirs[0, m, FIRST : FIRST + 1, :], own)

    def send_chunk(half, j):
        if half:
            shuffle_copy(j).start()
        for i in range(GROUP):
            k = chunk_at(j) * GROUP + i

            @pl.when(k > 0)
            def _():
                patch_copy(half, k).start()

    def exchange(half):
        def post(j, carry):
            swap_copy(half, j).wait_recv()
            pack_chunk(half, j)

            @pl.when(j > 0)
            def _():
                send_chunk(half, j - 1)

            return carry

        lax.fori_loop(0, chunks, post, 0)
        send_chunk(half, chunks - 1)
        got_ref[2 * me + half] = sent[half, me]

    def early():
        fill(0)
        to_scalars.wait()
        offer(0)
        for k in range(2 * STEPS - 1, rounds):
            if k > 2 * STEPS - 1:
                tell(k)
            hear(k)
        exchange(0)

    for s in range(STEPS):
        step(s, early if s == STEPS - 1 else None)
    fill(1)
    offer(1)
    exchange(1)

    def swapped(j, carry):
        swap_copy(0, j).wait_send()
        swap_copy(1, j).wait_send()
        shuffle_copy(j).wait()
        return carry

    lax.fori_loop(0, chunks, swapped, 0)
    near_tags = kept[:, TAG, :]
    far_tags = across[:, TAG, :]
    over = (near_tags > OVER / 2) | (far_tags > OVER / 2) | ((near_tags > -0.5) & (far_tags > -0.5))
    flag = jnp.max(jnp.where(over, OVER, 0.0), axis=0, keepdims=True)

    def pack_extra(d):
        m = lax.bitwise_xor(base, d)
        mine = kept[m]
        other = across[m]
        keep = ((mine[TAG:] > -0.5) & (far_chip == 0)) | ~(other[TAG:] > -0.5)
        extra[d] = jnp.where(keep, mine, other)
        extra[d, TAG : TAG + 1, :] = jnp.where(keep, mine[TAG:], other[TAG:]) + flag

    def mask_at(i):
        return lax.rem(i + count // 2, count)

    def post_extra(i, carry):
        pack_extra(peer(mask_at(i)))

        @pl.when((i > 0) & (mask_at(i - 1) > 0))
        def _():
            extra_copy(mask_at(i - 1)).start()

        return carry

    lax.fori_loop(0, count, post_extra, 0)
    extra_copy(mask_at(count - 1)).start()
    got_extra[me] = extra[me]

    def finish(k, carry):
        patch_copy(0, k).wait()
        patch_copy(1, k).wait()
        extra_copy(k).wait()
        return carry

    lax.fori_loop(1, count, finish, 0)

    def assemble(g, carry):
        for t in range(TILES):
            whole = got_ref.at[2 * count + 2 * g + t % 2]
            block = got_extra.at[g * GROUP + t]
            whole[t // 2 * MAIN : (t // 2 + 1) * MAIN, :] = block[:MAIN, :]
            low = 2 * MAIN + t // 2 * TAIL
            whole[low : low + TAIL, :] = block[MAIN : MAIN + TAIL, :]
        return carry

    lax.fori_loop(0, chunks, assemble, 0)
    source = lax.broadcasted_iota(jnp.int32, (2 * count, LANES), 0)
    wanted = lax.broadcasted_iota(jnp.int32, (2 * count, LANES), 1).astype(jnp.float32)
    first_hit = (got_ref[: 2 * count, MARK, :] == wanted) & (source % 2 == 0)
    index = jnp.sum(jnp.where(first_hit, source, 0), axis=0, keepdims=True)
    source = source[:count]
    extra_tags = got_extra[:, TAG, :]
    extra_hit = (extra_tags == wanted[:count]) & (source % GROUP == 0)
    place = source // GROUP * 2 + 2 * count
    index = index + jnp.sum(jnp.where(extra_hit, place, 0), axis=0, keepdims=True)
    over = jnp.max(extra_tags, axis=0, keepdims=True)
    row = lax.broadcasted_iota(jnp.int32, (8, LANES), 0)
    table_ref[...] = jnp.where(row == 0, index, jnp.where(over > OVER / 2, 1, 0))


def full_kernel(nb, nc, sidx, slot_of, pm, got_ref, table_ref, sent, send_sem, recv_sem):
    count = nb * nc
    me = lax.axis_index("blocks") * nc + lax.axis_index("cross")

    def device(d):
        return (d // nc, lax.rem(d, nc))

    barrier = pltpu.get_barrier_semaphore()

    def greet(k, carry):
        pl.semaphore_signal(barrier, inc=1, device_id=device(lax.bitwise_xor(me, k)), device_id_type=MESH)
        return carry

    lax.fori_loop(1, count, greet, 0)
    pl.semaphore_wait(barrier, count - 1)

    def pack(d, carry):
        for slot in range(2):
            p = sidx[2 * d + slot]
            sent[d, 2 * slot] = pm[p, :HALF]
            sent[d, 2 * slot + 1] = pm[p, HALF:]
            tag = jnp.full((1, LANES), slot_of[2 * d + slot].astype(jnp.float32), jnp.float32)
            sent[d, 2 * slot, MARK : MARK + 1, :] = tag
        return carry

    lax.fori_loop(0, count, pack, 0)

    def copy(k):
        d = lax.bitwise_xor(me, k)
        return pltpu.make_async_remote_copy(
            src_ref=sent.at[d], dst_ref=got_ref.at[pl.ds(4 * me, 4)], send_sem=send_sem.at[k],
            recv_sem=recv_sem.at[k], device_id=device(d), device_id_type=MESH)

    def post(k, carry):
        copy(k).start()
        return carry

    def finish(k, carry):
        copy(k).wait()
        return carry

    lax.fori_loop(1, count, post, 0)
    for i in range(4):
        got_ref[4 * me + i] = sent[me, i]
    lax.fori_loop(1, count, finish, 0)
    source = lax.broadcasted_iota(jnp.int32, (4 * count, LANES), 0)
    wanted = lax.broadcasted_iota(jnp.int32, (4 * count, LANES), 1).astype(jnp.float32)
    hit = (got_ref[:, MARK, :] == wanted) & (source % 2 == 0)
    index = jnp.sum(jnp.where(hit, source, 0), axis=0, keepdims=True)
    table_ref[...] = jnp.broadcast_to(index, table_ref.shape)


def unpack_kernel(ridx, got_ref, out_ref):
    for t in range(out_ref.shape[1]):
        base = ridx[0, t]
        for tile in range(TILES):
            block = got_ref.at[base + half_of(tile)]
            lanes = slice(tile * LANES, (tile + 1) * LANES)
            low = low_row(0, tile)
            out_ref[:MAIN, t, lanes] = block[low : low + MAIN, :]
            low = low_row(MAIN, tile)
            out_ref[MAIN:, t, lanes] = block[2 * MAIN :, :][low - 2 * MAIN : low - 2 * MAIN + TAIL]


def body(nb, nc, f_home, levels, plan):
    devices = nb * nc
    patches = f_home.shape[0]
    vmem = pl.BlockSpec(memory_space=pltpu.VMEM)
    smem = pl.BlockSpec(memory_space=pltpu.SMEM)
    state = (19, SPAN_PATCHES, 8, CELLS)
    small = (SPAN_PATCHES, 8, LANES)
    f32 = jnp.float32
    dma = pltpu.SemaphoreType.DMA
    half = (HALF, LANES)
    quarter = (QUARTER, LANES)
    rounds = max(2 * STEPS, (nb - 1).bit_length())
    limit = pltpu.CompilerParams(collective_id=0, has_side_effects=True, vmem_limit_bytes=60 * 1024 * 1024)
    got, packed, table = pl.pallas_call(
        lambda *refs: lattice_kernel(nb, nc, *refs),
        out_shape=(
            jax.ShapeDtypeStruct((2 * devices + 2 * devices // GROUP,) + half, f32),
            jax.ShapeDtypeStruct((patches, 2 * HALF, LANES), f32),
            jax.ShapeDtypeStruct((8, LANES), jnp.int32),
        ),
        in_specs=[smem, vmem, vmem],
        out_specs=(vmem, vmem, vmem),
        scratch_shapes=[
            pltpu.VMEM(state, f32),
            pltpu.VMEM(state, f32),
            pltpu.VMEM(state, f32),
            pltpu.VMEM((18,) + state[1:], f32),
            pltpu.VMEM((2, devices) + half, f32),
            pltpu.VMEM((2, devices) + half, f32),
            pltpu.VMEM((2, devices) + half, f32),
            pltpu.VMEM((devices,) + quarter, f32),
            pltpu.VMEM((devices,) + quarter, f32),
            pltpu.VMEM((devices,) + quarter, f32),
            pltpu.VMEM((devices,) + quarter, f32),
            pltpu.VMEM((devices,) + quarter, f32),
            pltpu.VMEM(small, f32),
            pltpu.VMEM((8, LANES), f32),
            pltpu.VMEM((3 * nc - 1, 8, LANES), f32),
            pltpu.VMEM((STEPS, 2, 5, 8, CELLS), f32),
            pltpu.VMEM((STEPS, 2, 5, 8, CELLS), f32),
            pltpu.VMEM((STEPS, 2, 5, 2, 8, LANES), f32),
            pltpu.VMEM((STEPS, 2, 5, 2, 8, LANES), f32),
            pltpu.VMEM((STEPS, len(DIAGONAL), 8, LANES), f32),
            pltpu.VMEM((STEPS, len(DIAGONAL), 8, LANES), f32),
            pltpu.VMEM((devices, LANES), jnp.int32),
            pltpu.SMEM((devices, LANES), jnp.int32),
            pltpu.VMEM((2, devices, LANES), f32),
            dma((STEPS, 8)),
            dma((STEPS, 8)),
            dma((3 * nc - 1,)),
            dma((3 * nc - 1,)),
            dma((2, devices)),
            dma((2, devices)),
            dma((devices,)),
            dma((devices,)),
            dma((2, devices // GROUP)),
            dma((2, devices // GROUP)),
            dma((devices // GROUP,)),
            dma((devices // GROUP,)),
            dma,
            pltpu.SemaphoreType.REGULAR((rounds,)),
            pltpu.SemaphoreType.REGULAR((rounds,)),
        ],
        compiler_params=limit,
    )(levels, plan[None, :], jnp.transpose(f_home, (1, 0, 2)))

    def unpack(table, got):
        return pl.pallas_call(
            unpack_kernel,
            out_shape=jax.ShapeDtypeStruct((19, patches, CELLS), f32),
            in_specs=[smem, vmem],
            out_specs=vmem,
            compiler_params=pltpu.CompilerParams(vmem_limit_bytes=40 * 1024 * 1024),
        )(table, got)

    def in_full(table, got, packed, plan):
        target = plan // patches
        order = jnp.arange(patches, dtype=jnp.int32)
        earlier = (target[:, None] == target[None, :]) & (order[None, :] < order[:, None])
        place = 2 * target + jnp.sum(earlier.astype(jnp.int32), axis=1)
        hit = place[None, :] == jnp.arange(2 * devices, dtype=jnp.int32)[:, None]
        sidx = jnp.sum(jnp.where(hit, order[None, :], 0), axis=1)
        slot_of = jnp.sum(jnp.where(hit, plan[None, :] % patches + 1, 0), axis=1) - 1
        got, table = pl.pallas_call(
            lambda *refs: full_kernel(nb, nc, *refs),
            out_shape=(
                jax.ShapeDtypeStruct((4 * devices,) + half, f32),
                jax.ShapeDtypeStruct((8, LANES), jnp.int32),
            ),
            in_specs=[smem, smem, vmem],
            out_specs=(vmem, vmem),
            scratch_shapes=[
                pltpu.VMEM((devices, 4) + half, f32), dma((devices,)), dma((devices,))
            ],
            compiler_params=pltpu.CompilerParams(collective_id=1, has_side_effects=True,
                                                 vmem_limit_bytes=48 * 1024 * 1024),
        )(sidx, slot_of, packed)
        return unpack(table, got)

    out = lax.cond(table[1, 0] > 0, in_full, lambda table, got, packed, plan: unpack(table, got),
                   table, got, packed, plan)
    return jnp.transpose(out, (1, 0, 2))


def solution(mesh):
    nb, nc = mesh.shape["blocks"], mesh.shape["cross"]
    in_specs = (P(("blocks", "cross"), None, None), P(("blocks", "cross")), P(("blocks", "cross")))
    out_specs = P(("blocks", "cross"), None, None)
    return jax.shard_map(
        lambda f, l, p: body(nb, nc, f, l, p),
        mesh=mesh, in_specs=in_specs, out_specs=out_specs, check_vma=False)
```

```python
import jax
import jax.numpy as jnp
from jax import lax
from jax.experimental import pallas as pl
from jax.experimental.pallas import tpu as pltpu
from jax.sharding import PartitionSpec as P

SPAN_PATCHES = 4
DEPTH_PATCHES = 8
STEPS = 2
CELLS = 512
VELOCITIES = (
    (0, 0, 0),
    (1, 0, 0),
    (-1, 0, 0),
    (0, 1, 0),
    (0, -1, 0),
    (0, 0, 1),
    (0, 0, -1),
    (1, 1, 0),
    (-1, -1, 0),
    (1, -1, 0),
    (-1, 1, 0),
    (1, 0, 1),
    (-1, 0, -1),
    (1, 0, -1),
    (-1, 0, 1),
    (0, 1, 1),
    (0, -1, -1),
    (0, 1, -1),
    (0, -1, 1),
)
WEIGHTS = (1.0 / 3.0,) + (1.0 / 18.0,) * 6 + (1.0 / 36.0,) * 12
TAU_COARSE = 0.55
TAU_FINE = 2.0 * TAU_COARSE - 0.5
RESCALE = TAU_FINE / (2.0 * TAU_COARSE)
INFLOW = 0.08
MESH = pl.DeviceIdType.MESH
MAIN = 16
TAIL = 3
HALF = 40
MARK = 38
FIRST = 39
QUARTER = 20
TAG = 19
OVER = 1000.0
GROUP = 4
LANES = 128
TILES = CELLS // LANES
Y_UP = [q for q in range(19) if VELOCITIES[q][1] == 1]
Y_DOWN = [q for q in range(19) if VELOCITIES[q][1] == -1]
X_UP = [q for q in range(19) if VELOCITIES[q][0] == 1]
X_DOWN = [q for q in range(19) if VELOCITIES[q][0] == -1]
DIAGONAL = [q for q in range(19) if VELOCITIES[q][0] and VELOCITIES[q][1]]


def relax_into(load, store, coef):
    f = [load(q) for q in range(19)]
    terms = list(f)
    while len(terms) > 1:
        pairs = [a + b for a, b in zip(terms[::2], terms[1::2])]
        terms = pairs + ([terms[-1]] if len(terms) % 2 else [])
    rho = terms[0]
    inv = 1.0 / rho
    u = []
    for axis in range(3):
        up = [f[q] for q in range(19) if VELOCITIES[q][axis] == 1]
        down = [f[q] for q in range(19) if VELOCITIES[q][axis] == -1]
        d = [a - b for a, b in zip(up, down)]
        u.append((((d[0] + d[1]) + (d[2] + d[3])) + d[4]) * inv)
    base = 1.0 - 1.5 * (u[0] * u[0] + u[1] * u[1] + u[2] * u[2])
    scaled = {w: w * rho for w in set(WEIGHTS)}
    for q in range(19):
        along = None
        for axis in range(3):
            e = VELOCITIES[q][axis]
            if e:
                term = u[axis] if e == 1 else -u[axis]
                along = term if along is None else along + term
        poly = base if along is None else base + along * (3.0 + 4.5 * along)
        balance = scaled[WEIGHTS[q]] * poly
        store(q, balance + coef(q) * (f[q] - balance))


def half_of(tile):
    return 1 if tile in (0, TILES - 1) else 0


def place_of(tile):
    return tile // 2 if half_of(tile) else tile - 1


def low_row(q, tile):
    place = place_of(tile)
    return place * MAIN + q if q < MAIN else 2 * MAIN + place * TAIL + q - MAIN


def lattice_kernel(nb, nc, level, plan_ref, f_ref, got_ref, pm, table_ref, st, pb, pb2, cq, sent, second, theirs,
                   away, kept, across, extra, got_extra, own_ref, lev_ref, lv, ys, yr, xs, xr, ds, dr, pick, pick_s, tags, send_sem, recv_sem, lsend, lrecv, psend,
                   precv, esend, erecv, csend, crecv, qsend, qrecv, pick_sem, up_sem, down_sem):
    others = nb * nc - 1
    rounds = max(2 * STEPS, (nb - 1).bit_length())
    b = lax.axis_index("blocks")
    c = lax.axis_index("cross")

    def at(dx, dy):
        return (lax.rem(b + dx + nb, nb), lax.rem(c + dy + nc, nc))

    me = b * nc + c

    def peer(k):
        return lax.bitwise_xor(me, k)

    def device(d):
        return (d // nc, lax.rem(d, nc))

    barrier = pltpu.get_barrier_semaphore()
    above = b < nb - 1
    below = b > 0

    def signal(sem, to):
        pl.semaphore_signal(sem, inc=1, device_id=to, device_id_type=MESH)

    for k in range(1, nc):
        signal(barrier, at(0, k))
    for there, dx in ((above, 1), (below, -1)):
        @pl.when(there)
        def _():
            for k in range(nc):
                signal(barrier, at(dx, k))

    def tell(k):
        hop = lax.shift_left(jnp.int32(1), jnp.int32(k))

        @pl.when(b + hop < nb)
        def _():
            signal(up_sem.at[k], (b + hop, c))

        @pl.when(b >= hop)
        def _():
            signal(down_sem.at[k], (b - hop, c))

    def hear(k):
        hop = lax.shift_left(jnp.int32(1), jnp.int32(k))

        @pl.when(b >= hop)
        def _():
            pl.semaphore_wait(up_sem.at[k], 1)

        @pl.when(b + hop < nb)
        def _():
            pl.semaphore_wait(down_sem.at[k], 1)

    patches = f_ref.shape[1]
    count = nb * nc
    target = lax.broadcasted_iota(jnp.int32, (count, patches), 0)
    where = jnp.broadcast_to(plan_ref[...], (count, patches))
    member = where // patches == target
    key = lax.broadcasted_iota(jnp.int32, (count, patches), 1) * patches + where % patches
    low_key = jnp.min(jnp.where(member, key, patches * patches), axis=1, keepdims=True)
    high_key = jnp.max(jnp.where(member, key, -1), axis=1, keepdims=True)
    some = high_key >= 0
    two = high_key > low_key
    column = lax.broadcasted_iota(jnp.int32, (count, LANES), 1)
    pick[...] = jnp.where(column == 0, jnp.where(some, low_key // patches, 0),
                          jnp.where(two, high_key // patches, 0))
    to_scalars = pltpu.make_async_copy(pick, pick_s, pick_sem)
    to_scalars.start()
    tags[0] = jnp.broadcast_to(jnp.where(some, low_key % patches, -1), (count, LANES)).astype(jnp.float32)
    tags[1] = jnp.broadcast_to(jnp.where(two, high_key % patches, -1), (count, LANES)).astype(jnp.float32)

    slot = lax.broadcasted_iota(jnp.int32, (8, LANES), 0)
    slot = slot + 8 * lax.broadcasted_iota(jnp.int32, (8, LANES), 1)
    brief = jnp.zeros((8, LANES), jnp.float32)
    for p in range(SPAN_PATCHES * 8):
        brief = jnp.where(slot == p, level[p].astype(jnp.float32), brief)
    lev_ref[...] = brief

    def spread(values, r):
        return jnp.broadcast_to(values[:, r : r + 1], (8, LANES))[None]

    own = jnp.concatenate([spread(brief, r) for r in range(SPAN_PATCHES)], axis=0)
    own_ref[...] = own
    for q in range(19):
        for r in range(SPAN_PATCHES):
            st[q, r] = f_ref[q, r * 8 : r * 8 + 8, :]
    gain = jnp.where(own > 0.5, (1.0 - 1.0 / TAU_FINE) / RESCALE, 1.0 - 1.0 / TAU_COARSE)
    lane = lax.broadcasted_iota(jnp.int32, (SPAN_PATCHES, 8, LANES), 2)
    lower = lane < 64
    half = lax.broadcasted_iota(jnp.int32, (2, 8, LANES), 2) < 64
    fine = own > 0.5
    in_tile = {
        (axis, e): (lane // 8 % 8 if axis == 1 else lane % 8) == (0 if e == 1 else 7)
        for axis in (1, 2) for e in (1, -1)
    }
    around = [(dx, dy) for dx in (-1, 0, 1) for dy in range(nc) if (dx, dy) != (0, 0)]

    def targets(far):
        scales = {}
        for dx in (-1, 0, 1):
            rows = [spread(far(dx, nc - 1), SPAN_PATCHES - 1)]
            rows += [own[r][None] if dx == 0 else spread(far(dx, 0), r) for r in range(SPAN_PATCHES)]
            rows += [spread(far(dx, 1 % nc), 0)]
            rows = [jnp.where(value > 0.5, RESCALE, 1.0) for value in rows]
            for dy in (-1, 0, 1):
                value = jnp.concatenate(rows[1 + dy : 1 + dy + SPAN_PATCHES], axis=0)
                for dz in (-1, 0, 1):
                    scales[dx, dy, dz] = pltpu.roll(value, (-dz) % 8, axis=1) if dz else value
        return scales

    def coefficient(q, tile, scales, rows):
        e = VELOCITIES[q]
        kinds = [{}]
        for axis in range(3):
            if e[axis] and (axis or tile == (TILES - 1 if e[0] == 1 else 0)):
                kinds = [{**k, axis: v} for k in kinds for v in (0, 1)]
        result = None
        for k in kinds:
            value = scales[tuple(e[a] * k.get(a, 0) for a in range(3))][rows]
            mask = None
            for axis, on in k.items():
                if on:
                    hit = in_tile[axis, -e[axis]] if axis else (~lower if e[0] == 1 else lower)
                    mask = hit[rows] if mask is None else mask & hit[rows]
            result = value if result is None else jnp.where(mask, value, result)
        return gain[rows] * result

    def lanes_of(tile):
        return slice(tile * LANES, (tile + 1) * LANES)

    everything = slice(0, SPAN_PATCHES)
    scales = targets(lambda dx, dy: jnp.zeros((8, LANES), jnp.float32))
    for q in range(1, 19):
        for tile in range(TILES):
            cq[q - 1, :, :, lanes_of(tile)] = coefficient(q, tile, scales, everything)

    def first(r, tiles):
        plain = jnp.where(own_ref[r] > 0.5, 1.0 - 1.0 / TAU_FINE, 1.0 - 1.0 / TAU_COARSE)
        for tile in tiles:
            lanes = lanes_of(tile)

            def put(q, value):
                pb[q, r, :, lanes] = value

            relax_into(lambda q: st[q, r, :, lanes], put,
                       lambda q: cq[q - 1, r, :, lanes] if q else plain)

    def first_rows(tiles, start, stop, stride=1):
        def one(n, carry):
            first(start + stride * n, tiles)
            return carry

        lax.fori_loop(0, (stop - start + stride - 1) // stride, one, 0)

    end_tiles = (0, TILES - 1)
    middle_tiles = tuple(range(1, TILES - 1))
    first_rows(end_tiles, 0, SPAN_PATCHES)
    first_rows(middle_tiles, 0, SPAN_PATCHES)
    pl.semaphore_wait(barrier, nc - 1 + nc * (jnp.where(above, 1, 0) + jnp.where(below, 1, 0)))
    tell(0)

    def start_to(there, copy):
        if there is None:
            copy.start()
        else:
            pl.when(there)(copy.start)

    def wait_for(outgoing, incoming, copy):
        if outgoing is None:
            copy.wait()
        else:
            pl.when(outgoing)(copy.wait_send)
            pl.when(incoming)(copy.wait_recv)

    def ends_of(dx):
        return {0: (None, None), 1: (above, below), -1: (below, above)}[dx]

    level_copies = []
    for n, (dx, dy) in enumerate(around):
        copy = pltpu.make_async_remote_copy(
            src_ref=lev_ref, dst_ref=lv.at[n], send_sem=lsend.at[n], recv_sem=lrecv.at[n],
            device_id=at(-dx, -dy), device_id_type=MESH)
        outgoing, incoming = ends_of(-dx)
        level_copies.append((outgoing, incoming, copy))

    def patch_copy(half, k):
        d = peer(k)
        rows = slice(0, MARK if half else FIRST)
        return pltpu.make_async_remote_copy(
            src_ref=sent.at[half, d, rows], dst_ref=got_ref.at[2 * me + half, rows],
            send_sem=psend.at[half], recv_sem=precv.at[half], device_id=device(d),
            device_id_type=MESH)

    def extra_copy(k):
        d = peer(k)
        return pltpu.make_async_remote_copy(
            src_ref=extra.at[d], dst_ref=got_extra.at[me], send_sem=esend,
            recv_sem=erecv, device_id=device(d), device_id_type=MESH)

    own_scale = jnp.where(fine, RESCALE, 1.0)
    kappa = gain / (1.0 - gain)

    def take_levels():
        for copy in level_copies:
            wait_for(*copy)
        scales = targets(lambda dx, dy: lv[around.index((dx, dy))])

        def refresh(q, tile, rows):
            cq[q - 1, rows, :, lanes_of(tile)] = coefficient(q, tile, scales, rows)

        for q in range(1, 19):
            e = VELOCITIES[q]
            outer_tile = {0: None, 1: TILES - 1, -1: 0}[e[0]]
            if e[0]:
                refresh(q, outer_tile, everything)
            if e[1]:
                r = SPAN_PATCHES - 1 if e[1] == 1 else 0
                for tile in range(TILES):
                    if tile != outer_tile:
                        refresh(q, tile, slice(r, r + 1))

    def spin(v, amount):
        return pltpu.roll(v, amount % LANES, axis=v.ndim - 1)

    def along_z(q, v, more=0):
        e = VELOCITIES[q][2]
        if not e:
            return spin(v, more) if more else v
        wrapped = pltpu.roll(spin(v, more - 7 * e), e % 8, axis=1)
        return jnp.where(in_tile[2, e][: v.shape[0]], wrapped, spin(v, more + e))

    def along_y(q, v, halo, more=0):
        e = VELOCITIES[q][1]
        moved = jnp.concatenate([halo, v[:-1]] if e == 1 else [v[1:], halo], axis=0)
        return jnp.where(in_tile[1, e], spin(moved, more - 56 * e), spin(v, more + 8 * e))

    def step(s, stage=None):
        copies = {"x": [], "y": []}

        def send(src, dst, n, dx, dy):
            copy = pltpu.make_async_remote_copy(
                src_ref=src, dst_ref=dst, send_sem=send_sem.at[s, n], recv_sem=recv_sem.at[s, n],
                device_id=at(dx, dy), device_id_type=MESH)
            outgoing, incoming = ends_of(dx)
            start_to(outgoing, copy)
            copies["x" if dx else "y"].append((outgoing, incoming, copy))

        parts = 2 if s == 0 else 1

        def face(q, rows, tile):
            spot = (q, rows, slice(0, 8), lanes_of(tile))
            values = [pb[spot]]
            if s == 0:
                values.append(kappa[rows] * (st[spot] - values[0]))
            return [along_z(q, v) for v in values]

        def send_x():
            for way, e, group in ((0, 1, X_UP), (1, -1, X_DOWN)):
                for n, q in enumerate(group):
                    for part_id, v in enumerate(face(q, everything, TILES - 1 if e == 1 else 0)):
                        turned = spin(v, 64)
                        if e == 1:
                            xs[s, way, part_id, n] = jnp.where(half, turned[:2], v[2:])
                        else:
                            xs[s, way, part_id, n] = jnp.where(half, v[:2], turned[2:])
                        if q in DIAGONAL:
                            edge = turned[SPAN_PATCHES - 1 if VELOCITIES[q][1] == 1 else 0]
                            ds[s, DIAGONAL.index(q), part_id] = edge
            for way, dx in ((0, 1), (1, -1)):
                send(xs.at[s, way, :parts], xr.at[s, way, :parts], 2 + way, dx, 0)
            for n, q in enumerate(DIAGONAL):
                send(ds.at[s, n, :parts], dr.at[s, n, :parts], 4 + n, *VELOCITIES[q][:2])

        def send_y():
            for way, e, group in ((0, 1, Y_UP), (1, -1, Y_DOWN)):
                r = SPAN_PATCHES - 1 if e == 1 else 0
                for n, q in enumerate(group):
                    for tile in range(TILES):
                        for part_id, v in enumerate(face(q, slice(r, r + 1), tile)):
                            ys[s, way, part_id, n, :, lanes_of(tile)] = v[0]
            for way, dy in ((0, 1), (1, -1)):
                send(ys.at[s, way, :parts], yr.at[s, way, :parts], way, 0, dy)

        def y_halo(e, n, tile):
            way, r = (0, 0) if e == 1 else (1, SPAN_PATCHES - 1)
            value = yr[s, way, 0, n, :, lanes_of(tile)]
            if s == 0:
                value = value + (own_scale[r] - 1.0) * yr[s, way, 1, n, :, lanes_of(tile)]
            return value[None]

        def x_halo(way, e, n, q):
            values = []
            for part_id in range(parts):
                h = xr[s, way, part_id, n]
                turned = spin(h, 64)
                halo = jnp.concatenate([h, turned] if e == 1 else [turned, h], axis=0)
                if q in DIAGONAL:
                    halo = along_y(q, halo, dr[s, DIAGONAL.index(q), part_id][None])
                values.append(halo)
            return values[0] + (own_scale - 1.0) * values[1] if s == 0 else values[0]

        if s == 0:
            send_x()
            send_y()
            for outgoing, _, copy in level_copies:
                start_to(outgoing, copy)
        elif stage is None:
            first_rows(end_tiles, 0, SPAN_PATCHES)
            send_x()
            send_y()
        else:
            first_rows(end_tiles, 0, SPAN_PATCHES, SPAN_PATCHES - 1)
            send_y()
            first_rows(end_tiles, 1, SPAN_PATCHES - 1)
            send_x()

        def shift(q):
            e = VELOCITIES[q]
            half_turn = 64 if e[0] else 0
            tiles = [along_z(q, pb[q, :, :, lanes_of(tile)], 0 if e[1] else half_turn) for tile in range(TILES)]
            if e[1]:
                n = (Y_UP if e[1] == 1 else Y_DOWN).index(q)
                tiles = [along_y(q, v, y_halo(e[1], n, tile), half_turn) for tile, v in enumerate(tiles)]
            if e[0]:
                turned = list(tiles)
                for tile in range(TILES):
                    if e[0] == 1:
                        tiles[tile] = jnp.where(lower, turned[tile - 1], turned[tile])
                    else:
                        tiles[tile] = jnp.where(lower, turned[tile], turned[(tile + 1) % TILES])
            for tile in range(TILES):
                st[q, :, :, lanes_of(tile)] = tiles[tile]

        for q in range(19):
            if not VELOCITIES[q][1]:
                shift(q)
        for copy in copies["y"]:
            wait_for(*copy)
        hear(2 * s)
        tell(2 * s + 1)
        for q in range(19):
            if VELOCITIES[q][1]:
                shift(q)

        def again(r, tiles):
            for tile in tiles:
                lanes = lanes_of(tile)

                def put(q, value):
                    pb2[q, r, :, lanes] = value

                relax_into(lambda q: st[q, r, :, lanes], put, lambda q: 1.0 - 1.0 / TAU_FINE)

        def settle(tiles):
            for q in range(19):
                e = VELOCITIES[q]
                amount = 64 * e[0] + 8 * e[1] + e[2]
                inside = fine
                for axis in (1, 2):
                    if e[axis]:
                        inside = inside & ~in_tile[axis, e[axis]]
                turned = {}

                def moved_from(tile):
                    if tile not in turned:
                        v = pb2[q, :, :, lanes_of(tile)]
                        turned[tile] = spin(v, amount) if amount else v
                    return turned[tile]

                for tile in tiles:
                    take = inside
                    value = moved_from(tile)
                    if e[0] == 1:
                        value = jnp.where(lower, moved_from((tile - 1) % TILES), value)
                        take = take & ~lower if tile == 0 else take
                    elif e[0] == -1:
                        value = jnp.where(lower, value, moved_from((tile + 1) % TILES))
                        take = take & lower if tile == TILES - 1 else take
                    lanes = lanes_of(tile)
                    st[q, :, :, lanes] = jnp.where(take, value, st[q, :, :, lanes])

        def middle(r, carry):
            again(r, range(1, TILES - 1))
            return carry

        def ends(r, carry):
            again(r, (0, TILES - 1))
            return carry

        lax.fori_loop(0, SPAN_PATCHES, middle, 0)
        lax.fori_loop(0, SPAN_PATCHES, ends, 0)
        settle(middle_tiles)
        if s == 0:
            take_levels()
        if stage is None:
            first_rows(middle_tiles, 0, SPAN_PATCHES)
        else:
            stage()
        for copy in copies["x"]:
            wait_for(*copy)
        if stage is None:
            hear(2 * s + 1)
            tell(2 * s + 2)
        for way, e, group in ((0, 1, X_UP), (1, -1, X_DOWN)):
            outside = b == (0 if e == 1 else nb - 1)
            for n, q in enumerate(group):
                halo = x_halo(way, e, n, q)
                along = e * INFLOW
                const = WEIGHTS[q] * (1.0 + 3.0 * along + 4.5 * along * along - 1.5 * INFLOW * INFLOW)
                halo = jnp.where(outside, jnp.full(halo.shape, const, jnp.float32), halo)
                lanes = lanes_of(0 if e == 1 else TILES - 1)
                keep = st[q, :, :, lanes]
                st[q, :, :, lanes] = jnp.where(lower, halo, keep) if e == 1 else jnp.where(lower, keep, halo)

        lax.fori_loop(0, SPAN_PATCHES, ends, 0)
        settle(end_tiles)

    flat = pm.reshape(pm.shape[0] * 2 * HALF, LANES)

    def fill(half):
        pm[:, half * HALF + 2 * MAIN : (half + 1) * HALF, :] = jnp.zeros(
            (pm.shape[0], HALF - 2 * MAIN, LANES), jnp.float32)
        for q in range(19):
            for r in range(SPAN_PATCHES):
                for tile in range(TILES):
                    if half_of(tile) == half:
                        row = r * 8 * 2 * HALF + half * HALF + low_row(q, tile)
                        flat[pl.ds(row, 8, stride=2 * HALF), :] = st[q, r, :, lanes_of(tile)]

    part = lax.rem(me, GROUP)
    base = me - part
    far_chip = part // nc
    chunks = count // GROUP

    def chunk_at(j):
        return lax.rem(j + chunks // 2, chunks)

    def rows_of(j):
        return pl.ds(chunk_at(j) * GROUP, GROUP)

    def swap_copy(half, j):
        return pltpu.make_async_remote_copy(
            src_ref=second.at[half, rows_of(j)], dst_ref=theirs.at[half, rows_of(j)],
            send_sem=csend.at[half], recv_sem=crecv.at[half, j], device_id=at(0, 1),
            device_id_type=MESH)

    def shuffle_copy(j):
        return pltpu.make_async_remote_copy(
            src_ref=away.at[rows_of(j)], dst_ref=across.at[rows_of(j)], send_sem=qsend,
            recv_sem=qrecv, device_id=device(lax.bitwise_xor(me, nc)), device_id_type=MESH)

    def tag_of(which, d):
        return tags[which, pl.ds(d, 1), :]

    def offer(half):
        def pack_second(j, carry):
            for i in range(GROUP):
                m = chunk_at(j) * GROUP + i
                d = lax.bitwise_xor(base, m)
                second[half, m] = pm[pick_s[d, 1], half * HALF : (half + 1) * HALF]
                if half == 0:
                    second[0, m, MARK : MARK + 1, :] = tag_of(1, d)
                    second[0, m, FIRST : FIRST + 1, :] = tag_of(0, d)

            @pl.when(j > 0)
            def _():
                swap_copy(half, j - 1).start()

            return carry

        lax.fori_loop(0, chunks, pack_second, 0)
        swap_copy(half, chunks - 1).start()

    zero = c == 0

    def pack_quarters(d, m, my_second, their_second, their_first, own):
        mine_extra = (my_second > -0.5) & (their_first > -0.5)
        their_extra = (their_second > -0.5) & own
        use_mine = mine_extra & (zero | ~their_extra)
        tag = jnp.where(use_mine, my_second, jnp.where(their_extra, their_second, -1.0))
        tag = jnp.where(mine_extra & their_extra, OVER, tag)
        p = pick_s[d, 1]
        for ref, t in ((kept, part), (away, lax.bitwise_xor(part, nc))):
            half = lax.rem(t, 2)
            place = t // 2
            top = pl.multiple_of(place * MAIN, 8)
            my_top = pl.multiple_of(half * HALF + place * MAIN, 8)
            my_low = pl.multiple_of(half * HALF + 2 * MAIN, 8)
            ref[m, :MAIN, :] = jnp.where(
                use_mine, pm[p, pl.ds(my_top, MAIN), :], theirs[half, m, pl.ds(top, MAIN), :])
            low = jnp.where(use_mine, pm[p, pl.ds(my_low, 8), :], theirs[half, m, 2 * MAIN : HALF, :])
            low = jnp.where(place == 1, pltpu.roll(low, 8 - TAIL, axis=0), low)
            ref[m, MAIN : MAIN + TAIL, :] = low[:TAIL]
            ref[m, TAG : TAG + 1, :] = tag

    def pack_chunk(half, j):
        for i in range(GROUP):
            k = chunk_at(j) * GROUP + i
            d = peer(k)
            m = lax.bitwise_xor(k, part)
            my_first = tag_of(0, d)
            their_second = theirs[0, m, MARK : MARK + 1, :]
            own = my_first > -0.5
            sent[half, d] = jnp.where(
                own, pm[pick_s[d, 0], half * HALF : (half + 1) * HALF], theirs[half, m])
            if half == 0:
                sent[0, d, MARK : MARK + 1, :] = jnp.where(own, my_first, their_second)
            else:
                pack_quarters(d, m, tag_of(1, d), their_second, theirs[0, m, FIRST : FIRST + 1, :], own)

    def send_chunk(half, j):
        if half:
            shuffle_copy(j).start()
        for i in range(GROUP):
            k = chunk_at(j) * GROUP + i

            @pl.when(k > 0)
            def _():
                patch_copy(half, k).start()

    def exchange(half):
        def post(j, carry):
            swap_copy(half, j).wait_recv()
            pack_chunk(half, j)

            @pl.when(j > 0)
            def _():
                send_chunk(half, j - 1)

            return carry

        lax.fori_loop(0, chunks, post, 0)
        send_chunk(half, chunks - 1)
        got_ref[2 * me + half] = sent[half, me]

    def early():
        fill(0)
        to_scalars.wait()
        offer(0)
        for k in range(2 * STEPS - 1, rounds):
            if k > 2 * STEPS - 1:
                tell(k)
            hear(k)
        exchange(0)

    for s in range(STEPS):
        step(s, early if s == STEPS - 1 else None)
    fill(1)
    offer(1)
    exchange(1)

    def waiter(ref, send, recv):
        return pltpu.make_async_remote_copy(
            src_ref=ref, dst_ref=ref, send_sem=send, recv_sem=recv, device_id=at(0, 1), device_id_type=MESH)

    for which in range(2):
        waiter(second.at[which], csend.at[which], csend.at[which]).wait_send()
    waiter(away, qsend, qrecv).wait_send()
    waiter(across, qsend, qrecv).wait_recv()
    near_tags = kept[:, TAG, :]
    far_tags = across[:, TAG, :]
    over = (near_tags > OVER / 2) | (far_tags > OVER / 2) | ((near_tags > -0.5) & (far_tags > -0.5))
    flag = jnp.max(jnp.where(over, OVER, 0.0), axis=0, keepdims=True)

    def pack_extra(d):
        m = lax.bitwise_xor(base, d)
        mine = kept[m]
        other = across[m]
        keep = ((mine[TAG:] > -0.5) & (far_chip == 0)) | ~(other[TAG:] > -0.5)
        extra[d] = jnp.where(keep, mine, other)
        extra[d, TAG : TAG + 1, :] = jnp.where(keep, mine[TAG:], other[TAG:]) + flag

    def mask_at(i):
        return lax.rem(i + count // 2, count)

    def post_extra(i, carry):
        pack_extra(peer(mask_at(i)))

        @pl.when((i > 0) & (mask_at(i - 1) > 0))
        def _():
            extra_copy(mask_at(i - 1)).start()

        return carry

    lax.fori_loop(0, count, post_extra, 0)
    extra_copy(mask_at(count - 1)).start()
    got_extra[me] = extra[me]

    for which, rows in ((0, FIRST), (1, MARK)):
        arrived = waiter(sent.at[which, 1:, :rows], psend.at[which], precv.at[which])
        arrived.wait_send()
        arrived.wait_recv()
    waiter(extra.at[1:], esend, erecv).wait_send()
    waiter(got_extra.at[1:], esend, erecv).wait_recv()

    def assemble(g, carry):
        for t in range(TILES):
            whole = got_ref.at[2 * count + 2 * g + t % 2]
            block = got_extra.at[g * GROUP + t]
            whole[t // 2 * MAIN : (t // 2 + 1) * MAIN, :] = block[:MAIN, :]
            low = 2 * MAIN + t // 2 * TAIL
            whole[low : low + TAIL, :] = block[MAIN : MAIN + TAIL, :]
        return carry

    lax.fori_loop(0, chunks, assemble, 0)
    source = lax.broadcasted_iota(jnp.int32, (2 * count, LANES), 0)
    wanted = lax.broadcasted_iota(jnp.int32, (2 * count, LANES), 1).astype(jnp.float32)
    first_hit = (got_ref[: 2 * count, MARK, :] == wanted) & (source % 2 == 0)
    index = jnp.sum(jnp.where(first_hit, source, 0), axis=0, keepdims=True)
    source = source[:count]
    extra_tags = got_extra[:, TAG, :]
    extra_hit = (extra_tags == wanted[:count]) & (source % GROUP == 0)
    place = source // GROUP * 2 + 2 * count
    index = index + jnp.sum(jnp.where(extra_hit, place, 0), axis=0, keepdims=True)
    over = jnp.max(extra_tags, axis=0, keepdims=True)
    row = lax.broadcasted_iota(jnp.int32, (8, LANES), 0)
    table_ref[...] = jnp.where(row == 0, index, jnp.where(over > OVER / 2, 1, 0))


def full_kernel(nb, nc, sidx, slot_of, pm, got_ref, table_ref, sent, send_sem, recv_sem):
    count = nb * nc
    me = lax.axis_index("blocks") * nc + lax.axis_index("cross")

    def device(d):
        return (d // nc, lax.rem(d, nc))

    barrier = pltpu.get_barrier_semaphore()

    def greet(k, carry):
        pl.semaphore_signal(barrier, inc=1, device_id=device(lax.bitwise_xor(me, k)), device_id_type=MESH)
        return carry

    lax.fori_loop(1, count, greet, 0)
    pl.semaphore_wait(barrier, count - 1)

    def pack(d, carry):
        for slot in range(2):
            p = sidx[2 * d + slot]
            sent[d, 2 * slot] = pm[p, :HALF]
            sent[d, 2 * slot + 1] = pm[p, HALF:]
            tag = jnp.full((1, LANES), slot_of[2 * d + slot].astype(jnp.float32), jnp.float32)
            sent[d, 2 * slot, MARK : MARK + 1, :] = tag
        return carry

    lax.fori_loop(0, count, pack, 0)

    def copy(k):
        d = lax.bitwise_xor(me, k)
        return pltpu.make_async_remote_copy(
            src_ref=sent.at[d], dst_ref=got_ref.at[pl.ds(4 * me, 4)], send_sem=send_sem.at[k],
            recv_sem=recv_sem.at[k], device_id=device(d), device_id_type=MESH)

    def post(k, carry):
        copy(k).start()
        return carry

    def finish(k, carry):
        copy(k).wait()
        return carry

    lax.fori_loop(1, count, post, 0)
    for i in range(4):
        got_ref[4 * me + i] = sent[me, i]
    lax.fori_loop(1, count, finish, 0)
    source = lax.broadcasted_iota(jnp.int32, (4 * count, LANES), 0)
    wanted = lax.broadcasted_iota(jnp.int32, (4 * count, LANES), 1).astype(jnp.float32)
    hit = (got_ref[:, MARK, :] == wanted) & (source % 2 == 0)
    index = jnp.sum(jnp.where(hit, source, 0), axis=0, keepdims=True)
    table_ref[...] = jnp.broadcast_to(index, table_ref.shape)


def unpack_kernel(ridx, got_ref, out_ref):
    for t in range(out_ref.shape[1]):
        base = ridx[0, t]
        for tile in range(TILES):
            block = got_ref.at[base + half_of(tile)]
            lanes = slice(tile * LANES, (tile + 1) * LANES)
            low = low_row(0, tile)
            out_ref[:MAIN, t, lanes] = block[low : low + MAIN, :]
            low = low_row(MAIN, tile)
            out_ref[MAIN:, t, lanes] = block[2 * MAIN :, :][low - 2 * MAIN : low - 2 * MAIN + TAIL]


def body(nb, nc, f_home, levels, plan):
    devices = nb * nc
    patches = f_home.shape[0]
    vmem = pl.BlockSpec(memory_space=pltpu.VMEM)
    smem = pl.BlockSpec(memory_space=pltpu.SMEM)
    state = (19, SPAN_PATCHES, 8, CELLS)
    small = (SPAN_PATCHES, 8, LANES)
    f32 = jnp.float32
    dma = pltpu.SemaphoreType.DMA
    half = (HALF, LANES)
    quarter = (QUARTER, LANES)
    rounds = max(2 * STEPS, (nb - 1).bit_length())
    limit = pltpu.CompilerParams(collective_id=0, has_side_effects=True, vmem_limit_bytes=60 * 1024 * 1024)
    got, packed, table = pl.pallas_call(
        lambda *refs: lattice_kernel(nb, nc, *refs),
        out_shape=(
            jax.ShapeDtypeStruct((2 * devices + 2 * devices // GROUP,) + half, f32),
            jax.ShapeDtypeStruct((patches, 2 * HALF, LANES), f32),
            jax.ShapeDtypeStruct((8, LANES), jnp.int32),
        ),
        in_specs=[smem, vmem, vmem],
        out_specs=(vmem, vmem, vmem),
        scratch_shapes=[
            pltpu.VMEM(state, f32),
            pltpu.VMEM(state, f32),
            pltpu.VMEM(state, f32),
            pltpu.VMEM((18,) + state[1:], f32),
            pltpu.VMEM((2, devices) + half, f32),
            pltpu.VMEM((2, devices) + half, f32),
            pltpu.VMEM((2, devices) + half, f32),
            pltpu.VMEM((devices,) + quarter, f32),
            pltpu.VMEM((devices,) + quarter, f32),
            pltpu.VMEM((devices,) + quarter, f32),
            pltpu.VMEM((devices,) + quarter, f32),
            pltpu.VMEM((devices,) + quarter, f32),
            pltpu.VMEM(small, f32),
            pltpu.VMEM((8, LANES), f32),
            pltpu.VMEM((3 * nc - 1, 8, LANES), f32),
            pltpu.VMEM((STEPS, 2, 2, 5, 8, CELLS), f32),
            pltpu.VMEM((STEPS, 2, 2, 5, 8, CELLS), f32),
            pltpu.VMEM((STEPS, 2, 2, 5, 2, 8, LANES), f32),
            pltpu.VMEM((STEPS, 2, 2, 5, 2, 8, LANES), f32),
            pltpu.VMEM((STEPS, len(DIAGONAL), 2, 8, LANES), f32),
            pltpu.VMEM((STEPS, len(DIAGONAL), 2, 8, LANES), f32),
            pltpu.VMEM((devices, LANES), jnp.int32),
            pltpu.SMEM((devices, LANES), jnp.int32),
            pltpu.VMEM((2, devices, LANES), f32),
            dma((STEPS, 8)),
            dma((STEPS, 8)),
            dma((3 * nc - 1,)),
            dma((3 * nc - 1,)),
            dma((2,)),
            dma((2,)),
            dma,
            dma,
            dma((2,)),
            dma((2, devices // GROUP)),
            dma,
            dma,
            dma,
            pltpu.SemaphoreType.REGULAR((rounds,)),
            pltpu.SemaphoreType.REGULAR((rounds,)),
        ],
        compiler_params=limit,
    )(levels, plan[None, :], jnp.transpose(f_home, (1, 0, 2)))

    def unpack(table, got):
        return pl.pallas_call(
            unpack_kernel,
            out_shape=jax.ShapeDtypeStruct((19, patches, CELLS), f32),
            in_specs=[smem, vmem],
            out_specs=vmem,
            compiler_params=pltpu.CompilerParams(vmem_limit_bytes=40 * 1024 * 1024),
        )(table, got)

    def in_full(table, got, packed, plan):
        target = plan // patches
        order = jnp.arange(patches, dtype=jnp.int32)
        earlier = (target[:, None] == target[None, :]) & (order[None, :] < order[:, None])
        place = 2 * target + jnp.sum(earlier.astype(jnp.int32), axis=1)
        hit = place[None, :] == jnp.arange(2 * devices, dtype=jnp.int32)[:, None]
        sidx = jnp.sum(jnp.where(hit, order[None, :], 0), axis=1)
        slot_of = jnp.sum(jnp.where(hit, plan[None, :] % patches + 1, 0), axis=1) - 1
        got, table = pl.pallas_call(
            lambda *refs: full_kernel(nb, nc, *refs),
            out_shape=(
                jax.ShapeDtypeStruct((4 * devices,) + half, f32),
                jax.ShapeDtypeStruct((8, LANES), jnp.int32),
            ),
            in_specs=[smem, smem, vmem],
            out_specs=(vmem, vmem),
            scratch_shapes=[
                pltpu.VMEM((devices, 4) + half, f32), dma((devices,)), dma((devices,))
            ],
            compiler_params=pltpu.CompilerParams(collective_id=1, has_side_effects=True,
                                                 vmem_limit_bytes=48 * 1024 * 1024),
        )(sidx, slot_of, packed)
        return unpack(table, got)

    out = lax.cond(table[1, 0] > 0, in_full, lambda table, got, packed, plan: unpack(table, got),
                   table, got, packed, plan)
    return jnp.transpose(out, (1, 0, 2))


def solution(mesh):
    nb, nc = mesh.shape["blocks"], mesh.shape["cross"]
    in_specs = (P(("blocks", "cross"), None, None), P(("blocks", "cross")), P(("blocks", "cross")))
    out_specs = P(("blocks", "cross"), None, None)
    return jax.shard_map(
        lambda f, l, p: body(nb, nc, f, l, p),
        mesh=mesh, in_specs=in_specs, out_specs=out_specs, check_vma=False)
```

```python
import jax
import jax.numpy as jnp
from jax import lax
from jax.experimental import pallas as pl
from jax.experimental.pallas import tpu as pltpu
from jax.sharding import PartitionSpec as P

SPAN_PATCHES = 4
DEPTH_PATCHES = 8
STEPS = 2
CELLS = 512
VELOCITIES = (
    (0, 0, 0),
    (1, 0, 0),
    (-1, 0, 0),
    (0, 1, 0),
    (0, -1, 0),
    (0, 0, 1),
    (0, 0, -1),
    (1, 1, 0),
    (-1, -1, 0),
    (1, -1, 0),
    (-1, 1, 0),
    (1, 0, 1),
    (-1, 0, -1),
    (1, 0, -1),
    (-1, 0, 1),
    (0, 1, 1),
    (0, -1, -1),
    (0, 1, -1),
    (0, -1, 1),
)
WEIGHTS = (1.0 / 3.0,) + (1.0 / 18.0,) * 6 + (1.0 / 36.0,) * 12
TAU_COARSE = 0.55
TAU_FINE = 2.0 * TAU_COARSE - 0.5
RESCALE = TAU_FINE / (2.0 * TAU_COARSE)
INFLOW = 0.08
MESH = pl.DeviceIdType.MESH
MAIN = 16
TAIL = 3
HALF = 40
MARK = 38
FIRST = 39
QUARTER = 20
TAG = 19
OVER = 1000.0
GROUP = 4
LANES = 128
TILES = CELLS // LANES
Y_UP = [q for q in range(19) if VELOCITIES[q][1] == 1]
Y_DOWN = [q for q in range(19) if VELOCITIES[q][1] == -1]
X_UP = [q for q in range(19) if VELOCITIES[q][0] == 1]
X_DOWN = [q for q in range(19) if VELOCITIES[q][0] == -1]
DIAGONAL = [q for q in range(19) if VELOCITIES[q][0] and VELOCITIES[q][1]]


def relax_into(load, store, coef):
    f = [load(q) for q in range(19)]
    terms = list(f)
    while len(terms) > 1:
        pairs = [a + b for a, b in zip(terms[::2], terms[1::2])]
        terms = pairs + ([terms[-1]] if len(terms) % 2 else [])
    rho = terms[0]
    inv = 1.0 / rho
    u = []
    for axis in range(3):
        up = [f[q] for q in range(19) if VELOCITIES[q][axis] == 1]
        down = [f[q] for q in range(19) if VELOCITIES[q][axis] == -1]
        d = [a - b for a, b in zip(up, down)]
        u.append((((d[0] + d[1]) + (d[2] + d[3])) + d[4]) * inv)
    base = 1.0 - 1.5 * (u[0] * u[0] + u[1] * u[1] + u[2] * u[2])
    scaled = {w: w * rho for w in set(WEIGHTS)}
    for q in range(19):
        along = None
        for axis in range(3):
            e = VELOCITIES[q][axis]
            if e:
                term = u[axis] if e == 1 else -u[axis]
                along = term if along is None else along + term
        poly = base if along is None else base + along * (3.0 + 4.5 * along)
        balance = scaled[WEIGHTS[q]] * poly
        store(q, balance + coef(q) * (f[q] - balance))


def half_of(tile):
    return 1 if tile in (0, TILES - 1) else 0


def place_of(tile):
    return tile // 2 if half_of(tile) else tile - 1


def low_row(q, tile):
    place = place_of(tile)
    return place * MAIN + q if q < MAIN else 2 * MAIN + place * TAIL + q - MAIN


def lattice_kernel(nb, nc, level, plan_ref, f_ref, got_ref, pm, table_ref, st, pb, pb2, cq, sent, second, theirs,
                   away, kept, across, extra, got_extra, own_ref, lev_ref, lv, ys, yr, xs, xr, ds, dr, pick, pick_s, tags, send_sem, recv_sem, lsend, lrecv, psend,
                   precv, esend, erecv, csend, crecv, qsend, qrecv, pick_sem, up_sem, down_sem):
    others = nb * nc - 1
    rounds = max(2 * STEPS, (nb - 1).bit_length())
    b = lax.axis_index("blocks")
    c = lax.axis_index("cross")

    def at(dx, dy):
        return (lax.rem(b + dx + nb, nb), lax.rem(c + dy + nc, nc))

    me = b * nc + c

    def peer(k):
        return lax.bitwise_xor(me, k)

    def device(d):
        return (d // nc, lax.rem(d, nc))

    barrier = pltpu.get_barrier_semaphore()
    above = b < nb - 1
    below = b > 0

    def signal(sem, to):
        pl.semaphore_signal(sem, inc=1, device_id=to, device_id_type=MESH)

    for k in range(1, nc):
        signal(barrier, at(0, k))
    for there, dx in ((above, 1), (below, -1)):
        @pl.when(there)
        def _():
            for k in range(nc):
                signal(barrier, at(dx, k))

    def tell(k):
        hop = lax.shift_left(jnp.int32(1), jnp.int32(k))

        @pl.when(b + hop < nb)
        def _():
            signal(up_sem.at[k], (b + hop, c))

        @pl.when(b >= hop)
        def _():
            signal(down_sem.at[k], (b - hop, c))

    def hear(k):
        hop = lax.shift_left(jnp.int32(1), jnp.int32(k))

        @pl.when(b >= hop)
        def _():
            pl.semaphore_wait(up_sem.at[k], 1)

        @pl.when(b + hop < nb)
        def _():
            pl.semaphore_wait(down_sem.at[k], 1)

    patches = f_ref.shape[1]
    count = nb * nc
    target = lax.broadcasted_iota(jnp.int32, (count, patches), 0)
    where = jnp.broadcast_to(plan_ref[...], (count, patches))
    member = where // patches == target
    key = lax.broadcasted_iota(jnp.int32, (count, patches), 1) * patches + where % patches
    low_key = jnp.min(jnp.where(member, key, patches * patches), axis=1, keepdims=True)
    high_key = jnp.max(jnp.where(member, key, -1), axis=1, keepdims=True)
    some = high_key >= 0
    two = high_key > low_key
    column = lax.broadcasted_iota(jnp.int32, (count, LANES), 1)
    pick[...] = jnp.where(column == 0, jnp.where(some, low_key // patches, 0),
                          jnp.where(two, high_key // patches, 0))
    to_scalars = pltpu.make_async_copy(pick, pick_s, pick_sem)
    to_scalars.start()
    tags[0] = jnp.broadcast_to(jnp.where(some, low_key % patches, -1), (count, LANES)).astype(jnp.float32)
    tags[1] = jnp.broadcast_to(jnp.where(two, high_key % patches, -1), (count, LANES)).astype(jnp.float32)

    slot = lax.broadcasted_iota(jnp.int32, (8, LANES), 0)
    slot = slot + 8 * lax.broadcasted_iota(jnp.int32, (8, LANES), 1)
    brief = jnp.zeros((8, LANES), jnp.float32)
    for p in range(SPAN_PATCHES * 8):
        brief = jnp.where(slot == p, level[p].astype(jnp.float32), brief)
    lev_ref[...] = brief

    def spread(values, r):
        return jnp.broadcast_to(values[:, r : r + 1], (8, LANES))[None]

    own = jnp.concatenate([spread(brief, r) for r in range(SPAN_PATCHES)], axis=0)
    own_ref[...] = own
    for q in range(19):
        for r in range(SPAN_PATCHES):
            st[q, r] = f_ref[q, r * 8 : r * 8 + 8, :]
    gain = jnp.where(own > 0.5, (1.0 - 1.0 / TAU_FINE) / RESCALE, 1.0 - 1.0 / TAU_COARSE)
    lane = lax.broadcasted_iota(jnp.int32, (SPAN_PATCHES, 8, LANES), 2)
    lower = lane < 64
    half = lax.broadcasted_iota(jnp.int32, (2, 8, LANES), 2) < 64
    fine = own > 0.5
    in_tile = {
        (axis, e): (lane // 8 % 8 if axis == 1 else lane % 8) == (0 if e == 1 else 7)
        for axis in (1, 2) for e in (1, -1)
    }
    around = [(dx, dy) for dx in (-1, 0, 1) for dy in range(nc) if (dx, dy) != (0, 0)]

    def targets(far):
        scales = {}
        for dx in (-1, 0, 1):
            rows = [spread(far(dx, nc - 1), SPAN_PATCHES - 1)]
            rows += [own[r][None] if dx == 0 else spread(far(dx, 0), r) for r in range(SPAN_PATCHES)]
            rows += [spread(far(dx, 1 % nc), 0)]
            rows = [jnp.where(value > 0.5, RESCALE, 1.0) for value in rows]
            for dy in (-1, 0, 1):
                value = jnp.concatenate(rows[1 + dy : 1 + dy + SPAN_PATCHES], axis=0)
                for dz in (-1, 0, 1):
                    scales[dx, dy, dz] = pltpu.roll(value, (-dz) % 8, axis=1) if dz else value
        return scales

    def coefficient(q, tile, scales, rows):
        e = VELOCITIES[q]
        kinds = [{}]
        for axis in range(3):
            if e[axis] and (axis or tile == (TILES - 1 if e[0] == 1 else 0)):
                kinds = [{**k, axis: v} for k in kinds for v in (0, 1)]
        result = None
        for k in kinds:
            value = scales[tuple(e[a] * k.get(a, 0) for a in range(3))][rows]
            mask = None
            for axis, on in k.items():
                if on:
                    hit = in_tile[axis, -e[axis]] if axis else (~lower if e[0] == 1 else lower)
                    mask = hit[rows] if mask is None else mask & hit[rows]
            result = value if result is None else jnp.where(mask, value, result)
        return gain[rows] * result

    def lanes_of(tile):
        return slice(tile * LANES, (tile + 1) * LANES)

    everything = slice(0, SPAN_PATCHES)
    scales = targets(lambda dx, dy: jnp.zeros((8, LANES), jnp.float32))
    for q in range(1, 19):
        for tile in range(TILES):
            cq[q - 1, :, :, lanes_of(tile)] = coefficient(q, tile, scales, everything)

    def first(r, tiles):
        plain = jnp.where(own_ref[r] > 0.5, 1.0 - 1.0 / TAU_FINE, 1.0 - 1.0 / TAU_COARSE)
        for tile in tiles:
            lanes = lanes_of(tile)

            def put(q, value):
                pb[q, r, :, lanes] = value

            relax_into(lambda q: st[q, r, :, lanes], put,
                       lambda q: cq[q - 1, r, :, lanes] if q else plain)

    def first_rows(tiles, start, stop, stride=1):
        def one(n, carry):
            first(start + stride * n, tiles)
            return carry

        lax.fori_loop(0, (stop - start + stride - 1) // stride, one, 0)

    end_tiles = (0, TILES - 1)
    middle_tiles = tuple(range(1, TILES - 1))
    first_rows(end_tiles, 0, SPAN_PATCHES)
    first_rows(middle_tiles, 0, SPAN_PATCHES)
    pl.semaphore_wait(barrier, nc - 1 + nc * (jnp.where(above, 1, 0) + jnp.where(below, 1, 0)))
    tell(0)

    def start_to(there, copy):
        if there is None:
            copy.start()
        else:
            pl.when(there)(copy.start)

    def wait_for(outgoing, incoming, copy):
        if outgoing is None:
            copy.wait()
        else:
            pl.when(outgoing)(copy.wait_send)
            pl.when(incoming)(copy.wait_recv)

    def ends_of(dx):
        return {0: (None, None), 1: (above, below), -1: (below, above)}[dx]

    def waiter(ref, send, recv):
        return pltpu.make_async_remote_copy(
            src_ref=ref, dst_ref=ref, send_sem=send, recv_sem=recv, device_id=at(0, 1), device_id_type=MESH)

    level_copies = []
    for n, (dx, dy) in enumerate(around):
        copy = pltpu.make_async_remote_copy(
            src_ref=lev_ref, dst_ref=lv.at[n], send_sem=lsend.at[dx + 1], recv_sem=lrecv.at[dx + 1],
            device_id=at(-dx, -dy), device_id_type=MESH)
        outgoing, incoming = ends_of(-dx)
        level_copies.append((outgoing, copy))

    def patch_copy(half, k):
        d = peer(k)
        rows = slice(0, MARK if half else FIRST)
        return pltpu.make_async_remote_copy(
            src_ref=sent.at[half, d, rows], dst_ref=got_ref.at[2 * me + half, rows],
            send_sem=psend.at[half], recv_sem=precv.at[half], device_id=device(d),
            device_id_type=MESH)

    def extra_copy(k):
        d = peer(k)
        return pltpu.make_async_remote_copy(
            src_ref=extra.at[d], dst_ref=got_extra.at[me], send_sem=esend,
            recv_sem=erecv, device_id=device(d), device_id_type=MESH)

    own_scale = jnp.where(fine, RESCALE, 1.0)
    kappa = gain / (1.0 - gain)

    def take_levels():
        for dx in (-1, 0, 1):
            some = nc if dx else nc - 1
            wait_for(*ends_of(-dx), waiter(lv.at[:some], lsend.at[dx + 1], lrecv.at[dx + 1]))
        scales = targets(lambda dx, dy: lv[around.index((dx, dy))])

        def refresh(q, tile, rows):
            cq[q - 1, rows, :, lanes_of(tile)] = coefficient(q, tile, scales, rows)

        for q in range(1, 19):
            e = VELOCITIES[q]
            outer_tile = {0: None, 1: TILES - 1, -1: 0}[e[0]]
            if e[0]:
                refresh(q, outer_tile, everything)
            if e[1]:
                r = SPAN_PATCHES - 1 if e[1] == 1 else 0
                for tile in range(TILES):
                    if tile != outer_tile:
                        refresh(q, tile, slice(r, r + 1))

    def spin(v, amount):
        return pltpu.roll(v, amount % LANES, axis=v.ndim - 1)

    def along_z(q, v, more=0):
        e = VELOCITIES[q][2]
        if not e:
            return spin(v, more) if more else v
        wrapped = pltpu.roll(spin(v, more - 7 * e), e % 8, axis=1)
        return jnp.where(in_tile[2, e][: v.shape[0]], wrapped, spin(v, more + e))

    def along_y(q, v, halo, more=0):
        e = VELOCITIES[q][1]
        moved = jnp.concatenate([halo, v[:-1]] if e == 1 else [v[1:], halo], axis=0)
        return jnp.where(in_tile[1, e], spin(moved, more - 56 * e), spin(v, more + 8 * e))

    def step(s, stage=None):
        def send(src, dst, dx, dy):
            copy = pltpu.make_async_remote_copy(
                src_ref=src, dst_ref=dst, send_sem=send_sem.at[s, dx + 1], recv_sem=recv_sem.at[s, dx + 1],
                device_id=at(dx, dy), device_id_type=MESH)
            start_to(ends_of(dx)[0], copy)

        def await_halos(dx):
            ref = pb2.at[: 3 * parts, :, :, :LANES] if dx else ys.at[s, :, :parts]
            wait_for(*ends_of(dx), waiter(ref, send_sem.at[s, dx + 1], recv_sem.at[s, dx + 1]))

        parts = 2 if s == 0 else 1

        def face(q, rows, tile):
            spot = (q, rows, slice(0, 8), lanes_of(tile))
            values = [pb[spot]]
            if s == 0:
                values.append(kappa[rows] * (st[spot] - values[0]))
            return [along_z(q, v) for v in values]

        def send_x():
            for way, e, group in ((0, 1, X_UP), (1, -1, X_DOWN)):
                for n, q in enumerate(group):
                    for part_id, v in enumerate(face(q, everything, TILES - 1 if e == 1 else 0)):
                        turned = spin(v, 64)
                        if e == 1:
                            xs[s, way, part_id, n] = jnp.where(half, turned[:2], v[2:])
                        else:
                            xs[s, way, part_id, n] = jnp.where(half, v[:2], turned[2:])
                        if q in DIAGONAL:
                            edge = turned[SPAN_PATCHES - 1 if VELOCITIES[q][1] == 1 else 0]
                            ds[s, DIAGONAL.index(q), part_id] = edge
            for way, dx in ((0, 1), (1, -1)):
                send(xs.at[s, way, :parts], xr.at[s, way, :parts], dx, 0)
            for n, q in enumerate(DIAGONAL):
                send(ds.at[s, n, :parts], dr.at[s, n, :parts], *VELOCITIES[q][:2])

        def send_y():
            for way, e, group in ((0, 1, Y_UP), (1, -1, Y_DOWN)):
                r = SPAN_PATCHES - 1 if e == 1 else 0
                for n, q in enumerate(group):
                    for tile in range(TILES):
                        for part_id, v in enumerate(face(q, slice(r, r + 1), tile)):
                            ys[s, way, part_id, n, :, lanes_of(tile)] = v[0]
            for way, dy in ((0, 1), (1, -1)):
                send(ys.at[s, way, :parts], yr.at[s, way, :parts], 0, dy)

        def y_halo(e, n, tile):
            way, r = (0, 0) if e == 1 else (1, SPAN_PATCHES - 1)
            value = yr[s, way, 0, n, :, lanes_of(tile)]
            if s == 0:
                value = value + (own_scale[r] - 1.0) * yr[s, way, 1, n, :, lanes_of(tile)]
            return value[None]

        def x_halo(way, e, n, q):
            values = []
            for part_id in range(parts):
                h = xr[s, way, part_id, n]
                turned = spin(h, 64)
                halo = jnp.concatenate([h, turned] if e == 1 else [turned, h], axis=0)
                if q in DIAGONAL:
                    halo = along_y(q, halo, dr[s, DIAGONAL.index(q), part_id][None])
                values.append(halo)
            return values[0] + (own_scale - 1.0) * values[1] if s == 0 else values[0]

        if s == 0:
            send_x()
            send_y()
            for outgoing, copy in level_copies:
                start_to(outgoing, copy)
        elif stage is None:
            first_rows(end_tiles, 0, SPAN_PATCHES)
            send_x()
            send_y()
        else:
            first_rows(end_tiles, 0, SPAN_PATCHES, SPAN_PATCHES - 1)
            send_y()
            first_rows(end_tiles, 1, SPAN_PATCHES - 1)
            send_x()

        def shift(q):
            e = VELOCITIES[q]
            half_turn = 64 if e[0] else 0
            tiles = [along_z(q, pb[q, :, :, lanes_of(tile)], 0 if e[1] else half_turn) for tile in range(TILES)]
            if e[1]:
                n = (Y_UP if e[1] == 1 else Y_DOWN).index(q)
                tiles = [along_y(q, v, y_halo(e[1], n, tile), half_turn) for tile, v in enumerate(tiles)]
            if e[0]:
                turned = list(tiles)
                for tile in range(TILES):
                    if e[0] == 1:
                        tiles[tile] = jnp.where(lower, turned[tile - 1], turned[tile])
                    else:
                        tiles[tile] = jnp.where(lower, turned[tile], turned[(tile + 1) % TILES])
            for tile in range(TILES):
                st[q, :, :, lanes_of(tile)] = tiles[tile]

        for q in range(19):
            if not VELOCITIES[q][1]:
                shift(q)
        await_halos(0)
        hear(2 * s)
        tell(2 * s + 1)
        for q in range(19):
            if VELOCITIES[q][1]:
                shift(q)

        def again(r, tiles):
            for tile in tiles:
                lanes = lanes_of(tile)

                def put(q, value):
                    pb2[q, r, :, lanes] = value

                relax_into(lambda q: st[q, r, :, lanes], put, lambda q: 1.0 - 1.0 / TAU_FINE)

        def settle(tiles):
            for q in range(19):
                e = VELOCITIES[q]
                amount = 64 * e[0] + 8 * e[1] + e[2]
                inside = fine
                for axis in (1, 2):
                    if e[axis]:
                        inside = inside & ~in_tile[axis, e[axis]]
                turned = {}

                def moved_from(tile):
                    if tile not in turned:
                        v = pb2[q, :, :, lanes_of(tile)]
                        turned[tile] = spin(v, amount) if amount else v
                    return turned[tile]

                for tile in tiles:
                    take = inside
                    value = moved_from(tile)
                    if e[0] == 1:
                        value = jnp.where(lower, moved_from((tile - 1) % TILES), value)
                        take = take & ~lower if tile == 0 else take
                    elif e[0] == -1:
                        value = jnp.where(lower, value, moved_from((tile + 1) % TILES))
                        take = take & lower if tile == TILES - 1 else take
                    lanes = lanes_of(tile)
                    st[q, :, :, lanes] = jnp.where(take, value, st[q, :, :, lanes])

        def middle(r, carry):
            again(r, range(1, TILES - 1))
            return carry

        def ends(r, carry):
            again(r, (0, TILES - 1))
            return carry

        lax.fori_loop(0, SPAN_PATCHES, middle, 0)
        lax.fori_loop(0, SPAN_PATCHES, ends, 0)
        settle(middle_tiles)
        if s == 0:
            take_levels()
        if stage is None:
            first_rows(middle_tiles, 0, SPAN_PATCHES)
        else:
            stage()
        await_halos(1)
        await_halos(-1)
        if stage is None:
            hear(2 * s + 1)
            tell(2 * s + 2)
        for way, e, group in ((0, 1, X_UP), (1, -1, X_DOWN)):
            outside = b == (0 if e == 1 else nb - 1)
            for n, q in enumerate(group):
                halo = x_halo(way, e, n, q)
                along = e * INFLOW
                const = WEIGHTS[q] * (1.0 + 3.0 * along + 4.5 * along * along - 1.5 * INFLOW * INFLOW)
                halo = jnp.where(outside, jnp.full(halo.shape, const, jnp.float32), halo)
                lanes = lanes_of(0 if e == 1 else TILES - 1)
                keep = st[q, :, :, lanes]
                st[q, :, :, lanes] = jnp.where(lower, halo, keep) if e == 1 else jnp.where(lower, keep, halo)

        lax.fori_loop(0, SPAN_PATCHES, ends, 0)
        settle(end_tiles)

    flat = pm.reshape(pm.shape[0] * 2 * HALF, LANES)

    def fill(half):
        pm[:, half * HALF + 2 * MAIN : (half + 1) * HALF, :] = jnp.zeros(
            (pm.shape[0], HALF - 2 * MAIN, LANES), jnp.float32)
        for q in range(19):
            for r in range(SPAN_PATCHES):
                for tile in range(TILES):
                    if half_of(tile) == half:
                        row = r * 8 * 2 * HALF + half * HALF + low_row(q, tile)
                        flat[pl.ds(row, 8, stride=2 * HALF), :] = st[q, r, :, lanes_of(tile)]

    part = lax.rem(me, GROUP)
    base = me - part
    far_chip = part // nc
    chunks = count // GROUP

    def chunk_at(j):
        return lax.rem(j + chunks // 2, chunks)

    def rows_of(j):
        return pl.ds(chunk_at(j) * GROUP, GROUP)

    def whole_swap():
        return pltpu.make_async_remote_copy(
            src_ref=second.at[1], dst_ref=theirs.at[1], send_sem=csend.at[1],
            recv_sem=crecv.at[chunks], device_id=at(0, 1), device_id_type=MESH)

    def swap_copy(half, j):
        return pltpu.make_async_remote_copy(
            src_ref=second.at[half, rows_of(j)], dst_ref=theirs.at[half, rows_of(j)],
            send_sem=csend.at[half], recv_sem=crecv.at[j], device_id=at(0, 1),
            device_id_type=MESH)

    def shuffle_copy(j):
        return pltpu.make_async_remote_copy(
            src_ref=away.at[rows_of(j)], dst_ref=across.at[rows_of(j)], send_sem=qsend,
            recv_sem=qrecv, device_id=device(lax.bitwise_xor(me, nc)), device_id_type=MESH)

    def tag_of(which, d):
        return tags[which, pl.ds(d, 1), :]

    def offer(half):
        def pack_second(j, carry):
            for i in range(GROUP):
                m = chunk_at(j) * GROUP + i
                d = lax.bitwise_xor(base, m)
                second[half, m] = pm[pick_s[d, 1], half * HALF : (half + 1) * HALF]
                if half == 0:
                    second[0, m, MARK : MARK + 1, :] = tag_of(1, d)
                    second[0, m, FIRST : FIRST + 1, :] = tag_of(0, d)

            if half == 0:
                @pl.when(j > 0)
                def _():
                    swap_copy(half, j - 1).start()

            return carry

        lax.fori_loop(0, chunks, pack_second, 0)
        if half == 0:
            swap_copy(half, chunks - 1).start()
        else:
            whole_swap().start()

    zero = c == 0

    def pack_quarters(d, m, my_second, their_second, their_first, own):
        mine_extra = (my_second > -0.5) & (their_first > -0.5)
        their_extra = (their_second > -0.5) & own
        use_mine = mine_extra & (zero | ~their_extra)
        tag = jnp.where(use_mine, my_second, jnp.where(their_extra, their_second, -1.0))
        tag = jnp.where(mine_extra & their_extra, OVER, tag)
        p = pick_s[d, 1]
        for ref, t in ((kept, part), (away, lax.bitwise_xor(part, nc))):
            half = lax.rem(t, 2)
            place = t // 2
            top = pl.multiple_of(place * MAIN, 8)
            my_top = pl.multiple_of(half * HALF + place * MAIN, 8)
            my_low = pl.multiple_of(half * HALF + 2 * MAIN, 8)
            ref[m, :MAIN, :] = jnp.where(
                use_mine, pm[p, pl.ds(my_top, MAIN), :], theirs[half, m, pl.ds(top, MAIN), :])
            low = jnp.where(use_mine, pm[p, pl.ds(my_low, 8), :], theirs[half, m, 2 * MAIN : HALF, :])
            low = jnp.where(place == 1, pltpu.roll(low, 8 - TAIL, axis=0), low)
            ref[m, MAIN : MAIN + TAIL, :] = low[:TAIL]
            ref[m, TAG : TAG + 1, :] = tag

    def pack_chunk(half, j):
        for i in range(GROUP):
            k = chunk_at(j) * GROUP + i
            d = peer(k)
            m = lax.bitwise_xor(k, part)
            my_first = tag_of(0, d)
            their_second = theirs[0, m, MARK : MARK + 1, :]
            own = my_first > -0.5
            sent[half, d] = jnp.where(
                own, pm[pick_s[d, 0], half * HALF : (half + 1) * HALF], theirs[half, m])
            if half == 0:
                sent[0, d, MARK : MARK + 1, :] = jnp.where(own, my_first, their_second)
            else:
                pack_quarters(d, m, tag_of(1, d), their_second, theirs[0, m, FIRST : FIRST + 1, :], own)

    def send_chunk(half, j):
        if half:
            shuffle_copy(j).start()
        for i in range(GROUP):
            k = chunk_at(j) * GROUP + i

            @pl.when(k > 0)
            def _():
                patch_copy(half, k).start()

    def exchange(half):
        if half:
            whole_swap().wait_recv()

        def post(j, carry):
            if half == 0:
                swap_copy(half, j).wait_recv()
            pack_chunk(half, j)

            @pl.when(j > 0)
            def _():
                send_chunk(half, j - 1)

            return carry

        lax.fori_loop(0, chunks, post, 0)
        send_chunk(half, chunks - 1)
        got_ref[2 * me + half] = sent[half, me]

    def early():
        fill(0)
        to_scalars.wait()
        offer(0)
        for k in range(2 * STEPS - 1, rounds):
            if k > 2 * STEPS - 1:
                tell(k)
            hear(k)
        exchange(0)

    for s in range(STEPS):
        step(s, early if s == STEPS - 1 else None)
    fill(1)
    offer(1)
    exchange(1)

    for which in range(2):
        waiter(second.at[which], csend.at[which], csend.at[which]).wait_send()
    waiter(away, qsend, qrecv).wait_send()
    waiter(across, qsend, qrecv).wait_recv()
    near_tags = kept[:, TAG, :]
    far_tags = across[:, TAG, :]
    over = (near_tags > OVER / 2) | (far_tags > OVER / 2) | ((near_tags > -0.5) & (far_tags > -0.5))
    flag = jnp.max(jnp.where(over, OVER, 0.0), axis=0, keepdims=True)

    def pack_extra(d):
        m = lax.bitwise_xor(base, d)
        mine = kept[m]
        other = across[m]
        keep = ((mine[TAG:] > -0.5) & (far_chip == 0)) | ~(other[TAG:] > -0.5)
        extra[d] = jnp.where(keep, mine, other)
        extra[d, TAG : TAG + 1, :] = jnp.where(keep, mine[TAG:], other[TAG:]) + flag

    def mask_at(i):
        return lax.rem(i + count // 2, count)

    def post_extra(i, carry):
        pack_extra(peer(mask_at(i)))

        @pl.when((i > 0) & (mask_at(i - 1) > 0))
        def _():
            extra_copy(mask_at(i - 1)).start()

        return carry

    lax.fori_loop(0, count, post_extra, 0)
    extra_copy(mask_at(count - 1)).start()
    got_extra[me] = extra[me]

    for which, rows in ((0, FIRST), (1, MARK)):
        arrived = waiter(sent.at[which, 1:, :rows], psend.at[which], precv.at[which])
        arrived.wait_send()
        arrived.wait_recv()
    waiter(extra.at[1:], esend, erecv).wait_send()
    waiter(got_extra.at[1:], esend, erecv).wait_recv()

    def assemble(g, carry):
        for t in range(TILES):
            whole = got_ref.at[2 * count + 2 * g + t % 2]
            block = got_extra.at[g * GROUP + t]
            whole[t // 2 * MAIN : (t // 2 + 1) * MAIN, :] = block[:MAIN, :]
            low = 2 * MAIN + t // 2 * TAIL
            whole[low : low + TAIL, :] = block[MAIN : MAIN + TAIL, :]
        return carry

    lax.fori_loop(0, chunks, assemble, 0)
    source = lax.broadcasted_iota(jnp.int32, (count, LANES), 0)
    wanted = lax.broadcasted_iota(jnp.int32, (count, LANES), 1).astype(jnp.float32)
    arrived_flat = got_ref.reshape(got_ref.shape[0] * HALF, LANES)
    first_hit = arrived_flat[pl.ds(MARK, count, stride=2 * HALF), :] == wanted
    index = jnp.sum(jnp.where(first_hit, 2 * source, 0), axis=0, keepdims=True)
    extra_tags = got_extra[:, TAG, :]
    extra_hit = (extra_tags == wanted) & (source % GROUP == 0)
    place = source // GROUP * 2 + 2 * count
    index = index + jnp.sum(jnp.where(extra_hit, place, 0), axis=0, keepdims=True)
    over = jnp.max(extra_tags, axis=0, keepdims=True)
    row = lax.broadcasted_iota(jnp.int32, (8, LANES), 0)
    table_ref[...] = jnp.where(row == 0, index, jnp.where(over > OVER / 2, 1, 0))


def full_kernel(nb, nc, sidx, slot_of, pm, got_ref, table_ref, sent, send_sem, recv_sem):
    count = nb * nc
    me = lax.axis_index("blocks") * nc + lax.axis_index("cross")

    def device(d):
        return (d // nc, lax.rem(d, nc))

    barrier = pltpu.get_barrier_semaphore()

    def greet(k, carry):
        pl.semaphore_signal(barrier, inc=1, device_id=device(lax.bitwise_xor(me, k)), device_id_type=MESH)
        return carry

    lax.fori_loop(1, count, greet, 0)
    pl.semaphore_wait(barrier, count - 1)

    def pack(d, carry):
        for slot in range(2):
            p = sidx[2 * d + slot]
            sent[d, 2 * slot] = pm[p, :HALF]
            sent[d, 2 * slot + 1] = pm[p, HALF:]
            tag = jnp.full((1, LANES), slot_of[2 * d + slot].astype(jnp.float32), jnp.float32)
            sent[d, 2 * slot, MARK : MARK + 1, :] = tag
        return carry

    lax.fori_loop(0, count, pack, 0)

    def copy(k):
        d = lax.bitwise_xor(me, k)
        return pltpu.make_async_remote_copy(
            src_ref=sent.at[d], dst_ref=got_ref.at[pl.ds(4 * me, 4)], send_sem=send_sem.at[k],
            recv_sem=recv_sem.at[k], device_id=device(d), device_id_type=MESH)

    def post(k, carry):
        copy(k).start()
        return carry

    def finish(k, carry):
        copy(k).wait()
        return carry

    lax.fori_loop(1, count, post, 0)
    for i in range(4):
        got_ref[4 * me + i] = sent[me, i]
    lax.fori_loop(1, count, finish, 0)
    source = lax.broadcasted_iota(jnp.int32, (4 * count, LANES), 0)
    wanted = lax.broadcasted_iota(jnp.int32, (4 * count, LANES), 1).astype(jnp.float32)
    hit = (got_ref[:, MARK, :] == wanted) & (source % 2 == 0)
    index = jnp.sum(jnp.where(hit, source, 0), axis=0, keepdims=True)
    table_ref[...] = jnp.broadcast_to(index, table_ref.shape)


def unpack_kernel(ridx, got_ref, out_ref):
    groups = out_ref.shape[1]
    flat = out_ref.reshape(19 * groups * TILES * 8, LANES)
    stride = groups * TILES * 8
    for t in range(groups * 8):
        base = ridx[0, t]
        for tile in range(TILES):
            block = got_ref.at[base + half_of(tile)]
            row = (t // 8 * TILES + tile) * 8 + t % 8
            place = place_of(tile)
            for q in range(0, MAIN, 8):
                flat[pl.ds(row + q * stride, 8, stride=stride), :] = block[place * MAIN + q : place * MAIN + q + 8, :]
            low = place * TAIL
            rest = block[2 * MAIN :, :][low : low + TAIL]
            flat[pl.ds(row + MAIN * stride, TAIL, stride=stride), :] = rest


def body(nb, nc, f_home, levels, plan):
    devices = nb * nc
    patches = f_home.shape[0]
    vmem = pl.BlockSpec(memory_space=pltpu.VMEM)
    smem = pl.BlockSpec(memory_space=pltpu.SMEM)
    state = (19, SPAN_PATCHES, 8, CELLS)
    small = (SPAN_PATCHES, 8, LANES)
    f32 = jnp.float32
    dma = pltpu.SemaphoreType.DMA
    half = (HALF, LANES)
    quarter = (QUARTER, LANES)
    rounds = max(2 * STEPS, (nb - 1).bit_length())
    limit = pltpu.CompilerParams(collective_id=0, has_side_effects=True, vmem_limit_bytes=60 * 1024 * 1024)
    got, packed, table = pl.pallas_call(
        lambda *refs: lattice_kernel(nb, nc, *refs),
        out_shape=(
            jax.ShapeDtypeStruct((2 * devices + 2 * devices // GROUP,) + half, f32),
            jax.ShapeDtypeStruct((patches, 2 * HALF, LANES), f32),
            jax.ShapeDtypeStruct((8, LANES), jnp.int32),
        ),
        in_specs=[smem, vmem, vmem],
        out_specs=(vmem, vmem, vmem),
        scratch_shapes=[
            pltpu.VMEM(state, f32),
            pltpu.VMEM(state, f32),
            pltpu.VMEM(state, f32),
            pltpu.VMEM((18,) + state[1:], f32),
            pltpu.VMEM((2, devices) + half, f32),
            pltpu.VMEM((2, devices) + half, f32),
            pltpu.VMEM((2, devices) + half, f32),
            pltpu.VMEM((devices,) + quarter, f32),
            pltpu.VMEM((devices,) + quarter, f32),
            pltpu.VMEM((devices,) + quarter, f32),
            pltpu.VMEM((devices,) + quarter, f32),
            pltpu.VMEM((devices,) + quarter, f32),
            pltpu.VMEM(small, f32),
            pltpu.VMEM((8, LANES), f32),
            pltpu.VMEM((3 * nc - 1, 8, LANES), f32),
            pltpu.VMEM((STEPS, 2, 2, 5, 8, CELLS), f32),
            pltpu.VMEM((STEPS, 2, 2, 5, 8, CELLS), f32),
            pltpu.VMEM((STEPS, 2, 2, 5, 2, 8, LANES), f32),
            pltpu.VMEM((STEPS, 2, 2, 5, 2, 8, LANES), f32),
            pltpu.VMEM((STEPS, len(DIAGONAL), 2, 8, LANES), f32),
            pltpu.VMEM((STEPS, len(DIAGONAL), 2, 8, LANES), f32),
            pltpu.VMEM((devices, LANES), jnp.int32),
            pltpu.SMEM((devices, LANES), jnp.int32),
            pltpu.VMEM((2, devices, LANES), f32),
            dma((STEPS, 3)),
            dma((STEPS, 3)),
            dma((3,)),
            dma((3,)),
            dma((2,)),
            dma((2,)),
            dma,
            dma,
            dma((2,)),
            dma((devices // GROUP + 1,)),
            dma,
            dma,
            dma,
            pltpu.SemaphoreType.REGULAR((rounds,)),
            pltpu.SemaphoreType.REGULAR((rounds,)),
        ],
        compiler_params=limit,
    )(levels, plan[None, :], jnp.transpose(f_home, (1, 0, 2)))

    def unpack(table, got):
        return pl.pallas_call(
            unpack_kernel,
            out_shape=jax.ShapeDtypeStruct((19, patches // 8, TILES, 8, LANES), f32),
            in_specs=[smem, vmem],
            out_specs=vmem,
            compiler_params=pltpu.CompilerParams(vmem_limit_bytes=40 * 1024 * 1024),
        )(table, got)

    def in_full(table, got, packed, plan):
        target = plan // patches
        order = jnp.arange(patches, dtype=jnp.int32)
        earlier = (target[:, None] == target[None, :]) & (order[None, :] < order[:, None])
        place = 2 * target + jnp.sum(earlier.astype(jnp.int32), axis=1)
        hit = place[None, :] == jnp.arange(2 * devices, dtype=jnp.int32)[:, None]
        sidx = jnp.sum(jnp.where(hit, order[None, :], 0), axis=1)
        slot_of = jnp.sum(jnp.where(hit, plan[None, :] % patches + 1, 0), axis=1) - 1
        got, table = pl.pallas_call(
            lambda *refs: full_kernel(nb, nc, *refs),
            out_shape=(
                jax.ShapeDtypeStruct((4 * devices,) + half, f32),
                jax.ShapeDtypeStruct((8, LANES), jnp.int32),
            ),
            in_specs=[smem, smem, vmem],
            out_specs=(vmem, vmem),
            scratch_shapes=[
                pltpu.VMEM((devices, 4) + half, f32), dma((devices,)), dma((devices,))
            ],
            compiler_params=pltpu.CompilerParams(collective_id=1, has_side_effects=True,
                                                 vmem_limit_bytes=48 * 1024 * 1024),
        )(sidx, slot_of, packed)
        return unpack(table, got)

    out = lax.cond(table[1, 0] > 0, in_full, lambda table, got, packed, plan: unpack(table, got),
                   table, got, packed, plan)
    return jnp.transpose(out, (1, 3, 0, 2, 4)).reshape(f_home.shape)


def solution(mesh):
    nb, nc = mesh.shape["blocks"], mesh.shape["cross"]
    in_specs = (P(("blocks", "cross"), None, None), P(("blocks", "cross")), P(("blocks", "cross")))
    out_specs = P(("blocks", "cross"), None, None)
    return jax.shard_map(
        lambda f, l, p: body(nb, nc, f, l, p),
        mesh=mesh, in_specs=in_specs, out_specs=out_specs, check_vma=False)
```

```python
import jax
import jax.numpy as jnp
from jax import lax
from jax.experimental import pallas as pl
from jax.experimental.pallas import tpu as pltpu
from jax.sharding import PartitionSpec as P

SPAN_PATCHES = 4
DEPTH_PATCHES = 8
STEPS = 2
CELLS = 512
VELOCITIES = (
    (0, 0, 0),
    (1, 0, 0),
    (-1, 0, 0),
    (0, 1, 0),
    (0, -1, 0),
    (0, 0, 1),
    (0, 0, -1),
    (1, 1, 0),
    (-1, -1, 0),
    (1, -1, 0),
    (-1, 1, 0),
    (1, 0, 1),
    (-1, 0, -1),
    (1, 0, -1),
    (-1, 0, 1),
    (0, 1, 1),
    (0, -1, -1),
    (0, 1, -1),
    (0, -1, 1),
)
WEIGHTS = (1.0 / 3.0,) + (1.0 / 18.0,) * 6 + (1.0 / 36.0,) * 12
TAU_COARSE = 0.55
TAU_FINE = 2.0 * TAU_COARSE - 0.5
RESCALE = TAU_FINE / (2.0 * TAU_COARSE)
INFLOW = 0.08
MESH = pl.DeviceIdType.MESH
MAIN = 16
TAIL = 3
HALF = 40
MARK = 38
FIRST = 39
QUARTER = 20
TAG = 19
OVER = 1000.0
GROUP = 4
LANES = 128
TILES = CELLS // LANES
Y_UP = [q for q in range(19) if VELOCITIES[q][1] == 1]
Y_DOWN = [q for q in range(19) if VELOCITIES[q][1] == -1]
X_UP = [q for q in range(19) if VELOCITIES[q][0] == 1]
X_DOWN = [q for q in range(19) if VELOCITIES[q][0] == -1]
DIAGONAL = [q for q in range(19) if VELOCITIES[q][0] and VELOCITIES[q][1]]


def relax_into(load, store, coef):
    f = [load(q) for q in range(19)]
    terms = list(f)
    while len(terms) > 1:
        pairs = [a + b for a, b in zip(terms[::2], terms[1::2])]
        terms = pairs + ([terms[-1]] if len(terms) % 2 else [])
    rho = terms[0]
    inv = 1.0 / rho
    u = []
    for axis in range(3):
        up = [f[q] for q in range(19) if VELOCITIES[q][axis] == 1]
        down = [f[q] for q in range(19) if VELOCITIES[q][axis] == -1]
        d = [a - b for a, b in zip(up, down)]
        u.append((((d[0] + d[1]) + (d[2] + d[3])) + d[4]) * inv)
    base = 1.0 - 1.5 * (u[0] * u[0] + u[1] * u[1] + u[2] * u[2])
    scaled = {w: w * rho for w in set(WEIGHTS)}
    for q in range(19):
        along = None
        for axis in range(3):
            e = VELOCITIES[q][axis]
            if e:
                term = u[axis] if e == 1 else -u[axis]
                along = term if along is None else along + term
        poly = base if along is None else base + along * (3.0 + 4.5 * along)
        balance = scaled[WEIGHTS[q]] * poly
        store(q, balance + coef(q) * (f[q] - balance))


def half_of(tile):
    return 1 if tile in (0, TILES - 1) else 0


def place_of(tile):
    return tile // 2 if half_of(tile) else tile - 1


def low_row(q, tile):
    place = place_of(tile)
    return place * MAIN + q if q < MAIN else 2 * MAIN + place * TAIL + q - MAIN


def lattice_kernel(nb, nc, level, plan_ref, f_ref, got_ref, pm, table_ref, st, pb, pb2, cq, sent, second, theirs,
                   away, kept, across, extra, got_extra, own_ref, lev_ref, lv, ys, yr, xs, xr, ds, dr, pick, pick_s, tags, send_sem, recv_sem, lsend, lrecv, psend,
                   precv, esend, erecv, csend, crecv, qsend, qrecv, pick_sem, up_sem, down_sem):
    others = nb * nc - 1
    rounds = max(2 * STEPS, (nb - 1).bit_length())
    b = lax.axis_index("blocks")
    c = lax.axis_index("cross")

    def at(dx, dy):
        return (lax.rem(b + dx + nb, nb), lax.rem(c + dy + nc, nc))

    me = b * nc + c

    def peer(k):
        return lax.bitwise_xor(me, k)

    def device(d):
        return (d // nc, lax.rem(d, nc))

    barrier = pltpu.get_barrier_semaphore()
    above = b < nb - 1
    below = b > 0

    def signal(sem, to):
        pl.semaphore_signal(sem, inc=1, device_id=to, device_id_type=MESH)

    for k in range(1, nc):
        signal(barrier, at(0, k))
    for there, dx in ((above, 1), (below, -1)):
        @pl.when(there)
        def _():
            for k in range(nc):
                signal(barrier, at(dx, k))

    def tell(k):
        hop = lax.shift_left(jnp.int32(1), jnp.int32(k))

        @pl.when(b + hop < nb)
        def _():
            signal(up_sem.at[k], (b + hop, c))

        @pl.when(b >= hop)
        def _():
            signal(down_sem.at[k], (b - hop, c))

    def hear(k):
        hop = lax.shift_left(jnp.int32(1), jnp.int32(k))

        @pl.when(b >= hop)
        def _():
            pl.semaphore_wait(up_sem.at[k], 1)

        @pl.when(b + hop < nb)
        def _():
            pl.semaphore_wait(down_sem.at[k], 1)

    patches = f_ref.shape[1]
    count = nb * nc
    target = lax.broadcasted_iota(jnp.int32, (count, patches), 0)
    where = jnp.broadcast_to(plan_ref[...], (count, patches))
    member = where // patches == target
    key = lax.broadcasted_iota(jnp.int32, (count, patches), 1) * patches + where % patches
    low_key = jnp.min(jnp.where(member, key, patches * patches), axis=1, keepdims=True)
    high_key = jnp.max(jnp.where(member, key, -1), axis=1, keepdims=True)
    some = high_key >= 0
    two = high_key > low_key
    column = lax.broadcasted_iota(jnp.int32, (count, LANES), 1)
    pick[...] = jnp.where(column == 0, jnp.where(some, low_key // patches, 0),
                          jnp.where(two, high_key // patches, 0))
    to_scalars = pltpu.make_async_copy(pick, pick_s, pick_sem)
    to_scalars.start()
    tags[0] = jnp.broadcast_to(jnp.where(some, low_key % patches, -1), (count, LANES)).astype(jnp.float32)
    tags[1] = jnp.broadcast_to(jnp.where(two, high_key % patches, -1), (count, LANES)).astype(jnp.float32)

    slot = lax.broadcasted_iota(jnp.int32, (8, LANES), 0)
    slot = slot + 8 * lax.broadcasted_iota(jnp.int32, (8, LANES), 1)
    brief = jnp.zeros((8, LANES), jnp.float32)
    for p in range(SPAN_PATCHES * 8):
        brief = jnp.where(slot == p, level[p].astype(jnp.float32), brief)
    lev_ref[...] = brief

    def spread(values, r):
        return jnp.broadcast_to(values[:, r : r + 1], (8, LANES))[None]

    own = jnp.concatenate([spread(brief, r) for r in range(SPAN_PATCHES)], axis=0)
    own_ref[...] = own
    for q in range(19):
        for r in range(SPAN_PATCHES):
            st[q, r] = f_ref[q, r * 8 : r * 8 + 8, :]
    gain = jnp.where(own > 0.5, (1.0 - 1.0 / TAU_FINE) / RESCALE, 1.0 - 1.0 / TAU_COARSE)
    lane = lax.broadcasted_iota(jnp.int32, (SPAN_PATCHES, 8, LANES), 2)
    lower = lane < 64
    half = lax.broadcasted_iota(jnp.int32, (2, 8, LANES), 2) < 64
    fine = own > 0.5
    in_tile = {
        (axis, e): (lane // 8 % 8 if axis == 1 else lane % 8) == (0 if e == 1 else 7)
        for axis in (1, 2) for e in (1, -1)
    }
    around = [(dx, dy) for dx in (-1, 0, 1) for dy in range(nc) if (dx, dy) != (0, 0)]

    def targets(far):
        scales = {}
        for dx in (-1, 0, 1):
            rows = [spread(far(dx, nc - 1), SPAN_PATCHES - 1)]
            rows += [own[r][None] if dx == 0 else spread(far(dx, 0), r) for r in range(SPAN_PATCHES)]
            rows += [spread(far(dx, 1 % nc), 0)]
            rows = [jnp.where(value > 0.5, RESCALE, 1.0) for value in rows]
            for dy in (-1, 0, 1):
                value = jnp.concatenate(rows[1 + dy : 1 + dy + SPAN_PATCHES], axis=0)
                for dz in (-1, 0, 1):
                    scales[dx, dy, dz] = pltpu.roll(value, (-dz) % 8, axis=1) if dz else value
        return scales

    def coefficient(q, tile, scales, rows):
        e = VELOCITIES[q]
        kinds = [{}]
        for axis in range(3):
            if e[axis] and (axis or tile == (TILES - 1 if e[0] == 1 else 0)):
                kinds = [{**k, axis: v} for k in kinds for v in (0, 1)]
        result = None
        for k in kinds:
            value = scales[tuple(e[a] * k.get(a, 0) for a in range(3))][rows]
            mask = None
            for axis, on in k.items():
                if on:
                    hit = in_tile[axis, -e[axis]] if axis else (~lower if e[0] == 1 else lower)
                    mask = hit[rows] if mask is None else mask & hit[rows]
            result = value if result is None else jnp.where(mask, value, result)
        return gain[rows] * result

    def lanes_of(tile):
        return slice(tile * LANES, (tile + 1) * LANES)

    everything = slice(0, SPAN_PATCHES)
    scales = targets(lambda dx, dy: jnp.zeros((8, LANES), jnp.float32))
    for q in range(1, 19):
        for tile in range(TILES):
            cq[q - 1, :, :, lanes_of(tile)] = coefficient(q, tile, scales, everything)

    def first(r, tiles):
        plain = jnp.where(own_ref[r] > 0.5, 1.0 - 1.0 / TAU_FINE, 1.0 - 1.0 / TAU_COARSE)
        for tile in tiles:
            lanes = lanes_of(tile)

            def put(q, value):
                pb[q, r, :, lanes] = value

            relax_into(lambda q: st[q, r, :, lanes], put,
                       lambda q: cq[q - 1, r, :, lanes] if q else plain)

    def first_rows(tiles, start, stop, stride=1):
        def one(n, carry):
            first(start + stride * n, tiles)
            return carry

        lax.fori_loop(0, (stop - start + stride - 1) // stride, one, 0)

    end_tiles = (0, TILES - 1)
    middle_tiles = tuple(range(1, TILES - 1))
    first_rows(end_tiles, 0, SPAN_PATCHES)
    first_rows(middle_tiles, 0, SPAN_PATCHES)
    pl.semaphore_wait(barrier, nc - 1 + nc * (jnp.where(above, 1, 0) + jnp.where(below, 1, 0)))
    tell(0)

    def start_to(there, copy):
        if there is None:
            copy.start()
        else:
            pl.when(there)(copy.start)

    def wait_for(outgoing, incoming, copy):
        if outgoing is None:
            copy.wait()
        else:
            pl.when(outgoing)(copy.wait_send)
            pl.when(incoming)(copy.wait_recv)

    def ends_of(dx):
        return {0: (None, None), 1: (above, below), -1: (below, above)}[dx]

    def waiter(ref, send, recv):
        return pltpu.make_async_remote_copy(
            src_ref=ref, dst_ref=ref, send_sem=send, recv_sem=recv, device_id=at(0, 1), device_id_type=MESH)

    level_copies = []
    for n, (dx, dy) in enumerate(around):
        copy = pltpu.make_async_remote_copy(
            src_ref=lev_ref, dst_ref=lv.at[n], send_sem=lsend.at[dx + 1], recv_sem=lrecv.at[dx + 1],
            device_id=at(-dx, -dy), device_id_type=MESH)
        outgoing, incoming = ends_of(-dx)
        level_copies.append((outgoing, copy))

    def patch_copy(half, k):
        d = peer(k)
        rows = slice(0, MARK if half else FIRST)
        return pltpu.make_async_remote_copy(
            src_ref=sent.at[half, d, rows], dst_ref=got_ref.at[2 * me + half, rows],
            send_sem=psend.at[half], recv_sem=precv.at[half], device_id=device(d),
            device_id_type=MESH)

    def extra_copy(k):
        d = peer(k)
        return pltpu.make_async_remote_copy(
            src_ref=extra.at[d], dst_ref=got_extra.at[me], send_sem=esend,
            recv_sem=erecv, device_id=device(d), device_id_type=MESH)

    own_scale = jnp.where(fine, RESCALE, 1.0)
    kappa = gain / (1.0 - gain)

    def take_levels():
        for dx in (-1, 0, 1):
            some = nc if dx else nc - 1
            wait_for(*ends_of(-dx), waiter(lv.at[:some], lsend.at[dx + 1], lrecv.at[dx + 1]))
        scales = targets(lambda dx, dy: lv[around.index((dx, dy))])

        def refresh(q, tile, rows):
            cq[q - 1, rows, :, lanes_of(tile)] = coefficient(q, tile, scales, rows)

        for q in range(1, 19):
            e = VELOCITIES[q]
            outer_tile = {0: None, 1: TILES - 1, -1: 0}[e[0]]
            if e[0]:
                refresh(q, outer_tile, everything)
            if e[1]:
                r = SPAN_PATCHES - 1 if e[1] == 1 else 0
                for tile in range(TILES):
                    if tile != outer_tile:
                        refresh(q, tile, slice(r, r + 1))

    def spin(v, amount):
        return pltpu.roll(v, amount % LANES, axis=v.ndim - 1)

    def along_z(q, v, more=0):
        e = VELOCITIES[q][2]
        if not e:
            return spin(v, more) if more else v
        wrapped = pltpu.roll(spin(v, more - 7 * e), e % 8, axis=1)
        return jnp.where(in_tile[2, e][: v.shape[0]], wrapped, spin(v, more + e))

    def along_y(q, v, halo, more=0):
        e = VELOCITIES[q][1]
        moved = jnp.concatenate([halo, v[:-1]] if e == 1 else [v[1:], halo], axis=0)
        return jnp.where(in_tile[1, e], spin(moved, more - 56 * e), spin(v, more + 8 * e))

    def step(s, stage=None):
        def send(src, dst, dx, dy):
            copy = pltpu.make_async_remote_copy(
                src_ref=src, dst_ref=dst, send_sem=send_sem.at[s, dx + 1], recv_sem=recv_sem.at[s, dx + 1],
                device_id=at(dx, dy), device_id_type=MESH)
            start_to(ends_of(dx)[0], copy)

        def await_halos(dx):
            ref = pb2.at[: 3 * parts, :, :, :LANES] if dx else ys.at[s, :, :parts]
            wait_for(*ends_of(dx), waiter(ref, send_sem.at[s, dx + 1], recv_sem.at[s, dx + 1]))

        parts = 2 if s == 0 else 1

        def face(q, rows, tile):
            spot = (q, rows, slice(0, 8), lanes_of(tile))
            values = [pb[spot]]
            if s == 0:
                values.append(kappa[rows] * (st[spot] - values[0]))
            return [along_z(q, v) for v in values]

        def send_x():
            for way, e, group in ((0, 1, X_UP), (1, -1, X_DOWN)):
                for n, q in enumerate(group):
                    for part_id, v in enumerate(face(q, everything, TILES - 1 if e == 1 else 0)):
                        turned = spin(v, 64)
                        if e == 1:
                            xs[s, way, part_id, n] = jnp.where(half, turned[:2], v[2:])
                        else:
                            xs[s, way, part_id, n] = jnp.where(half, v[:2], turned[2:])
                        if q in DIAGONAL:
                            edge = turned[SPAN_PATCHES - 1 if VELOCITIES[q][1] == 1 else 0]
                            ds[s, DIAGONAL.index(q), part_id] = edge
            for way, dx in ((0, 1), (1, -1)):
                send(xs.at[s, way, :parts], xr.at[s, way, :parts], dx, 0)
            for n, q in enumerate(DIAGONAL):
                send(ds.at[s, n, :parts], dr.at[s, n, :parts], *VELOCITIES[q][:2])

        def send_y():
            for way, e, group in ((0, 1, Y_UP), (1, -1, Y_DOWN)):
                r = SPAN_PATCHES - 1 if e == 1 else 0
                for n, q in enumerate(group):
                    for tile in range(TILES):
                        for part_id, v in enumerate(face(q, slice(r, r + 1), tile)):
                            ys[s, way, part_id, n, :, lanes_of(tile)] = v[0]
            for way, dy in ((0, 1), (1, -1)):
                send(ys.at[s, way, :parts], yr.at[s, way, :parts], 0, dy)

        def y_halo(e, n, tile):
            way, r = (0, 0) if e == 1 else (1, SPAN_PATCHES - 1)
            value = yr[s, way, 0, n, :, lanes_of(tile)]
            if s == 0:
                value = value + (own_scale[r] - 1.0) * yr[s, way, 1, n, :, lanes_of(tile)]
            return value[None]

        def x_halo(way, e, n, q):
            values = []
            for part_id in range(parts):
                h = xr[s, way, part_id, n]
                turned = spin(h, 64)
                halo = jnp.concatenate([h, turned] if e == 1 else [turned, h], axis=0)
                if q in DIAGONAL:
                    halo = along_y(q, halo, dr[s, DIAGONAL.index(q), part_id][None])
                values.append(halo)
            return values[0] + (own_scale - 1.0) * values[1] if s == 0 else values[0]

        if s == 0:
            send_x()
            send_y()
            for outgoing, copy in level_copies:
                start_to(outgoing, copy)
        elif stage is None:
            first_rows(end_tiles, 0, SPAN_PATCHES)
            send_x()
            send_y()
        else:
            first_rows(end_tiles, 0, SPAN_PATCHES, SPAN_PATCHES - 1)
            send_y()
            first_rows(end_tiles, 1, SPAN_PATCHES - 1)
            send_x()

        def shift(q):
            e = VELOCITIES[q]
            half_turn = 64 if e[0] else 0
            tiles = [along_z(q, pb[q, :, :, lanes_of(tile)], 0 if e[1] else half_turn) for tile in range(TILES)]
            if e[1]:
                n = (Y_UP if e[1] == 1 else Y_DOWN).index(q)
                tiles = [along_y(q, v, y_halo(e[1], n, tile), half_turn) for tile, v in enumerate(tiles)]
            if e[0]:
                turned = list(tiles)
                for tile in range(TILES):
                    if e[0] == 1:
                        tiles[tile] = jnp.where(lower, turned[tile - 1], turned[tile])
                    else:
                        tiles[tile] = jnp.where(lower, turned[tile], turned[(tile + 1) % TILES])
            for tile in range(TILES):
                st[q, :, :, lanes_of(tile)] = tiles[tile]

        for q in range(19):
            if not VELOCITIES[q][1]:
                shift(q)
        await_halos(0)
        hear(2 * s)
        tell(2 * s + 1)
        for q in range(19):
            if VELOCITIES[q][1]:
                shift(q)

        def again(r, tiles):
            for tile in tiles:
                lanes = lanes_of(tile)

                def put(q, value):
                    pb2[q, r, :, lanes] = value

                relax_into(lambda q: st[q, r, :, lanes], put, lambda q: 1.0 - 1.0 / TAU_FINE)

        def settle(tiles):
            for q in range(19):
                e = VELOCITIES[q]
                amount = 64 * e[0] + 8 * e[1] + e[2]
                inside = fine
                for axis in (1, 2):
                    if e[axis]:
                        inside = inside & ~in_tile[axis, e[axis]]
                turned = {}

                def moved_from(tile):
                    if tile not in turned:
                        v = pb2[q, :, :, lanes_of(tile)]
                        turned[tile] = spin(v, amount) if amount else v
                    return turned[tile]

                for tile in tiles:
                    take = inside
                    value = moved_from(tile)
                    if e[0] == 1:
                        value = jnp.where(lower, moved_from((tile - 1) % TILES), value)
                        take = take & ~lower if tile == 0 else take
                    elif e[0] == -1:
                        value = jnp.where(lower, value, moved_from((tile + 1) % TILES))
                        take = take & lower if tile == TILES - 1 else take
                    lanes = lanes_of(tile)
                    st[q, :, :, lanes] = jnp.where(take, value, st[q, :, :, lanes])

        def middle(r, carry):
            again(r, range(1, TILES - 1))
            return carry

        def ends(r, carry):
            again(r, (0, TILES - 1))
            return carry

        lax.fori_loop(0, SPAN_PATCHES, middle, 0)
        lax.fori_loop(0, SPAN_PATCHES, ends, 0)
        settle(middle_tiles)
        if s == 0:
            take_levels()
        if stage is None:
            first_rows(middle_tiles, 0, SPAN_PATCHES)
        else:
            stage()
        await_halos(1)
        await_halos(-1)
        if stage is None:
            hear(2 * s + 1)
            tell(2 * s + 2)
        for way, e, group in ((0, 1, X_UP), (1, -1, X_DOWN)):
            outside = b == (0 if e == 1 else nb - 1)
            for n, q in enumerate(group):
                halo = x_halo(way, e, n, q)
                along = e * INFLOW
                const = WEIGHTS[q] * (1.0 + 3.0 * along + 4.5 * along * along - 1.5 * INFLOW * INFLOW)
                halo = jnp.where(outside, jnp.full(halo.shape, const, jnp.float32), halo)
                lanes = lanes_of(0 if e == 1 else TILES - 1)
                keep = st[q, :, :, lanes]
                st[q, :, :, lanes] = jnp.where(lower, halo, keep) if e == 1 else jnp.where(lower, keep, halo)

        lax.fori_loop(0, SPAN_PATCHES, ends, 0)
        settle(end_tiles)

    flat = pm.reshape(pm.shape[0] * 2 * HALF, LANES)

    def fill(half):
        pm[:, half * HALF + 2 * MAIN : (half + 1) * HALF, :] = jnp.zeros(
            (pm.shape[0], HALF - 2 * MAIN, LANES), jnp.float32)
        for q in range(19):
            for r in range(SPAN_PATCHES):
                for tile in range(TILES):
                    if half_of(tile) == half:
                        row = r * 8 * 2 * HALF + half * HALF + low_row(q, tile)
                        flat[pl.ds(row, 8, stride=2 * HALF), :] = st[q, r, :, lanes_of(tile)]

    part = lax.rem(me, GROUP)
    base = me - part
    far_chip = part // nc
    chunks = count // GROUP

    def chunk_at(j):
        return lax.rem(j + chunks // 2, chunks)

    def rows_of(j):
        return pl.ds(chunk_at(j) * GROUP, GROUP)

    def whole_swap():
        return pltpu.make_async_remote_copy(
            src_ref=second.at[1], dst_ref=theirs.at[1], send_sem=csend.at[1],
            recv_sem=crecv.at[chunks], device_id=at(0, 1), device_id_type=MESH)

    def swap_copy(half, j):
        return pltpu.make_async_remote_copy(
            src_ref=second.at[half, rows_of(j)], dst_ref=theirs.at[half, rows_of(j)],
            send_sem=csend.at[half], recv_sem=crecv.at[j], device_id=at(0, 1),
            device_id_type=MESH)

    def shuffle_copy(j):
        return pltpu.make_async_remote_copy(
            src_ref=away.at[rows_of(j)], dst_ref=across.at[rows_of(j)], send_sem=qsend,
            recv_sem=qrecv, device_id=device(lax.bitwise_xor(me, nc)), device_id_type=MESH)

    def tag_of(which, d):
        return tags[which, pl.ds(d, 1), :]

    def offer(half):
        def pack_second(j, carry):
            for i in range(GROUP):
                m = chunk_at(j) * GROUP + i
                d = lax.bitwise_xor(base, m)
                second[half, m] = pm[pick_s[d, 1], half * HALF : (half + 1) * HALF]
                if half == 0:
                    second[0, m, MARK : MARK + 1, :] = tag_of(1, d)
                    second[0, m, FIRST : FIRST + 1, :] = tag_of(0, d)

            if half == 0:
                @pl.when(j > 0)
                def _():
                    swap_copy(half, j - 1).start()

            return carry

        lax.fori_loop(0, chunks, pack_second, 0)
        if half == 0:
            swap_copy(half, chunks - 1).start()
        else:
            whole_swap().start()

    zero = c == 0

    def pack_quarters(d, m, my_second, their_second, their_first, own):
        mine_extra = (my_second > -0.5) & (their_first > -0.5)
        their_extra = (their_second > -0.5) & own
        use_mine = mine_extra & (zero | ~their_extra)
        tag = jnp.where(use_mine, my_second, jnp.where(their_extra, their_second, -1.0))
        tag = jnp.where(mine_extra & their_extra, OVER, tag)
        p = pick_s[d, 1]
        for ref, t in ((kept, part), (away, lax.bitwise_xor(part, nc))):
            half = lax.rem(t, 2)
            place = t // 2
            top = pl.multiple_of(place * MAIN, 8)
            my_top = pl.multiple_of(half * HALF + place * MAIN, 8)
            my_low = pl.multiple_of(half * HALF + 2 * MAIN, 8)
            ref[m, :MAIN, :] = jnp.where(
                use_mine, pm[p, pl.ds(my_top, MAIN), :], theirs[half, m, pl.ds(top, MAIN), :])
            low = jnp.where(use_mine, pm[p, pl.ds(my_low, 8), :], theirs[half, m, 2 * MAIN : HALF, :])
            low = jnp.where(place == 1, pltpu.roll(low, 8 - TAIL, axis=0), low)
            ref[m, MAIN : MAIN + TAIL, :] = low[:TAIL]
            ref[m, TAG : TAG + 1, :] = tag

    def pack_chunk(half, j):
        for i in range(GROUP):
            k = chunk_at(j) * GROUP + i
            d = peer(k)
            m = lax.bitwise_xor(k, part)
            my_first = tag_of(0, d)
            their_second = theirs[0, m, MARK : MARK + 1, :]
            own = my_first > -0.5
            sent[half, d] = jnp.where(
                own, pm[pick_s[d, 0], half * HALF : (half + 1) * HALF], theirs[half, m])
            if half == 0:
                sent[0, d, MARK : MARK + 1, :] = jnp.where(own, my_first, their_second)
            else:
                pack_quarters(d, m, tag_of(1, d), their_second, theirs[0, m, FIRST : FIRST + 1, :], own)

    def send_chunk(half, j):
        if half:
            shuffle_copy(j).start()
        for i in range(GROUP):
            k = chunk_at(j) * GROUP + i

            @pl.when(k > 0)
            def _():
                patch_copy(half, k).start()

    def exchange(half):
        if half:
            whole_swap().wait_recv()

        def post(j, carry):
            if half == 0:
                swap_copy(half, j).wait_recv()
            pack_chunk(half, j)

            @pl.when(j > 0)
            def _():
                send_chunk(half, j - 1)

            return carry

        lax.fori_loop(0, chunks, post, 0)
        send_chunk(half, chunks - 1)
        got_ref[2 * me + half] = sent[half, me]

    def early():
        fill(0)
        to_scalars.wait()
        offer(0)
        for k in range(2 * STEPS - 1, rounds):
            if k > 2 * STEPS - 1:
                tell(k)
            hear(k)
        exchange(0)

    for s in range(STEPS):
        step(s, early if s == STEPS - 1 else None)
    fill(1)
    offer(1)
    exchange(1)

    for which in range(2):
        waiter(second.at[which], csend.at[which], csend.at[which]).wait_send()
    waiter(away, qsend, qrecv).wait_send()
    waiter(across, qsend, qrecv).wait_recv()
    near_tags = kept[:, TAG, :]
    far_tags = across[:, TAG, :]
    over = (near_tags > OVER / 2) | (far_tags > OVER / 2) | ((near_tags > -0.5) & (far_tags > -0.5))
    flag = jnp.max(jnp.where(over, OVER, 0.0), axis=0, keepdims=True)

    def pack_extra(d):
        m = lax.bitwise_xor(base, d)
        mine = kept[m]
        other = across[m]
        keep = ((mine[TAG:] > -0.5) & (far_chip == 0)) | ~(other[TAG:] > -0.5)
        extra[d] = jnp.where(keep, mine, other)
        extra[d, TAG : TAG + 1, :] = jnp.where(keep, mine[TAG:], other[TAG:]) + flag

    def mask_at(i):
        return lax.rem(i + count // 2, count)

    def post_extra(i, carry):
        pack_extra(peer(mask_at(i)))

        @pl.when((i > 0) & (mask_at(i - 1) > 0))
        def _():
            extra_copy(mask_at(i - 1)).start()

        return carry

    lax.fori_loop(0, count, post_extra, 0)
    extra_copy(mask_at(count - 1)).start()
    got_extra[me] = extra[me]

    for which, rows in ((0, FIRST), (1, MARK)):
        arrived = waiter(sent.at[which, 1:, :rows], psend.at[which], precv.at[which])
        arrived.wait_send()
        arrived.wait_recv()
    waiter(extra.at[1:], esend, erecv).wait_send()
    waiter(got_extra.at[1:], esend, erecv).wait_recv()

    def assemble(g, carry):
        for t in range(TILES):
            whole = got_ref.at[2 * count + 2 * g + t % 2]
            block = got_extra.at[g * GROUP + t]
            whole[t // 2 * MAIN : (t // 2 + 1) * MAIN, :] = block[:MAIN, :]
            low = 2 * MAIN + t // 2 * TAIL
            whole[low : low + TAIL, :] = block[MAIN : MAIN + TAIL, :]
        return carry

    lax.fori_loop(0, chunks, assemble, 0)
    source = lax.broadcasted_iota(jnp.int32, (count, LANES), 0)
    wanted = lax.broadcasted_iota(jnp.int32, (count, LANES), 1).astype(jnp.float32)
    arrived_flat = got_ref.reshape(got_ref.shape[0] * HALF, LANES)
    first_hit = arrived_flat[pl.ds(MARK, count, stride=2 * HALF), :] == wanted
    index = jnp.sum(jnp.where(first_hit, 2 * source, 0), axis=0, keepdims=True)
    extra_tags = got_extra[:, TAG, :]
    extra_hit = (extra_tags == wanted) & (source % GROUP == 0)
    place = source // GROUP * 2 + 2 * count
    index = index + jnp.sum(jnp.where(extra_hit, place, 0), axis=0, keepdims=True)
    over = jnp.max(extra_tags, axis=0, keepdims=True)
    row = lax.broadcasted_iota(jnp.int32, (8, LANES), 0)
    table_ref[...] = jnp.where(row == 0, index, jnp.where(over > OVER / 2, 1, 0))


def full_kernel(nb, nc, sidx, slot_of, pm, got_ref, table_ref, sent, send_sem, recv_sem):
    count = nb * nc
    me = lax.axis_index("blocks") * nc + lax.axis_index("cross")

    def device(d):
        return (d // nc, lax.rem(d, nc))

    barrier = pltpu.get_barrier_semaphore()

    def greet(k, carry):
        pl.semaphore_signal(barrier, inc=1, device_id=device(lax.bitwise_xor(me, k)), device_id_type=MESH)
        return carry

    lax.fori_loop(1, count, greet, 0)
    pl.semaphore_wait(barrier, count - 1)

    def pack(d, carry):
        for slot in range(2):
            p = sidx[2 * d + slot]
            sent[d, 2 * slot] = pm[p, :HALF]
            sent[d, 2 * slot + 1] = pm[p, HALF:]
            tag = jnp.full((1, LANES), slot_of[2 * d + slot].astype(jnp.float32), jnp.float32)
            sent[d, 2 * slot, MARK : MARK + 1, :] = tag
        return carry

    lax.fori_loop(0, count, pack, 0)

    def copy(k):
        d = lax.bitwise_xor(me, k)
        return pltpu.make_async_remote_copy(
            src_ref=sent.at[d], dst_ref=got_ref.at[pl.ds(4 * me, 4)], send_sem=send_sem.at[k],
            recv_sem=recv_sem.at[k], device_id=device(d), device_id_type=MESH)

    def post(k, carry):
        copy(k).start()
        return carry

    def finish(k, carry):
        copy(k).wait()
        return carry

    lax.fori_loop(1, count, post, 0)
    for i in range(4):
        got_ref[4 * me + i] = sent[me, i]
    lax.fori_loop(1, count, finish, 0)
    source = lax.broadcasted_iota(jnp.int32, (4 * count, LANES), 0)
    wanted = lax.broadcasted_iota(jnp.int32, (4 * count, LANES), 1).astype(jnp.float32)
    hit = (got_ref[:, MARK, :] == wanted) & (source % 2 == 0)
    index = jnp.sum(jnp.where(hit, source, 0), axis=0, keepdims=True)
    table_ref[...] = jnp.broadcast_to(index, table_ref.shape)


def unpack_kernel(ridx, got_ref, out_ref):
    for t in range(out_ref.shape[1]):
        base = ridx[0, t]
        for tile in range(TILES):
            block = got_ref.at[base + half_of(tile)]
            lanes = slice(tile * LANES, (tile + 1) * LANES)
            low = low_row(0, tile)
            out_ref[:MAIN, t, lanes] = block[low : low + MAIN, :]
            low = low_row(MAIN, tile)
            out_ref[MAIN:, t, lanes] = block[2 * MAIN :, :][low - 2 * MAIN : low - 2 * MAIN + TAIL]


def body(nb, nc, f_home, levels, plan):
    devices = nb * nc
    patches = f_home.shape[0]
    vmem = pl.BlockSpec(memory_space=pltpu.VMEM)
    smem = pl.BlockSpec(memory_space=pltpu.SMEM)
    state = (19, SPAN_PATCHES, 8, CELLS)
    small = (SPAN_PATCHES, 8, LANES)
    f32 = jnp.float32
    dma = pltpu.SemaphoreType.DMA
    half = (HALF, LANES)
    quarter = (QUARTER, LANES)
    rounds = max(2 * STEPS, (nb - 1).bit_length())
    limit = pltpu.CompilerParams(collective_id=0, has_side_effects=True, vmem_limit_bytes=60 * 1024 * 1024)
    got, packed, table = pl.pallas_call(
        lambda *refs: lattice_kernel(nb, nc, *refs),
        out_shape=(
            jax.ShapeDtypeStruct((2 * devices + 2 * devices // GROUP,) + half, f32),
            jax.ShapeDtypeStruct((patches, 2 * HALF, LANES), f32),
            jax.ShapeDtypeStruct((8, LANES), jnp.int32),
        ),
        in_specs=[smem, vmem, vmem],
        out_specs=(vmem, vmem, vmem),
        scratch_shapes=[
            pltpu.VMEM(state, f32),
            pltpu.VMEM(state, f32),
            pltpu.VMEM(state, f32),
            pltpu.VMEM((18,) + state[1:], f32),
            pltpu.VMEM((2, devices) + half, f32),
            pltpu.VMEM((2, devices) + half, f32),
            pltpu.VMEM((2, devices) + half, f32),
            pltpu.VMEM((devices,) + quarter, f32),
            pltpu.VMEM((devices,) + quarter, f32),
            pltpu.VMEM((devices,) + quarter, f32),
            pltpu.VMEM((devices,) + quarter, f32),
            pltpu.VMEM((devices,) + quarter, f32),
            pltpu.VMEM(small, f32),
            pltpu.VMEM((8, LANES), f32),
            pltpu.VMEM((3 * nc - 1, 8, LANES), f32),
            pltpu.VMEM((STEPS, 2, 2, 5, 8, CELLS), f32),
            pltpu.VMEM((STEPS, 2, 2, 5, 8, CELLS), f32),
            pltpu.VMEM((STEPS, 2, 2, 5, 2, 8, LANES), f32),
            pltpu.VMEM((STEPS, 2, 2, 5, 2, 8, LANES), f32),
            pltpu.VMEM((STEPS, len(DIAGONAL), 2, 8, LANES), f32),
            pltpu.VMEM((STEPS, len(DIAGONAL), 2, 8, LANES), f32),
            pltpu.VMEM((devices, LANES), jnp.int32),
            pltpu.SMEM((devices, LANES), jnp.int32),
            pltpu.VMEM((2, devices, LANES), f32),
            dma((STEPS, 3)),
            dma((STEPS, 3)),
            dma((3,)),
            dma((3,)),
            dma((2,)),
            dma((2,)),
            dma,
            dma,
            dma((2,)),
            dma((devices // GROUP + 1,)),
            dma,
            dma,
            dma,
            pltpu.SemaphoreType.REGULAR((rounds,)),
            pltpu.SemaphoreType.REGULAR((rounds,)),
        ],
        compiler_params=limit,
    )(levels, plan[None, :], jnp.transpose(f_home, (1, 0, 2)))

    def unpack(table, got):
        return pl.pallas_call(
            unpack_kernel,
            out_shape=jax.ShapeDtypeStruct((19, patches, CELLS), f32),
            in_specs=[smem, vmem],
            out_specs=vmem,
            compiler_params=pltpu.CompilerParams(vmem_limit_bytes=40 * 1024 * 1024),
        )(table, got)

    def in_full(table, got, packed, plan):
        target = plan // patches
        order = jnp.arange(patches, dtype=jnp.int32)
        earlier = (target[:, None] == target[None, :]) & (order[None, :] < order[:, None])
        place = 2 * target + jnp.sum(earlier.astype(jnp.int32), axis=1)
        hit = place[None, :] == jnp.arange(2 * devices, dtype=jnp.int32)[:, None]
        sidx = jnp.sum(jnp.where(hit, order[None, :], 0), axis=1)
        slot_of = jnp.sum(jnp.where(hit, plan[None, :] % patches + 1, 0), axis=1) - 1
        got, table = pl.pallas_call(
            lambda *refs: full_kernel(nb, nc, *refs),
            out_shape=(
                jax.ShapeDtypeStruct((4 * devices,) + half, f32),
                jax.ShapeDtypeStruct((8, LANES), jnp.int32),
            ),
            in_specs=[smem, smem, vmem],
            out_specs=(vmem, vmem),
            scratch_shapes=[
                pltpu.VMEM((devices, 4) + half, f32), dma((devices,)), dma((devices,))
            ],
            compiler_params=pltpu.CompilerParams(collective_id=1, has_side_effects=True,
                                                 vmem_limit_bytes=48 * 1024 * 1024),
        )(sidx, slot_of, packed)
        return unpack(table, got)

    out = lax.cond(table[1, 0] > 0, in_full, lambda table, got, packed, plan: unpack(table, got),
                   table, got, packed, plan)
    return jnp.transpose(out, (1, 0, 2))


def solution(mesh):
    nb, nc = mesh.shape["blocks"], mesh.shape["cross"]
    in_specs = (P(("blocks", "cross"), None, None), P(("blocks", "cross")), P(("blocks", "cross")))
    out_specs = P(("blocks", "cross"), None, None)
    return jax.shard_map(
        lambda f, l, p: body(nb, nc, f, l, p),
        mesh=mesh, in_specs=in_specs, out_specs=out_specs, check_vma=False)
```

```python
import jax
import jax.numpy as jnp
from jax import lax
from jax.experimental import pallas as pl
from jax.experimental.pallas import tpu as pltpu
from jax.sharding import PartitionSpec as P

SPAN_PATCHES = 4
DEPTH_PATCHES = 8
STEPS = 2
CELLS = 512
VELOCITIES = (
    (0, 0, 0),
    (1, 0, 0),
    (-1, 0, 0),
    (0, 1, 0),
    (0, -1, 0),
    (0, 0, 1),
    (0, 0, -1),
    (1, 1, 0),
    (-1, -1, 0),
    (1, -1, 0),
    (-1, 1, 0),
    (1, 0, 1),
    (-1, 0, -1),
    (1, 0, -1),
    (-1, 0, 1),
    (0, 1, 1),
    (0, -1, -1),
    (0, 1, -1),
    (0, -1, 1),
)
WEIGHTS = (1.0 / 3.0,) + (1.0 / 18.0,) * 6 + (1.0 / 36.0,) * 12
TAU_COARSE = 0.55
TAU_FINE = 2.0 * TAU_COARSE - 0.5
RESCALE = TAU_FINE / (2.0 * TAU_COARSE)
INFLOW = 0.08
MESH = pl.DeviceIdType.MESH
MAIN = 16
TAIL = 3
HALF = 40
MARK = 38
FIRST = 39
QUARTER = 20
TAG = 19
OVER = 1000.0
GROUP = 4
LANES = 128
TILES = CELLS // LANES
Y_UP = [q for q in range(19) if VELOCITIES[q][1] == 1]
Y_DOWN = [q for q in range(19) if VELOCITIES[q][1] == -1]
X_UP = [q for q in range(19) if VELOCITIES[q][0] == 1]
X_DOWN = [q for q in range(19) if VELOCITIES[q][0] == -1]
DIAGONAL = [q for q in range(19) if VELOCITIES[q][0] and VELOCITIES[q][1]]


def relax_into(load, store, coef):
    f = [load(q) for q in range(19)]
    terms = list(f)
    while len(terms) > 1:
        pairs = [a + b for a, b in zip(terms[::2], terms[1::2])]
        terms = pairs + ([terms[-1]] if len(terms) % 2 else [])
    rho = terms[0]
    inv = 1.0 / rho
    u = []
    for axis in range(3):
        up = [f[q] for q in range(19) if VELOCITIES[q][axis] == 1]
        down = [f[q] for q in range(19) if VELOCITIES[q][axis] == -1]
        d = [a - b for a, b in zip(up, down)]
        u.append((((d[0] + d[1]) + (d[2] + d[3])) + d[4]) * inv)
    base = 1.0 - 1.5 * (u[0] * u[0] + u[1] * u[1] + u[2] * u[2])
    scaled = {w: w * rho for w in set(WEIGHTS)}
    for q in range(19):
        along = None
        for axis in range(3):
            e = VELOCITIES[q][axis]
            if e:
                term = u[axis] if e == 1 else -u[axis]
                along = term if along is None else along + term
        poly = base if along is None else base + along * (3.0 + 4.5 * along)
        balance = scaled[WEIGHTS[q]] * poly
        store(q, balance + coef(q) * (f[q] - balance))


def half_of(tile):
    return 1 if tile in (0, TILES - 1) else 0


def place_of(tile):
    return tile // 2 if half_of(tile) else tile - 1


def low_row(q, tile):
    place = place_of(tile)
    return place * MAIN + q if q < MAIN else 2 * MAIN + place * TAIL + q - MAIN


def lattice_kernel(nb, nc, level, plan_ref, f_ref, got_ref, pm, table_ref, st, pb, pb2, cq, sent, second, theirs,
                   away, kept, across, extra, got_extra, own_ref, lev_ref, lv, ys, yr, xs, xr, ds, dr, pick, pick_s, tags, send_sem, recv_sem, lsend, lrecv, psend,
                   precv, esend, erecv, csend, crecv, qsend, qrecv, pick_sem, up_sem, down_sem):
    others = nb * nc - 1
    rounds = max(2 * STEPS, (nb - 1).bit_length())
    b = lax.axis_index("blocks")
    c = lax.axis_index("cross")

    def at(dx, dy):
        return (lax.rem(b + dx + nb, nb), lax.rem(c + dy + nc, nc))

    me = b * nc + c

    def peer(k):
        return lax.bitwise_xor(me, k)

    def device(d):
        return (d // nc, lax.rem(d, nc))

    barrier = pltpu.get_barrier_semaphore()
    above = b < nb - 1
    below = b > 0

    def signal(sem, to):
        pl.semaphore_signal(sem, inc=1, device_id=to, device_id_type=MESH)

    for k in range(1, nc):
        signal(barrier, at(0, k))
    for there, dx in ((above, 1), (below, -1)):
        @pl.when(there)
        def _():
            for k in range(nc):
                signal(barrier, at(dx, k))

    def tell(k):
        hop = lax.shift_left(jnp.int32(1), jnp.int32(k))

        @pl.when(b + hop < nb)
        def _():
            signal(up_sem.at[k], (b + hop, c))

        @pl.when(b >= hop)
        def _():
            signal(down_sem.at[k], (b - hop, c))

    def hear(k):
        hop = lax.shift_left(jnp.int32(1), jnp.int32(k))

        @pl.when(b >= hop)
        def _():
            pl.semaphore_wait(up_sem.at[k], 1)

        @pl.when(b + hop < nb)
        def _():
            pl.semaphore_wait(down_sem.at[k], 1)

    patches = f_ref.shape[1]
    count = nb * nc
    target = lax.broadcasted_iota(jnp.int32, (count, patches), 0)
    where = jnp.broadcast_to(plan_ref[...], (count, patches))
    member = where // patches == target
    key = lax.broadcasted_iota(jnp.int32, (count, patches), 1) * patches + where % patches
    low_key = jnp.min(jnp.where(member, key, patches * patches), axis=1, keepdims=True)
    high_key = jnp.max(jnp.where(member, key, -1), axis=1, keepdims=True)
    some = high_key >= 0
    two = high_key > low_key
    column = lax.broadcasted_iota(jnp.int32, (count, LANES), 1)
    pick[...] = jnp.where(column == 0, jnp.where(some, low_key // patches, 0),
                          jnp.where(two, high_key // patches, 0))
    to_scalars = pltpu.make_async_copy(pick, pick_s, pick_sem)
    to_scalars.start()
    tags[0] = jnp.broadcast_to(jnp.where(some, low_key % patches, -1), (count, LANES)).astype(jnp.float32)
    tags[1] = jnp.broadcast_to(jnp.where(two, high_key % patches, -1), (count, LANES)).astype(jnp.float32)

    slot = lax.broadcasted_iota(jnp.int32, (8, LANES), 0)
    slot = slot + 8 * lax.broadcasted_iota(jnp.int32, (8, LANES), 1)
    brief = jnp.zeros((8, LANES), jnp.float32)
    for p in range(SPAN_PATCHES * 8):
        brief = jnp.where(slot == p, level[p].astype(jnp.float32), brief)
    lev_ref[...] = brief

    def spread(values, r):
        return jnp.broadcast_to(values[:, r : r + 1], (8, LANES))[None]

    own = jnp.concatenate([spread(brief, r) for r in range(SPAN_PATCHES)], axis=0)
    own_ref[...] = own
    for q in range(19):
        for r in range(SPAN_PATCHES):
            st[q, r] = f_ref[q, r * 8 : r * 8 + 8, :]
    gain = jnp.where(own > 0.5, (1.0 - 1.0 / TAU_FINE) / RESCALE, 1.0 - 1.0 / TAU_COARSE)
    lane = lax.broadcasted_iota(jnp.int32, (SPAN_PATCHES, 8, LANES), 2)
    lower = lane < 64
    half = lax.broadcasted_iota(jnp.int32, (2, 8, LANES), 2) < 64
    fine = own > 0.5
    in_tile = {
        (axis, e): (lane // 8 % 8 if axis == 1 else lane % 8) == (0 if e == 1 else 7)
        for axis in (1, 2) for e in (1, -1)
    }
    around = [(dx, dy) for dx in (-1, 0, 1) for dy in range(nc) if (dx, dy) != (0, 0)]

    def targets(far):
        scales = {}
        for dx in (-1, 0, 1):
            rows = [spread(far(dx, nc - 1), SPAN_PATCHES - 1)]
            rows += [own[r][None] if dx == 0 else spread(far(dx, 0), r) for r in range(SPAN_PATCHES)]
            rows += [spread(far(dx, 1 % nc), 0)]
            rows = [jnp.where(value > 0.5, RESCALE, 1.0) for value in rows]
            for dy in (-1, 0, 1):
                value = jnp.concatenate(rows[1 + dy : 1 + dy + SPAN_PATCHES], axis=0)
                for dz in (-1, 0, 1):
                    scales[dx, dy, dz] = pltpu.roll(value, (-dz) % 8, axis=1) if dz else value
        return scales

    def coefficient(q, tile, scales, rows):
        e = VELOCITIES[q]
        kinds = [{}]
        for axis in range(3):
            if e[axis] and (axis or tile == (TILES - 1 if e[0] == 1 else 0)):
                kinds = [{**k, axis: v} for k in kinds for v in (0, 1)]
        result = None
        for k in kinds:
            value = scales[tuple(e[a] * k.get(a, 0) for a in range(3))][rows]
            mask = None
            for axis, on in k.items():
                if on:
                    hit = in_tile[axis, -e[axis]] if axis else (~lower if e[0] == 1 else lower)
                    mask = hit[rows] if mask is None else mask & hit[rows]
            result = value if result is None else jnp.where(mask, value, result)
        return gain[rows] * result

    def lanes_of(tile):
        return slice(tile * LANES, (tile + 1) * LANES)

    everything = slice(0, SPAN_PATCHES)
    scales = targets(lambda dx, dy: jnp.zeros((8, LANES), jnp.float32))
    for q in range(1, 19):
        for tile in range(TILES):
            cq[q - 1, :, :, lanes_of(tile)] = coefficient(q, tile, scales, everything)

    def first(r, tiles):
        plain = jnp.where(own_ref[r] > 0.5, 1.0 - 1.0 / TAU_FINE, 1.0 - 1.0 / TAU_COARSE)
        for tile in tiles:
            lanes = lanes_of(tile)

            def put(q, value):
                pb[q, r, :, lanes] = value

            relax_into(lambda q: st[q, r, :, lanes], put,
                       lambda q: cq[q - 1, r, :, lanes] if q else plain)

    def first_rows(tiles, start, stop, stride=1):
        def one(n, carry):
            first(start + stride * n, tiles)
            return carry

        lax.fori_loop(0, (stop - start + stride - 1) // stride, one, 0)

    end_tiles = (0, TILES - 1)
    middle_tiles = tuple(range(1, TILES - 1))
    first_rows(end_tiles, 0, SPAN_PATCHES)
    first_rows(middle_tiles, 0, SPAN_PATCHES)
    pl.semaphore_wait(barrier, nc - 1 + nc * (jnp.where(above, 1, 0) + jnp.where(below, 1, 0)))
    tell(0)

    def start_to(there, copy):
        if there is None:
            copy.start()
        else:
            pl.when(there)(copy.start)

    def wait_for(outgoing, incoming, copy):
        if outgoing is None:
            copy.wait()
        else:
            pl.when(outgoing)(copy.wait_send)
            pl.when(incoming)(copy.wait_recv)

    def ends_of(dx):
        return {0: (None, None), 1: (above, below), -1: (below, above)}[dx]

    def waiter(ref, send, recv):
        return pltpu.make_async_remote_copy(
            src_ref=ref, dst_ref=ref, send_sem=send, recv_sem=recv, device_id=at(0, 1), device_id_type=MESH)

    level_copies = []
    for n, (dx, dy) in enumerate(around):
        copy = pltpu.make_async_remote_copy(
            src_ref=lev_ref, dst_ref=lv.at[n], send_sem=lsend.at[dx + 1], recv_sem=lrecv.at[dx + 1],
            device_id=at(-dx, -dy), device_id_type=MESH)
        outgoing, incoming = ends_of(-dx)
        level_copies.append((outgoing, copy))

    def patch_copy(half, k):
        d = peer(k)
        rows = slice(0, MARK if half else FIRST)
        return pltpu.make_async_remote_copy(
            src_ref=sent.at[half, d, rows], dst_ref=got_ref.at[2 * me + half, rows],
            send_sem=psend.at[half], recv_sem=precv.at[half], device_id=device(d),
            device_id_type=MESH)

    def extra_copy(k):
        d = peer(k)
        return pltpu.make_async_remote_copy(
            src_ref=extra.at[d], dst_ref=got_extra.at[me], send_sem=esend,
            recv_sem=erecv, device_id=device(d), device_id_type=MESH)

    own_scale = jnp.where(fine, RESCALE, 1.0)
    kappa = gain / (1.0 - gain)

    def take_levels():
        for dx in (-1, 0, 1):
            some = nc if dx else nc - 1
            wait_for(*ends_of(-dx), waiter(lv.at[:some], lsend.at[dx + 1], lrecv.at[dx + 1]))
        scales = targets(lambda dx, dy: lv[around.index((dx, dy))])

        def refresh(q, tile, rows):
            cq[q - 1, rows, :, lanes_of(tile)] = coefficient(q, tile, scales, rows)

        for q in range(1, 19):
            e = VELOCITIES[q]
            outer_tile = {0: None, 1: TILES - 1, -1: 0}[e[0]]
            if e[0]:
                refresh(q, outer_tile, everything)
            if e[1]:
                r = SPAN_PATCHES - 1 if e[1] == 1 else 0
                for tile in range(TILES):
                    if tile != outer_tile:
                        refresh(q, tile, slice(r, r + 1))

    def spin(v, amount):
        return pltpu.roll(v, amount % LANES, axis=v.ndim - 1)

    def along_z(q, v, more=0):
        e = VELOCITIES[q][2]
        if not e:
            return spin(v, more) if more else v
        wrapped = pltpu.roll(spin(v, more - 7 * e), e % 8, axis=1)
        return jnp.where(in_tile[2, e][: v.shape[0]], wrapped, spin(v, more + e))

    def along_y(q, v, halo, more=0):
        e = VELOCITIES[q][1]
        moved = jnp.concatenate([halo, v[:-1]] if e == 1 else [v[1:], halo], axis=0)
        return jnp.where(in_tile[1, e], spin(moved, more - 56 * e), spin(v, more + 8 * e))

    def step(s, stage=None):
        def send(src, dst, dx, dy):
            copy = pltpu.make_async_remote_copy(
                src_ref=src, dst_ref=dst, send_sem=send_sem.at[s, dx + 1], recv_sem=recv_sem.at[s, dx + 1],
                device_id=at(dx, dy), device_id_type=MESH)
            start_to(ends_of(dx)[0], copy)

        def await_halos(dx):
            ref = pb2.at[: 3 * parts, :, :, :LANES] if dx else ys.at[s, :, :parts]
            wait_for(*ends_of(dx), waiter(ref, send_sem.at[s, dx + 1], recv_sem.at[s, dx + 1]))

        parts = 2 if s == 0 else 1

        def face(q, rows, tile):
            spot = (q, rows, slice(0, 8), lanes_of(tile))
            values = [pb[spot]]
            if s == 0:
                values.append(kappa[rows] * (st[spot] - values[0]))
            return [along_z(q, v) for v in values]

        def send_x():
            for way, e, group in ((0, 1, X_UP), (1, -1, X_DOWN)):
                for n, q in enumerate(group):
                    for part_id, v in enumerate(face(q, everything, TILES - 1 if e == 1 else 0)):
                        turned = spin(v, 64)
                        if e == 1:
                            xs[s, way, part_id, n] = jnp.where(half, turned[:2], v[2:])
                        else:
                            xs[s, way, part_id, n] = jnp.where(half, v[:2], turned[2:])
                        if q in DIAGONAL:
                            edge = turned[SPAN_PATCHES - 1 if VELOCITIES[q][1] == 1 else 0]
                            ds[s, DIAGONAL.index(q), part_id] = edge
            for way, dx in ((0, 1), (1, -1)):
                send(xs.at[s, way, :parts], xr.at[s, way, :parts], dx, 0)
            for n, q in enumerate(DIAGONAL):
                send(ds.at[s, n, :parts], dr.at[s, n, :parts], *VELOCITIES[q][:2])

        def send_y():
            for way, e, group in ((0, 1, Y_UP), (1, -1, Y_DOWN)):
                r = SPAN_PATCHES - 1 if e == 1 else 0
                for n, q in enumerate(group):
                    for tile in range(TILES):
                        for part_id, v in enumerate(face(q, slice(r, r + 1), tile)):
                            ys[s, way, part_id, n, :, lanes_of(tile)] = v[0]
            for way, dy in ((0, 1), (1, -1)):
                send(ys.at[s, way, :parts], yr.at[s, way, :parts], 0, dy)

        def y_halo(e, n, tile):
            way, r = (0, 0) if e == 1 else (1, SPAN_PATCHES - 1)
            value = yr[s, way, 0, n, :, lanes_of(tile)]
            if s == 0:
                value = value + (own_scale[r] - 1.0) * yr[s, way, 1, n, :, lanes_of(tile)]
            return value[None]

        def x_halo(way, e, n, q):
            values = []
            for part_id in range(parts):
                h = xr[s, way, part_id, n]
                turned = spin(h, 64)
                halo = jnp.concatenate([h, turned] if e == 1 else [turned, h], axis=0)
                if q in DIAGONAL:
                    halo = along_y(q, halo, dr[s, DIAGONAL.index(q), part_id][None])
                values.append(halo)
            return values[0] + (own_scale - 1.0) * values[1] if s == 0 else values[0]

        if s == 0:
            send_x()
            send_y()
            for outgoing, copy in level_copies:
                start_to(outgoing, copy)
        elif stage is None:
            first_rows(end_tiles, 0, SPAN_PATCHES)
            send_x()
            send_y()
        else:
            first_rows(end_tiles, 0, SPAN_PATCHES, SPAN_PATCHES - 1)
            send_y()
            first_rows(end_tiles, 1, SPAN_PATCHES - 1)
            send_x()

        def shift(q):
            e = VELOCITIES[q]
            half_turn = 64 if e[0] else 0
            tiles = [along_z(q, pb[q, :, :, lanes_of(tile)], 0 if e[1] else half_turn) for tile in range(TILES)]
            if e[1]:
                n = (Y_UP if e[1] == 1 else Y_DOWN).index(q)
                tiles = [along_y(q, v, y_halo(e[1], n, tile), half_turn) for tile, v in enumerate(tiles)]
            if e[0]:
                turned = list(tiles)
                for tile in range(TILES):
                    if e[0] == 1:
                        tiles[tile] = jnp.where(lower, turned[tile - 1], turned[tile])
                    else:
                        tiles[tile] = jnp.where(lower, turned[tile], turned[(tile + 1) % TILES])
            for tile in range(TILES):
                st[q, :, :, lanes_of(tile)] = tiles[tile]

        for q in range(19):
            if not VELOCITIES[q][1]:
                shift(q)
        await_halos(0)
        hear(2 * s)
        tell(2 * s + 1)
        for q in range(19):
            if VELOCITIES[q][1]:
                shift(q)

        def again(r, tiles):
            for tile in tiles:
                lanes = lanes_of(tile)

                def put(q, value):
                    pb2[q, r, :, lanes] = value

                relax_into(lambda q: st[q, r, :, lanes], put, lambda q: 1.0 - 1.0 / TAU_FINE)

        def settle(tiles):
            for q in range(19):
                e = VELOCITIES[q]
                amount = 64 * e[0] + 8 * e[1] + e[2]
                inside = fine
                for axis in (1, 2):
                    if e[axis]:
                        inside = inside & ~in_tile[axis, e[axis]]
                turned = {}

                def moved_from(tile):
                    if tile not in turned:
                        v = pb2[q, :, :, lanes_of(tile)]
                        turned[tile] = spin(v, amount) if amount else v
                    return turned[tile]

                for tile in tiles:
                    take = inside
                    value = moved_from(tile)
                    if e[0] == 1:
                        value = jnp.where(lower, moved_from((tile - 1) % TILES), value)
                        take = take & ~lower if tile == 0 else take
                    elif e[0] == -1:
                        value = jnp.where(lower, value, moved_from((tile + 1) % TILES))
                        take = take & lower if tile == TILES - 1 else take
                    lanes = lanes_of(tile)
                    st[q, :, :, lanes] = jnp.where(take, value, st[q, :, :, lanes])

        def middle(r, carry):
            again(r, range(1, TILES - 1))
            return carry

        def ends(r, carry):
            again(r, (0, TILES - 1))
            return carry

        lax.fori_loop(0, SPAN_PATCHES, middle, 0)
        lax.fori_loop(0, SPAN_PATCHES, ends, 0)
        settle(middle_tiles)
        if s == 0:
            take_levels()
        if stage is None:
            first_rows(middle_tiles, 0, SPAN_PATCHES)
        else:
            stage()
        await_halos(1)
        await_halos(-1)
        if stage is None:
            hear(2 * s + 1)
            tell(2 * s + 2)
        for way, e, group in ((0, 1, X_UP), (1, -1, X_DOWN)):
            outside = b == (0 if e == 1 else nb - 1)
            for n, q in enumerate(group):
                halo = x_halo(way, e, n, q)
                along = e * INFLOW
                const = WEIGHTS[q] * (1.0 + 3.0 * along + 4.5 * along * along - 1.5 * INFLOW * INFLOW)
                halo = jnp.where(outside, jnp.full(halo.shape, const, jnp.float32), halo)
                lanes = lanes_of(0 if e == 1 else TILES - 1)
                keep = st[q, :, :, lanes]
                st[q, :, :, lanes] = jnp.where(lower, halo, keep) if e == 1 else jnp.where(lower, keep, halo)

        lax.fori_loop(0, SPAN_PATCHES, ends, 0)
        settle(end_tiles)

    flat = pm.reshape(pm.shape[0] * 2 * HALF, LANES)

    def fill(half):
        pm[:, half * HALF + 2 * MAIN : (half + 1) * HALF, :] = jnp.zeros(
            (pm.shape[0], HALF - 2 * MAIN, LANES), jnp.float32)
        for q in range(19):
            for r in range(SPAN_PATCHES):
                for tile in range(TILES):
                    if half_of(tile) == half:
                        row = r * 8 * 2 * HALF + half * HALF + low_row(q, tile)
                        flat[pl.ds(row, 8, stride=2 * HALF), :] = st[q, r, :, lanes_of(tile)]

    part = lax.rem(me, GROUP)
    base = me - part
    far_chip = part // nc
    chunks = count // GROUP

    def chunk_at(j):
        return lax.rem(j + chunks // 2, chunks)

    def rows_of(j):
        return pl.ds(chunk_at(j) * GROUP, GROUP)

    def whole_swap():
        return pltpu.make_async_remote_copy(
            src_ref=second.at[1], dst_ref=theirs.at[1], send_sem=csend.at[1],
            recv_sem=crecv.at[chunks], device_id=at(0, 1), device_id_type=MESH)

    def swap_copy(half, j):
        return pltpu.make_async_remote_copy(
            src_ref=second.at[half, rows_of(j)], dst_ref=theirs.at[half, rows_of(j)],
            send_sem=csend.at[half], recv_sem=crecv.at[j], device_id=at(0, 1),
            device_id_type=MESH)

    def shuffle_copy(j):
        return pltpu.make_async_remote_copy(
            src_ref=away.at[rows_of(j)], dst_ref=across.at[rows_of(j)], send_sem=qsend,
            recv_sem=qrecv, device_id=device(lax.bitwise_xor(me, nc)), device_id_type=MESH)

    def tag_of(which, d):
        return tags[which, pl.ds(d, 1), :]

    def offer(half):
        def pack_second(j, carry):
            for i in range(GROUP):
                m = chunk_at(j) * GROUP + i
                d = lax.bitwise_xor(base, m)
                second[half, m] = pm[pick_s[d, 1], half * HALF : (half + 1) * HALF]
                if half == 0:
                    second[0, m, MARK : MARK + 1, :] = tag_of(1, d)
                    second[0, m, FIRST : FIRST + 1, :] = tag_of(0, d)

            if half == 0:
                @pl.when(j > 0)
                def _():
                    swap_copy(half, j - 1).start()

            return carry

        lax.fori_loop(0, chunks, pack_second, 0)
        if half == 0:
            swap_copy(half, chunks - 1).start()
        else:
            whole_swap().start()

    zero = c == 0

    def pack_quarters(d, m, my_second, their_second, their_first, own):
        mine_extra = (my_second > -0.5) & (their_first > -0.5)
        their_extra = (their_second > -0.5) & own
        use_mine = mine_extra & (zero | ~their_extra)
        tag = jnp.where(use_mine, my_second, jnp.where(their_extra, their_second, -1.0))
        tag = jnp.where(mine_extra & their_extra, OVER, tag)
        p = pick_s[d, 1]
        for ref, t in ((kept, part), (away, lax.bitwise_xor(part, nc))):
            half = lax.rem(t, 2)
            place = t // 2
            top = pl.multiple_of(place * MAIN, 8)
            my_top = pl.multiple_of(half * HALF + place * MAIN, 8)
            my_low = pl.multiple_of(half * HALF + 2 * MAIN, 8)
            ref[m, :MAIN, :] = jnp.where(
                use_mine, pm[p, pl.ds(my_top, MAIN), :], theirs[half, m, pl.ds(top, MAIN), :])
            low = jnp.where(use_mine, pm[p, pl.ds(my_low, 8), :], theirs[half, m, 2 * MAIN : HALF, :])
            low = jnp.where(place == 1, pltpu.roll(low, 8 - TAIL, axis=0), low)
            ref[m, MAIN : MAIN + TAIL, :] = low[:TAIL]
            ref[m, TAG : TAG + 1, :] = tag

    def pack_chunk(half, j):
        for i in range(GROUP):
            k = chunk_at(j) * GROUP + i
            d = peer(k)
            m = lax.bitwise_xor(k, part)
            my_first = tag_of(0, d)
            their_second = theirs[0, m, MARK : MARK + 1, :]
            own = my_first > -0.5
            sent[half, d] = jnp.where(
                own, pm[pick_s[d, 0], half * HALF : (half + 1) * HALF], theirs[half, m])
            if half == 0:
                sent[0, d, MARK : MARK + 1, :] = jnp.where(own, my_first, their_second)
            else:
                pack_quarters(d, m, tag_of(1, d), their_second, theirs[0, m, FIRST : FIRST + 1, :], own)

    def send_chunk(half, j):
        if half:
            shuffle_copy(j).start()
        for i in range(GROUP):
            k = chunk_at(j) * GROUP + i

            @pl.when(k > 0)
            def _():
                patch_copy(half, k).start()

    def exchange(half):
        if half:
            whole_swap().wait_recv()

        def post(j, carry):
            if half == 0:
                swap_copy(half, j).wait_recv()
            pack_chunk(half, j)

            @pl.when(j > 0)
            def _():
                send_chunk(half, j - 1)

            return carry

        lax.fori_loop(0, chunks, post, 0)
        send_chunk(half, chunks - 1)
        got_ref[2 * me + half] = sent[half, me]

    def early():
        fill(0)
        to_scalars.wait()
        offer(0)
        for k in range(2 * STEPS - 1, rounds):
            if k > 2 * STEPS - 1:
                tell(k)
            hear(k)
        exchange(0)

    for s in range(STEPS):
        step(s, early if s == STEPS - 1 else None)
    fill(1)
    offer(1)
    exchange(1)

    for which in range(2):
        waiter(second.at[which], csend.at[which], csend.at[which]).wait_send()
    waiter(away, qsend, qrecv).wait_send()
    waiter(across, qsend, qrecv).wait_recv()
    near_tags = kept[:, TAG, :]
    far_tags = across[:, TAG, :]
    over = (near_tags > OVER / 2) | (far_tags > OVER / 2) | ((near_tags > -0.5) & (far_tags > -0.5))
    flag = jnp.max(jnp.where(over, OVER, 0.0), axis=0, keepdims=True)

    def pack_extra(d):
        m = lax.bitwise_xor(base, d)
        mine = kept[m]
        other = across[m]
        keep = ((mine[TAG:] > -0.5) & (far_chip == 0)) | ~(other[TAG:] > -0.5)
        extra[d] = jnp.where(keep, mine, other)
        extra[d, TAG : TAG + 1, :] = jnp.where(keep, mine[TAG:], other[TAG:]) + flag

    def mask_at(i):
        return lax.rem(i + count // 2, count)

    def post_extra(i, carry):
        pack_extra(peer(mask_at(i)))

        @pl.when((i > 0) & (mask_at(i - 1) > 0))
        def _():
            extra_copy(mask_at(i - 1)).start()

        return carry

    lax.fori_loop(0, count, post_extra, 0)
    extra_copy(mask_at(count - 1)).start()
    got_extra[me] = extra[me]

    for which, rows in ((0, FIRST), (1, MARK)):
        arrived = waiter(sent.at[which, 1:, :rows], psend.at[which], precv.at[which])
        arrived.wait_send()
        arrived.wait_recv()
    waiter(extra.at[1:], esend, erecv).wait_send()
    waiter(got_extra.at[1:], esend, erecv).wait_recv()

    def assemble(g, carry):
        for t in range(TILES):
            whole = got_ref.at[2 * count + 2 * g + t % 2]
            block = got_extra.at[g * GROUP + t]
            whole[t // 2 * MAIN : (t // 2 + 1) * MAIN, :] = block[:MAIN, :]
            low = 2 * MAIN + t // 2 * TAIL
            whole[low : low + TAIL, :] = block[MAIN : MAIN + TAIL, :]
        return carry

    lax.fori_loop(0, chunks, assemble, 0, unroll=True)
    source = lax.broadcasted_iota(jnp.int32, (count, LANES), 0)
    wanted = lax.broadcasted_iota(jnp.int32, (count, LANES), 1).astype(jnp.float32)
    arrived_flat = got_ref.reshape(got_ref.shape[0] * HALF, LANES)
    first_hit = arrived_flat[pl.ds(MARK, count, stride=2 * HALF), :] == wanted
    index = jnp.sum(jnp.where(first_hit, 2 * source, 0), axis=0, keepdims=True)
    extra_tags = got_extra[:, TAG, :]
    extra_hit = (extra_tags == wanted) & (source % GROUP == 0)
    place = source // GROUP * 2 + 2 * count
    index = index + jnp.sum(jnp.where(extra_hit, place, 0), axis=0, keepdims=True)
    over = jnp.max(extra_tags, axis=0, keepdims=True)
    row = lax.broadcasted_iota(jnp.int32, (8, LANES), 0)
    table_ref[...] = jnp.where(row == 0, index, jnp.where(over > OVER / 2, 1, 0))


def full_kernel(nb, nc, sidx, slot_of, pm, got_ref, table_ref, sent, send_sem, recv_sem):
    count = nb * nc
    me = lax.axis_index("blocks") * nc + lax.axis_index("cross")

    def device(d):
        return (d // nc, lax.rem(d, nc))

    barrier = pltpu.get_barrier_semaphore()

    def greet(k, carry):
        pl.semaphore_signal(barrier, inc=1, device_id=device(lax.bitwise_xor(me, k)), device_id_type=MESH)
        return carry

    lax.fori_loop(1, count, greet, 0)
    pl.semaphore_wait(barrier, count - 1)

    def pack(d, carry):
        for slot in range(2):
            p = sidx[2 * d + slot]
            sent[d, 2 * slot] = pm[p, :HALF]
            sent[d, 2 * slot + 1] = pm[p, HALF:]
            tag = jnp.full((1, LANES), slot_of[2 * d + slot].astype(jnp.float32), jnp.float32)
            sent[d, 2 * slot, MARK : MARK + 1, :] = tag
        return carry

    lax.fori_loop(0, count, pack, 0)

    def copy(k):
        d = lax.bitwise_xor(me, k)
        return pltpu.make_async_remote_copy(
            src_ref=sent.at[d], dst_ref=got_ref.at[pl.ds(4 * me, 4)], send_sem=send_sem.at[k],
            recv_sem=recv_sem.at[k], device_id=device(d), device_id_type=MESH)

    def post(k, carry):
        copy(k).start()
        return carry

    def finish(k, carry):
        copy(k).wait()
        return carry

    lax.fori_loop(1, count, post, 0)
    for i in range(4):
        got_ref[4 * me + i] = sent[me, i]
    lax.fori_loop(1, count, finish, 0)
    source = lax.broadcasted_iota(jnp.int32, (4 * count, LANES), 0)
    wanted = lax.broadcasted_iota(jnp.int32, (4 * count, LANES), 1).astype(jnp.float32)
    hit = (got_ref[:, MARK, :] == wanted) & (source % 2 == 0)
    index = jnp.sum(jnp.where(hit, source, 0), axis=0, keepdims=True)
    table_ref[...] = jnp.broadcast_to(index, table_ref.shape)


def unpack_kernel(ridx, got_ref, out_ref):
    for t in range(out_ref.shape[1]):
        base = ridx[0, t]
        for tile in range(TILES):
            block = got_ref.at[base + half_of(tile)]
            lanes = slice(tile * LANES, (tile + 1) * LANES)
            low = low_row(0, tile)
            out_ref[:MAIN, t, lanes] = block[low : low + MAIN, :]
            low = low_row(MAIN, tile)
            out_ref[MAIN:, t, lanes] = block[2 * MAIN :, :][low - 2 * MAIN : low - 2 * MAIN + TAIL]


def body(nb, nc, f_home, levels, plan):
    devices = nb * nc
    patches = f_home.shape[0]
    vmem = pl.BlockSpec(memory_space=pltpu.VMEM)
    smem = pl.BlockSpec(memory_space=pltpu.SMEM)
    state = (19, SPAN_PATCHES, 8, CELLS)
    small = (SPAN_PATCHES, 8, LANES)
    f32 = jnp.float32
    dma = pltpu.SemaphoreType.DMA
    half = (HALF, LANES)
    quarter = (QUARTER, LANES)
    rounds = max(2 * STEPS, (nb - 1).bit_length())
    limit = pltpu.CompilerParams(collective_id=0, has_side_effects=True, vmem_limit_bytes=60 * 1024 * 1024)
    got, packed, table = pl.pallas_call(
        lambda *refs: lattice_kernel(nb, nc, *refs),
        out_shape=(
            jax.ShapeDtypeStruct((2 * devices + 2 * devices // GROUP,) + half, f32),
            jax.ShapeDtypeStruct((patches, 2 * HALF, LANES), f32),
            jax.ShapeDtypeStruct((8, LANES), jnp.int32),
        ),
        in_specs=[smem, vmem, vmem],
        out_specs=(vmem, vmem, vmem),
        scratch_shapes=[
            pltpu.VMEM(state, f32),
            pltpu.VMEM(state, f32),
            pltpu.VMEM(state, f32),
            pltpu.VMEM((18,) + state[1:], f32),
            pltpu.VMEM((2, devices) + half, f32),
            pltpu.VMEM((2, devices) + half, f32),
            pltpu.VMEM((2, devices) + half, f32),
            pltpu.VMEM((devices,) + quarter, f32),
            pltpu.VMEM((devices,) + quarter, f32),
            pltpu.VMEM((devices,) + quarter, f32),
            pltpu.VMEM((devices,) + quarter, f32),
            pltpu.VMEM((devices,) + quarter, f32),
            pltpu.VMEM(small, f32),
            pltpu.VMEM((8, LANES), f32),
            pltpu.VMEM((3 * nc - 1, 8, LANES), f32),
            pltpu.VMEM((STEPS, 2, 2, 5, 8, CELLS), f32),
            pltpu.VMEM((STEPS, 2, 2, 5, 8, CELLS), f32),
            pltpu.VMEM((STEPS, 2, 2, 5, 2, 8, LANES), f32),
            pltpu.VMEM((STEPS, 2, 2, 5, 2, 8, LANES), f32),
            pltpu.VMEM((STEPS, len(DIAGONAL), 2, 8, LANES), f32),
            pltpu.VMEM((STEPS, len(DIAGONAL), 2, 8, LANES), f32),
            pltpu.VMEM((devices, LANES), jnp.int32),
            pltpu.SMEM((devices, LANES), jnp.int32),
            pltpu.VMEM((2, devices, LANES), f32),
            dma((STEPS, 3)),
            dma((STEPS, 3)),
            dma((3,)),
            dma((3,)),
            dma((2,)),
            dma((2,)),
            dma,
            dma,
            dma((2,)),
            dma((devices // GROUP + 1,)),
            dma,
            dma,
            dma,
            pltpu.SemaphoreType.REGULAR((rounds,)),
            pltpu.SemaphoreType.REGULAR((rounds,)),
        ],
        compiler_params=limit,
    )(levels, plan[None, :], jnp.transpose(f_home, (1, 0, 2)))

    def unpack(table, got):
        return pl.pallas_call(
            unpack_kernel,
            out_shape=jax.ShapeDtypeStruct((19, patches, CELLS), f32),
            in_specs=[smem, vmem],
            out_specs=vmem,
            compiler_params=pltpu.CompilerParams(vmem_limit_bytes=40 * 1024 * 1024),
        )(table, got)

    def in_full(table, got, packed, plan):
        target = plan // patches
        order = jnp.arange(patches, dtype=jnp.int32)
        earlier = (target[:, None] == target[None, :]) & (order[None, :] < order[:, None])
        place = 2 * target + jnp.sum(earlier.astype(jnp.int32), axis=1)
        hit = place[None, :] == jnp.arange(2 * devices, dtype=jnp.int32)[:, None]
        sidx = jnp.sum(jnp.where(hit, order[None, :], 0), axis=1)
        slot_of = jnp.sum(jnp.where(hit, plan[None, :] % patches + 1, 0), axis=1) - 1
        got, table = pl.pallas_call(
            lambda *refs: full_kernel(nb, nc, *refs),
            out_shape=(
                jax.ShapeDtypeStruct((4 * devices,) + half, f32),
                jax.ShapeDtypeStruct((8, LANES), jnp.int32),
            ),
            in_specs=[smem, smem, vmem],
            out_specs=(vmem, vmem),
            scratch_shapes=[
                pltpu.VMEM((devices, 4) + half, f32), dma((devices,)), dma((devices,))
            ],
            compiler_params=pltpu.CompilerParams(collective_id=1, has_side_effects=True,
                                                 vmem_limit_bytes=48 * 1024 * 1024),
        )(sidx, slot_of, packed)
        return unpack(table, got)

    out = lax.cond(table[1, 0] > 0, in_full, lambda table, got, packed, plan: unpack(table, got),
                   table, got, packed, plan)
    return jnp.transpose(out, (1, 0, 2))


def solution(mesh):
    nb, nc = mesh.shape["blocks"], mesh.shape["cross"]
    in_specs = (P(("blocks", "cross"), None, None), P(("blocks", "cross")), P(("blocks", "cross")))
    out_specs = P(("blocks", "cross"), None, None)
    return jax.shard_map(
        lambda f, l, p: body(nb, nc, f, l, p),
        mesh=mesh, in_specs=in_specs, out_specs=out_specs, check_vma=False)
```
